32 devices in a mesh: rep: 4 (over y, x), grp: 8 (over z, core).
Axes of the slice: x: 2, y: 2, z: 4, core: 2. Of those that a mesh axis runs over, the one named last changes fastest.
Arguments:
- tokens: bfloat16 [4, 2048, 1024], P('rep', 'grp'), may hold values from -6 to 6
- segments: int32 [4, 2048], P('rep'), may hold values from 0 to 2, never falling along the last dimension, each value on 1 to 1024 neighbouring positions
- input_gain: bfloat16 [1024], P('grp'), may hold values from 0.5 to 1.5
- attention_in: bfloat16 [1024, 768], P('grp'), may hold values from -0.1875 to 0.1875
- attention_out: bfloat16 [512, 1024], P('grp'), may hold values from -2 to 2
- mixer_in: bfloat16 [1024, 3352], P('grp'), may hold values from -0.1875 to 0.1875
- filter_taps: bfloat16 [4, 1792], P(None, 'grp'), may hold values from -3 to 3
- filter_bias: bfloat16 [1792], P('grp'), may hold values from -3 to 3
- step_bias: float32 [24], replicated, may hold values from -6 to -2
- decay_log: float32 [24], replicated, may hold values from -3 to 1.5
- skip_scale: float32 [24], replicated, may hold values from 0.5 to 1.5
- mixer_gain: bfloat16 [1536], P('grp'), may hold values from 0.5 to 1.5
- mixer_out: bfloat16 [1536, 1024], P('grp'), may hold values from -0.15625 to 0.15625
- feed_gain: bfloat16 [1024], P('grp'), may hold values from 0.5 to 1.5
- gate_up: bfloat16 [1024, 4096], P('grp'), may hold values from -0.1875 to 0.1875
- down_proj: bfloat16 [2048, 1024], P('grp'), may hold values from -0.125 to 0.125
- cotangent: bfloat16 [4, 2048, 1024], P('rep', 'grp'), may hold values from -6 to 6
Outputs:
- out: bfloat16 [4, 2048, 1024], P('rep', 'grp')
- d_tokens: float32 [4, 2048, 1024], P('rep', 'grp')
- grad_input_gain: float32 [1024], P('grp')
- grad_attention_in: float32 [1024, 768], P('grp')
- grad_attention_out: float32 [512, 1024], P('grp')
- grad_mixer_in: float32 [1024, 3352], P('grp')
- grad_filter_taps: float32 [4, 1792], P(None, 'grp')
- grad_filter_bias: float32 [1792], P('grp')
- grad_step_bias: float32 [24], replicated
- grad_decay_log: float32 [24], replicated
- grad_skip_scale: float32 [24], replicated
- grad_mixer_gain: float32 [1536], P('grp')
- grad_mixer_out: float32 [1536, 1024], P('grp')
- grad_feed_gain: float32 [1024], P('grp')
- grad_gate_up: float32 [1024, 4096], P('grp')
- grad_down_proj: float32 [2048, 1024], P('grp')
The draws below stay inside these ranges and needn't reach their ends.
Inputs may be any that keep to these rules, and one draw needn't show every extreme that they name: `segments`: within a sequence the document number never falls, so each document is a run of consecutive tokens, at most 1024 long; some document is exactly that long.
All inputs are finite; a program needn't handle non-finite values.
Results may differ from the reference program's by a relative error of at most 0.025.
Values may be sent and summed in bfloat16 or wider, within the bound.
A program may use at most 256 MiB of HBM per device.

```python
import math
from functools import partial
import jax
import jax.numpy as jnp
import numpy as np
from jax import lax

D = 1024
HEADS = 8
KV_HEADS = 2
HEAD = 64
SSM_HEADS = 24
SSM_HEAD = 64
STATE = 128
CONV = 4
FF = 2048
SPAN = 256
LEN = 2048
SEQS = 4
QKV = 768
XBC = 1792
IN_W = 3352
N_GRP = 8


def block_scale(rng, dims, shards, smallest, top_value):
    level, own = 1.0, jax.random.fold_in(rng, 6)
    for axis_at, shards_of in shards:
        steps = jnp.exp(jax.random.uniform(jax.random.fold_in(own, axis_at), (shards_of,), jnp.float32, smallest / len(shards), top_value / len(shards)))
        level = level * jnp.repeat(steps, dims[axis_at] // shards_of).reshape([-1 if axis == axis_at else 1 for axis in range(len(dims))])
    return level


def profile(number_of, total, bound, lean):
    weights = [(1 << 20) // math.isqrt(standing ** lean) + 1 for standing in range(2, number_of + 1)]
    surplus, given = total - bound - (number_of - 1), [1] * (number_of - 1)
    while surplus > 0:
        candidates = [i for i in range(number_of - 1) if given[i] < bound]
        mass, left = sum([weights[i] for i in candidates]), surplus
        for i in candidates:
            extra = min(bound - given[i], max(1, left * weights[i] // mass), surplus)
            given[i] = given[i] + extra
            surplus = surplus - extra
    return np.array([bound] + given)


def uneven(key, number_of, total, reach, slope):
    if number_of == 2:
        one = jax.random.randint(key, (), max(1, total - reach), min(reach, total - 1) + 1)
        return jnp.stack([one, total - one])
    lengths = jnp.asarray(profile(number_of, total, reach, slope), jnp.int32)
    couples = (number_of - 1) // 2
    donor, sink = lengths[1:1 + 2 * couples:2], lengths[2:2 + 2 * couples:2]
    room = jnp.minimum(donor - 1, reach - sink)
    passed = jax.random.randint(jax.random.fold_in(key, 1), (couples,), 0, 1 << 20) % (room + 1)
    lengths = lengths.at[1:1 + 2 * couples:2].set(donor - passed).at[2:2 + 2 * couples:2].set(sink + passed)
    return lengths[jax.random.permutation(jax.random.fold_in(key, 2), number_of)]


def scatter_about(key, extent, width, limit, split=(), held_as=jnp.bfloat16):
    entries = jax.random.normal(key, extent, jnp.float32) * width
    if len(split) > 0:
        entries = block_scale(key, extent, split, -0.22, 0.18) * entries
    return jnp.clip(entries, min=-limit, max=limit).astype(held_as)


def setup_inputs(seed: int = 0) -> dict:
    splits = jax.random.split(jax.random.key(seed), 18)
    return {
        "tokens": scatter_about(splits[0], (SEQS, LEN, D), 1.0, 6.0, ((0, 4), (1, 8))),
        "segments": jax.vmap(lambda own: jnp.searchsorted(jnp.cumsum(uneven(own, 3, LEN, LEN // 2, 0)), jnp.arange(LEN), side="right"))(jax.random.split(splits[1], SEQS)).reshape((SEQS, LEN)).astype(jnp.int32),
        "input_gain": jnp.clip(1.0 + 0.1 * jax.random.normal(splits[2], (D,), jnp.float32), 0.5, 1.5).astype(jnp.bfloat16),
        "attention_in": scatter_about(splits[3], (D, QKV), D ** -0.5, 0.1875, ((0, 8),)),
        "attention_out": scatter_about(splits[4], (HEADS * HEAD, D), (HEADS * HEAD // 64) ** -0.5, 2.0, ((0, 8),)),
        "mixer_in": scatter_about(splits[5], (D, IN_W), D ** -0.5, 0.1875, ((0, 8),)),
        "filter_taps": scatter_about(splits[6], (CONV, XBC), CONV ** -0.5, 3.0, ((1, 8),)),
        "filter_bias": scatter_about(splits[7], (XBC,), 0.5, 3.0, ((0, 8),)),
        "step_bias": jnp.clip(jax.random.uniform(splits[8], (SSM_HEADS,), jnp.float32, -6.0, -2.0), -6.0, -2.0),
        "decay_log": jnp.clip(jax.random.uniform(splits[9], (SSM_HEADS,), jnp.float32, -3.0, 1.5), -3.0, 1.5),
        "skip_scale": jnp.clip(jax.random.uniform(splits[10], (SSM_HEADS,), jnp.float32, 0.5, 1.5), 0.5, 1.5),
        "mixer_gain": jnp.clip(1.0 + 0.1 * jax.random.normal(splits[11], (SSM_HEADS * SSM_HEAD,), jnp.float32), 0.5, 1.5).astype(jnp.bfloat16),
        "mixer_out": scatter_about(splits[12], (SSM_HEADS * SSM_HEAD, D), (SSM_HEADS * SSM_HEAD) ** -0.5, 0.15625, ((0, 8),)),
        "feed_gain": jnp.clip(1.0 + 0.1 * jax.random.normal(splits[13], (D,), jnp.float32), 0.5, 1.5).astype(jnp.bfloat16),
        "gate_up": scatter_about(splits[14], (D, 2 * FF), D ** -0.5, 0.1875, ((0, 8),)),
        "down_proj": scatter_about(splits[15], (FF, D), FF ** -0.5, 0.125, ((0, 8),)),
        "cotangent": scatter_about(splits[16], (SEQS, LEN, D), 1.0, 6.0, ((0, 4), (1, 8))),
    }


NORM_EPS = 1e-05
ROPE_BASE = 100000000000.0
HIGHEST = lax.Precision.HIGHEST

def rms_scale(values, scales):
    return values * lax.rsqrt(lax.optimization_barrier(jnp.mean(values * values, axis=-1, keepdims=True)) + NORM_EPS) * scales

def rope_tables(positions, head_width):
    indices = jnp.arange(head_width // 2, dtype=jnp.float32)
    frequency = ROPE_BASE ** (-2.0 * indices / head_width)
    angles = positions.astype(jnp.float32)[:, None] * frequency[None, :]
    return (jnp.cos(angles), jnp.sin(angles))

def rotate(values, cosine_table, sine_table):
    middle = values.shape[-1] // 2
    lower_half = values[..., :middle]
    upper_half = values[..., middle:]
    cos_rows = cosine_table[:, None, :]
    sin_rows = sine_table[:, None, :]
    return jnp.concatenate([lower_half * cos_rows - upper_half * sin_rows, upper_half * cos_rows + lower_half * sin_rows], axis=-1)

def mixer_inputs(extended, step_raw, taps, tap_bias, step_bias, seg_ext):
    span_rows = step_raw.shape[1]
    tap_count = taps.shape[0]
    own_doc = seg_ext[:, tap_count - 1:]
    summed = jnp.zeros((extended.shape[0], span_rows, extended.shape[2]), jnp.float32) + tap_bias
    for offset in range(tap_count):
        same_doc = (seg_ext[:, offset:offset + span_rows] == own_doc)[..., None]
        summed = summed + jnp.where(same_doc, extended[:, offset:offset + span_rows] * taps[offset], 0.0)
    active = jax.nn.silu(summed)
    step_sizes = jax.nn.softplus(step_raw + step_bias)
    inner_width = SSM_HEADS * SSM_HEAD
    heads_x = active[..., :inner_width].reshape(active.shape[0], span_rows, SSM_HEADS, SSM_HEAD)
    return (heads_x, active[..., inner_width:inner_width + STATE], active[..., inner_width + STATE:], step_sizes)

def span_states(heads_x, input_map, step_sizes, decay_log, seg_ext):
    doc_ids = seg_ext[:, CONV - 1:]
    log_rates = step_sizes * -jnp.exp(decay_log)
    running = jnp.cumsum(log_rates, axis=1)
    final_sum = running[:, -1:, :]
    tail_doc = doc_ids[:, -1:]
    state_weights = jnp.where((doc_ids == tail_doc)[..., None], jnp.exp(final_sum - running), 0.0) * step_sizes
    states = jnp.einsum('sqhp,sqn->shpn', state_weights[..., None] * heads_x, input_map, precision=HIGHEST)
    carried = jnp.where(tail_doc == seg_ext[:, CONV - 2:CONV - 1], jnp.exp(final_sum[:, 0, :]), 0.0)
    return (carried, states)

def span_output(heads_x, input_map, output_map, step_sizes, decay_log, skip_scale, start_state, seg_ext):
    doc_ids = seg_ext[:, CONV - 1:]
    prior_doc = seg_ext[:, CONV - 2:CONV - 1]
    span_rows = doc_ids.shape[1]
    log_rates = step_sizes * -jnp.exp(decay_log)
    running = jnp.cumsum(log_rates, axis=1)
    running_heads = jnp.swapaxes(running, 1, 2)
    token_order = jnp.arange(span_rows)
    allowed = (token_order[:, None] >= token_order[None, :]) & (doc_ids[:, :, None] == doc_ids[:, None, :])
    allowed = allowed[:, None, :, :]
    spread = running_heads[:, :, :, None] - running_heads[:, :, None, :]
    decays = jnp.where(allowed, jnp.exp(jnp.where(allowed, spread, 0.0)), 0.0)
    gram_matrix = jnp.einsum('stn,sun->stu', output_map, input_map, precision=HIGHEST)
    mixing = decays * gram_matrix[:, None, :, :] * jnp.swapaxes(step_sizes, 1, 2)[:, :, None, :]
    result = jnp.einsum('shtu,suhp->sthp', mixing, heads_x, precision=HIGHEST)
    entering = jnp.where((doc_ids == prior_doc)[..., None], jnp.exp(running), 0.0)
    result = result + entering[..., None] * jnp.einsum('stn,shpn->sthp', output_map, start_state, precision=HIGHEST)
    return result + skip_scale[:, None] * heads_x

def gated_norm(mixed, gate_part, scales):
    flat_mixed = mixed.reshape(gate_part.shape)
    return rms_scale(flat_mixed * jax.nn.silu(gate_part), scales)

def swiglu(gate_vals, up_vals):
    return jax.nn.silu(gate_vals) * up_vals

def attend(queries, keys, values, allowed):
    group_count, row_count, head_width = queries.shape
    flat_queries = queries.reshape(group_count * row_count, head_width)
    scores = (jnp.dot(flat_queries, keys.T, preferred_element_type=jnp.float32) * HEAD ** (-0.5)).reshape(group_count, row_count, -1)
    scores = jnp.where(allowed[None], scores, -jnp.inf)
    log_total = jnp.log(lax.optimization_barrier(jnp.sum(jnp.exp(scores), axis=-1)))
    weights_low = jnp.exp(scores - log_total[..., None]).astype(jnp.bfloat16)
    output = jnp.dot(weights_low.reshape(group_count * row_count, -1), values, preferred_element_type=jnp.float32)
    return (output.reshape(group_count, row_count, head_width).astype(jnp.bfloat16), log_total)

def attend_back(queries, keys, values, allowed, log_total, output, grad_out):
    group_count, row_count, head_width = queries.shape
    flat_queries = queries.reshape(group_count * row_count, head_width)
    scores = (jnp.dot(flat_queries, keys.T, preferred_element_type=jnp.float32) * HEAD ** (-0.5)).reshape(group_count, row_count, -1)
    probs_full = jnp.where(allowed[None], jnp.exp(scores - log_total[..., None]), 0.0)
    grad_flat = grad_out.reshape(group_count * row_count, head_width)
    grad_values = jnp.dot(probs_full.astype(jnp.bfloat16).reshape(group_count * row_count, -1).T, grad_flat, preferred_element_type=jnp.float32)
    grad_probs = jnp.dot(grad_flat, values.T, preferred_element_type=jnp.float32).reshape(group_count, row_count, -1)
    centre = lax.optimization_barrier(jnp.sum(grad_out.astype(jnp.float32) * output.astype(jnp.float32), axis=-1))
    grad_scores = (probs_full * (grad_probs - centre[..., None]) * HEAD ** (-0.5)).astype(jnp.bfloat16).reshape(group_count * row_count, -1)
    grad_queries = jnp.dot(grad_scores, keys, preferred_element_type=jnp.float32).reshape(group_count, row_count, head_width)
    grad_keys = jnp.dot(grad_scores.T, flat_queries, preferred_element_type=jnp.float32)
    return (grad_queries, grad_keys, grad_values)

def forward_link(state_now, element):
    return (element[0][:, None, None] * state_now + element[1], state_now)

def backward_link(grad_now, element):
    return (element[1] + element[0][:, None, None] * grad_now, grad_now)

def reference(tokens, segments, input_gain, attention_in, attention_out, mixer_in, filter_taps, filter_bias, step_bias, decay_log, skip_scale, mixer_gain, mixer_out, feed_gain, gate_up, down_proj, cotangent):
    inner_width = SSM_HEADS * SSM_HEAD
    xbc_width = inner_width + 2 * STATE
    query_width = HEADS * HEAD
    kv_width = KV_HEADS * HEAD
    group_size = HEADS // KV_HEADS
    rim_rows = CONV - 1
    cosine_table, sine_table = rope_tables(jnp.arange(LEN), HEAD)
    key_order = jnp.arange(LEN)
    block_rows = (jnp.arange(N_GRP)[:, None] * SPAN + jnp.arange(SPAN + rim_rows)[None, :]).reshape(-1)
    starts_at = jnp.arange(N_GRP) * SPAN
    gain_in = input_gain.astype(jnp.float32)
    gain_mix = mixer_gain.astype(jnp.float32)
    gain_feed = feed_gain.astype(jnp.float32)
    taps_float = filter_taps.astype(jnp.float32)
    tap_bias = filter_bias.astype(jnp.float32)
    turner = partial(rotate, cosine_table=cosine_table, sine_table=sine_table)

    def one_sequence(totals, inputs):
        seq_tokens, seq_docs, seq_grad = inputs
        token_float = seq_tokens.astype(jnp.float32)
        normed, norm_back = jax.vjp(rms_scale, token_float, gain_in)
        normed_low = normed.astype(jnp.bfloat16)
        projected = jnp.dot(normed_low, attention_in, preferred_element_type=jnp.float32)
        query_raw = projected[:, :query_width].reshape(LEN, HEADS, HEAD)
        key_raw = projected[:, query_width:query_width + kv_width].reshape(LEN, KV_HEADS, HEAD)
        value_low = projected[:, query_width + kv_width:].astype(jnp.bfloat16).reshape(LEN, KV_HEADS, HEAD)
        query_rot, query_back = jax.vjp(turner, query_raw)
        key_rot, key_back = jax.vjp(turner, key_raw)
        query_low = query_rot.astype(jnp.bfloat16)
        key_low = key_rot.astype(jnp.bfloat16)
        query_blocks = query_low.reshape(N_GRP, SPAN, KV_HEADS, group_size, HEAD).transpose(0, 2, 3, 1, 4)
        keys_heads = key_low.transpose(1, 0, 2)
        values_heads = value_low.transpose(1, 0, 2)

        def visible_for(block_start):
            query_pos = block_start + jnp.arange(SPAN)
            return (key_order[None, :] <= query_pos[:, None]) & (seq_docs[None, :] == seq_docs[query_pos][:, None])

        def forward_block(packed):
            block_queries, block_start = packed
            visible = visible_for(block_start)
            results = [attend(block_queries[head_index], keys_heads[head_index], values_heads[head_index], visible) for head_index in range(KV_HEADS)]
            return (jnp.stack([result_pair[0] for result_pair in results]), jnp.stack([result_pair[1] for result_pair in results]))
        attn_blocks, lse_blocks = lax.map(forward_block, (query_blocks, starts_at))
        attended = attn_blocks.transpose(0, 3, 1, 2, 4).reshape(LEN, query_width)
        mix_proj = jnp.dot(normed_low, mixer_in, preferred_element_type=jnp.float32)
        gate_part = mix_proj[:, :inner_width].reshape(N_GRP, SPAN, inner_width)
        conv_low = mix_proj[:, inner_width:inner_width + xbc_width].astype(jnp.bfloat16)
        step_raw = mix_proj[:, inner_width + xbc_width:].reshape(N_GRP, SPAN, SSM_HEADS)
        padded = jnp.concatenate([jnp.zeros((rim_rows, xbc_width), jnp.bfloat16), conv_low], axis=0)
        extended = padded[block_rows].reshape(N_GRP, SPAN + rim_rows, xbc_width).astype(jnp.float32)
        padded_docs = jnp.concatenate([jnp.full((rim_rows,), -1, jnp.int32), seq_docs], axis=0)
        seg_ext = padded_docs[block_rows].reshape(N_GRP, SPAN + rim_rows)
        (heads_x, input_map, output_map, step_sizes), prep_back = jax.vjp(partial(mixer_inputs, seg_ext=seg_ext), extended, step_raw, taps_float, tap_bias, step_bias)
        (carried, states), states_back = jax.vjp(partial(span_states, seg_ext=seg_ext), heads_x, input_map, step_sizes, decay_log)
        empty_state = jnp.zeros(states.shape[1:], jnp.float32)
        final_state, entering = lax.scan(forward_link, empty_state, (carried, states))
        mixed, output_back = jax.vjp(partial(span_output, seg_ext=seg_ext), heads_x, input_map, output_map, step_sizes, decay_log, skip_scale, entering)
        normed_mix, gate_back = jax.vjp(gated_norm, mixed, gate_part, gain_mix)
        normed_mix_low = normed_mix.reshape(LEN, inner_width).astype(jnp.bfloat16)
        hidden = token_float + jnp.dot(attended, attention_out, preferred_element_type=jnp.float32) + jnp.dot(normed_mix_low, mixer_out, preferred_element_type=jnp.float32)
        normed_feed, feed_back = jax.vjp(rms_scale, hidden, gain_feed)
        normed_feed_low = normed_feed.astype(jnp.bfloat16)
        gate_vals = jnp.dot(normed_feed_low, gate_up, preferred_element_type=jnp.float32)
        activation, act_back = jax.vjp(swiglu, gate_vals[:, :FF], gate_vals[:, FF:])
        activation_low = activation.astype(jnp.bfloat16)
        out_seq = (hidden + jnp.dot(activation_low, down_proj, preferred_element_type=jnp.float32)).astype(jnp.bfloat16)
        grad_down = jnp.dot(activation_low.T, seq_grad, preferred_element_type=jnp.float32)
        grad_act = jnp.dot(seq_grad, down_proj.T, preferred_element_type=jnp.float32)
        grad_gate, grad_upper = act_back(grad_act)
        grad_gu = jnp.concatenate([grad_gate, grad_upper], axis=-1).astype(jnp.bfloat16)
        grad_gate_up = jnp.dot(normed_feed_low.T, grad_gu, preferred_element_type=jnp.float32)
        grad_feed_in = jnp.dot(grad_gu, gate_up.T, preferred_element_type=jnp.float32)
        grad_hidden_norm, grad_feed = feed_back(grad_feed_in)
        grad_hidden = seq_grad.astype(jnp.float32) + grad_hidden_norm
        grad_hidden_low = grad_hidden.astype(jnp.bfloat16)
        grad_attn_out = jnp.dot(attended.T, grad_hidden_low, preferred_element_type=jnp.float32)
        grad_attended = jnp.dot(grad_hidden_low, attention_out.T, preferred_element_type=jnp.float32).astype(jnp.bfloat16)
        grad_mix_out = jnp.dot(normed_mix_low.T, grad_hidden_low, preferred_element_type=jnp.float32)
        grad_normed_mix = jnp.dot(grad_hidden_low, mixer_out.T, preferred_element_type=jnp.float32)
        grad_mixed, grad_gate_part, grad_mix_gain = gate_back(grad_normed_mix.reshape(N_GRP, SPAN, inner_width))
        grad_x_one, grad_in_one, grad_out_map, grad_step_one, grad_log_one, grad_skip, grad_entering = output_back(grad_mixed)
        first_grad, later = lax.scan(backward_link, empty_state, (carried, grad_entering), reverse=True)
        grad_carried = lax.optimization_barrier(jnp.sum(later * entering, axis=(2, 3)))
        grad_x_two, grad_in_two, grad_step_two, grad_log_two = states_back((grad_carried, later))
        grad_extended, grad_step_raw, grad_taps, grad_tap_bias, grad_step_bias = prep_back((grad_x_one + grad_x_two, grad_in_one + grad_in_two, grad_out_map, grad_step_one + grad_step_two))
        grad_conv = jnp.zeros((LEN + rim_rows, xbc_width), jnp.float32).at[block_rows].add(grad_extended.reshape(-1, xbc_width))[rim_rows:]
        grad_mix_proj = jnp.concatenate([grad_gate_part.reshape(LEN, inner_width), grad_conv, grad_step_raw.reshape(LEN, SSM_HEADS)], axis=-1).astype(jnp.bfloat16)
        grad_mix_in = jnp.dot(normed_low.T, grad_mix_proj, preferred_element_type=jnp.float32)
        grad_normed_m = jnp.dot(grad_mix_proj, mixer_in.T, preferred_element_type=jnp.float32)
        grad_blocks = grad_attended.reshape(N_GRP, SPAN, KV_HEADS, group_size, HEAD).transpose(0, 2, 3, 1, 4)

        def backward_block(packed):
            block_queries, block_out, block_lse, block_grad, block_start = packed
            visible = visible_for(block_start)
            results = [attend_back(block_queries[head_index], keys_heads[head_index], values_heads[head_index], visible, block_lse[head_index], block_out[head_index], block_grad[head_index]) for head_index in range(KV_HEADS)]
            return tuple((jnp.stack([entry[part_index] for entry in results]) for part_index in range(3)))
        grad_q_blocks, grad_k_blocks, grad_v_blocks = lax.map(backward_block, (query_blocks, attn_blocks, lse_blocks, grad_blocks, starts_at))
        grad_query = grad_q_blocks.transpose(0, 3, 1, 2, 4).reshape(LEN, HEADS, HEAD)
        grad_key = lax.optimization_barrier(jnp.sum(grad_k_blocks, axis=0)).transpose(1, 0, 2)
        grad_value = lax.optimization_barrier(jnp.sum(grad_v_blocks, axis=0)).transpose(1, 0, 2)
        grad_query_raw, = query_back(grad_query)
        grad_key_raw, = key_back(grad_key)
        grad_projected = jnp.concatenate([grad_query_raw.reshape(LEN, query_width), grad_key_raw.reshape(LEN, kv_width), grad_value.reshape(LEN, kv_width)], axis=-1).astype(jnp.bfloat16)
        grad_attn_in = jnp.dot(normed_low.T, grad_projected, preferred_element_type=jnp.float32)
        grad_normed_a = jnp.dot(grad_projected, attention_in.T, preferred_element_type=jnp.float32)
        grad_token_norm, grad_gain_in = norm_back(grad_normed_a + grad_normed_m)
        grad_token = grad_hidden + grad_token_norm
        terms = (grad_gain_in, grad_attn_in, grad_attn_out, grad_mix_in, grad_taps, grad_tap_bias, grad_step_bias, grad_log_one + grad_log_two, grad_skip, grad_mix_gain, grad_mix_out, grad_feed, grad_gate_up, grad_down)
        return (tuple((total + term for total, term in zip(totals, terms))), (out_seq, grad_token))
    zero_totals = (jnp.zeros(input_gain.shape, jnp.float32), jnp.zeros(attention_in.shape, jnp.float32), jnp.zeros(attention_out.shape, jnp.float32), jnp.zeros(mixer_in.shape, jnp.float32), jnp.zeros(filter_taps.shape, jnp.float32), jnp.zeros(filter_bias.shape, jnp.float32), jnp.zeros(step_bias.shape, jnp.float32), jnp.zeros(decay_log.shape, jnp.float32), jnp.zeros(skip_scale.shape, jnp.float32), jnp.zeros(mixer_gain.shape, jnp.float32), jnp.zeros(mixer_out.shape, jnp.float32), jnp.zeros(feed_gain.shape, jnp.float32), jnp.zeros(gate_up.shape, jnp.float32), jnp.zeros(down_proj.shape, jnp.float32))
    totals, outputs = lax.scan(one_sequence, zero_totals, (tokens, segments, cotangent))
    return (outputs[0], outputs[1], totals[0], totals[1], totals[2], totals[3], totals[4], totals[5], totals[6], totals[7], totals[8], totals[9], totals[10], totals[11], totals[12], totals[13])
```

```python
import functools
from functools import partial

import jax
import jax.numpy as jnp
from jax import lax
from jax.experimental import pallas as pl
from jax.experimental.pallas import tpu as pltpu
from jax.sharding import PartitionSpec as P

HEADS = 8
KV_HEADS = 2
HEAD = 64
SSM_HEADS = 24
SSM_HEAD = 64
STATE = 128
CONV = 4
FF = 2048


NORM_EPS = 1e-05
ROPE_BASE = 100000000000.0
HIGHEST = lax.Precision.HIGHEST


def shifted(value, axis, steps):
    count = lax.axis_size(axis)
    leading, last = (max(0, -steps), min(count, count - steps))
    return lax.ppermute(value, axis, [(source, source + steps) for source in range(leading, last)])


def prefix(array, axis, combine, identity, reverse):
    peers, position = (lax.axis_size(axis), lax.axis_index(axis))
    everything = jax.tree.map(lambda part: lax.all_gather(part, axis), array)
    start = jax.tree.map(
        lambda part, zero: jnp.broadcast_to(jnp.asarray(zero, part.dtype), part.shape),
        array,
        identity,
    )

    def hop(k, before):
        at = peers - 1 - k if reverse else k
        reached = at > position if reverse else at < position
        new = combine(before, jax.tree.map(lambda part: part[at], everything))
        return jax.tree.map(lambda a, b: jnp.where(reached, a, b), new, before)

    return lax.fori_loop(0, peers, hop, start)


def rms_scale(values, scales):
    return values * lax.rsqrt(jnp.mean(values * values, axis=-1, keepdims=True) + NORM_EPS) * scales


def rope_tables(positions, head_width):
    indices = jnp.arange(head_width // 2, dtype=jnp.float32)
    frequency = ROPE_BASE ** (-2.0 * indices / head_width)
    angles = positions.astype(jnp.float32)[:, None] * frequency[None, :]
    return (jnp.cos(angles), jnp.sin(angles))


def rotate(values, cosine_table, sine_table):
    middle = values.shape[-1] // 2
    lower_half = values[..., :middle]
    upper_half = values[..., middle:]
    cos_rows = cosine_table[:, None, :]
    sin_rows = sine_table[:, None, :]
    return jnp.concatenate(
        [
            lower_half * cos_rows - upper_half * sin_rows,
            upper_half * cos_rows + lower_half * sin_rows,
        ],
        axis=-1,
    )


def mixer_inputs(extended, step_raw, taps, tap_bias, step_bias, seg_ext):
    span_rows = step_raw.shape[1]
    tap_count = taps.shape[0]
    own_doc = seg_ext[:, tap_count - 1 :]
    summed = jnp.zeros((extended.shape[0], span_rows, extended.shape[2]), jnp.float32) + tap_bias
    for offset in range(tap_count):
        same_doc = (seg_ext[:, offset : offset + span_rows] == own_doc)[..., None]
        summed = summed + jnp.where(
            same_doc, extended[:, offset : offset + span_rows] * taps[offset], 0.0
        )
    active = jax.nn.silu(summed)
    step_sizes = jax.nn.softplus(step_raw + step_bias)
    inner_width = SSM_HEADS * SSM_HEAD
    heads_x = active[..., :inner_width].reshape(active.shape[0], span_rows, SSM_HEADS, SSM_HEAD)
    return (
        heads_x,
        active[..., inner_width : inner_width + STATE],
        active[..., inner_width + STATE :],
        step_sizes,
    )


def span_states(heads_x, input_map, step_sizes, decay_log, seg_ext):
    doc_ids = seg_ext[:, CONV - 1 :]
    log_rates = step_sizes * -jnp.exp(decay_log)
    running = jnp.cumsum(log_rates, axis=1)
    final_sum = running[:, -1:, :]
    tail_doc = doc_ids[:, -1:]
    state_weights = (
        jnp.where((doc_ids == tail_doc)[..., None], jnp.exp(final_sum - running), 0.0) * step_sizes
    )
    states = jnp.einsum(
        "sqhp,sqn->shpn", state_weights[..., None] * heads_x, input_map, precision=HIGHEST
    )
    carried = jnp.where(
        tail_doc == seg_ext[:, CONV - 2 : CONV - 1], jnp.exp(final_sum[:, 0, :]), 0.0
    )
    return (carried, states)


def span_output(
    heads_x, input_map, output_map, step_sizes, decay_log, skip_scale, start_state, seg_ext
):
    doc_ids = seg_ext[:, CONV - 1 :]
    prior_doc = seg_ext[:, CONV - 2 : CONV - 1]
    span_rows = doc_ids.shape[1]
    log_rates = step_sizes * -jnp.exp(decay_log)
    running = jnp.cumsum(log_rates, axis=1)
    running_heads = jnp.swapaxes(running, 1, 2)
    token_order = jnp.arange(span_rows)
    allowed = (token_order[:, None] >= token_order[None, :]) & (
        doc_ids[:, :, None] == doc_ids[:, None, :]
    )
    allowed = allowed[:, None, :, :]
    spread = running_heads[:, :, :, None] - running_heads[:, :, None, :]
    decays = jnp.where(allowed, jnp.exp(jnp.where(allowed, spread, 0.0)), 0.0)
    gram_matrix = jnp.einsum("stn,sun->stu", output_map, input_map, precision=HIGHEST)
    mixing = decays * gram_matrix[:, None, :, :] * jnp.swapaxes(step_sizes, 1, 2)[:, :, None, :]
    result = jnp.einsum("shtu,suhp->sthp", mixing, heads_x, precision=HIGHEST)
    entering = jnp.where((doc_ids == prior_doc)[..., None], jnp.exp(running), 0.0)
    result = result + entering[..., None] * jnp.einsum(
        "stn,shpn->sthp", output_map, start_state, precision=HIGHEST
    )
    return result + skip_scale[:, None] * heads_x


def gated_norm(mixed, gate_part, scales):
    flat_mixed = mixed.reshape(gate_part.shape)
    return rms_scale(flat_mixed * jax.nn.silu(gate_part), scales)


def swiglu(gate_vals, up_vals):
    return jax.nn.silu(gate_vals) * up_vals


def attend(queries, keys, values, allowed):
    group_count, row_count, head_width = queries.shape
    flat_queries = queries.reshape(group_count * row_count, head_width)
    scores = (
        jnp.dot(flat_queries, keys.T, preferred_element_type=jnp.float32) * HEAD ** (-0.5)
    ).reshape(group_count, row_count, -1)
    scores = jnp.where(allowed[None], scores, -jnp.inf)
    log_total = jnp.log(jnp.sum(jnp.exp(scores), axis=-1))
    weights_low = jnp.exp(scores - log_total[..., None]).astype(jnp.bfloat16)
    output = jnp.dot(
        weights_low.reshape(group_count * row_count, -1), values, preferred_element_type=jnp.float32
    )
    return (output.reshape(group_count, row_count, head_width).astype(jnp.bfloat16), log_total)


def attend_back(queries, keys, values, allowed, log_total, output, grad_out):
    group_count, row_count, head_width = queries.shape
    flat_queries = queries.reshape(group_count * row_count, head_width)
    scores = (
        jnp.dot(flat_queries, keys.T, preferred_element_type=jnp.float32) * HEAD ** (-0.5)
    ).reshape(group_count, row_count, -1)
    probs_full = jnp.where(allowed[None], jnp.exp(scores - log_total[..., None]), 0.0)
    grad_flat = grad_out.reshape(group_count * row_count, head_width)
    grad_values = jnp.dot(
        probs_full.astype(jnp.bfloat16).reshape(group_count * row_count, -1).T,
        grad_flat,
        preferred_element_type=jnp.float32,
    )
    grad_probs = jnp.dot(grad_flat, values.T, preferred_element_type=jnp.float32).reshape(
        group_count, row_count, -1
    )
    centre = jnp.sum(grad_out.astype(jnp.float32) * output.astype(jnp.float32), axis=-1)
    grad_scores = (
        (probs_full * (grad_probs - centre[..., None]) * HEAD ** (-0.5))
        .astype(jnp.bfloat16)
        .reshape(group_count * row_count, -1)
    )
    grad_queries = jnp.dot(grad_scores, keys, preferred_element_type=jnp.float32).reshape(
        group_count, row_count, head_width
    )
    grad_keys = jnp.dot(grad_scores.T, flat_queries, preferred_element_type=jnp.float32)
    return (grad_queries, grad_keys, grad_values)


def attend_item(packed):
    return attend(packed[0], packed[1], packed[2], packed[3])


def attend_back_item(packed):
    return attend_back(packed[0], packed[1], packed[2], packed[3], packed[4], packed[5], packed[6])


def chain_combine(earlier, later):
    return (earlier[0] * later[0], earlier[1] * later[0][:, :, None, None] + later[1])


MESH = pl.DeviceIdType.MESH
VMEM_LIMIT = 60 * 1024 * 1024


def seat():
    rep, grp = lax.axis_index("rep"), lax.axis_index("grp")
    chips = lax.axis_size("grp") // 2
    quarter = lax.rem(rep, 4)
    base = rep - quarter
    flip_x = quarter + 1 - 2 * lax.rem(quarter, 2)
    flip_y = lax.rem(quarter + 2, 4)
    chip, core = lax.div(grp, 2), lax.rem(grp, 2)
    return dict(
        quarter=quarter,
        qx=flip_x,
        qy=flip_y,
        qd=lax.rem(flip_x + 2, 4),
        chip=chip,
        core=core,
        x={"rep": base + flip_x},
        y={"rep": base + flip_y},
        partner={"grp": chip * 2 + 1 - core},
        along=[{"grp": lax.rem(chip + k, chips) * 2 + core} for k in range(chips)],
        chip_to=[lax.rem(chip + k, chips) for k in range(chips)],
        chip_from=[lax.rem(chip - k + chips, chips) for k in range(chips)],
    )


def remote(source, target, sent, arrived, device):
    return pltpu.make_async_remote_copy(
        src_ref=source,
        dst_ref=target,
        send_sem=sent,
        recv_sem=arrived,
        device_id=device,
        device_id_type=MESH,
    )


def greet(me, extra=()):
    barrier = pltpu.get_barrier_semaphore()
    others = [me["x"], me["y"], me["partner"], *me["along"][1:], *extra]
    for device in others:
        pl.semaphore_signal(barrier, inc=1, device_id=device, device_id_type=MESH)
    pl.semaphore_wait(barrier, len(others))


def near_first(chips):
    return sorted(range(1, chips), key=lambda k: min(k, chips - k))


def gather_kernel(count, whole, chips, *refs):
    ins, outs = refs[:count], refs[count : 2 * count]
    zs, zr, xs, xr, ys, yr, ds, dr, cs, cr, ls = refs[2 * count :]
    me = seat()
    greet(me)
    own = me["chip"] * 2 + me["core"]
    order = near_first(chips)
    along, over_x, over_y, diagonal, across, local = {}, {}, {}, {}, {}, []
    for m in range(count):
        local.append(pltpu.make_async_copy(ins[m], outs[m].at[own], ls.at[m]))
        local[-1].start()
        for k in order:
            part = ins[m] if whole[m] else ins[m].at[me["quarter"]]
            place = outs[m].at[own] if whole[m] else outs[m].at[own, me["quarter"]]
            along[m, k] = remote(part, place, zs.at[m, k], zr.at[m, k], me["along"][k])
            along[m, k].start()
        across[m, 0] = remote(ins[m], outs[m].at[own], cs.at[m, 0], cr.at[m, 0], me["partner"])
        across[m, 0].start()
    for step in range(count + 2):
        m = step
        if m < count:
            for k in order:
                along[m, k].wait_recv()
                if whole[m]:
                    continue
                piece = outs[m].at[me["chip_from"][k] * 2 + me["core"], me["quarter"]]
                over_x[m, k] = remote(piece, piece, xs.at[m, k], xr.at[m, k], me["x"])
                over_y[m, k] = remote(piece, piece, ys.at[m, k], yr.at[m, k], me["y"])
                over_x[m, k].start()
                over_y[m, k].start()
        m = step - 1
        if 0 <= m < count and not whole[m]:
            for k in order:
                block = outs[m].at[me["chip_from"][k] * 2 + me["core"]]
                if (m + k) % 2 == 0:
                    over_x[m, k].wait_recv()
                    piece, device = block.at[me["qx"]], me["y"]
                else:
                    over_y[m, k].wait_recv()
                    piece, device = block.at[me["qy"]], me["x"]
                diagonal[m, k] = remote(piece, piece, ds.at[m, k], dr.at[m, k], device)
                diagonal[m, k].start()
        m = step - 2
        if 0 <= m < count:
            for k in order:
                block = outs[m].at[me["chip_from"][k] * 2 + me["core"]]
                if not whole[m]:
                    if (m + k) % 2 == 0:
                        over_y[m, k].wait_recv()
                    else:
                        over_x[m, k].wait_recv()
                    diagonal[m, k].wait_recv()
                across[m, k] = remote(block, block, cs.at[m, k], cr.at[m, k], me["partner"])
                across[m, k].start()
    for copy in across.values():
        copy.wait_recv()
    for copies in (along, over_x, over_y, diagonal, across):
        for copy in copies.values():
            copy.wait_send()
    for copy in local:
        copy.wait()


def gather_group(shards, whole):
    group = lax.axis_size("grp")
    chips = group // 2
    count = len(shards)
    cut = [
        shard[None] if flag else shard.reshape(4, shard.shape[0] // 4, shard.shape[1])
        for shard, flag in zip(shards, whole)
    ]
    sems = [pltpu.SemaphoreType.DMA((count, chips))] * 10 + [pltpu.SemaphoreType.DMA((count,))]
    full = pl.pallas_call(
        functools.partial(gather_kernel, count, whole, chips),
        out_shape=[jax.ShapeDtypeStruct((group, *part.shape), part.dtype) for part in cut],
        in_specs=[pl.BlockSpec(memory_space=pltpu.VMEM)] * count,
        out_specs=[pl.BlockSpec(memory_space=pl.ANY)] * count,
        scratch_shapes=sems,
        compiler_params=pltpu.CompilerParams(
            collective_id=0, has_side_effects=True, vmem_limit_bytes=VMEM_LIMIT
        ),
        name="gather_group",
    )(*cut)
    return [part.reshape(-1, part.shape[-1]) for part in full]


def reduce_kernel(count, routes, chips, extras, *refs):
    parts, outs = refs[:count], refs[count : 2 * count]
    rest = refs[2 * count :]
    one, staged, two, total, slots = (rest[i * count : (i + 1) * count] for i in range(5))
    extra_in = rest[5 * count : 6 * count] if extras > 1 else ()
    sems = rest[(6 if extras > 1 else 5) * count :]
    s1, r1, s2, r2, zs, zr, es, er, gs, gr = sems
    me = seat()
    rep = lax.axis_index("rep")
    reps = lax.axis_size("rep")
    beyond = [{"rep": lax.rem(rep + 4 * e, reps)} for e in range(1, extras)]
    greet(me, beyond)
    first, second, along, other, spread = {}, {}, {}, {}, {}
    for m in range(count):
        device, mine = (me["x"], me["qx"]) if routes[m] == 0 else (me["y"], me["qy"])
        for i, q in enumerate((mine, me["qd"])):
            first[m, i] = remote(parts[m].at[q], one[m].at[i], s1.at[m, i], r1.at[m, i], device)
        first[m, 1].start()
        first[m, 0].start()

    def over_chips(body):
        lax.fori_loop(0, chips, lambda j, _: (body(j), 0)[1], 0)

    def f32(value):
        return value.astype(jnp.float32)

    for step in range(count + 3):
        m = step
        if m < count:
            device, q = (me["y"], me["qy"]) if routes[m] == 0 else (me["x"], me["qx"])
            first[m, 1].wait_recv()

            def add_first(j, m=m, q=q):
                staged[m][j] = (f32(parts[m][q, j]) + f32(one[m][1, j])).astype(jnp.bfloat16)

            over_chips(add_first)
            second[m] = remote(staged[m], two[m], s2.at[m], r2.at[m], device)
            second[m].start()
        m = step - 1
        if 0 <= m < count:
            first[m, 0].wait_recv()
            second[m].wait_recv()

            def add_second(j, m=m):
                value = f32(parts[m][me["quarter"], j]) + f32(one[m][0, j]) + f32(two[m][j])
                total[m][j] = value.astype(jnp.bfloat16)

            over_chips(add_second)
            for k in near_first(chips):
                along[m, k] = remote(
                    total[m].at[me["chip_to"][k]],
                    slots[m].at[k],
                    zs.at[m, k],
                    zr.at[m, k],
                    me["along"][k],
                )
                along[m, k].start()
        m = step - 2
        if 0 <= m < count:
            value = f32(total[m][me["chip"]])
            for k in near_first(chips):
                along[m, k].wait_recv()
                value = value + f32(slots[m][k])
            if extras > 1:
                extra_in[m][0] = value.astype(jnp.bfloat16)
                for e in range(1, extras):
                    other[m, e] = remote(
                        extra_in[m].at[0],
                        extra_in[m].at[e],
                        es.at[m, e],
                        er.at[m, e],
                        beyond[e - 1],
                    )
                    other[m, e].start()
                for e in range(1, extras):
                    other[m, e].wait_recv()
                    value = value + f32(extra_in[m][e])
            outs[m][me["quarter"]] = value.astype(jnp.bfloat16)
            piece = outs[m].at[me["quarter"]]
            for i, device in enumerate((me["x"], me["y"])):
                spread[m, i] = remote(piece, piece, gs.at[m, i], gr.at[m, i], device)
                spread[m, i].start()
        m = step - 3
        if 0 <= m < count:
            spread[m, routes[m]].wait_recv()
            q, device = (me["qx"], me["y"]) if routes[m] == 0 else (me["qy"], me["x"])
            piece = outs[m].at[q]
            spread[m, 2] = remote(piece, piece, gs.at[m, 2], gr.at[m, 2], device)
            spread[m, 2].start()
    for m in range(count):
        spread[m, 1 - routes[m]].wait_recv()
        spread[m, 2].wait_recv()
    for copies in (first, second, along, other, spread):
        for copy in copies.values():
            copy.wait_send()


def reduce_group(parts, routes):
    chips = lax.axis_size("grp") // 2
    extras = lax.axis_size("rep") // 4
    count = len(parts)
    half = jnp.bfloat16
    piece = [part.shape[2:] for part in parts]
    scratch = [pltpu.VMEM((2, chips, *shape), half) for shape in piece]
    scratch += [pltpu.VMEM((chips, *shape), half) for shape in piece]
    scratch += [pltpu.VMEM((chips, *shape), half) for shape in piece]
    scratch += [pltpu.VMEM((chips, *shape), half) for shape in piece]
    scratch += [pltpu.VMEM((chips, *shape), half) for shape in piece]
    if extras > 1:
        scratch += [pltpu.VMEM((extras, *shape), half) for shape in piece]
    dma = pltpu.SemaphoreType.DMA
    scratch += [dma((count, 2)), dma((count, 2)), dma((count,)), dma((count,))]
    scratch += [dma((count, chips)), dma((count, chips)), dma((count, extras)), dma((count, extras))]
    scratch += [dma((count, 3)), dma((count, 3))]
    sums = pl.pallas_call(
        functools.partial(reduce_kernel, count, routes, chips, extras),
        out_shape=[jax.ShapeDtypeStruct((4, *shape), half) for shape in piece],
        in_specs=[pl.BlockSpec(memory_space=pltpu.VMEM)] * count,
        out_specs=[pl.BlockSpec(memory_space=pltpu.VMEM)] * count,
        scratch_shapes=scratch,
        compiler_params=pltpu.CompilerParams(
            collective_id=1, has_side_effects=True, vmem_limit_bytes=VMEM_LIMIT
        ),
        name="reduce_group",
    )(*parts)
    return [total.reshape(-1, total.shape[-1]).astype(jnp.float32) for total in sums]


def swap_cores(value):
    group = lax.axis_size("grp")
    return lax.ppermute(value, "grp", [(i, i + 1 - 2 * (i % 2)) for i in range(group)])


def rows_by_core(activation):
    tokens, features = activation.shape
    chips = lax.axis_size("grp") // 2
    core = lax.rem(lax.axis_index("grp"), 2)
    turned = activation.T.reshape(chips, 2, 4, features // (8 * chips), tokens)
    own = lax.dynamic_index_in_dim(turned, core, 1, keepdims=False)
    other = lax.dynamic_index_in_dim(turned, 1 - core, 1, keepdims=False)
    own = own.transpose(1, 0, 2, 3).reshape(features // 2, tokens)
    other = other.transpose(1, 0, 2, 3).reshape(features // 2, tokens)
    return jnp.concatenate([own, swap_cores(other)], axis=1)


def both_tokens(value):
    return jnp.concatenate([value, swap_cores(value)], axis=0)


def weight_grad(rows, value):
    chips = lax.axis_size("grp") // 2
    grad = jnp.dot(rows, value, preferred_element_type=jnp.float32).astype(jnp.bfloat16)
    return grad.reshape(4, chips, -1, value.shape[1])


def shards(
    tokens,
    segments,
    input_gain,
    attention_in,
    attention_out,
    mixer_in,
    filter_taps,
    filter_bias,
    step_bias,
    decay_log,
    skip_scale,
    mixer_gain,
    mixer_out,
    feed_gain,
    gate_up,
    down_proj,
    cotangent,
):
    seq_count, span_len, model_width = tokens.shape
    row_count = seq_count * span_len
    seq_len = segments.shape[1]
    group_devices = lax.axis_size("grp")
    position = lax.axis_index("grp") * span_len
    inner_width = SSM_HEADS * SSM_HEAD
    xbc_width = inner_width + 2 * STATE
    query_width = HEADS * HEAD
    kv_width = KV_HEADS * HEAD
    group_size = HEADS // KV_HEADS
    rim_rows = CONV - 1
    small = [input_gain, filter_taps.reshape(-1), filter_bias, mixer_gain, feed_gain]
    sizes = [part.shape[0] for part in small]
    packed = jnp.concatenate(small)
    packed = jnp.pad(packed, (0, -packed.shape[0] % 2048)).reshape(-1, 128)
    full_attn_in, full_mix_in, full_small, full_gate_up, full_down, full_mix_out, full_attn_out = (
        gather_group(
            [attention_in, mixer_in, packed, gate_up, down_proj, mixer_out, attention_out],
            [False, False, True, False, False, False, False],
        )
    )
    full_small = full_small.reshape(group_devices, -1)
    starts = [sum(sizes[:i]) for i in range(len(sizes) + 1)]
    pieces = [full_small[:, starts[i] : starts[i + 1]] for i in range(len(sizes))]
    full_gain_in, full_tap_bias, full_mix_gain, full_feed_gain = (
        pieces[i].reshape(-1) for i in (0, 2, 3, 4)
    )
    full_taps = pieces[1].reshape(group_devices, CONV, -1).transpose(1, 0, 2).reshape(CONV, -1)
    back_attn_in, back_attn_out, back_mix_in = full_attn_in, full_attn_out, full_mix_in
    back_mix_out, back_gate_up, back_down = full_mix_out, full_gate_up, full_down
    offsets = position + jnp.arange(span_len, dtype=jnp.int32)
    token_float = tokens.reshape(row_count, model_width).astype(jnp.float32)
    normed, norm_back = jax.vjp(rms_scale, token_float, full_gain_in.astype(jnp.float32))
    normed_low = normed.astype(jnp.bfloat16)
    projected = jnp.dot(normed_low, full_attn_in, preferred_element_type=jnp.float32).reshape(
        seq_count, span_len, -1
    )
    cosine_table, sine_table = rope_tables(offsets, HEAD)
    turner = partial(rotate, cosine_table=cosine_table, sine_table=sine_table)
    query_raw = projected[..., :query_width].reshape(seq_count, span_len, HEADS, HEAD)
    key_raw = projected[..., query_width : query_width + kv_width].reshape(
        seq_count, span_len, KV_HEADS, HEAD
    )
    value_part = projected[..., query_width + kv_width :]
    query_rot, query_back = jax.vjp(turner, query_raw)
    key_rot, key_back = jax.vjp(turner, key_raw)
    query_low = query_rot.astype(jnp.bfloat16)
    kv_local = jnp.concatenate(
        [key_rot.reshape(seq_count, span_len, kv_width), value_part], axis=-1
    ).astype(jnp.bfloat16)
    kv_all = lax.all_gather(kv_local, "grp", axis=1, tiled=True)
    queries_grouped = (
        query_low.reshape(seq_count, span_len, KV_HEADS, group_size, HEAD)
        .transpose(0, 2, 3, 1, 4)
        .reshape(seq_count * KV_HEADS, group_size, span_len, HEAD)
    )
    keys_grouped = (
        kv_all[..., :kv_width]
        .reshape(seq_count, seq_len, KV_HEADS, HEAD)
        .transpose(0, 2, 1, 3)
        .reshape(seq_count * KV_HEADS, seq_len, HEAD)
    )
    values_grouped = (
        kv_all[..., kv_width:]
        .reshape(seq_count, seq_len, KV_HEADS, HEAD)
        .transpose(0, 2, 1, 3)
        .reshape(seq_count * KV_HEADS, seq_len, HEAD)
    )
    query_docs = lax.dynamic_slice_in_dim(segments, position, span_len, 1)
    key_order = jnp.arange(seq_len, dtype=jnp.int32)
    visible = (key_order[None, None, :] <= offsets[None, :, None]) & (
        segments[:, None, :] == query_docs[:, :, None]
    )
    visible_grouped = jnp.repeat(visible, KV_HEADS, axis=0)
    attn_heads, attn_lse = lax.map(
        attend_item, (queries_grouped, keys_grouped, values_grouped, visible_grouped)
    )
    attended = (
        attn_heads.reshape(seq_count, KV_HEADS, group_size, span_len, HEAD)
        .transpose(0, 3, 1, 2, 4)
        .reshape(row_count, query_width)
    )
    mix_proj = jnp.dot(normed_low, full_mix_in, preferred_element_type=jnp.float32).reshape(
        seq_count, span_len, -1
    )
    gate_part = mix_proj[..., :inner_width]
    conv_low = mix_proj[..., inner_width : inner_width + xbc_width].astype(jnp.bfloat16)
    step_raw = mix_proj[..., inner_width + xbc_width :]
    rim_in = shifted(conv_low[:, span_len - rim_rows :], "grp", 1)
    extended = jnp.concatenate([rim_in, conv_low], axis=1).astype(jnp.float32)
    padded_docs = jnp.concatenate(
        [jnp.full((seq_count, rim_rows), -1, jnp.int32), segments], axis=1
    )
    seg_ext = lax.dynamic_slice_in_dim(padded_docs, position, span_len + rim_rows, 1)
    (heads_x, input_map, output_map, step_sizes), prep_back = jax.vjp(
        partial(mixer_inputs, seg_ext=seg_ext),
        extended,
        step_raw,
        full_taps.astype(jnp.float32),
        full_tap_bias.astype(jnp.float32),
        step_bias,
    )
    (carried, states), states_back = jax.vjp(
        partial(span_states, seg_ext=seg_ext), heads_x, input_map, step_sizes, decay_log
    )
    entering = prefix(
        (carried, states),
        "grp",
        chain_combine,
        (jnp.ones_like(carried), jnp.zeros_like(states)),
        False,
    )[1]
    mixed, output_back = jax.vjp(
        partial(span_output, seg_ext=seg_ext),
        heads_x,
        input_map,
        output_map,
        step_sizes,
        decay_log,
        skip_scale,
        entering,
    )
    normed_mix, gate_back = jax.vjp(gated_norm, mixed, gate_part, full_mix_gain.astype(jnp.float32))
    normed_mix_low = normed_mix.reshape(row_count, inner_width).astype(jnp.bfloat16)
    hidden = (
        token_float
        + jnp.dot(attended, full_attn_out, preferred_element_type=jnp.float32)
        + jnp.dot(normed_mix_low, full_mix_out, preferred_element_type=jnp.float32)
    )
    normed_feed, feed_back = jax.vjp(rms_scale, hidden, full_feed_gain.astype(jnp.float32))
    normed_feed_low = normed_feed.astype(jnp.bfloat16)
    gate_vals = jnp.dot(normed_feed_low, full_gate_up, preferred_element_type=jnp.float32)
    activation, act_back = jax.vjp(swiglu, gate_vals[:, :FF], gate_vals[:, FF:])
    activation_low = activation.astype(jnp.bfloat16)
    out_rows = (
        hidden + jnp.dot(activation_low, full_down, preferred_element_type=jnp.float32)
    ).astype(jnp.bfloat16)
    grad_rows = cotangent.reshape(row_count, model_width)
    rows_both = both_tokens(grad_rows)
    grad_down = weight_grad(rows_by_core(activation_low), rows_both)
    grad_act = jnp.dot(grad_rows, back_down.T, preferred_element_type=jnp.float32)
    grad_gate, grad_upper = act_back(grad_act)
    grad_gu = jnp.concatenate([grad_gate, grad_upper], axis=-1).astype(jnp.bfloat16)
    feed_rows = rows_by_core(normed_feed_low)
    gu_both = both_tokens(grad_gu)
    grad_gate_w = weight_grad(feed_rows, gu_both[:, :FF])
    grad_up_w = weight_grad(feed_rows, gu_both[:, FF:])
    grad_feed_in = jnp.dot(grad_gu, back_gate_up.T, preferred_element_type=jnp.float32)
    grad_hidden_norm, grad_feed = feed_back(grad_feed_in)
    grad_hidden = grad_rows.astype(jnp.float32) + grad_hidden_norm
    grad_hidden_low = grad_hidden.astype(jnp.bfloat16)
    hidden_both = both_tokens(grad_hidden_low)
    grad_attn_out = weight_grad(rows_by_core(attended), hidden_both)
    grad_attended = jnp.dot(
        grad_hidden_low, back_attn_out.T, preferred_element_type=jnp.float32
    ).astype(jnp.bfloat16)
    grad_mix_out = weight_grad(rows_by_core(normed_mix_low), hidden_both)
    grad_normed_mix = jnp.dot(grad_hidden_low, back_mix_out.T, preferred_element_type=jnp.float32)
    grad_mixed, grad_gate_part, grad_mix_gain = gate_back(
        grad_normed_mix.reshape(seq_count, span_len, inner_width)
    )
    grad_x_one, grad_in_one, grad_out_map, grad_step_one, grad_log_one, grad_skip, grad_entering = (
        output_back(grad_mixed)
    )
    later = prefix(
        (carried, grad_entering),
        "grp",
        chain_combine,
        (jnp.ones_like(carried), jnp.zeros_like(grad_entering)),
        True,
    )[1]
    grad_carried = jnp.sum(later * entering, axis=(2, 3))
    grad_x_two, grad_in_two, grad_step_two, grad_log_two = states_back((grad_carried, later))
    grad_extended, grad_step_raw, grad_taps, grad_tap_bias, grad_step_bias = prep_back(
        (
            grad_x_one + grad_x_two,
            grad_in_one + grad_in_two,
            grad_out_map,
            grad_step_one + grad_step_two,
        )
    )
    rim_back = shifted(grad_extended[:, :rim_rows], "grp", -1)
    grad_conv = grad_extended[:, rim_rows:] + jnp.pad(
        rim_back, ((0, 0), (span_len - rim_rows, 0), (0, 0))
    )
    grad_mix_proj = jnp.concatenate(
        [
            grad_gate_part.reshape(row_count, inner_width),
            grad_conv.reshape(row_count, xbc_width),
            grad_step_raw.reshape(row_count, SSM_HEADS),
        ],
        axis=-1,
    ).astype(jnp.bfloat16)
    normed_rows = rows_by_core(normed_low)
    mix_both = both_tokens(grad_mix_proj)
    grad_mix_one = weight_grad(normed_rows, mix_both[:, :inner_width])
    grad_mix_two = weight_grad(normed_rows, mix_both[:, inner_width:])
    grad_normed_m = jnp.dot(grad_mix_proj, back_mix_in.T, preferred_element_type=jnp.float32)
    grad_grouped = (
        grad_attended.reshape(seq_count, span_len, KV_HEADS, group_size, HEAD)
        .transpose(0, 2, 3, 1, 4)
        .reshape(seq_count * KV_HEADS, group_size, span_len, HEAD)
    )
    grad_query_g, grad_key_g, grad_value_g = lax.map(
        attend_back_item,
        (
            queries_grouped,
            keys_grouped,
            values_grouped,
            visible_grouped,
            attn_lse,
            attn_heads,
            grad_grouped,
        ),
    )
    grad_query = (
        grad_query_g.reshape(seq_count, KV_HEADS, group_size, span_len, HEAD)
        .transpose(0, 3, 1, 2, 4)
        .reshape(seq_count, span_len, HEADS, HEAD)
    )
    grad_key_all = (
        grad_key_g.reshape(seq_count, KV_HEADS, seq_len, HEAD)
        .transpose(0, 2, 1, 3)
        .reshape(seq_count, seq_len, kv_width)
    )
    grad_value_all = (
        grad_value_g.reshape(seq_count, KV_HEADS, seq_len, HEAD)
        .transpose(0, 2, 1, 3)
        .reshape(seq_count, seq_len, kv_width)
    )
    grad_kv_all = jnp.concatenate([grad_key_all, grad_value_all], axis=-1)
    grad_kv_own = lax.psum_scatter(
        grad_kv_all.astype(jnp.bfloat16), "grp", scatter_dimension=1, tiled=True
    ).astype(jnp.float32)
    (grad_query_raw,) = query_back(grad_query)
    (grad_key_raw,) = key_back(
        grad_kv_own[..., :kv_width].reshape(seq_count, span_len, KV_HEADS, HEAD)
    )
    grad_projected = jnp.concatenate(
        [
            grad_query_raw.reshape(row_count, query_width),
            grad_key_raw.reshape(row_count, kv_width),
            grad_kv_own[..., kv_width:].reshape(row_count, kv_width),
        ],
        axis=-1,
    ).astype(jnp.bfloat16)
    grad_attn_in = weight_grad(normed_rows, both_tokens(grad_projected))
    grad_normed_a = jnp.dot(grad_projected, back_attn_in.T, preferred_element_type=jnp.float32)
    grad_token_norm, grad_gain_in = norm_back(grad_normed_a + grad_normed_m)
    grad_token = grad_hidden + grad_token_norm
    heads = jnp.concatenate([grad_step_bias, grad_log_one + grad_log_two, grad_skip])
    parts = [grad_gain_in, grad_taps.reshape(-1), grad_tap_bias, grad_mix_gain, grad_feed, heads]
    lengths = [part.shape[0] for part in parts]
    summed = lax.psum(jnp.concatenate(parts), ("rep", "grp"))
    marks = [sum(lengths[:i]) for i in range(len(lengths) + 1)]
    sums = [summed[marks[i] : marks[i + 1]] for i in range(len(lengths))]
    index = lax.axis_index("grp")

    def own_part(value):
        size = value.shape[-1] // group_devices
        return lax.dynamic_slice_in_dim(value, index * size, size, value.ndim - 1)

    own_gate, own_up, own_down, own_attn_out, own_mix_out, own_mix_one, own_mix_two, own_attn_in = (
        reduce_group(
            [
                grad_gate_w,
                grad_up_w,
                grad_down,
                grad_attn_out,
                grad_mix_out,
                grad_mix_one,
                grad_mix_two,
                grad_attn_in,
            ],
            (0, 1, 0, 1, 1, 1, 0, 0),
        )
    )
    return (
        out_rows.reshape(seq_count, span_len, model_width),
        grad_token.reshape(seq_count, span_len, model_width),
        own_part(sums[0]),
        own_attn_in,
        own_attn_out,
        jnp.concatenate([own_mix_one, own_mix_two], axis=1),
        own_part(sums[1].reshape(CONV, -1)),
        own_part(sums[2]),
        sums[5][:SSM_HEADS],
        sums[5][SSM_HEADS : 2 * SSM_HEADS],
        sums[5][2 * SSM_HEADS :],
        own_part(sums[3]),
        own_mix_out,
        own_part(sums[4]),
        jnp.concatenate([own_gate, own_up], axis=1),
        own_down,
    )


def solution(mesh):
    return jax.shard_map(
        shards,
        mesh=mesh,
        in_specs=(
            P("rep", "grp", None),
            P("rep", None),
            P("grp"),
            P("grp", None),
            P("grp", None),
            P("grp", None),
            P(None, "grp"),
            P("grp"),
            P(),
            P(),
            P(),
            P("grp"),
            P("grp", None),
            P("grp"),
            P("grp", None),
            P("grp", None),
            P("rep", "grp", None),
        ),
        out_specs=(
            P("rep", "grp", None),
            P("rep", "grp", None),
            P("grp"),
            P("grp", None),
            P("grp", None),
            P("grp", None),
            P(None, "grp"),
            P("grp"),
            P(),
            P(),
            P(),
            P("grp"),
            P("grp", None),
            P("grp"),
            P("grp", None),
            P("grp", None),
        ),
        check_vma=False,
    )
```

```python
import functools
from functools import partial

import jax
import jax.numpy as jnp
from jax import lax
from jax.experimental import pallas as pl
from jax.experimental.pallas import tpu as pltpu
from jax.sharding import PartitionSpec as P

HEADS = 8
KV_HEADS = 2
HEAD = 64
SSM_HEADS = 24
SSM_HEAD = 64
STATE = 128
CONV = 4
FF = 2048


NORM_EPS = 1e-05
ROPE_BASE = 100000000000.0
HIGHEST = lax.Precision.HIGHEST


def shifted(value, axis, steps):
    count = lax.axis_size(axis)
    leading, last = (max(0, -steps), min(count, count - steps))
    return lax.ppermute(value, axis, [(source, source + steps) for source in range(leading, last)])


def rms_scale(values, scales):
    return values * lax.rsqrt(jnp.mean(values * values, axis=-1, keepdims=True) + NORM_EPS) * scales


def rope_tables(positions, head_width):
    indices = jnp.arange(head_width // 2, dtype=jnp.float32)
    frequency = ROPE_BASE ** (-2.0 * indices / head_width)
    angles = positions.astype(jnp.float32)[:, None] * frequency[None, :]
    return (jnp.cos(angles), jnp.sin(angles))


def rotate(values, cosine_table, sine_table):
    middle = values.shape[-1] // 2
    lower_half = values[..., :middle]
    upper_half = values[..., middle:]
    cos_rows = cosine_table[:, None, :]
    sin_rows = sine_table[:, None, :]
    return jnp.concatenate(
        [
            lower_half * cos_rows - upper_half * sin_rows,
            upper_half * cos_rows + lower_half * sin_rows,
        ],
        axis=-1,
    )


def mixer_inputs(extended, step_raw, taps, tap_bias, step_bias, seg_ext):
    span_rows = step_raw.shape[1]
    tap_count = taps.shape[0]
    own_doc = seg_ext[:, tap_count - 1 :]
    summed = jnp.zeros((extended.shape[0], span_rows, extended.shape[2]), jnp.float32) + tap_bias
    for offset in range(tap_count):
        same_doc = (seg_ext[:, offset : offset + span_rows] == own_doc)[..., None]
        summed = summed + jnp.where(
            same_doc, extended[:, offset : offset + span_rows] * taps[offset], 0.0
        )
    return jax.nn.silu(summed), jax.nn.softplus(step_raw + step_bias)


def gated_norm(mixed, gate_part, scales):
    flat_mixed = mixed.reshape(gate_part.shape)
    return rms_scale(flat_mixed * jax.nn.silu(gate_part), scales)


def swiglu(gate_vals, up_vals):
    return jax.nn.silu(gate_vals) * up_vals


MESH = pl.DeviceIdType.MESH
HIDDEN = -1e30
VMEM_LIMIT = 60 * 1024 * 1024


def seat():
    rep, grp = lax.axis_index("rep"), lax.axis_index("grp")
    chips = lax.axis_size("grp") // 2
    quarter = lax.rem(rep, 4)
    base = rep - quarter
    flip_x = quarter + 1 - 2 * lax.rem(quarter, 2)
    flip_y = lax.rem(quarter + 2, 4)
    chip, core = lax.div(grp, 2), lax.rem(grp, 2)
    return dict(
        quarter=quarter,
        qx=flip_x,
        qy=flip_y,
        qd=lax.rem(flip_x + 2, 4),
        chip=chip,
        core=core,
        x={"rep": base + flip_x},
        y={"rep": base + flip_y},
        partner={"grp": chip * 2 + 1 - core},
        along=[{"grp": lax.rem(chip + k, chips) * 2 + core} for k in range(chips)],
        chip_to=[lax.rem(chip + k, chips) for k in range(chips)],
        chip_from=[lax.rem(chip - k + chips, chips) for k in range(chips)],
    )


def remote(source, target, sent, arrived, device):
    return pltpu.make_async_remote_copy(
        src_ref=source,
        dst_ref=target,
        send_sem=sent,
        recv_sem=arrived,
        device_id=device,
        device_id_type=MESH,
    )


def greet(me, extra=()):
    barrier = pltpu.get_barrier_semaphore()
    others = [me["x"], me["y"], me["partner"], *me["along"][1:], *extra]
    for device in others:
        pl.semaphore_signal(barrier, inc=1, device_id=device, device_id_type=MESH)
    pl.semaphore_wait(barrier, len(others))


def near_first(chips):
    return sorted(range(1, chips), key=lambda k: min(k, chips - k))


def gather_kernel(count, whole, chips, *refs):
    ins, outs = refs[:count], refs[count : 2 * count]
    zs, zr, xs, xr, ys, yr, ds, dr, cs, cr, ls = refs[2 * count :]
    me = seat()
    greet(me)
    own = me["chip"] * 2 + me["core"]
    order = near_first(chips)
    along, over_x, over_y, diagonal, across, local = {}, {}, {}, {}, {}, []
    for m in range(count):
        local.append(pltpu.make_async_copy(ins[m], outs[m].at[own], ls.at[m]))
        local[-1].start()
        for k in order:
            part = ins[m] if whole[m] else ins[m].at[me["quarter"]]
            place = outs[m].at[own] if whole[m] else outs[m].at[own, me["quarter"]]
            along[m, k] = remote(part, place, zs.at[m, k], zr.at[m, k], me["along"][k])
            along[m, k].start()
        across[m, 0] = remote(ins[m], outs[m].at[own], cs.at[m, 0], cr.at[m, 0], me["partner"])
        across[m, 0].start()
    for step in range(count + 2):
        m = step
        if m < count:
            for k in order:
                along[m, k].wait_recv()
                if whole[m]:
                    continue
                piece = outs[m].at[me["chip_from"][k] * 2 + me["core"], me["quarter"]]
                over_x[m, k] = remote(piece, piece, xs.at[m, k], xr.at[m, k], me["x"])
                over_y[m, k] = remote(piece, piece, ys.at[m, k], yr.at[m, k], me["y"])
                over_x[m, k].start()
                over_y[m, k].start()
        m = step - 1
        if 0 <= m < count and not whole[m]:
            for k in order:
                block = outs[m].at[me["chip_from"][k] * 2 + me["core"]]
                if (m + k) % 2 == 0:
                    over_x[m, k].wait_recv()
                    piece, device = block.at[me["qx"]], me["y"]
                else:
                    over_y[m, k].wait_recv()
                    piece, device = block.at[me["qy"]], me["x"]
                diagonal[m, k] = remote(piece, piece, ds.at[m, k], dr.at[m, k], device)
                diagonal[m, k].start()
        m = step - 2
        if 0 <= m < count:
            for k in order:
                block = outs[m].at[me["chip_from"][k] * 2 + me["core"]]
                if not whole[m]:
                    if (m + k) % 2 == 0:
                        over_y[m, k].wait_recv()
                    else:
                        over_x[m, k].wait_recv()
                    diagonal[m, k].wait_recv()
                across[m, k] = remote(block, block, cs.at[m, k], cr.at[m, k], me["partner"])
                across[m, k].start()
    for copy in across.values():
        copy.wait_recv()
    for copies in (along, over_x, over_y, diagonal, across):
        for copy in copies.values():
            copy.wait_send()
    for copy in local:
        copy.wait()


def gather_group(shards, whole):
    group = lax.axis_size("grp")
    chips = group // 2
    count = len(shards)
    cut = [
        shard[None] if flag else shard.reshape(4, shard.shape[0] // 4, shard.shape[1])
        for shard, flag in zip(shards, whole)
    ]
    sems = [pltpu.SemaphoreType.DMA((count, chips))] * 10 + [pltpu.SemaphoreType.DMA((count,))]
    full = pl.pallas_call(
        functools.partial(gather_kernel, count, whole, chips),
        out_shape=[jax.ShapeDtypeStruct((group, *part.shape), part.dtype) for part in cut],
        in_specs=[pl.BlockSpec(memory_space=pltpu.VMEM)] * count,
        out_specs=[pl.BlockSpec(memory_space=pl.ANY)] * count,
        scratch_shapes=sems,
        compiler_params=pltpu.CompilerParams(
            collective_id=0, has_side_effects=True, vmem_limit_bytes=VMEM_LIMIT
        ),
        name="gather_group",
    )(*cut)
    return [part.reshape(-1, part.shape[-1]) for part in full]


def reduce_kernel(count, routes, chips, extras, *refs):
    parts, outs = refs[:count], refs[count : 2 * count]
    rest = refs[2 * count :]
    one, staged, two, total, slots = (rest[i * count : (i + 1) * count] for i in range(5))
    extra_in = rest[5 * count : 6 * count] if extras > 1 else ()
    sems = rest[(6 if extras > 1 else 5) * count :]
    s1, r1, s2, r2, zs, zr, es, er, gs, gr = sems
    me = seat()
    rep = lax.axis_index("rep")
    reps = lax.axis_size("rep")
    beyond = [{"rep": lax.rem(rep + 4 * e, reps)} for e in range(1, extras)]
    greet(me, beyond)
    first, second, along, other, spread = {}, {}, {}, {}, {}
    for m in range(count):
        device, mine = (me["x"], me["qx"]) if routes[m] == 0 else (me["y"], me["qy"])
        for i, q in enumerate((mine, me["qd"])):
            first[m, i] = remote(parts[m].at[q], one[m].at[i], s1.at[m, i], r1.at[m, i], device)
        first[m, 1].start()
        first[m, 0].start()

    def over_chips(body):
        lax.fori_loop(0, chips, lambda j, _: (body(j), 0)[1], 0)

    def f32(value):
        return value.astype(jnp.float32)

    for step in range(count + 3):
        m = step
        if m < count:
            device, q = (me["y"], me["qy"]) if routes[m] == 0 else (me["x"], me["qx"])
            first[m, 1].wait_recv()

            def add_first(j, m=m, q=q):
                staged[m][j] = (f32(parts[m][q, j]) + f32(one[m][1, j])).astype(jnp.bfloat16)

            over_chips(add_first)
            second[m] = remote(staged[m], two[m], s2.at[m], r2.at[m], device)
            second[m].start()
        m = step - 1
        if 0 <= m < count:
            first[m, 0].wait_recv()
            second[m].wait_recv()

            def add_second(j, m=m):
                value = f32(parts[m][me["quarter"], j]) + f32(one[m][0, j]) + f32(two[m][j])
                total[m][j] = value.astype(jnp.bfloat16)

            over_chips(add_second)
            for k in near_first(chips):
                along[m, k] = remote(
                    total[m].at[me["chip_to"][k]],
                    slots[m].at[k],
                    zs.at[m, k],
                    zr.at[m, k],
                    me["along"][k],
                )
                along[m, k].start()
        m = step - 2
        if 0 <= m < count:
            value = f32(total[m][me["chip"]])
            for k in near_first(chips):
                along[m, k].wait_recv()
                value = value + f32(slots[m][k])
            if extras > 1:
                extra_in[m][0] = value.astype(jnp.bfloat16)
                for e in range(1, extras):
                    other[m, e] = remote(
                        extra_in[m].at[0],
                        extra_in[m].at[e],
                        es.at[m, e],
                        er.at[m, e],
                        beyond[e - 1],
                    )
                    other[m, e].start()
                for e in range(1, extras):
                    other[m, e].wait_recv()
                    value = value + f32(extra_in[m][e])
            outs[m][me["quarter"]] = value.astype(jnp.bfloat16)
            piece = outs[m].at[me["quarter"]]
            for i, device in enumerate((me["x"], me["y"])):
                spread[m, i] = remote(piece, piece, gs.at[m, i], gr.at[m, i], device)
                spread[m, i].start()
        m = step - 3
        if 0 <= m < count:
            spread[m, routes[m]].wait_recv()
            q, device = (me["qx"], me["y"]) if routes[m] == 0 else (me["qy"], me["x"])
            piece = outs[m].at[q]
            spread[m, 2] = remote(piece, piece, gs.at[m, 2], gr.at[m, 2], device)
            spread[m, 2].start()
    for m in range(count):
        spread[m, 1 - routes[m]].wait_recv()
        spread[m, 2].wait_recv()
    for copies in (first, second, along, other, spread):
        for copy in copies.values():
            copy.wait_send()


def reduce_group(parts, routes):
    chips = lax.axis_size("grp") // 2
    extras = lax.axis_size("rep") // 4
    count = len(parts)
    half = jnp.bfloat16
    piece = [part.shape[2:] for part in parts]
    scratch = [pltpu.VMEM((2, chips, *shape), half) for shape in piece]
    scratch += [pltpu.VMEM((chips, *shape), half) for shape in piece]
    scratch += [pltpu.VMEM((chips, *shape), half) for shape in piece]
    scratch += [pltpu.VMEM((chips, *shape), half) for shape in piece]
    scratch += [pltpu.VMEM((chips, *shape), half) for shape in piece]
    if extras > 1:
        scratch += [pltpu.VMEM((extras, *shape), half) for shape in piece]
    dma = pltpu.SemaphoreType.DMA
    scratch += [dma((count, 2)), dma((count, 2)), dma((count,)), dma((count,))]
    scratch += [dma((count, chips)), dma((count, chips)), dma((count, extras)), dma((count, extras))]
    scratch += [dma((count, 3)), dma((count, 3))]
    sums = pl.pallas_call(
        functools.partial(reduce_kernel, count, routes, chips, extras),
        out_shape=[jax.ShapeDtypeStruct((4, *shape), half) for shape in piece],
        in_specs=[pl.BlockSpec(memory_space=pltpu.VMEM)] * count,
        out_specs=[pl.BlockSpec(memory_space=pltpu.VMEM)] * count,
        scratch_shapes=scratch,
        compiler_params=pltpu.CompilerParams(
            collective_id=1, has_side_effects=True, vmem_limit_bytes=VMEM_LIMIT
        ),
        name="reduce_group",
    )(*parts)
    return [total.reshape(-1, total.shape[-1]).astype(jnp.float32) for total in sums]


def axis_seat():
    grp = lax.axis_index("grp")
    return lax.div(grp, 2), lax.rem(grp, 2)


def greet_group():
    size, grp = lax.axis_size("grp"), lax.axis_index("grp")
    barrier = pltpu.get_barrier_semaphore()
    for k in range(1, size):
        device = {"grp": lax.rem(grp + k, size)}
        pl.semaphore_signal(barrier, inc=1, device_id=device, device_id_type=MESH)
    pl.semaphore_wait(barrier, size - 1)


def lanes(shape):
    return lax.broadcasted_iota(jnp.int32, shape, len(shape) - 1)


def pair_columns(columns, pair):
    rows = columns.shape[0]
    low = jnp.broadcast_to(columns[:, 2 * pair : 2 * pair + 1], (rows, 128))
    high = jnp.broadcast_to(columns[:, 2 * pair + 1 : 2 * pair + 2], (rows, 128))
    return jnp.where(lanes((rows, 128)) < 64, low, high)


def dot_rows(left, right):
    return lax.dot_general(
        left, right, (((1,), (1,)), ((), ())), preferred_element_type=jnp.float32
    )


def dot_plain(left, right):
    return jnp.dot(left, right, preferred_element_type=jnp.float32)


def align_heads(source, target, scale):
    for pair in range(HEADS // 2):
        both = source[:, pair * 128 : (pair + 1) * 128].astype(jnp.float32) * scale
        swapped = pltpu.roll(both, 64, 1)
        for odd in range(2):
            head = 2 * pair + odd
            group = head // (HEADS // KV_HEADS)
            value = both if odd == group else swapped
            keep = lanes(value.shape) // 64 == group
            target[head] = jnp.where(keep, value, 0.0).astype(jnp.bfloat16)


def slot_plan(reach):
    return [(0, 0)] + [(k, core) for k in range(1, reach + 1) for core in (1, 0)]


def slot_live(slot, chip, core, reach):
    back, side = slot
    if back == 0:
        return core == 1
    live = chip - back >= 0
    if back == reach and side == 0:
        live = jnp.logical_and(live, core == 0)
    return live


def same_document(key_column, query_row, causal):
    size = query_row.shape[-1]
    allowed = key_column == query_row
    if causal:
        rows = lax.broadcasted_iota(jnp.int32, (size, size), 0)
        allowed = jnp.logical_and(allowed, rows <= lanes((size, size)))
    return jnp.where(allowed, 0.0, HIDDEN)


def mix_forward_kernel(
    reach,
    chips,
    q_ref,
    kv_ref,
    segc_ref,
    segr_ref,
    act_ref,
    dt_ref,
    run_ref,
    runt_ref,
    e_ref,
    wd_ref,
    car_ref,
    skip_ref,
    att_ref,
    attt_ref,
    inv_ref,
    mixed_ref,
    ent_ref,
    kvw_ref,
    qa,
    bias,
    vt,
    ot,
    total,
    xdt,
    xw,
    runb,
    gram,
    own_state,
    half_out,
    half_in,
    car_in,
    chip_out,
    chip_car,
    chip_in,
    chip_car_in,
    enter_out,
    acc,
    ka_s,
    ka_r,
    kp_s,
    kp_r,
    ha_s,
    ha_r,
    ca_s,
    ca_r,
    en_s,
    en_r,
):
    chip, core = axis_seat()
    grp = lax.axis_index("grp")
    span = q_ref.shape[0]
    inner = SSM_HEADS * SSM_HEAD
    half = inner // 2
    partner = {"grp": chip * 2 + 1 - core}

    def ahead(k):
        return {"grp": lax.rem(grp + 2 * k, 2 * chips)}

    greet_group()
    own_kv = remote(kv_ref, kvw_ref.at[0, core], kp_s.at[0], kp_r.at[0], partner)
    own_kv.start()
    kv_along = {}
    for k in range(1, reach + 1):
        kv_along[k] = remote(kv_ref, kvw_ref.at[k, core], ka_s.at[k], ka_r.at[k], ahead(k))
        pl.when(chip + k < chips)(kv_along[k].start)
    kvw_ref[0, core] = kv_ref[...]

    weight = wd_ref[...] * dt_ref[...]
    for pair in range(SSM_HEADS // 2):
        at = slice(pair * 128, (pair + 1) * 128)
        x_pair = act_ref[:, at]
        xdt[:, at] = (x_pair * pair_columns(dt_ref, pair)).astype(jnp.bfloat16)
        xw[:, at] = (x_pair * pair_columns(weight, pair)).astype(jnp.bfloat16)
    in_map = act_ref[:, inner : inner + STATE]
    out_map = act_ref[:, inner + STATE :]
    out_low = out_map.astype(jnp.bfloat16)
    in_turned = in_map.T.astype(jnp.bfloat16)
    for i in range(2):
        own_state[i] = dot_plain(in_turned, xw[:, i * half : (i + 1) * half])
    half_out[...] = own_state[1 - core].astype(jnp.bfloat16)
    align_heads(q_ref, qa, HEAD**-0.5)
    ot[...] = jnp.zeros_like(ot)
    total[...] = jnp.zeros_like(total)
    half_car = remote(car_ref.at[1 - core], car_in, ha_s.at[0], ha_r.at[0], partner)
    half_state = remote(half_out, half_in, ha_s.at[1], ha_r.at[1], partner)
    half_car.start()
    half_state.start()

    def attend_slot(keys, values, key_docs, causal):
        bias[...] = same_document(key_docs, segr_ref[...], causal)
        vt[...] = values.astype(jnp.float32).T.astype(jnp.bfloat16)

        def per_head(head, _):
            group = lax.div(head, HEADS // KV_HEADS)
            scores = dot_rows(keys[...], qa[head]) + bias[...]
            weights = jnp.exp(scores)
            total[head] += jnp.sum(weights, axis=0, keepdims=True)
            rows = pl.ds(pl.multiple_of(group * HEAD, HEAD), HEAD)
            into = pl.ds(pl.multiple_of(head * HEAD, HEAD), HEAD)
            ot[into, :] += dot_plain(vt[rows, :], weights.astype(jnp.bfloat16))
            return 0

        lax.fori_loop(0, HEADS, per_head, 0)

    def attend_ref(ref, key_docs, causal):
        attend_slot(ref.at[:, 0:128], ref[:, 128:256], key_docs, causal)

    attend_ref(kv_ref, segc_ref[2 * reach + core], True)

    half_car.wait_recv()
    half_state.wait_recv()
    mine, theirs = own_state[core], half_in[...].astype(jnp.float32)
    car_mine, car_theirs = car_ref[core], car_in[...]
    first = core == 0
    car_0 = jnp.where(first, car_mine, car_theirs)
    car_1 = jnp.where(first, car_theirs, car_mine)
    state_0 = jnp.where(first, mine, theirs)
    state_1 = jnp.where(first, theirs, mine)
    chip_out[...] = (state_1 + car_1[0:1] * state_0).astype(jnp.bfloat16)
    chip_car[...] = car_0 * car_1

    for head in range(SSM_HEADS):
        runb[head] = jnp.broadcast_to(run_ref[:, head : head + 1], (span, 128))
    gram[...] = lax.dot_general(
        out_map, in_map, (((1,), (1,)), ((), ())), precision=HIGHEST,
        preferred_element_type=jnp.float32,
    )
    state_along = {}
    for k in range(1, reach + 1):
        state_along[k] = (
            remote(chip_out, chip_in.at[k], ca_s.at[k, 0], ca_r.at[k, 0], ahead(k)),
            remote(chip_car, chip_car_in.at[k], ca_s.at[k, 1], ca_r.at[k, 1], ahead(k)),
        )
        for copy in state_along[k]:
            pl.when(chip + k < chips)(copy.start)

    kv_pass = {}
    for k in range(1, reach + 1):
        place = kvw_ref.at[k, core]
        kv_pass[k] = remote(place, place, kp_s.at[k], kp_r.at[k], partner)

        def hand_on(k=k):
            kv_along[k].wait_recv()
            kv_pass[k].start()

        pl.when(chip - k >= 0)(hand_on)

    rows = lax.broadcasted_iota(jnp.int32, (span, span), 0)
    allowed = jnp.logical_and(segc_ref[2 * reach + core] == segr_ref[...], rows >= lanes((span, span)))
    bias[...] = jnp.where(allowed, 0.0, HIDDEN)

    def intra(quad, _):
        at = pl.ds(pl.multiple_of(quad * 256, 256), 256)
        value = jnp.zeros((span, 256), jnp.float32)
        for i in range(4):
            head = quad * 4 + i
            column = runb[head]
            spread = jnp.concatenate([column] * (span // 128), axis=1) - runt_ref[head]
            mixing = (jnp.exp(spread + bias[...]) * gram[...]).astype(jnp.bfloat16)
            part = dot_plain(mixing, xdt[:, at])
            value = jnp.where(lanes((span, 256)) // 64 == i, part, value)
        mixed_ref[:, at] = value + skip_ref[:, at] * act_ref[:, at]
        return 0

    lax.fori_loop(0, SSM_HEADS // 4, intra, 0)

    own_kv.wait_recv()
    for index, slot in enumerate(slot_plan(reach)):
        back, side = slot
        if slot == (1, 1):
            acc[...] = jnp.zeros_like(acc)
            for k in range(reach, 0, -1):

                def take(k=k):
                    for copy in state_along[k]:
                        copy.wait_recv()
                    acc[...] = chip_in[k].astype(jnp.float32) + chip_car_in[k, 0:1] * acc[...]

                pl.when(chip - k >= 0)(take)
            enter_0, enter_1 = acc[...], state_0 + car_0[0:1] * acc[...]
            ent_ref[core] = jnp.where(first, enter_0, enter_1)
            enter_out[...] = jnp.where(first, enter_1, enter_0)
            for k in range(1, reach + 1):
                pl.when(chip - k >= 0)(kv_pass[k].wait_recv)

        def visit(back=back, side=side):
            ref = kvw_ref.at[back, side]
            attend_ref(ref, segc_ref[2 * (reach - back) + side], False)

        pl.when(slot_live(slot, chip, core, reach))(visit)
        if slot == (1, 1):
            enter_pass = remote(enter_out, ent_ref.at[core], en_s, en_r, partner)
            enter_pass.start()

    for head in range(HEADS):
        inverse = 1.0 / total[head]
        inv_ref[head] = inverse
        into = slice(head * HEAD, (head + 1) * HEAD)
        ot[into, :] = ot[into, :] * inverse
    attt_ref[...] = ot[...].astype(jnp.bfloat16)
    for pair in range(HEADS // 2):
        at = slice(pair * 128, (pair + 1) * 128)
        att_ref[:, at] = ot[at, :].T.astype(jnp.bfloat16)

    enter_pass.wait_recv()
    for i in range(2):
        carried_in = dot_plain(out_low, ent_ref[i].astype(jnp.bfloat16))
        for j in range(SSM_HEADS // 4):
            pair = i * (SSM_HEADS // 4) + j
            at = slice(pair * 128, (pair + 1) * 128)
            part = carried_in[:, j * 128 : (j + 1) * 128]
            mixed_ref[:, at] += pair_columns(e_ref, pair) * part

    own_kv.wait_send()
    half_car.wait_send()
    half_state.wait_send()
    enter_pass.wait_send()
    for k in range(1, reach + 1):

        def sent(k=k):
            kv_along[k].wait_send()
            for copy in state_along[k]:
                copy.wait_send()

        pl.when(chip + k < chips)(sent)
        pl.when(chip - k >= 0)(kv_pass[k].wait_send)


def mix_forward(reach, q, kv, segc, segr, act, dt, run, runt, e, wd, car, skip):
    chips = lax.axis_size("grp") // 2
    span = q.shape[0]
    inner = SSM_HEADS * SSM_HEAD
    half = inner // 2
    f32, low = jnp.float32, jnp.bfloat16
    shape = jax.ShapeDtypeStruct
    dma = pltpu.SemaphoreType.DMA
    vmem = pltpu.VMEM
    outs = [
        shape((span, HEADS * HEAD), low),
        shape((HEADS * HEAD, span), low),
        shape((HEADS, 1, span), f32),
        shape((span, inner), f32),
        shape((2, STATE, half), f32),
        shape((reach + 1, 2, span, kv.shape[1]), low),
    ]
    scratch = [
        vmem((HEADS, span, 128), low),
        vmem((span, span), f32),
        vmem((128, span), low),
        vmem((HEADS * HEAD, span), f32),
        vmem((HEADS, 1, span), f32),
        vmem((span, inner), low),
        vmem((span, inner), low),
        vmem((SSM_HEADS, span, 128), f32),
        vmem((span, span), f32),
        vmem((2, STATE, half), f32),
        vmem((STATE, half), low),
        vmem((STATE, half), low),
        vmem((8, half), f32),
        vmem((STATE, half), low),
        vmem((8, half), f32),
        vmem((reach + 1, STATE, half), low),
        vmem((reach + 1, 8, half), f32),
        vmem((STATE, half), f32),
        vmem((STATE, half), f32),
        dma((reach + 1,)),
        dma((reach + 1,)),
        dma((reach + 1,)),
        dma((reach + 1,)),
        dma((2,)),
        dma((2,)),
        dma((reach + 1, 2)),
        dma((reach + 1, 2)),
        dma,
        dma,
    ]
    return pl.pallas_call(
        functools.partial(mix_forward_kernel, reach, chips),
        out_shape=outs,
        in_specs=[pl.BlockSpec(memory_space=pltpu.VMEM)] * 12,
        out_specs=[pl.BlockSpec(memory_space=pltpu.VMEM)] * len(outs),
        scratch_shapes=scratch,
        compiler_params=pltpu.CompilerParams(
            collective_id=2, has_side_effects=True, vmem_limit_bytes=VMEM_LIMIT
        ),
        name="mix_forward",
    )(q, kv, segc, segr, act, dt, run, runt, e, wd, car, skip)


def mix_backward_kernel(
    reach,
    chips,
    q_ref,
    kvw_ref,
    segc_ref,
    segr_ref,
    act_ref,
    dt_ref,
    run_ref,
    runt_ref,
    e_ref,
    wd_ref,
    car_ref,
    skip_ref,
    attt_ref,
    inv_ref,
    ent_ref,
    gout_ref,
    gmix_ref,
    rate_ref,
    dq_ref,
    dkv_ref,
    dact_ref,
    ddt_ref,
    heads_ref,
    qa,
    da,
    bias,
    kt,
    dqt,
    centre,
    dk,
    dv,
    part_out,
    part_in,
    sum_out,
    sum_in,
    xdt,
    xw,
    ge,
    runb,
    gramt,
    dgram,
    own_grad,
    half_out,
    half_in,
    car_in,
    chip_out,
    chip_car,
    chip_in,
    chip_car_in,
    later_out,
    later,
    acc,
    qrow,
    qcol,
    dxdt,
    sums,
    fold_ref,
    pp_s,
    pp_r,
    pa_s,
    pa_r,
    ha_s,
    ha_r,
    ca_s,
    ca_r,
    la_s,
    la_r,
):
    chip, core = axis_seat()
    grp = lax.axis_index("grp")
    span = q_ref.shape[0]
    inner = SSM_HEADS * SSM_HEAD
    half = inner // 2
    low = jnp.bfloat16
    partner = {"grp": chip * 2 + 1 - core}
    first = core == 0

    def behind(k):
        return {"grp": lax.rem(grp - 2 * k + 2 * chips, 2 * chips)}

    greet_group()
    in_map = act_ref[:, inner : inner + STATE]
    out_map = act_ref[:, inner + STATE :]
    in_low, out_low = in_map.astype(low), out_map.astype(low)
    weight = wd_ref[...] * dt_ref[...]
    for pair in range(SSM_HEADS // 2):
        at = slice(pair * 128, (pair + 1) * 128)
        x_pair = act_ref[:, at]
        ge[:, at] = (gmix_ref[:, at] * pair_columns(e_ref, pair)).astype(low)
        xdt[:, at] = (x_pair * pair_columns(dt_ref, pair)).astype(low)
        xw[:, at] = (x_pair * pair_columns(weight, pair)).astype(low)
    out_turned = out_map.T.astype(low)
    for i in range(2):
        own_grad[i] = dot_plain(out_turned, ge[:, i * half : (i + 1) * half])
    half_out[...] = own_grad[1 - core].astype(low)
    align_heads(q_ref, qa, HEAD**-0.5)
    align_heads(gout_ref, da, 1.0)
    half_car = remote(car_ref.at[1 - core], car_in, ha_s.at[0], ha_r.at[0], partner)
    half_grad = remote(half_out, half_in, ha_s.at[1], ha_r.at[1], partner)
    half_car.start()
    half_grad.start()

    for pair in range(HEADS // 2):
        at = slice(pair * 128, (pair + 1) * 128)
        product = gout_ref[:, at].astype(jnp.float32).T * attt_ref[at, :].astype(jnp.float32)
        for odd in range(2):
            rows = product[odd * HEAD : (odd + 1) * HEAD]
            centre[2 * pair + odd] = jnp.sum(rows, axis=0, keepdims=True)
    dqt[...] = jnp.zeros_like(dqt)

    def attend_back(ref, key_docs, causal):
        bias[...] = same_document(key_docs, segr_ref[...], causal)
        kt[...] = ref[:, 0:128].astype(jnp.float32).T.astype(low)
        dk[...] = jnp.zeros_like(dk)
        dv[...] = jnp.zeros_like(dv)

        def per_head(head, _):
            group = lax.div(head, HEADS // KV_HEADS)
            scores = dot_rows(ref[:, 0:128], qa[head]) + bias[...]
            probs = jnp.exp(scores) * inv_ref[head]
            grad_probs = dot_rows(ref[:, 128:256], da[head])
            grad_scores = (probs * (grad_probs - centre[head])).astype(low)
            dv[...] += dot_plain(probs.astype(low), da[head])
            dk[...] += dot_plain(grad_scores, qa[head])
            rows = pl.ds(pl.multiple_of(group * HEAD, HEAD), HEAD)
            into = pl.ds(pl.multiple_of(head * HEAD, HEAD), HEAD)
            dqt[into, :] += dot_plain(kt[rows, :], grad_scores)
            return 0

        lax.fori_loop(0, HEADS, per_head, 0)

    passed, sent_on = {}, {}

    def pass_slot(back, side):
        live = slot_live((back, side), chip, core, reach)

        def compute():
            attend_back(kvw_ref.at[back, side], segc_ref[2 * (reach - back) + side], False)
            part_out[back, side, :, 0:128] = dk[...].astype(low)
            part_out[back, side, :, 128:256] = dv[...].astype(low)

        pl.when(live)(compute)

    def start_part(back):
        for side in (0, 1):
            passed[back, side] = remote(
                part_out.at[back, side],
                part_in.at[back],
                pp_s.at[back],
                pp_r.at[back],
                partner,
            )
            live = slot_live((back, side), chip, core, reach)
            pl.when(jnp.logical_and(live, core != side))(passed[back, side].start)

    def send_sum(back):
        both = chip - back >= 0
        partner_has = jnp.logical_and(both, core == 1) if back == reach else both

        def add_partner():
            passed[back, 0].wait_recv()
            value = part_out[back, core].astype(jnp.float32) + part_in[back].astype(jnp.float32)
            sum_out[back] = value.astype(low)

        pl.when(partner_has)(add_partner)
        if back == reach:

            def alone():
                sum_out[back] = part_out[back, core]

            pl.when(jnp.logical_and(both, core == 0))(alone)

    def send_sum_start(back):
        sent_on[back] = remote(
            sum_out.at[back], sum_in.at[back], pa_s.at[back], pa_r.at[back], behind(back)
        )
        pl.when(chip - back >= 0)(sent_on[back].start)

    pass_slot(reach, 1)

    half_car.wait_recv()
    half_grad.wait_recv()
    mine, theirs = own_grad[core], half_in[...].astype(jnp.float32)
    car_mine, car_theirs = car_ref[core], car_in[...]
    car_0 = jnp.where(first, car_mine, car_theirs)
    car_1 = jnp.where(first, car_theirs, car_mine)
    grad_0 = jnp.where(first, mine, theirs)
    grad_1 = jnp.where(first, theirs, mine)
    chip_out[...] = (grad_0 + car_0[0:1] * grad_1).astype(low)
    chip_car[...] = car_0 * car_1
    pass_slot(reach, 0)
    state_along = {}
    for k in range(1, reach + 1):
        state_along[k] = (
            remote(chip_out, chip_in.at[k], ca_s.at[k, 0], ca_r.at[k, 0], behind(k)),
            remote(chip_car, chip_car_in.at[k], ca_s.at[k, 1], ca_r.at[k, 1], behind(k)),
        )
        for copy in state_along[k]:
            pl.when(chip - k >= 0)(copy.start)
    start_part(reach)
    for back in range(reach - 1, 0, -1):
        pass_slot(back, 1)
        send_sum(back + 1)
        pass_slot(back, 0)
        send_sum_start(back + 1)
        start_part(back)
    pass_slot(0, 0)
    start_part(0)
    send_sum(1)

    for head in range(SSM_HEADS):
        runb[head] = jnp.broadcast_to(run_ref[:, head : head + 1], (span, 128))
    send_sum_start(1)
    bias[...] = same_document(segc_ref[2 * reach + core], segr_ref[...], True)
    gramt[...] = lax.dot_general(
        in_map, out_map, (((1,), (1,)), ((), ())), precision=HIGHEST,
        preferred_element_type=jnp.float32,
    )
    dgram[...] = jnp.zeros_like(dgram)
    qcol[...] = jnp.zeros_like(qcol)
    qrow[...] = jnp.zeros_like(qrow)
    heads_of = lax.broadcasted_iota(jnp.int32, (inner, 128), 0) // SSM_HEAD
    fold_ref[...] = jnp.where(heads_of == lanes((inner, 128)), 1.0, 0.0)

    def intra(quad, _):
        at = pl.ds(pl.multiple_of(quad * 256, 256), 256)
        grads = gmix_ref[:, at].astype(low)
        inputs = xdt[:, at]
        place = lanes((span, 256)) // 64
        value = jnp.zeros((span, 256), jnp.float32)
        for i in range(4):
            head = quad * 4 + i
            column = runb[head]
            spread = runt_ref[head] - jnp.concatenate([column] * (span // 128), axis=1)
            decay = jnp.exp(spread + bias[...])
            mixing = decay * gramt[...]
            alone = jnp.where(place == i, inputs, jnp.zeros_like(inputs))
            grad_mixing = dot_rows(alone, grads)
            dgram[...] += decay * grad_mixing
            product = mixing * grad_mixing
            qrow[pl.ds(head, 1), :] = jnp.sum(product, axis=0, keepdims=True)
            by_row = jnp.sum(product, axis=1, keepdims=True)
            qcol[...] = jnp.where(lanes((span, 128)) == head, by_row, qcol[...])
            part = dot_plain(mixing.astype(low), grads)
            value = jnp.where(place == i, part, value)
        dxdt[:, at] = value
        return 0

    lax.fori_loop(0, SSM_HEADS // 4, intra, 0)

    acc[...] = jnp.zeros_like(acc)
    for k in range(reach, 0, -1):

        def take(k=k):
            for copy in state_along[k]:
                copy.wait_recv()
            acc[...] = chip_in[k].astype(jnp.float32) + chip_car_in[k, 0:1] * acc[...]

        pl.when(chip + k < chips)(take)
    later_1, later_0 = acc[...], grad_1 + car_1[0:1] * acc[...]
    later[core] = jnp.where(first, later_0, later_1)
    later_out[...] = jnp.where(first, later_1, later_0)

    attend_back(kvw_ref.at[0, core], segc_ref[2 * reach + core], True)
    later_pass = remote(later_out, later.at[core], la_s, la_r, partner)
    later_pass.start()
    for pair in range(HEADS // 2):
        at = slice(pair * 128, (pair + 1) * 128)
        dq_ref[:, at] = dqt[at, :].T * HEAD**-0.5

    dkv_ref[:, 0:128] = dk[...]
    dkv_ref[:, 128:256] = dv[...]

    def add_zero():
        passed[0, 0].wait_recv()
        dkv_ref[...] += part_in[0].astype(jnp.float32)

    pl.when(core == 0)(add_zero)
    for k in range(1, reach + 1):

        def add_ahead(k=k):
            sent_on[k].wait_recv()
            dkv_ref[...] += sum_in[k].astype(jnp.float32)

        pl.when(chip + k < chips)(add_ahead)

    grad_low = dgram[...].astype(low)
    grad_in = dot_plain(grad_low, out_low)
    grad_out = dot_plain(dgram[...].T.astype(low), in_low)
    later_pass.wait_recv()
    carried = jnp.zeros((1, 128), jnp.float32)
    for i in range(2):
        entering = ent_ref[i]
        grads = later[i]
        carried = carried + lax.dot_general(
            jnp.sum(entering * grads, axis=0, keepdims=True),
            fold_ref[i * half : (i + 1) * half],
            (((1,), (0,)), ((), ())),
            precision=HIGHEST,
            preferred_element_type=jnp.float32,
        )
        enter_low, later_low = entering.astype(low), grads.astype(low)
        own = slice(i * half, (i + 1) * half)
        grad_out = grad_out + dot_rows(ge[:, own], enter_low)
        grad_in = grad_in + dot_rows(xw[:, own], later_low)
        reached = dot_plain(out_low, enter_low)
        grad_xw = dot_plain(in_low, later_low)
        for j in range(SSM_HEADS // 4):
            pair = i * (SSM_HEADS // 4) + j
            at = slice(pair * 128, (pair + 1) * 128)
            x_pair, g_pair = act_ref[:, at], gmix_ref[:, at]
            part = grad_xw[:, j * 128 : (j + 1) * 128]
            inside = dxdt[:, at]
            dact_ref[:, at] = (
                skip_ref[:, at] * g_pair
                + pair_columns(dt_ref, pair) * inside
                + pair_columns(weight, pair) * part
            )
            sums[0, :, at] = x_pair * inside
            sums[1, :, at] = x_pair * part
            sums[2, :, at] = g_pair * reached[:, j * 128 : (j + 1) * 128]
            sums[3, :, at] = x_pair * g_pair
    dact_ref[:, inner : inner + STATE] = grad_in
    dact_ref[:, inner + STATE :] = grad_out

    def fold(value):
        return lax.dot_general(
            value, fold_ref[...], (((1,), (0,)), ((), ())), precision=HIGHEST,
            preferred_element_type=jnp.float32,
        )

    x_inside, x_part, g_reached = fold(sums[0]), fold(sums[1]), fold(sums[2])
    skip_sum = fold(jnp.broadcast_to(jnp.sum(sums[3], axis=0, keepdims=True), (8, inner)))
    w_part = weight * x_part
    drun = qrow[...].T - qcol[...] + e_ref[...] * g_reached - w_part
    last = jnp.sum(w_part, axis=0, keepdims=True) + rate_ref[1:2] * carried
    rows = lax.broadcasted_iota(jnp.int32, (span, 128), 0)
    drun = jnp.where(rows == span - 1, drun + last, drun)
    upper = lax.broadcasted_iota(jnp.int32, (span, span), 0) <= lanes((span, span))
    drate = lax.dot_general(
        jnp.where(upper, 1.0, 0.0), drun, (((1,), (0,)), ((), ())), precision=HIGHEST,
        preferred_element_type=jnp.float32,
    )
    rate = rate_ref[0:1]
    ddt_ref[...] = x_inside + wd_ref[...] * x_part + rate * drate
    heads_ref[...] = jnp.zeros_like(heads_ref)
    heads_ref[0:1] = jnp.sum(rate * dt_ref[...] * drate, axis=0, keepdims=True)
    heads_ref[1:2] = skip_sum[0:1]

    half_car.wait_send()
    half_grad.wait_send()
    later_pass.wait_send()
    for k in range(1, reach + 1):

        def sent(k=k):
            sent_on[k].wait_send()
            for copy in state_along[k]:
                copy.wait_send()

        pl.when(chip - k >= 0)(sent)
    for back in range(reach + 1):
        for side in (0, 1):
            if (back, side) in ((0, 1),):
                continue
            live = slot_live((back, side), chip, core, reach)
            pl.when(jnp.logical_and(live, core != side))(passed[back, side].wait_send)


def mix_backward(reach, *operands):
    chips = lax.axis_size("grp") // 2
    span = operands[0].shape[0]
    inner = SSM_HEADS * SSM_HEAD
    half = inner // 2
    kv_width = 2 * KV_HEADS * HEAD
    f32, low = jnp.float32, jnp.bfloat16
    shape = jax.ShapeDtypeStruct
    dma = pltpu.SemaphoreType.DMA
    vmem = pltpu.VMEM
    outs = [
        shape((span, HEADS * HEAD), f32),
        shape((span, kv_width), f32),
        shape((span, inner + 2 * STATE), f32),
        shape((span, 128), f32),
        shape((8, 128), f32),
    ]
    scratch = [
        vmem((HEADS, span, 128), low),
        vmem((HEADS, span, 128), low),
        vmem((span, span), f32),
        vmem((128, span), low),
        vmem((HEADS * HEAD, span), f32),
        vmem((HEADS, 1, span), f32),
        vmem((span, 128), f32),
        vmem((span, 128), f32),
        vmem((reach + 1, 2, span, kv_width), low),
        vmem((reach + 1, span, kv_width), low),
        vmem((reach + 1, span, kv_width), low),
        vmem((reach + 1, span, kv_width), low),
        vmem((span, inner), low),
        vmem((span, inner), low),
        vmem((span, inner), low),
        vmem((SSM_HEADS, span, 128), f32),
        vmem((span, span), f32),
        vmem((span, span), f32),
        vmem((2, STATE, half), f32),
        vmem((STATE, half), low),
        vmem((STATE, half), low),
        vmem((8, half), f32),
        vmem((STATE, half), low),
        vmem((8, half), f32),
        vmem((reach + 1, STATE, half), low),
        vmem((reach + 1, 8, half), f32),
        vmem((STATE, half), f32),
        vmem((2, STATE, half), f32),
        vmem((STATE, half), f32),
        vmem((128, span), f32),
        vmem((span, 128), f32),
        vmem((span, inner), f32),
        vmem((4, span, inner), f32),
        vmem((inner, 128), f32),
        dma((reach + 1,)),
        dma((reach + 1,)),
        dma((reach + 1,)),
        dma((reach + 1,)),
        dma((2,)),
        dma((2,)),
        dma((reach + 1, 2)),
        dma((reach + 1, 2)),
        dma,
        dma,
    ]
    return pl.pallas_call(
        functools.partial(mix_backward_kernel, reach, chips),
        out_shape=outs,
        in_specs=[pl.BlockSpec(memory_space=pltpu.VMEM)] * len(operands),
        out_specs=[pl.BlockSpec(memory_space=pltpu.VMEM)] * len(outs),
        scratch_shapes=scratch,
        compiler_params=pltpu.CompilerParams(
            collective_id=3, has_side_effects=True, vmem_limit_bytes=VMEM_LIMIT
        ),
        name="mix_backward",
    )(*operands)


def swap_cores(value):
    group = lax.axis_size("grp")
    return lax.ppermute(value, "grp", [(i, i + 1 - 2 * (i % 2)) for i in range(group)])


def rows_by_core(activation):
    return turned_rows(activation.T)


def turned_rows(turned):
    features, tokens = turned.shape
    chips = lax.axis_size("grp") // 2
    core = lax.rem(lax.axis_index("grp"), 2)
    turned = turned.reshape(chips, 2, 4, features // (8 * chips), tokens)
    own = lax.dynamic_index_in_dim(turned, core, 1, keepdims=False)
    other = lax.dynamic_index_in_dim(turned, 1 - core, 1, keepdims=False)
    own = own.transpose(1, 0, 2, 3).reshape(features // 2, tokens)
    other = other.transpose(1, 0, 2, 3).reshape(features // 2, tokens)
    return jnp.concatenate([own, swap_cores(other)], axis=1)


def both_tokens(value):
    return jnp.concatenate([value, swap_cores(value)], axis=0)


def weight_grad(rows, value):
    chips = lax.axis_size("grp") // 2
    grad = jnp.dot(rows, value, preferred_element_type=jnp.float32).astype(jnp.bfloat16)
    return grad.reshape(4, chips, -1, value.shape[1])


def shards(
    tokens,
    segments,
    input_gain,
    attention_in,
    attention_out,
    mixer_in,
    filter_taps,
    filter_bias,
    step_bias,
    decay_log,
    skip_scale,
    mixer_gain,
    mixer_out,
    feed_gain,
    gate_up,
    down_proj,
    cotangent,
):
    seq_count, span_len, model_width = tokens.shape
    row_count = seq_count * span_len
    seq_len = segments.shape[1]
    group_devices = lax.axis_size("grp")
    position = lax.axis_index("grp") * span_len
    inner_width = SSM_HEADS * SSM_HEAD
    xbc_width = inner_width + 2 * STATE
    query_width = HEADS * HEAD
    kv_width = KV_HEADS * HEAD
    rim_rows = CONV - 1
    small = [input_gain, filter_taps.reshape(-1), filter_bias, mixer_gain, feed_gain]
    sizes = [part.shape[0] for part in small]
    packed = jnp.concatenate(small)
    packed = jnp.pad(packed, (0, -packed.shape[0] % 2048)).reshape(-1, 128)
    full_attn_in, full_mix_in, full_small, full_gate_up, full_down, full_mix_out, full_attn_out = (
        gather_group(
            [attention_in, mixer_in, packed, gate_up, down_proj, mixer_out, attention_out],
            [False, False, True, False, False, False, False],
        )
    )
    full_small = full_small.reshape(group_devices, -1)
    starts = [sum(sizes[:i]) for i in range(len(sizes) + 1)]
    pieces = [full_small[:, starts[i] : starts[i + 1]] for i in range(len(sizes))]
    full_gain_in, full_tap_bias, full_mix_gain, full_feed_gain = (
        pieces[i].reshape(-1) for i in (0, 2, 3, 4)
    )
    full_taps = pieces[1].reshape(group_devices, CONV, -1).transpose(1, 0, 2).reshape(CONV, -1)
    back_attn_in, back_attn_out, back_mix_in = full_attn_in, full_attn_out, full_mix_in
    back_mix_out, back_gate_up, back_down = full_mix_out, full_gate_up, full_down
    offsets = position + jnp.arange(span_len, dtype=jnp.int32)
    token_float = tokens.reshape(row_count, model_width).astype(jnp.float32)
    normed, norm_back = jax.vjp(rms_scale, token_float, full_gain_in.astype(jnp.float32))
    normed_low = normed.astype(jnp.bfloat16)
    projected = jnp.dot(normed_low, full_attn_in, preferred_element_type=jnp.float32).reshape(
        seq_count, span_len, -1
    )
    cosine_table, sine_table = rope_tables(offsets, HEAD)
    turner = partial(rotate, cosine_table=cosine_table, sine_table=sine_table)
    query_raw = projected[..., :query_width].reshape(seq_count, span_len, HEADS, HEAD)
    key_raw = projected[..., query_width : query_width + kv_width].reshape(
        seq_count, span_len, KV_HEADS, HEAD
    )
    value_part = projected[..., query_width + kv_width :]
    query_rot, query_back = jax.vjp(turner, query_raw)
    key_rot, key_back = jax.vjp(turner, key_raw)
    query_low = query_rot.astype(jnp.bfloat16)
    kv_local = jnp.concatenate(
        [key_rot.reshape(seq_count, span_len, kv_width), value_part], axis=-1
    ).astype(jnp.bfloat16)
    mix_proj = jnp.dot(normed_low, full_mix_in, preferred_element_type=jnp.float32).reshape(
        seq_count, span_len, -1
    )
    gate_part = mix_proj[..., :inner_width]
    conv_low = mix_proj[..., inner_width : inner_width + xbc_width].astype(jnp.bfloat16)
    step_raw = mix_proj[..., inner_width + xbc_width :]
    rim_in = shifted(conv_low[:, span_len - rim_rows :], "grp", 1)
    extended = jnp.concatenate([rim_in, conv_low], axis=1).astype(jnp.float32)
    padded_docs = jnp.concatenate(
        [jnp.full((seq_count, rim_rows), -1, jnp.int32), segments], axis=1
    )
    seg_ext = lax.dynamic_slice_in_dim(padded_docs, position, span_len + rim_rows, 1)
    (active, step_sizes), prep_back = jax.vjp(
        partial(mixer_inputs, seg_ext=seg_ext),
        extended,
        step_raw,
        full_taps.astype(jnp.float32),
        full_tap_bias.astype(jnp.float32),
        step_bias,
    )
    reach = min(seq_len // (4 * span_len), group_devices // 2 - 1)
    chip = lax.axis_index("grp") // 2
    docs = jnp.concatenate([jnp.full((2 * reach * span_len,), -1, jnp.int32), segments[0]])
    window = lax.dynamic_slice_in_dim(docs, 2 * chip * span_len, 2 * (reach + 1) * span_len)
    window = window.reshape(2 * (reach + 1), span_len, 1)
    own_docs = seg_ext[0, rim_rows:]
    prior_doc = seg_ext[0, rim_rows - 1]
    rate_scale = -jnp.exp(decay_log)
    steps = step_sizes[0]
    order = jnp.arange(span_len)
    before = (order[:, None] >= order[None, :]).astype(jnp.float32)
    running = jnp.dot(before, steps * rate_scale, precision=HIGHEST)
    final = running[-1:]
    enter_decay = jnp.where((own_docs == prior_doc)[:, None], jnp.exp(running), 0.0)
    tail_decay = jnp.where((own_docs == own_docs[-1])[:, None], jnp.exp(final - running), 0.0)
    carried = jnp.where(own_docs[-1] == prior_doc, jnp.exp(final[0]), 0.0)
    carried_lanes = jnp.broadcast_to(
        jnp.repeat(carried, SSM_HEAD).reshape(2, 1, inner_width // 2), (2, 8, inner_width // 2)
    )

    def wide(value):
        return jnp.pad(value, ((0, 0), (0, 128 - value.shape[1])))

    query_rows = query_low.reshape(row_count, query_width)
    recurrence = (
        active[0],
        wide(steps),
        wide(running),
        running.T.reshape(SSM_HEADS, 1, span_len),
        wide(enter_decay),
        wide(tail_decay),
        carried_lanes,
        jnp.repeat(skip_scale, SSM_HEAD)[None, :],
    )
    attended, attended_turned, inverse_total, mixed, entering, kv_window = mix_forward(
        reach, query_rows, kv_local[0], window, own_docs[None, :], *recurrence
    )
    mixed = mixed[None]
    normed_mix, gate_back = jax.vjp(gated_norm, mixed, gate_part, full_mix_gain.astype(jnp.float32))
    normed_mix_low = normed_mix.reshape(row_count, inner_width).astype(jnp.bfloat16)
    hidden = (
        token_float
        + jnp.dot(attended, full_attn_out, preferred_element_type=jnp.float32)
        + jnp.dot(normed_mix_low, full_mix_out, preferred_element_type=jnp.float32)
    )
    normed_feed, feed_back = jax.vjp(rms_scale, hidden, full_feed_gain.astype(jnp.float32))
    normed_feed_low = normed_feed.astype(jnp.bfloat16)
    gate_vals = jnp.dot(normed_feed_low, full_gate_up, preferred_element_type=jnp.float32)
    activation, act_back = jax.vjp(swiglu, gate_vals[:, :FF], gate_vals[:, FF:])
    activation_low = activation.astype(jnp.bfloat16)
    out_rows = (
        hidden + jnp.dot(activation_low, full_down, preferred_element_type=jnp.float32)
    ).astype(jnp.bfloat16)
    grad_rows = cotangent.reshape(row_count, model_width)
    rows_both = both_tokens(grad_rows)
    grad_down = weight_grad(rows_by_core(activation_low), rows_both)
    grad_act = jnp.dot(grad_rows, back_down.T, preferred_element_type=jnp.float32)
    grad_gate, grad_upper = act_back(grad_act)
    grad_gu = jnp.concatenate([grad_gate, grad_upper], axis=-1).astype(jnp.bfloat16)
    feed_rows = rows_by_core(normed_feed_low)
    gu_both = both_tokens(grad_gu)
    grad_gate_w = weight_grad(feed_rows, gu_both[:, :FF])
    grad_up_w = weight_grad(feed_rows, gu_both[:, FF:])
    grad_feed_in = jnp.dot(grad_gu, back_gate_up.T, preferred_element_type=jnp.float32)
    grad_hidden_norm, grad_feed = feed_back(grad_feed_in)
    grad_hidden = grad_rows.astype(jnp.float32) + grad_hidden_norm
    grad_hidden_low = grad_hidden.astype(jnp.bfloat16)
    hidden_both = both_tokens(grad_hidden_low)
    grad_attn_out = weight_grad(turned_rows(attended_turned), hidden_both)
    grad_attended = jnp.dot(
        grad_hidden_low, back_attn_out.T, preferred_element_type=jnp.float32
    ).astype(jnp.bfloat16)
    grad_mix_out = weight_grad(rows_by_core(normed_mix_low), hidden_both)
    grad_normed_mix = jnp.dot(grad_hidden_low, back_mix_out.T, preferred_element_type=jnp.float32)
    grad_mixed, grad_gate_part, grad_mix_gain = gate_back(
        grad_normed_mix.reshape(seq_count, span_len, inner_width)
    )
    heads_scale = jnp.pad(jnp.stack([rate_scale, carried]), ((0, 6), (0, 128 - SSM_HEADS)))
    grad_query, grad_kv_own, grad_active, grad_steps, grad_heads = mix_backward(
        reach,
        query_rows,
        kv_window,
        window,
        own_docs[None, :],
        *recurrence,
        attended_turned,
        inverse_total,
        entering,
        grad_attended,
        grad_mixed.reshape(row_count, inner_width),
        heads_scale,
    )
    grad_query = grad_query.reshape(seq_count, span_len, HEADS, HEAD)
    grad_kv_own = grad_kv_own.reshape(seq_count, span_len, 2 * kv_width)
    grad_extended, grad_step_raw, grad_taps, grad_tap_bias, grad_step_bias = prep_back(
        (grad_active[None], grad_steps[None, :, :SSM_HEADS])
    )
    rim_back = shifted(grad_extended[:, :rim_rows], "grp", -1)
    grad_conv = grad_extended[:, rim_rows:] + jnp.pad(
        rim_back, ((0, 0), (span_len - rim_rows, 0), (0, 0))
    )
    grad_mix_proj = jnp.concatenate(
        [
            grad_gate_part.reshape(row_count, inner_width),
            grad_conv.reshape(row_count, xbc_width),
            grad_step_raw.reshape(row_count, SSM_HEADS),
        ],
        axis=-1,
    ).astype(jnp.bfloat16)
    normed_rows = rows_by_core(normed_low)
    mix_both = both_tokens(grad_mix_proj)
    grad_mix_one = weight_grad(normed_rows, mix_both[:, :inner_width])
    grad_mix_two = weight_grad(normed_rows, mix_both[:, inner_width:])
    grad_normed_m = jnp.dot(grad_mix_proj, back_mix_in.T, preferred_element_type=jnp.float32)
    (grad_query_raw,) = query_back(grad_query)
    (grad_key_raw,) = key_back(
        grad_kv_own[..., :kv_width].reshape(seq_count, span_len, KV_HEADS, HEAD)
    )
    grad_projected = jnp.concatenate(
        [
            grad_query_raw.reshape(row_count, query_width),
            grad_key_raw.reshape(row_count, kv_width),
            grad_kv_own[..., kv_width:].reshape(row_count, kv_width),
        ],
        axis=-1,
    ).astype(jnp.bfloat16)
    grad_attn_in = weight_grad(normed_rows, both_tokens(grad_projected))
    grad_normed_a = jnp.dot(grad_projected, back_attn_in.T, preferred_element_type=jnp.float32)
    grad_token_norm, grad_gain_in = norm_back(grad_normed_a + grad_normed_m)
    grad_token = grad_hidden + grad_token_norm
    heads = jnp.concatenate([grad_step_bias, grad_heads[0, :SSM_HEADS], grad_heads[1, :SSM_HEADS]])
    parts = [grad_gain_in, grad_taps.reshape(-1), grad_tap_bias, grad_mix_gain, grad_feed, heads]
    lengths = [part.shape[0] for part in parts]
    summed = lax.psum(jnp.concatenate(parts), ("rep", "grp"))
    marks = [sum(lengths[:i]) for i in range(len(lengths) + 1)]
    sums = [summed[marks[i] : marks[i + 1]] for i in range(len(lengths))]
    index = lax.axis_index("grp")

    def own_part(value):
        size = value.shape[-1] // group_devices
        return lax.dynamic_slice_in_dim(value, index * size, size, value.ndim - 1)

    own_gate, own_up, own_down, own_attn_out, own_mix_out, own_mix_one, own_mix_two, own_attn_in = (
        reduce_group(
            [
                grad_gate_w,
                grad_up_w,
                grad_down,
                grad_attn_out,
                grad_mix_out,
                grad_mix_one,
                grad_mix_two,
                grad_attn_in,
            ],
            (0, 1, 0, 1, 1, 1, 0, 0),
        )
    )
    return (
        out_rows.reshape(seq_count, span_len, model_width),
        grad_token.reshape(seq_count, span_len, model_width),
        own_part(sums[0]),
        own_attn_in,
        own_attn_out,
        jnp.concatenate([own_mix_one, own_mix_two], axis=1),
        own_part(sums[1].reshape(CONV, -1)),
        own_part(sums[2]),
        sums[5][:SSM_HEADS],
        sums[5][SSM_HEADS : 2 * SSM_HEADS],
        sums[5][2 * SSM_HEADS :],
        own_part(sums[3]),
        own_mix_out,
        own_part(sums[4]),
        jnp.concatenate([own_gate, own_up], axis=1),
        own_down,
    )


def solution(mesh):
    return jax.shard_map(
        shards,
        mesh=mesh,
        in_specs=(
            P("rep", "grp", None),
            P("rep", None),
            P("grp"),
            P("grp", None),
            P("grp", None),
            P("grp", None),
            P(None, "grp"),
            P("grp"),
            P(),
            P(),
            P(),
            P("grp"),
            P("grp", None),
            P("grp"),
            P("grp", None),
            P("grp", None),
            P("rep", "grp", None),
        ),
        out_specs=(
            P("rep", "grp", None),
            P("rep", "grp", None),
            P("grp"),
            P("grp", None),
            P("grp", None),
            P("grp", None),
            P(None, "grp"),
            P("grp"),
            P(),
            P(),
            P(),
            P("grp"),
            P("grp", None),
            P("grp"),
            P("grp", None),
            P("grp", None),
        ),
        check_vma=False,
    )
```

```python
import functools
import math
from functools import partial

import jax
import jax.numpy as jnp
from jax import lax
from jax.experimental import pallas as pl
from jax.experimental.pallas import tpu as pltpu
from jax.sharding import PartitionSpec as P

HEADS = 8
KV_HEADS = 2
HEAD = 64
SSM_HEADS = 24
SSM_HEAD = 64
STATE = 128
CONV = 4
FF = 2048


NORM_EPS = 1e-05
ROPE_BASE = 100000000000.0
HIGHEST = lax.Precision.HIGHEST


def shifted(value, axis, steps):
    count = lax.axis_size(axis)
    leading, last = (max(0, -steps), min(count, count - steps))
    return lax.ppermute(value, axis, [(source, source + steps) for source in range(leading, last)])


def rms_scale(values, scales):
    return values * lax.rsqrt(jnp.mean(values * values, axis=-1, keepdims=True) + NORM_EPS) * scales


def rope_tables(positions, head_width):
    indices = jnp.arange(head_width // 2, dtype=jnp.float32)
    frequency = ROPE_BASE ** (-2.0 * indices / head_width)
    angles = positions.astype(jnp.float32)[:, None] * frequency[None, :]
    return (jnp.cos(angles), jnp.sin(angles))


def rotate(values, cosine_table, sine_table):
    middle = values.shape[-1] // 2
    lower_half = values[..., :middle]
    upper_half = values[..., middle:]
    cos_rows = cosine_table[:, None, :]
    sin_rows = sine_table[:, None, :]
    return jnp.concatenate(
        [
            lower_half * cos_rows - upper_half * sin_rows,
            upper_half * cos_rows + lower_half * sin_rows,
        ],
        axis=-1,
    )


def mixer_inputs(extended, step_raw, taps, tap_bias, step_bias, seg_ext):
    span_rows = step_raw.shape[1]
    tap_count = taps.shape[0]
    own_doc = seg_ext[:, tap_count - 1 :]
    summed = jnp.zeros((extended.shape[0], span_rows, extended.shape[2]), jnp.float32) + tap_bias
    for offset in range(tap_count):
        same_doc = (seg_ext[:, offset : offset + span_rows] == own_doc)[..., None]
        summed = summed + jnp.where(
            same_doc, extended[:, offset : offset + span_rows] * taps[offset], 0.0
        )
    return jax.nn.silu(summed), jax.nn.softplus(step_raw + step_bias)


def gated_norm(mixed, gate_part, scales):
    flat_mixed = mixed.reshape(gate_part.shape)
    return rms_scale(flat_mixed * jax.nn.silu(gate_part), scales)


def swiglu(gate_vals, up_vals):
    return jax.nn.silu(gate_vals) * up_vals


MESH = pl.DeviceIdType.MESH
HIDDEN = -1e30
VMEM_LIMIT = 67043328
TAIL_LAG = 1


def seat():
    rep, grp = lax.axis_index("rep"), lax.axis_index("grp")
    chips = lax.axis_size("grp") // 2
    quarter = lax.rem(rep, 4)
    base = rep - quarter
    flip_x = quarter + 1 - 2 * lax.rem(quarter, 2)
    flip_y = lax.rem(quarter + 2, 4)
    chip, core = lax.div(grp, 2), lax.rem(grp, 2)
    return dict(
        quarter=quarter,
        qx=flip_x,
        qy=flip_y,
        qd=lax.rem(flip_x + 2, 4),
        chip=chip,
        core=core,
        x={"rep": base + flip_x},
        y={"rep": base + flip_y},
        partner={"grp": chip * 2 + 1 - core},
        along=[{"grp": lax.rem(chip + k, chips) * 2 + core} for k in range(chips)],
        chip_to=[lax.rem(chip + k, chips) for k in range(chips)],
        chip_from=[lax.rem(chip - k + chips, chips) for k in range(chips)],
    )


def remote(source, target, sent, arrived, device):
    return pltpu.make_async_remote_copy(
        src_ref=source,
        dst_ref=target,
        send_sem=sent,
        recv_sem=arrived,
        device_id=device,
        device_id_type=MESH,
    )


def greet(me, extra=()):
    barrier = pltpu.get_barrier_semaphore()
    others = [me["x"], me["y"], me["partner"], *me["along"][1:], *extra]
    for device in others:
        pl.semaphore_signal(barrier, inc=1, device_id=device, device_id_type=MESH)
    pl.semaphore_wait(barrier, len(others))


def near_first(chips):
    return sorted(range(1, chips), key=lambda k: min(k, chips - k))


def gather_kernel(count, whole, chips, *refs):
    ins, outs = refs[:count], refs[count : 2 * count]
    zs, zr, xs, xr, ys, yr, ds, dr, cs, cr, ls = refs[2 * count :]
    me = seat()
    greet(me)
    own = me["chip"] * 2 + me["core"]
    order = near_first(chips)
    along, over_x, over_y, diagonal, across, local = {}, {}, {}, {}, {}, []
    for m in range(count):
        local.append(pltpu.make_async_copy(ins[m], outs[m].at[own], ls.at[m]))
        local[-1].start()
        for k in order:
            part = ins[m] if whole[m] else ins[m].at[me["quarter"]]
            place = outs[m].at[own] if whole[m] else outs[m].at[own, me["quarter"]]
            along[m, k] = remote(part, place, zs.at[m, k], zr.at[m, k], me["along"][k])
            along[m, k].start()
        across[m, 0] = remote(ins[m], outs[m].at[own], cs.at[m, 0], cr.at[m, 0], me["partner"])
        across[m, 0].start()
    for step in range(count + 2):
        m = step
        if m < count:
            for k in order:
                along[m, k].wait_recv()
                if whole[m]:
                    continue
                piece = outs[m].at[me["chip_from"][k] * 2 + me["core"], me["quarter"]]
                over_x[m, k] = remote(piece, piece, xs.at[m, k], xr.at[m, k], me["x"])
                over_y[m, k] = remote(piece, piece, ys.at[m, k], yr.at[m, k], me["y"])
                over_x[m, k].start()
                over_y[m, k].start()
        m = step - 1
        if 0 <= m < count and not whole[m]:
            for k in order:
                block = outs[m].at[me["chip_from"][k] * 2 + me["core"]]
                if (m + k) % 2 == 0:
                    over_x[m, k].wait_recv()
                    piece, device = block.at[me["qx"]], me["y"]
                else:
                    over_y[m, k].wait_recv()
                    piece, device = block.at[me["qy"]], me["x"]
                diagonal[m, k] = remote(piece, piece, ds.at[m, k], dr.at[m, k], device)
                diagonal[m, k].start()
        m = step - 2
        if 0 <= m < count:
            for k in order:
                block = outs[m].at[me["chip_from"][k] * 2 + me["core"]]
                if not whole[m]:
                    if (m + k) % 2 == 0:
                        over_y[m, k].wait_recv()
                    else:
                        over_x[m, k].wait_recv()
                    diagonal[m, k].wait_recv()
                across[m, k] = remote(block, block, cs.at[m, k], cr.at[m, k], me["partner"])
                across[m, k].start()
    for copy in across.values():
        copy.wait_recv()
    for copies in (along, over_x, over_y, diagonal, across):
        for copy in copies.values():
            copy.wait_send()
    for copy in local:
        copy.wait()


def gather_group(shards, whole):
    group = lax.axis_size("grp")
    chips = group // 2
    count = len(shards)
    cut = [
        shard[None] if flag else shard.reshape(4, shard.shape[0] // 4, shard.shape[1])
        for shard, flag in zip(shards, whole)
    ]
    sems = [pltpu.SemaphoreType.DMA((count, chips))] * 10 + [pltpu.SemaphoreType.DMA((count,))]
    full = pl.pallas_call(
        functools.partial(gather_kernel, count, whole, chips),
        out_shape=[jax.ShapeDtypeStruct((group, *part.shape), part.dtype) for part in cut],
        in_specs=[pl.BlockSpec(memory_space=pltpu.VMEM)] * count,
        out_specs=[pl.BlockSpec(memory_space=pl.ANY)] * count,
        scratch_shapes=sems,
        compiler_params=pltpu.CompilerParams(
            collective_id=0, has_side_effects=True, vmem_limit_bytes=VMEM_LIMIT
        ),
        name="gather_group",
    )(*cut)
    return [part.reshape(-1, part.shape[-1]) for part in full]


def f32(value):
    return value.astype(jnp.float32)


def turn_rows(source, turned, chips, piece, is_turned):
    features = source.shape[0] if is_turned else source.shape[1]
    width = math.lcm(128, piece)
    for start in range(0, features, width):
        if is_turned:
            value = f32(source[start : start + width, :])
        else:
            value = f32(source[:, start : start + width]).T
        for i in range(width // piece):
            at = start // piece + i
            chip, core, quarter = at // 8, (at // 4) % 2, at % 4
            block = value[i * piece : (i + 1) * piece].astype(jnp.bfloat16)
            turned[core, quarter, chip * piece : (chip + 1) * piece, :] = block


class GradPlan:
    def __init__(self, lefts, turned, rights, chunks):
        self.chips = lax.axis_size("grp") // 2
        self.extras = lax.axis_size("rep") // 4
        self.lefts, self.turned, self.rights, self.chunks = lefts, turned, rights, chunks
        self.tokens = rights[0].shape[0]
        sizes = [x.shape[0] if flag else x.shape[1] for x, flag in zip(lefts, turned)]
        self.rows = [size // 8 for size in sizes]
        self.piece = [size // (8 * self.chips) for size in sizes]

    def operands(self):
        return [*self.lefts, *self.rights]

    def outs(self):
        return [
            jax.ShapeDtypeStruct((4, self.piece[a], width), jnp.bfloat16)
            for a, _, _, width in self.chunks
        ]

    def scratch(self):
        low, vmem, dma = jnp.bfloat16, pltpu.VMEM, pltpu.SemaphoreType.DMA
        lefts, rights, count = len(self.lefts), len(self.rights), len(self.chunks)
        work = [vmem((2, 4, rows, self.tokens), low) for rows in self.rows]
        work += [vmem((4, rows, self.tokens), low) for rows in self.rows]
        work += [vmem(right.shape, low) for right in self.rights]
        shapes = [(self.rows[a], self.piece[a], width) for a, _, _, width in self.chunks]
        work += [vmem((4, rows, width), low) for rows, _, width in shapes]
        work += [vmem((2, rows, width), low) for rows, _, width in shapes]
        work += [vmem((rows, width), low) for rows, _, width in shapes]
        work += [vmem((self.chips, piece, width), low) for _, piece, width in shapes]
        work += [vmem((self.chips - 1, piece, width), low) for _, piece, width in shapes]
        if self.extras > 1:
            work += [vmem((self.extras, piece, width), low) for _, piece, width in shapes]
        sems = [dma((lefts,))] * 2 + [dma((rights,))] * 2
        sems += [dma((count, 2)), dma((count, 2)), dma((count,)), dma((count,))]
        sems += [dma((count, self.chips))] * 2 + [dma((count, self.extras))] * 2
        sems += [dma((count, 3))] * 2
        return [*work, *sems]

    def steps(self, me, ins, outs, scratch, lag=2):
        chips, extras, count = self.chips, self.extras, len(self.chunks)
        lefts, rights = ins[: len(self.lefts)], ins[len(self.lefts) :]
        groups = []
        for size in (len(lefts), len(lefts), len(rights), *[count] * (6 if extras > 1 else 5)):
            groups.append(scratch[:size])
            scratch = scratch[size:]
        turned, turned_in, rights_in, parts, one, two, total, slots = groups[:8]
        extra_in = groups[8] if extras > 1 else ()
        la_s, la_r, ri_s, ri_r, s1, r1, s2, r2, zs, zr, es, er, gs, gr = scratch
        core = me["core"]
        reps, rep = lax.axis_size("rep"), lax.axis_index("rep")
        beyond = [{"rep": lax.rem(rep + 4 * e, reps)} for e in range(1, extras)]
        swap_left, swap_right = {}, {}
        for n in range(len(rights)):
            swap_right[n] = remote(rights[n], rights_in[n], ri_s.at[n], ri_r.at[n], me["partner"])
            swap_right[n].start()
        for n in range(len(lefts)):
            turn_rows(lefts[n], turned[n], chips, self.piece[n], self.turned[n])
            swap_left[n] = remote(
                turned[n].at[1 - core], turned_in[n], la_s.at[n], la_r.at[n], me["partner"]
            )
            if n > 0:
                swap_left[n - 1].start()
            yield
        swap_left[len(lefts) - 1].start()
        have = set()
        first, second, along, other, spread = {}, {}, {}, {}, {}

        def form(m):
            a, b, start, width = self.chunks[m]
            for key, copy in (("left", a), swap_left[a]), (("right", b), swap_right[b]):
                if key not in have:
                    have.add(key)
                    copy.wait_recv()
            at = slice(start, start + width)

            def quarter(q, _):
                value = dot_plain(turned[a][core, q], rights[b][:, at])
                value = value + dot_plain(turned_in[a][q], rights_in[b][:, at])
                parts[m][q] = value.astype(jnp.bfloat16)
                return 0

            lax.fori_loop(0, 4, quarter, 0)

        def send_first(m):
            device, mine = (me["x"], me["qx"]) if m % 2 == 0 else (me["y"], me["qy"])
            for i, q in ((1, me["qd"]), (0, mine)):
                first[m, i] = remote(
                    parts[m].at[q], one[m].at[i], s1.at[m, i], r1.at[m, i], device
                )
                first[m, i].start()

        def send_second(m):
            rows = self.rows[self.chunks[m][0]]
            device, q = (me["y"], me["qy"]) if m % 2 == 0 else (me["x"], me["qx"])
            first[m, 1].wait_recv()

            def add(j, _):
                at = pl.ds(pl.multiple_of(j * 64, 64), 64)
                value = f32(parts[m][q, at, :]) + f32(one[m][1, at, :])
                parts[m][q, at, :] = value.astype(jnp.bfloat16)
                return 0

            lax.fori_loop(0, rows // 64, add, 0)
            second[m] = remote(parts[m].at[q], two[m], s2.at[m], r2.at[m], device)
            second[m].start()

        def send_along(m):
            piece = self.piece[self.chunks[m][0]]
            first[m, 0].wait_recv()
            second[m].wait_recv()
            for j in range(chips):
                at = slice(j * piece, (j + 1) * piece)
                value = f32(parts[m][me["quarter"], at, :]) + f32(one[m][0, at, :]) + f32(two[m][at, :])
                total[m][j] = value.astype(jnp.bfloat16)
            for k in near_first(chips):
                along[m, k] = remote(
                    total[m].at[me["chip_to"][k]],
                    slots[m].at[k - 1],
                    zs.at[m, k],
                    zr.at[m, k],
                    me["along"][k],
                )
                along[m, k].start()

        def send_spread(m):
            value = f32(total[m][me["chip"]])
            for k in near_first(chips):
                along[m, k].wait_recv()
                value = value + f32(slots[m][k - 1])
            if extras > 1:
                extra_in[m][0] = value.astype(jnp.bfloat16)
                for e in range(1, extras):
                    other[m, e] = remote(
                        extra_in[m].at[0],
                        extra_in[m].at[e],
                        es.at[m, e],
                        er.at[m, e],
                        beyond[e - 1],
                    )
                    other[m, e].start()
                for e in range(1, extras):
                    other[m, e].wait_recv()
                    value = value + f32(extra_in[m][e])
            outs[m][me["quarter"]] = value.astype(jnp.bfloat16)
            piece = outs[m].at[me["quarter"]]
            for i, device in enumerate((me["x"], me["y"])):
                spread[m, i] = remote(piece, piece, gs.at[m, i], gr.at[m, i], device)
                spread[m, i].start()

        def send_diagonal(m):
            way = m % 2
            spread[m, way].wait_recv()
            q, device = (me["qx"], me["y"]) if way == 0 else (me["qy"], me["x"])
            piece = outs[m].at[q]
            spread[m, 2] = remote(piece, piece, gs.at[m, 2], gr.at[m, 2], device)
            spread[m, 2].start()

        stages = (send_second, send_along, send_spread, send_diagonal)
        for step in range(count + lag * len(stages)):
            if step < count:
                form(step)
                send_first(step)
            for n, stage in enumerate(stages):
                m = step - lag * (n + 1)
                if 0 <= m < count:
                    stage(m)
            yield
        for m in range(count):
            spread[m, 1 - m % 2].wait_recv()
            spread[m, 2].wait_recv()
        for copies in (swap_left, swap_right, first, second, along, other, spread):
            for copy in copies.values():
                copy.wait_send()
        yield


def small_steps(me, chips, extras, vec, out, stage, slots, sems, more):
    ss, sr, zs, zr = sems
    copies = []
    value = vec[...]
    hops = [me["x"], me["y"], me["partner"]]
    for i, device in enumerate(hops):
        stage[i] = value
        copies.append(remote(stage.at[i], slots.at[i], ss.at[i], sr.at[i], device))
        copies[-1].start()
        yield
        copies[-1].wait_recv()
        value = value + slots[i]
    if extras > 1:
        stage[3] = value
        for e in range(1, extras):
            at = 3 + chips + e
            copies.append(remote(stage.at[3], slots.at[at], ss.at[2 + e], sr.at[2 + e], more[e - 1]))
            copies[-1].start()
        yield
        for e in range(1, extras):
            copies[-e].wait_recv()
        for e in range(1, extras):
            value = value + slots[3 + chips + e]
    stage[4] = value
    along = []
    for k in near_first(chips):
        along.append(remote(stage.at[4], slots.at[3 + k], zs.at[k], zr.at[k], me["along"][k]))
        along[-1].start()
    yield
    for copy in along:
        copy.wait_recv()
    for k in range(1, chips):
        value = value + slots[3 + k]
    out[...] = value
    for copy in copies + along:
        copy.wait_send()
    yield


def run_out(steps):
    for _ in steps:
        pass


def tail_kernel(plan, *refs):
    cut = (len(plan.operands()), 1, len(plan.chunks), 1)
    groups = []
    for size in cut:
        groups.append(refs[:size])
        refs = refs[size:]
    (vec,), (total,) = groups[1], groups[3]
    stage, slots = refs[-6:-4]
    me = seat()
    rep, reps = lax.axis_index("rep"), lax.axis_size("rep")
    beyond = [{"rep": lax.rem(rep + 4 * e, reps)} for e in range(1, plan.extras)]
    greet(me, beyond)
    large = plan.steps(me, groups[0], groups[2], refs[:-6], lag=TAIL_LAG)
    small = small_steps(me, plan.chips, plan.extras, vec, total, stage, slots, refs[-4:], beyond)
    for _ in small:
        next(large, None)
    run_out(large)


def sum_gradients(plan, vec):
    dma = pltpu.SemaphoreType.DMA
    chips, extras = plan.chips, plan.extras
    small = [
        pltpu.VMEM((5, *vec.shape), vec.dtype),
        pltpu.VMEM((3 + chips + extras, *vec.shape), vec.dtype),
    ]
    small += [dma((2 + extras,)), dma((2 + extras,)), dma((chips,)), dma((chips,))]
    count = len(plan.chunks)
    *sums, total = pl.pallas_call(
        functools.partial(tail_kernel, plan),
        out_shape=[*plan.outs(), jax.ShapeDtypeStruct(vec.shape, vec.dtype)],
        in_specs=[pl.BlockSpec(memory_space=pltpu.VMEM)] * (len(plan.operands()) + 1),
        out_specs=[pl.BlockSpec(memory_space=pltpu.VMEM)] * (count + 1),
        scratch_shapes=[*plan.scratch(), *small],
        compiler_params=pltpu.CompilerParams(
            collective_id=1, has_side_effects=True, vmem_limit_bytes=VMEM_LIMIT
        ),
        name="sum_gradients",
    )(*plan.operands(), vec)
    return sums, total


def shard_rows(totals):
    wide = [total.reshape(-1, total.shape[-1]) for total in totals]
    return jnp.concatenate(wide, axis=1).astype(jnp.float32)


def column_chunks(left, right, columns, pieces):
    width = columns // pieces // 128 * 128
    starts = [i * width for i in range(pieces)] + [columns]
    return [(left, right, low, high - low) for low, high in zip(starts, starts[1:])]


def axis_seat():
    grp = lax.axis_index("grp")
    return lax.div(grp, 2), lax.rem(grp, 2)


def greet_group(extra=()):
    size, grp = lax.axis_size("grp"), lax.axis_index("grp")
    barrier = pltpu.get_barrier_semaphore()
    others = [{"grp": lax.rem(grp + k, size)} for k in range(1, size)] + list(extra)
    for device in others:
        pl.semaphore_signal(barrier, inc=1, device_id=device, device_id_type=MESH)
    pl.semaphore_wait(barrier, len(others))


def lanes(shape):
    return lax.broadcasted_iota(jnp.int32, shape, len(shape) - 1)


def pair_columns(columns, pair):
    rows = columns.shape[0]
    low = jnp.broadcast_to(columns[:, 2 * pair : 2 * pair + 1], (rows, 128))
    high = jnp.broadcast_to(columns[:, 2 * pair + 1 : 2 * pair + 2], (rows, 128))
    return jnp.where(lanes((rows, 128)) < 64, low, high)


def dot_rows(left, right):
    return lax.dot_general(
        left, right, (((1,), (1,)), ((), ())), preferred_element_type=jnp.float32
    )


def dot_plain(left, right):
    return jnp.dot(left, right, preferred_element_type=jnp.float32)


def align_heads(source, target, scale):
    for pair in range(HEADS // 2):
        both = source[:, pair * 128 : (pair + 1) * 128].astype(jnp.float32) * scale
        swapped = pltpu.roll(both, 64, 1)
        for odd in range(2):
            head = 2 * pair + odd
            group = head // (HEADS // KV_HEADS)
            value = both if odd == group else swapped
            keep = lanes(value.shape) // 64 == group
            target[head] = jnp.where(keep, value, 0.0).astype(jnp.bfloat16)


def slot_plan(reach):
    return [(0, 0)] + [(k, core) for k in range(1, reach + 1) for core in (1, 0)]


def slot_live(slot, chip, core, reach):
    back, side = slot
    if back == 0:
        return core == 1
    live = chip - back >= 0
    if back == reach and side == 0:
        live = jnp.logical_and(live, core == 0)
    return live


def same_document(key_column, query_row, causal):
    size = query_row.shape[-1]
    allowed = key_column == query_row
    if causal:
        rows = lax.broadcasted_iota(jnp.int32, (size, size), 0)
        allowed = jnp.logical_and(allowed, rows <= lanes((size, size)))
    return jnp.where(allowed, 0.0, HIDDEN)


def mix_forward_kernel(
    reach,
    chips,
    q_ref,
    kv_ref,
    segc_ref,
    segr_ref,
    act_ref,
    dt_ref,
    run_ref,
    runt_ref,
    e_ref,
    wd_ref,
    car_ref,
    skip_ref,
    att_ref,
    attt_ref,
    inv_ref,
    mixed_ref,
    ent_ref,
    kvw_ref,
    qa,
    bias,
    vt,
    ot,
    total,
    xdt,
    xw,
    runb,
    gram,
    own_state,
    half_out,
    half_in,
    car_in,
    chip_out,
    chip_car,
    chip_in,
    chip_car_in,
    enter_out,
    acc,
    ka_s,
    ka_r,
    kp_s,
    kp_r,
    ha_s,
    ha_r,
    ca_s,
    ca_r,
    en_s,
    en_r,
):
    chip, core = axis_seat()
    grp = lax.axis_index("grp")
    span = q_ref.shape[0]
    inner = SSM_HEADS * SSM_HEAD
    half = inner // 2
    partner = {"grp": chip * 2 + 1 - core}

    def ahead(k):
        return {"grp": lax.rem(grp + 2 * k, 2 * chips)}

    greet_group()
    own_kv = remote(kv_ref, kvw_ref.at[0, core], kp_s.at[0], kp_r.at[0], partner)
    own_kv.start()
    kv_along = {}
    for k in range(1, reach + 1):
        kv_along[k] = remote(kv_ref, kvw_ref.at[k, core], ka_s.at[k], ka_r.at[k], ahead(k))
        pl.when(chip + k < chips)(kv_along[k].start)
    kvw_ref[0, core] = kv_ref[...]

    weight = wd_ref[...] * dt_ref[...]
    for pair in range(SSM_HEADS // 2):
        at = slice(pair * 128, (pair + 1) * 128)
        x_pair = act_ref[:, at]
        xdt[:, at] = (x_pair * pair_columns(dt_ref, pair)).astype(jnp.bfloat16)
        xw[:, at] = (x_pair * pair_columns(weight, pair)).astype(jnp.bfloat16)
    in_map = act_ref[:, inner : inner + STATE]
    out_map = act_ref[:, inner + STATE :]
    out_low = out_map.astype(jnp.bfloat16)
    in_turned = in_map.T.astype(jnp.bfloat16)
    for i in range(2):
        own_state[i] = dot_plain(in_turned, xw[:, i * half : (i + 1) * half])
    half_out[...] = own_state[1 - core].astype(jnp.bfloat16)
    align_heads(q_ref, qa, HEAD**-0.5)
    ot[...] = jnp.zeros_like(ot)
    total[...] = jnp.zeros_like(total)
    half_car = remote(car_ref.at[1 - core], car_in, ha_s.at[0], ha_r.at[0], partner)
    half_state = remote(half_out, half_in, ha_s.at[1], ha_r.at[1], partner)
    half_car.start()
    half_state.start()

    def attend_slot(keys, values, key_docs, causal):
        bias[...] = same_document(key_docs, segr_ref[...], causal)
        vt[...] = values.astype(jnp.float32).T.astype(jnp.bfloat16)

        def per_head(head, _):
            group = lax.div(head, HEADS // KV_HEADS)
            scores = dot_rows(keys[...], qa[head]) + bias[...]
            weights = jnp.exp(scores)
            total[head] += jnp.sum(weights, axis=0, keepdims=True)
            rows = pl.ds(pl.multiple_of(group * HEAD, HEAD), HEAD)
            into = pl.ds(pl.multiple_of(head * HEAD, HEAD), HEAD)
            ot[into, :] += dot_plain(vt[rows, :], weights.astype(jnp.bfloat16))
            return 0

        lax.fori_loop(0, HEADS, per_head, 0)

    def attend_ref(ref, key_docs, causal):
        attend_slot(ref.at[:, 0:128], ref[:, 128:256], key_docs, causal)

    attend_ref(kv_ref, segc_ref[2 * reach + core], True)

    half_car.wait_recv()
    half_state.wait_recv()
    mine, theirs = own_state[core], half_in[...].astype(jnp.float32)
    car_mine, car_theirs = car_ref[core], car_in[...]
    first = core == 0
    car_0 = jnp.where(first, car_mine, car_theirs)
    car_1 = jnp.where(first, car_theirs, car_mine)
    state_0 = jnp.where(first, mine, theirs)
    state_1 = jnp.where(first, theirs, mine)
    chip_out[...] = (state_1 + car_1[0:1] * state_0).astype(jnp.bfloat16)
    chip_car[...] = car_0 * car_1

    for head in range(SSM_HEADS):
        runb[head] = jnp.broadcast_to(run_ref[:, head : head + 1], (span, 128))
    gram[...] = lax.dot_general(
        out_map, in_map, (((1,), (1,)), ((), ())), precision=HIGHEST,
        preferred_element_type=jnp.float32,
    )
    state_along = {}
    for k in range(1, reach + 1):
        state_along[k] = (
            remote(chip_out, chip_in.at[k], ca_s.at[k, 0], ca_r.at[k, 0], ahead(k)),
            remote(chip_car, chip_car_in.at[k], ca_s.at[k, 1], ca_r.at[k, 1], ahead(k)),
        )
        for copy in state_along[k]:
            pl.when(chip + k < chips)(copy.start)

    kv_pass = {}
    for k in range(1, reach + 1):
        place = kvw_ref.at[k, core]
        kv_pass[k] = remote(place, place, kp_s.at[k], kp_r.at[k], partner)

        def hand_on(k=k):
            kv_along[k].wait_recv()
            kv_pass[k].start()

        pl.when(chip - k >= 0)(hand_on)

    rows = lax.broadcasted_iota(jnp.int32, (span, span), 0)
    allowed = jnp.logical_and(segc_ref[2 * reach + core] == segr_ref[...], rows >= lanes((span, span)))
    bias[...] = jnp.where(allowed, 0.0, HIDDEN)

    def intra(quad, _):
        at = pl.ds(pl.multiple_of(quad * 256, 256), 256)
        value = jnp.zeros((span, 256), jnp.float32)
        for i in range(4):
            head = quad * 4 + i
            column = runb[head]
            spread = jnp.concatenate([column] * (span // 128), axis=1) - runt_ref[head]
            mixing = (jnp.exp(spread + bias[...]) * gram[...]).astype(jnp.bfloat16)
            part = dot_plain(mixing, xdt[:, at])
            value = jnp.where(lanes((span, 256)) // 64 == i, part, value)
        mixed_ref[:, at] = value + skip_ref[:, at] * act_ref[:, at]
        return 0

    lax.fori_loop(0, SSM_HEADS // 4, intra, 0)

    own_kv.wait_recv()
    for index, slot in enumerate(slot_plan(reach)):
        back, side = slot
        if slot == (1, 1):
            acc[...] = jnp.zeros_like(acc)
            for k in range(reach, 0, -1):

                def take(k=k):
                    for copy in state_along[k]:
                        copy.wait_recv()
                    acc[...] = chip_in[k].astype(jnp.float32) + chip_car_in[k, 0:1] * acc[...]

                pl.when(chip - k >= 0)(take)
            enter_0, enter_1 = acc[...], state_0 + car_0[0:1] * acc[...]
            ent_ref[core] = jnp.where(first, enter_0, enter_1)
            enter_out[...] = jnp.where(first, enter_1, enter_0)
            for k in range(1, reach + 1):
                pl.when(chip - k >= 0)(kv_pass[k].wait_recv)

        def visit(back=back, side=side):
            ref = kvw_ref.at[back, side]
            attend_ref(ref, segc_ref[2 * (reach - back) + side], False)

        pl.when(slot_live(slot, chip, core, reach))(visit)
        if slot == (1, 1):
            enter_pass = remote(enter_out, ent_ref.at[core], en_s, en_r, partner)
            enter_pass.start()

    for head in range(HEADS):
        inverse = 1.0 / total[head]
        inv_ref[head] = inverse
        into = slice(head * HEAD, (head + 1) * HEAD)
        ot[into, :] = ot[into, :] * inverse
    attt_ref[...] = ot[...].astype(jnp.bfloat16)
    for pair in range(HEADS // 2):
        at = slice(pair * 128, (pair + 1) * 128)
        att_ref[:, at] = ot[at, :].T.astype(jnp.bfloat16)

    enter_pass.wait_recv()
    for i in range(2):
        carried_in = dot_plain(out_low, ent_ref[i].astype(jnp.bfloat16))
        for j in range(SSM_HEADS // 4):
            pair = i * (SSM_HEADS // 4) + j
            at = slice(pair * 128, (pair + 1) * 128)
            part = carried_in[:, j * 128 : (j + 1) * 128]
            mixed_ref[:, at] += pair_columns(e_ref, pair) * part

    own_kv.wait_send()
    half_car.wait_send()
    half_state.wait_send()
    enter_pass.wait_send()
    for k in range(1, reach + 1):

        def sent(k=k):
            kv_along[k].wait_send()
            for copy in state_along[k]:
                copy.wait_send()

        pl.when(chip + k < chips)(sent)
        pl.when(chip - k >= 0)(kv_pass[k].wait_send)


def mix_forward(reach, q, kv, segc, segr, act, dt, run, runt, e, wd, car, skip):
    chips = lax.axis_size("grp") // 2
    span = q.shape[0]
    inner = SSM_HEADS * SSM_HEAD
    half = inner // 2
    f32, low = jnp.float32, jnp.bfloat16
    shape = jax.ShapeDtypeStruct
    dma = pltpu.SemaphoreType.DMA
    vmem = pltpu.VMEM
    outs = [
        shape((span, HEADS * HEAD), low),
        shape((HEADS * HEAD, span), low),
        shape((HEADS, 1, span), f32),
        shape((span, inner), f32),
        shape((2, STATE, half), f32),
        shape((reach + 1, 2, span, kv.shape[1]), low),
    ]
    scratch = [
        vmem((HEADS, span, 128), low),
        vmem((span, span), f32),
        vmem((128, span), low),
        vmem((HEADS * HEAD, span), f32),
        vmem((HEADS, 1, span), f32),
        vmem((span, inner), low),
        vmem((span, inner), low),
        vmem((SSM_HEADS, span, 128), f32),
        vmem((span, span), f32),
        vmem((2, STATE, half), f32),
        vmem((STATE, half), low),
        vmem((STATE, half), low),
        vmem((8, half), f32),
        vmem((STATE, half), low),
        vmem((8, half), f32),
        vmem((reach + 1, STATE, half), low),
        vmem((reach + 1, 8, half), f32),
        vmem((STATE, half), f32),
        vmem((STATE, half), f32),
        dma((reach + 1,)),
        dma((reach + 1,)),
        dma((reach + 1,)),
        dma((reach + 1,)),
        dma((2,)),
        dma((2,)),
        dma((reach + 1, 2)),
        dma((reach + 1, 2)),
        dma,
        dma,
    ]
    return pl.pallas_call(
        functools.partial(mix_forward_kernel, reach, chips),
        out_shape=outs,
        in_specs=[pl.BlockSpec(memory_space=pltpu.VMEM)] * 12,
        out_specs=[pl.BlockSpec(memory_space=pltpu.VMEM)] * len(outs),
        scratch_shapes=scratch,
        compiler_params=pltpu.CompilerParams(
            collective_id=2, has_side_effects=True, vmem_limit_bytes=VMEM_LIMIT
        ),
        name="mix_forward",
    )(q, kv, segc, segr, act, dt, run, runt, e, wd, car, skip)


def mix_backward_kernel(reach, plan, *refs):
    chips, extras = plan.chips, plan.extras
    many = len(plan.chunks)
    cut = [18, len(plan.operands()), 5, many, 44]
    groups = []
    for size in cut:
        groups.append(refs[:size])
        refs = refs[size:]
    (
        q_ref,
        kvw_ref,
        segc_ref,
        segr_ref,
        act_ref,
        dt_ref,
        run_ref,
        runt_ref,
        e_ref,
        wd_ref,
        car_ref,
        skip_ref,
        attt_ref,
        inv_ref,
        ent_ref,
        gout_ref,
        gmix_ref,
        rate_ref,
    ) = groups[0]
    (
        dq_ref,
        dkv_ref,
        dact_ref,
        ddt_ref,
        heads_ref,
    ) = groups[2]
    (
        qa,
        da,
        bias,
        kt,
        dqt,
        centre,
        dk,
        dv,
        part_out,
        part_in,
        sum_out,
        sum_in,
        xdt,
        xw,
        ge,
        runb,
        gramt,
        dgram,
        own_grad,
        half_out,
        half_in,
        car_in,
        chip_out,
        chip_car,
        chip_in,
        chip_car_in,
        later_out,
        later,
        acc,
        qrow,
        qcol,
        dxdt,
        sums,
        fold_ref,
        pp_s,
        pp_r,
        pa_s,
        pa_r,
        ha_s,
        ha_r,
        ca_s,
        ca_r,
        la_s,
        la_r,
    ) = groups[4]
    me = seat()
    rep, reps = lax.axis_index("rep"), lax.axis_size("rep")
    beyond = [{"rep": lax.rem(rep + 4 * e, reps)} for e in range(1, extras)]
    reduction = plan.steps(me, groups[1], groups[3], refs)
    chip, core = axis_seat()
    grp = lax.axis_index("grp")
    span = q_ref.shape[0]
    inner = SSM_HEADS * SSM_HEAD
    half = inner // 2
    low = jnp.bfloat16
    partner = {"grp": chip * 2 + 1 - core}
    first = core == 0

    def behind(k):
        return {"grp": lax.rem(grp - 2 * k + 2 * chips, 2 * chips)}

    greet_group([me["x"], me["y"], *beyond])
    next(reduction)
    in_map = act_ref[:, inner : inner + STATE]
    out_map = act_ref[:, inner + STATE :]
    in_low, out_low = in_map.astype(low), out_map.astype(low)
    weight = wd_ref[...] * dt_ref[...]
    for pair in range(SSM_HEADS // 2):
        at = slice(pair * 128, (pair + 1) * 128)
        x_pair = act_ref[:, at]
        ge[:, at] = (gmix_ref[:, at] * pair_columns(e_ref, pair)).astype(low)
        xdt[:, at] = (x_pair * pair_columns(dt_ref, pair)).astype(low)
        xw[:, at] = (x_pair * pair_columns(weight, pair)).astype(low)
    out_turned = out_map.T.astype(low)
    for i in range(2):
        own_grad[i] = dot_plain(out_turned, ge[:, i * half : (i + 1) * half])
    half_out[...] = own_grad[1 - core].astype(low)
    align_heads(q_ref, qa, HEAD**-0.5)
    align_heads(gout_ref, da, 1.0)
    half_car = remote(car_ref.at[1 - core], car_in, ha_s.at[0], ha_r.at[0], partner)
    half_grad = remote(half_out, half_in, ha_s.at[1], ha_r.at[1], partner)
    half_car.start()
    half_grad.start()

    next(reduction, None)
    for pair in range(HEADS // 2):
        at = slice(pair * 128, (pair + 1) * 128)
        product = gout_ref[:, at].astype(jnp.float32).T * attt_ref[at, :].astype(jnp.float32)
        for odd in range(2):
            rows = product[odd * HEAD : (odd + 1) * HEAD]
            centre[2 * pair + odd] = jnp.sum(rows, axis=0, keepdims=True)
    dqt[...] = jnp.zeros_like(dqt)

    def attend_back(ref, key_docs, causal):
        bias[...] = same_document(key_docs, segr_ref[...], causal)
        kt[...] = ref[:, 0:128].astype(jnp.float32).T.astype(low)
        dk[...] = jnp.zeros_like(dk)
        dv[...] = jnp.zeros_like(dv)

        def per_head(head, _):
            group = lax.div(head, HEADS // KV_HEADS)
            scores = dot_rows(ref[:, 0:128], qa[head]) + bias[...]
            probs = jnp.exp(scores) * inv_ref[head]
            grad_probs = dot_rows(ref[:, 128:256], da[head])
            grad_scores = (probs * (grad_probs - centre[head])).astype(low)
            dv[...] += dot_plain(probs.astype(low), da[head])
            dk[...] += dot_plain(grad_scores, qa[head])
            rows = pl.ds(pl.multiple_of(group * HEAD, HEAD), HEAD)
            into = pl.ds(pl.multiple_of(head * HEAD, HEAD), HEAD)
            dqt[into, :] += dot_plain(kt[rows, :], grad_scores)
            return 0

        lax.fori_loop(0, HEADS // 2, per_head, 0)
        lax.fori_loop(HEADS // 2, HEADS, per_head, 0)

    passed, sent_on = {}, {}

    def pass_slot(back, side):
        live = slot_live((back, side), chip, core, reach)

        def compute():
            attend_back(kvw_ref.at[back, side], segc_ref[2 * (reach - back) + side], False)
            part_out[back, side, :, 0:128] = dk[...].astype(low)
            part_out[back, side, :, 128:256] = dv[...].astype(low)

        pl.when(live)(compute)

    def start_part(back):
        for side in (0, 1):
            passed[back, side] = remote(
                part_out.at[back, side],
                part_in.at[back],
                pp_s.at[back],
                pp_r.at[back],
                partner,
            )
            live = slot_live((back, side), chip, core, reach)
            pl.when(jnp.logical_and(live, core != side))(passed[back, side].start)

    def send_sum(back):
        both = chip - back >= 0
        partner_has = jnp.logical_and(both, core == 1) if back == reach else both

        def add_partner():
            passed[back, 0].wait_recv()
            value = part_out[back, core].astype(jnp.float32) + part_in[back].astype(jnp.float32)
            sum_out[back] = value.astype(low)

        pl.when(partner_has)(add_partner)
        if back == reach:

            def alone():
                sum_out[back] = part_out[back, core]

            pl.when(jnp.logical_and(both, core == 0))(alone)

    def send_sum_start(back):
        sent_on[back] = remote(
            sum_out.at[back], sum_in.at[back], pa_s.at[back], pa_r.at[back], behind(back)
        )
        pl.when(chip - back >= 0)(sent_on[back].start)

    next(reduction, None)
    pass_slot(reach, 1)
    next(reduction, None)

    half_car.wait_recv()
    half_grad.wait_recv()
    mine, theirs = own_grad[core], half_in[...].astype(jnp.float32)
    car_mine, car_theirs = car_ref[core], car_in[...]
    car_0 = jnp.where(first, car_mine, car_theirs)
    car_1 = jnp.where(first, car_theirs, car_mine)
    grad_0 = jnp.where(first, mine, theirs)
    grad_1 = jnp.where(first, theirs, mine)
    chip_out[...] = (grad_0 + car_0[0:1] * grad_1).astype(low)
    chip_car[...] = car_0 * car_1
    pass_slot(reach, 0)
    next(reduction, None)
    state_along = {}
    for k in range(1, reach + 1):
        state_along[k] = (
            remote(chip_out, chip_in.at[k], ca_s.at[k, 0], ca_r.at[k, 0], behind(k)),
            remote(chip_car, chip_car_in.at[k], ca_s.at[k, 1], ca_r.at[k, 1], behind(k)),
        )
        for copy in state_along[k]:
            pl.when(chip - k >= 0)(copy.start)
    start_part(reach)
    for back in range(reach - 1, 0, -1):
        pass_slot(back, 1)
        next(reduction, None)
        send_sum(back + 1)
        pass_slot(back, 0)
        next(reduction, None)
        send_sum_start(back + 1)
        start_part(back)
    pass_slot(0, 0)
    next(reduction, None)
    start_part(0)
    send_sum(1)

    for head in range(SSM_HEADS):
        runb[head] = jnp.broadcast_to(run_ref[:, head : head + 1], (span, 128))
    send_sum_start(1)
    bias[...] = same_document(segc_ref[2 * reach + core], segr_ref[...], True)
    gramt[...] = lax.dot_general(
        in_map, out_map, (((1,), (1,)), ((), ())), precision=HIGHEST,
        preferred_element_type=jnp.float32,
    )
    dgram[...] = jnp.zeros_like(dgram)
    qcol[...] = jnp.zeros_like(qcol)
    qrow[...] = jnp.zeros_like(qrow)
    heads_of = lax.broadcasted_iota(jnp.int32, (inner, 128), 0) // SSM_HEAD
    fold_ref[...] = jnp.where(heads_of == lanes((inner, 128)), 1.0, 0.0).astype(low)

    def intra(quad, _):
        at = pl.ds(pl.multiple_of(quad * 256, 256), 256)
        grads = gmix_ref[:, at].astype(low)
        inputs = xdt[:, at]
        place = lanes((span, 256)) // 64
        value = jnp.zeros((span, 256), jnp.float32)
        for i in range(4):
            head = quad * 4 + i
            column = runb[head]
            spread = runt_ref[head] - jnp.concatenate([column] * (span // 128), axis=1)
            decay = jnp.exp(spread + bias[...])
            mixing = decay * gramt[...]
            alone = jnp.where(place == i, inputs, jnp.zeros_like(inputs))
            grad_mixing = dot_rows(alone, grads)
            dgram[...] += decay * grad_mixing
            product = mixing * grad_mixing
            qrow[pl.ds(head, 1), :] = jnp.sum(product, axis=0, keepdims=True)
            by_row = jnp.sum(product, axis=1, keepdims=True)
            qcol[...] = jnp.where(lanes((span, 128)) == head, by_row, qcol[...])
            part = dot_plain(mixing.astype(low), grads)
            value = jnp.where(place == i, part, value)
        dxdt[:, at] = value
        return 0

    for quad in range(SSM_HEADS // 4):
        lax.fori_loop(quad, quad + 1, intra, 0)
        next(reduction, None)

    acc[...] = jnp.zeros_like(acc)
    for k in range(reach, 0, -1):

        def take(k=k):
            for copy in state_along[k]:
                copy.wait_recv()
            acc[...] = chip_in[k].astype(jnp.float32) + chip_car_in[k, 0:1] * acc[...]

        pl.when(chip + k < chips)(take)
    later_1, later_0 = acc[...], grad_1 + car_1[0:1] * acc[...]
    later[core] = jnp.where(first, later_0, later_1)
    later_out[...] = jnp.where(first, later_1, later_0)

    attend_back(kvw_ref.at[0, core], segc_ref[2 * reach + core], True)
    next(reduction, None)
    later_pass = remote(later_out, later.at[core], la_s, la_r, partner)
    later_pass.start()
    for pair in range(HEADS // 2):
        at = slice(pair * 128, (pair + 1) * 128)
        dq_ref[:, at] = dqt[at, :].T * HEAD**-0.5

    dkv_ref[:, 0:128] = dk[...]
    dkv_ref[:, 128:256] = dv[...]

    def add_zero():
        passed[0, 0].wait_recv()
        dkv_ref[...] += part_in[0].astype(jnp.float32)

    pl.when(core == 0)(add_zero)
    for k in range(1, reach + 1):

        def add_ahead(k=k):
            sent_on[k].wait_recv()
            dkv_ref[...] += sum_in[k].astype(jnp.float32)

        pl.when(chip + k < chips)(add_ahead)

    grad_low = dgram[...].astype(low)
    grad_in = dot_plain(grad_low, out_low)
    grad_out = dot_plain(dgram[...].T.astype(low), in_low)
    later_pass.wait_recv()

    def fold(value, own):
        high = value.astype(low)
        rest = (value - high.astype(jnp.float32)).astype(low)
        return dot_plain(high, fold_ref[own, :]) + dot_plain(rest, fold_ref[own, :])

    carried = jnp.zeros((1, 128), jnp.float32)
    skip_sum = jnp.zeros((8, 128), jnp.float32)
    x_inside, x_part, g_reached = (jnp.zeros((span, 128), jnp.float32) for _ in range(3))
    for i in range(2):
        entering = ent_ref[i]
        grads = later[i]
        own = slice(i * half, (i + 1) * half)
        by_lane = jnp.sum(entering * grads, axis=0, keepdims=True)
        carried = carried + fold(jnp.broadcast_to(by_lane, (8, half)), own)[0:1]
        enter_low, later_low = entering.astype(low), grads.astype(low)
        grad_out = grad_out + dot_rows(ge[:, own], enter_low)
        grad_in = grad_in + dot_rows(xw[:, own], later_low)
        reached = dot_plain(out_low, enter_low)
        grad_xw = dot_plain(in_low, later_low)
        for j in range(SSM_HEADS // 4):
            pair = i * (SSM_HEADS // 4) + j
            at = slice(pair * 128, (pair + 1) * 128)
            here = slice(j * 128, (j + 1) * 128)
            x_pair, g_pair = act_ref[:, at], gmix_ref[:, at]
            part = grad_xw[:, here]
            inside = dxdt[:, at]
            dact_ref[:, at] = (
                skip_ref[:, at] * g_pair
                + pair_columns(dt_ref, pair) * inside
                + pair_columns(weight, pair) * part
            )
            sums[0, :, here] = x_pair * inside
            sums[1, :, here] = x_pair * part
            sums[2, :, here] = g_pair * reached[:, here]
            sums[3, :, here] = x_pair * g_pair
        x_inside, x_part, g_reached = (
            total + fold(sums[n], own) for n, total in enumerate((x_inside, x_part, g_reached))
        )
        by_lane = jnp.sum(sums[3], axis=0, keepdims=True)
        skip_sum = skip_sum + fold(jnp.broadcast_to(by_lane, (8, half)), own)
    dact_ref[:, inner : inner + STATE] = grad_in
    dact_ref[:, inner + STATE :] = grad_out

    w_part = weight * x_part
    drun = qrow[...].T - qcol[...] + e_ref[...] * g_reached - w_part
    last = jnp.sum(w_part, axis=0, keepdims=True) + rate_ref[1:2] * carried
    rows = lax.broadcasted_iota(jnp.int32, (span, 128), 0)
    drun = jnp.where(rows == span - 1, drun + last, drun)
    upper = lax.broadcasted_iota(jnp.int32, (span, span), 0) <= lanes((span, span))
    drate = lax.dot_general(
        jnp.where(upper, 1.0, 0.0), drun, (((1,), (0,)), ((), ())), precision=HIGHEST,
        preferred_element_type=jnp.float32,
    )
    rate = rate_ref[0:1]
    ddt_ref[...] = x_inside + wd_ref[...] * x_part + rate * drate
    heads_ref[...] = jnp.zeros_like(heads_ref)
    heads_ref[0:1] = jnp.sum(rate * dt_ref[...] * drate, axis=0, keepdims=True)
    heads_ref[1:2] = skip_sum[0:1]

    run_out(reduction)
    half_car.wait_send()
    half_grad.wait_send()
    later_pass.wait_send()
    for k in range(1, reach + 1):

        def sent(k=k):
            sent_on[k].wait_send()
            for copy in state_along[k]:
                copy.wait_send()

        pl.when(chip - k >= 0)(sent)
    for back in range(reach + 1):
        for side in (0, 1):
            if (back, side) in ((0, 1),):
                continue
            live = slot_live((back, side), chip, core, reach)
            pl.when(jnp.logical_and(live, core != side))(passed[back, side].wait_send)


def mix_backward(reach, operands, plan):
    sums = plan.outs()
    chips = lax.axis_size("grp") // 2
    span = operands[0].shape[0]
    inner = SSM_HEADS * SSM_HEAD
    half = inner // 2
    kv_width = 2 * KV_HEADS * HEAD
    f32, low = jnp.float32, jnp.bfloat16
    shape = jax.ShapeDtypeStruct
    dma = pltpu.SemaphoreType.DMA
    vmem = pltpu.VMEM
    outs = [
        shape((span, HEADS * HEAD), f32),
        shape((span, kv_width), f32),
        shape((span, inner + 2 * STATE), f32),
        shape((span, 128), f32),
        shape((8, 128), f32),
    ]
    scratch = [
        vmem((HEADS, span, 128), low),
        vmem((HEADS, span, 128), low),
        vmem((span, span), f32),
        vmem((128, span), low),
        vmem((HEADS * HEAD, span), f32),
        vmem((HEADS, 1, span), f32),
        vmem((span, 128), f32),
        vmem((span, 128), f32),
        vmem((reach + 1, 2, span, kv_width), low),
        vmem((reach + 1, span, kv_width), low),
        vmem((reach + 1, span, kv_width), low),
        vmem((reach + 1, span, kv_width), low),
        vmem((span, inner), low),
        vmem((span, inner), low),
        vmem((span, inner), low),
        vmem((SSM_HEADS, span, 128), f32),
        vmem((span, span), f32),
        vmem((span, span), f32),
        vmem((2, STATE, half), f32),
        vmem((STATE, half), low),
        vmem((STATE, half), low),
        vmem((8, half), f32),
        vmem((STATE, half), low),
        vmem((8, half), f32),
        vmem((reach + 1, STATE, half), low),
        vmem((reach + 1, 8, half), f32),
        vmem((STATE, half), f32),
        vmem((2, STATE, half), f32),
        vmem((STATE, half), f32),
        vmem((128, span), f32),
        vmem((span, 128), f32),
        vmem((span, inner), f32),
        vmem((4, span, half), f32),
        vmem((inner, 128), low),
        dma((reach + 1,)),
        dma((reach + 1,)),
        dma((reach + 1,)),
        dma((reach + 1,)),
        dma((2,)),
        dma((2,)),
        dma((reach + 1, 2)),
        dma((reach + 1, 2)),
        dma,
        dma,
    ]
    results = pl.pallas_call(
        functools.partial(mix_backward_kernel, reach, plan),
        out_shape=[*outs, *sums],
        in_specs=[pl.BlockSpec(memory_space=pltpu.VMEM)] * (len(operands) + len(plan.operands())),
        out_specs=[pl.BlockSpec(memory_space=pltpu.VMEM)] * (len(outs) + len(sums)),
        scratch_shapes=[*scratch, *plan.scratch()],
        compiler_params=pltpu.CompilerParams(
            collective_id=3, has_side_effects=True, vmem_limit_bytes=VMEM_LIMIT
        ),
        name="mix_backward",
    )(*operands, *plan.operands())
    return results[: len(outs)], results[len(outs) :]


def shards(
    tokens,
    segments,
    input_gain,
    attention_in,
    attention_out,
    mixer_in,
    filter_taps,
    filter_bias,
    step_bias,
    decay_log,
    skip_scale,
    mixer_gain,
    mixer_out,
    feed_gain,
    gate_up,
    down_proj,
    cotangent,
):
    seq_count, span_len, model_width = tokens.shape
    row_count = seq_count * span_len
    seq_len = segments.shape[1]
    group_devices = lax.axis_size("grp")
    position = lax.axis_index("grp") * span_len
    inner_width = SSM_HEADS * SSM_HEAD
    xbc_width = inner_width + 2 * STATE
    query_width = HEADS * HEAD
    kv_width = KV_HEADS * HEAD
    rim_rows = CONV - 1
    small = [input_gain, filter_taps.reshape(-1), filter_bias, mixer_gain, feed_gain]
    sizes = [part.shape[0] for part in small]
    packed = jnp.concatenate(small)
    packed = jnp.pad(packed, (0, -packed.shape[0] % 2048)).reshape(-1, 128)
    full_attn_in, full_mix_in, full_small, full_gate_up, full_down, full_mix_out, full_attn_out = (
        gather_group(
            [attention_in, mixer_in, packed, gate_up, down_proj, mixer_out, attention_out],
            [False, False, True, False, False, False, False],
        )
    )
    full_small = full_small.reshape(group_devices, -1)
    starts = [sum(sizes[:i]) for i in range(len(sizes) + 1)]
    pieces = [full_small[:, starts[i] : starts[i + 1]] for i in range(len(sizes))]
    full_gain_in, full_tap_bias, full_mix_gain, full_feed_gain = (
        pieces[i].reshape(-1) for i in (0, 2, 3, 4)
    )
    full_taps = pieces[1].reshape(group_devices, CONV, -1).transpose(1, 0, 2).reshape(CONV, -1)
    back_attn_in, back_attn_out, back_mix_in = full_attn_in, full_attn_out, full_mix_in
    back_mix_out, back_gate_up, back_down = full_mix_out, full_gate_up, full_down
    offsets = position + jnp.arange(span_len, dtype=jnp.int32)
    token_float = tokens.reshape(row_count, model_width).astype(jnp.float32)
    normed, norm_back = jax.vjp(rms_scale, token_float, full_gain_in.astype(jnp.float32))
    normed_low = normed.astype(jnp.bfloat16)
    projected = jnp.dot(normed_low, full_attn_in, preferred_element_type=jnp.float32).reshape(
        seq_count, span_len, -1
    )
    cosine_table, sine_table = rope_tables(offsets, HEAD)
    turner = partial(rotate, cosine_table=cosine_table, sine_table=sine_table)
    query_raw = projected[..., :query_width].reshape(seq_count, span_len, HEADS, HEAD)
    key_raw = projected[..., query_width : query_width + kv_width].reshape(
        seq_count, span_len, KV_HEADS, HEAD
    )
    value_part = projected[..., query_width + kv_width :]
    query_rot, query_back = jax.vjp(turner, query_raw)
    key_rot, key_back = jax.vjp(turner, key_raw)
    query_low = query_rot.astype(jnp.bfloat16)
    kv_local = jnp.concatenate(
        [key_rot.reshape(seq_count, span_len, kv_width), value_part], axis=-1
    ).astype(jnp.bfloat16)
    mix_proj = jnp.dot(normed_low, full_mix_in, preferred_element_type=jnp.float32).reshape(
        seq_count, span_len, -1
    )
    gate_part = mix_proj[..., :inner_width]
    conv_low = mix_proj[..., inner_width : inner_width + xbc_width].astype(jnp.bfloat16)
    step_raw = mix_proj[..., inner_width + xbc_width :]
    rim_in = shifted(conv_low[:, span_len - rim_rows :], "grp", 1)
    extended = jnp.concatenate([rim_in, conv_low], axis=1).astype(jnp.float32)
    padded_docs = jnp.concatenate(
        [jnp.full((seq_count, rim_rows), -1, jnp.int32), segments], axis=1
    )
    seg_ext = lax.dynamic_slice_in_dim(padded_docs, position, span_len + rim_rows, 1)
    (active, step_sizes), prep_back = jax.vjp(
        partial(mixer_inputs, seg_ext=seg_ext),
        extended,
        step_raw,
        full_taps.astype(jnp.float32),
        full_tap_bias.astype(jnp.float32),
        step_bias,
    )
    reach = min(seq_len // (4 * span_len), group_devices // 2 - 1)
    chip = lax.axis_index("grp") // 2
    docs = jnp.concatenate([jnp.full((2 * reach * span_len,), -1, jnp.int32), segments[0]])
    window = lax.dynamic_slice_in_dim(docs, 2 * chip * span_len, 2 * (reach + 1) * span_len)
    window = window.reshape(2 * (reach + 1), span_len, 1)
    own_docs = seg_ext[0, rim_rows:]
    prior_doc = seg_ext[0, rim_rows - 1]
    rate_scale = -jnp.exp(decay_log)
    steps = step_sizes[0]
    order = jnp.arange(span_len)
    before = (order[:, None] >= order[None, :]).astype(jnp.float32)
    running = jnp.dot(before, steps * rate_scale, precision=HIGHEST)
    final = running[-1:]
    enter_decay = jnp.where((own_docs == prior_doc)[:, None], jnp.exp(running), 0.0)
    tail_decay = jnp.where((own_docs == own_docs[-1])[:, None], jnp.exp(final - running), 0.0)
    carried = jnp.where(own_docs[-1] == prior_doc, jnp.exp(final[0]), 0.0)
    carried_lanes = jnp.broadcast_to(
        jnp.repeat(carried, SSM_HEAD).reshape(2, 1, inner_width // 2), (2, 8, inner_width // 2)
    )

    def wide(value):
        return jnp.pad(value, ((0, 0), (0, 128 - value.shape[1])))

    query_rows = query_low.reshape(row_count, query_width)
    recurrence = (
        active[0],
        wide(steps),
        wide(running),
        running.T.reshape(SSM_HEADS, 1, span_len),
        wide(enter_decay),
        wide(tail_decay),
        carried_lanes,
        jnp.repeat(skip_scale, SSM_HEAD)[None, :],
    )
    attended, attended_turned, inverse_total, mixed, entering, kv_window = mix_forward(
        reach, query_rows, kv_local[0], window, own_docs[None, :], *recurrence
    )
    mixed = mixed[None]
    normed_mix, gate_back = jax.vjp(gated_norm, mixed, gate_part, full_mix_gain.astype(jnp.float32))
    normed_mix_low = normed_mix.reshape(row_count, inner_width).astype(jnp.bfloat16)
    hidden = (
        token_float
        + jnp.dot(attended, full_attn_out, preferred_element_type=jnp.float32)
        + jnp.dot(normed_mix_low, full_mix_out, preferred_element_type=jnp.float32)
    )
    normed_feed, feed_back = jax.vjp(rms_scale, hidden, full_feed_gain.astype(jnp.float32))
    normed_feed_low = normed_feed.astype(jnp.bfloat16)
    gate_vals = jnp.dot(normed_feed_low, full_gate_up, preferred_element_type=jnp.float32)
    activation, act_back = jax.vjp(swiglu, gate_vals[:, :FF], gate_vals[:, FF:])
    activation_low = activation.astype(jnp.bfloat16)
    out_rows = (
        hidden + jnp.dot(activation_low, full_down, preferred_element_type=jnp.float32)
    ).astype(jnp.bfloat16)
    grad_rows = cotangent.reshape(row_count, model_width)
    grad_act = jnp.dot(grad_rows, back_down.T, preferred_element_type=jnp.float32)
    grad_gate, grad_upper = act_back(grad_act)
    grad_gu = jnp.concatenate([grad_gate, grad_upper], axis=-1).astype(jnp.bfloat16)
    grad_feed_in = jnp.dot(grad_gu, back_gate_up.T, preferred_element_type=jnp.float32)
    grad_hidden_norm, grad_feed = feed_back(grad_feed_in)
    grad_hidden = grad_rows.astype(jnp.float32) + grad_hidden_norm
    grad_hidden_low = grad_hidden.astype(jnp.bfloat16)
    grad_attended = jnp.dot(
        grad_hidden_low, back_attn_out.T, preferred_element_type=jnp.float32
    ).astype(jnp.bfloat16)
    grad_normed_mix = jnp.dot(grad_hidden_low, back_mix_out.T, preferred_element_type=jnp.float32)
    grad_mixed, grad_gate_part, grad_mix_gain = gate_back(
        grad_normed_mix.reshape(seq_count, span_len, inner_width)
    )
    heads_scale = jnp.pad(jnp.stack([rate_scale, carried]), ((0, 6), (0, 128 - SSM_HEADS)))
    operands = (
        query_rows,
        kv_window,
        window,
        own_docs[None, :],
        *recurrence,
        attended_turned,
        inverse_total,
        entering,
        grad_attended,
        grad_mixed.reshape(row_count, inner_width),
        heads_scale,
    )
    early = GradPlan(
        [normed_feed_low, activation_low, normed_mix_low, attended_turned],
        [False, False, False, True],
        [grad_gu, grad_rows, grad_hidden_low],
        [
            *column_chunks(0, 0, 2 * FF, 4),
            *column_chunks(1, 1, model_width, 2),
            *column_chunks(2, 2, model_width, 2),
            (3, 2, 0, model_width),
        ],
    )
    (grad_query, grad_kv_own, grad_active, grad_steps, grad_heads), early_sums = mix_backward(
        reach, operands, early
    )
    grad_query = grad_query.reshape(seq_count, span_len, HEADS, HEAD)
    grad_kv_own = grad_kv_own.reshape(seq_count, span_len, 2 * kv_width)
    grad_extended, grad_step_raw, grad_taps, grad_tap_bias, grad_step_bias = prep_back(
        (grad_active[None], grad_steps[None, :, :SSM_HEADS])
    )
    rim_back = shifted(grad_extended[:, :rim_rows], "grp", -1)
    grad_conv = grad_extended[:, rim_rows:] + jnp.pad(
        rim_back, ((0, 0), (span_len - rim_rows, 0), (0, 0))
    )
    grad_mix_proj = jnp.concatenate(
        [
            grad_gate_part.reshape(row_count, inner_width),
            grad_conv.reshape(row_count, xbc_width),
            grad_step_raw.reshape(row_count, SSM_HEADS),
        ],
        axis=-1,
    ).astype(jnp.bfloat16)
    grad_normed_m = jnp.dot(grad_mix_proj, back_mix_in.T, preferred_element_type=jnp.float32)
    (grad_query_raw,) = query_back(grad_query)
    (grad_key_raw,) = key_back(
        grad_kv_own[..., :kv_width].reshape(seq_count, span_len, KV_HEADS, HEAD)
    )
    grad_projected = jnp.concatenate(
        [
            grad_query_raw.reshape(row_count, query_width),
            grad_key_raw.reshape(row_count, kv_width),
            grad_kv_own[..., kv_width:].reshape(row_count, kv_width),
        ],
        axis=-1,
    ).astype(jnp.bfloat16)
    grad_normed_a = jnp.dot(grad_projected, back_attn_in.T, preferred_element_type=jnp.float32)
    grad_token_norm, grad_gain_in = norm_back(grad_normed_a + grad_normed_m)
    grad_token = grad_hidden + grad_token_norm
    heads = jnp.concatenate([grad_step_bias, grad_heads[0, :SSM_HEADS], grad_heads[1, :SSM_HEADS]])
    parts = [grad_gain_in, grad_taps.reshape(-1), grad_tap_bias, grad_mix_gain, grad_feed, heads]
    lengths = [part.shape[0] for part in parts]
    vec = jnp.concatenate(parts)
    vec = jnp.pad(vec, (0, -vec.shape[0] % 1024)).reshape(-1, 128)
    late = GradPlan(
        [normed_low],
        [False],
        [grad_mix_proj, grad_projected],
        [*column_chunks(0, 0, grad_mix_proj.shape[1], 5), (0, 1, 0, grad_projected.shape[1])],
    )
    late_sums, summed = sum_gradients(late, vec)
    summed = summed.reshape(-1)
    marks = [sum(lengths[:i]) for i in range(len(lengths) + 1)]
    sums = [summed[marks[i] : marks[i + 1]] for i in range(len(lengths))]
    index = lax.axis_index("grp")

    def own_part(value):
        size = value.shape[-1] // group_devices
        return lax.dynamic_slice_in_dim(value, index * size, size, value.ndim - 1)

    own_gate_up, own_down = shard_rows(early_sums[:4]), shard_rows(early_sums[4:6])
    own_mix_out, own_attn_out = shard_rows(early_sums[6:8]), shard_rows(early_sums[8:])
    own_mix_in, own_attn_in = shard_rows(late_sums[:-1]), shard_rows(late_sums[-1:])
    return (
        out_rows.reshape(seq_count, span_len, model_width),
        grad_token.reshape(seq_count, span_len, model_width),
        own_part(sums[0]),
        own_attn_in,
        own_attn_out,
        own_mix_in,
        own_part(sums[1].reshape(CONV, -1)),
        own_part(sums[2]),
        sums[5][:SSM_HEADS],
        sums[5][SSM_HEADS : 2 * SSM_HEADS],
        sums[5][2 * SSM_HEADS :],
        own_part(sums[3]),
        own_mix_out,
        own_part(sums[4]),
        own_gate_up,
        own_down,
    )


def solution(mesh):
    return jax.shard_map(
        shards,
        mesh=mesh,
        in_specs=(
            P("rep", "grp", None),
            P("rep", None),
            P("grp"),
            P("grp", None),
            P("grp", None),
            P("grp", None),
            P(None, "grp"),
            P("grp"),
            P(),
            P(),
            P(),
            P("grp"),
            P("grp", None),
            P("grp"),
            P("grp", None),
            P("grp", None),
            P("rep", "grp", None),
        ),
        out_specs=(
            P("rep", "grp", None),
            P("rep", "grp", None),
            P("grp"),
            P("grp", None),
            P("grp", None),
            P("grp", None),
            P(None, "grp"),
            P("grp"),
            P(),
            P(),
            P(),
            P("grp"),
            P("grp", None),
            P("grp"),
            P("grp", None),
            P("grp", None),
        ),
        check_vma=False,
    )
```

```python
import functools
import math
from functools import partial

import jax
import jax.numpy as jnp
from jax import lax
from jax.experimental import pallas as pl
from jax.experimental.pallas import tpu as pltpu
from jax.sharding import PartitionSpec as P

HEADS = 8
KV_HEADS = 2
HEAD = 64
SSM_HEADS = 24
SSM_HEAD = 64
STATE = 128
CONV = 4
FF = 2048


NORM_EPS = 1e-05
ROPE_BASE = 100000000000.0
HIGHEST = lax.Precision.HIGHEST


def shifted(value, axis, steps):
    count = lax.axis_size(axis)
    leading, last = (max(0, -steps), min(count, count - steps))
    return lax.ppermute(value, axis, [(source, source + steps) for source in range(leading, last)])


def rms_scale(values, scales):
    return values * lax.rsqrt(jnp.mean(values * values, axis=-1, keepdims=True) + NORM_EPS) * scales


def rope_tables(positions, head_width):
    indices = jnp.arange(head_width // 2, dtype=jnp.float32)
    frequency = ROPE_BASE ** (-2.0 * indices / head_width)
    angles = positions.astype(jnp.float32)[:, None] * frequency[None, :]
    return (jnp.cos(angles), jnp.sin(angles))


def rotate(values, cosine_table, sine_table):
    middle = values.shape[-1] // 2
    lower_half = values[..., :middle]
    upper_half = values[..., middle:]
    cos_rows = cosine_table[:, None, :]
    sin_rows = sine_table[:, None, :]
    return jnp.concatenate(
        [
            lower_half * cos_rows - upper_half * sin_rows,
            upper_half * cos_rows + lower_half * sin_rows,
        ],
        axis=-1,
    )


def mixer_inputs(extended, step_raw, taps, tap_bias, step_bias, seg_ext):
    span_rows = step_raw.shape[1]
    tap_count = taps.shape[0]
    own_doc = seg_ext[:, tap_count - 1 :]
    summed = jnp.zeros((extended.shape[0], span_rows, extended.shape[2]), jnp.float32) + tap_bias
    for offset in range(tap_count):
        same_doc = (seg_ext[:, offset : offset + span_rows] == own_doc)[..., None]
        summed = summed + jnp.where(
            same_doc, extended[:, offset : offset + span_rows] * taps[offset], 0.0
        )
    return jax.nn.silu(summed), jax.nn.softplus(step_raw + step_bias)


def gated_norm(mixed, gate_part, scales):
    flat_mixed = mixed.reshape(gate_part.shape)
    return rms_scale(flat_mixed * jax.nn.silu(gate_part), scales)


def swiglu(gate_vals, up_vals):
    return jax.nn.silu(gate_vals) * up_vals


MESH = pl.DeviceIdType.MESH
HIDDEN = -1e30
VMEM_LIMIT = 67043328
TAIL_LAG = 2
WINDOW = 2


def seat():
    rep, grp = lax.axis_index("rep"), lax.axis_index("grp")
    chips = lax.axis_size("grp") // 2
    quarter = lax.rem(rep, 4)
    base = rep - quarter
    flip_x = quarter + 1 - 2 * lax.rem(quarter, 2)
    flip_y = lax.rem(quarter + 2, 4)
    chip, core = lax.div(grp, 2), lax.rem(grp, 2)
    return dict(
        quarter=quarter,
        qx=flip_x,
        qy=flip_y,
        qd=lax.rem(flip_x + 2, 4),
        chip=chip,
        core=core,
        x={"rep": base + flip_x},
        y={"rep": base + flip_y},
        partner={"grp": chip * 2 + 1 - core},
        along=[{"grp": lax.rem(chip + k, chips) * 2 + core} for k in range(chips)],
        chip_to=[lax.rem(chip + k, chips) for k in range(chips)],
        chip_from=[lax.rem(chip - k + chips, chips) for k in range(chips)],
    )


def remote(source, target, sent, arrived, device):
    return pltpu.make_async_remote_copy(
        src_ref=source,
        dst_ref=target,
        send_sem=sent,
        recv_sem=arrived,
        device_id=device,
        device_id_type=MESH,
    )


def greet(me, extra=()):
    barrier = pltpu.get_barrier_semaphore()
    others = [me["x"], me["y"], me["partner"], *me["along"][1:], *extra]
    for device in others:
        pl.semaphore_signal(barrier, inc=1, device_id=device, device_id_type=MESH)
    pl.semaphore_wait(barrier, len(others))


def near_first(chips):
    return sorted(range(1, chips), key=lambda k: min(k, chips - k))


class Gather:
    def __init__(self, shards, chunks, pack):
        self.group = lax.axis_size("grp")
        self.chips = self.group // 2
        self.cut = [s.reshape(4, s.shape[0] // 4, s.shape[1]) for s in shards]
        self.chunks = chunks
        self.pack = pack

    def outs(self):
        shape = jax.ShapeDtypeStruct
        return [shape((self.group, *part.shape), part.dtype) for part in self.cut]

    def scratch(self):
        dma = pltpu.SemaphoreType.DMA
        count = len(self.chunks) + 1
        own = [pltpu.VMEM(part.shape, part.dtype) for part in self.cut]
        return [*own, *[dma((count, self.chips))] * 10, dma((len(self.cut), 2))]

    def steps(self, me, ins, pack, packs, outs, scratch):
        chips, count = self.chips, len(self.chunks)
        own_copy = scratch[: len(ins)]
        zs, zr, xs, xr, ys, yr, ds, dr, cs, cr, ls = scratch[len(ins) :]
        own = me["chip"] * 2 + me["core"]
        order = near_first(chips)
        along, over_x, over_y, diagonal, self.across = {}, {}, {}, {}, {}

        def part(m, ref):
            n, start, width = self.chunks[m]
            return ref if width == outs[n].shape[-1] else ref.at[..., start : start + width]

        def weight(m):
            return self.chunks[m][0]

        def start_along(m):
            source = part(m, ins[weight(m)].at[me["quarter"]])
            place = part(m, outs[weight(m)].at[own, me["quarter"]])
            for k in order:
                along[m, k] = remote(source, place, zs.at[m, k], zr.at[m, k], me["along"][k])
                along[m, k].start()

        def block(m, k):
            return outs[weight(m)].at[me["chip_from"][k] * 2 + me["core"]]

        for k in order:
            along[count, k] = remote(
                pack, packs.at[own], zs.at[count, k], zr.at[count, k], me["along"][k]
            )
            along[count, k].start()
        self.across[count, 0] = remote(
            pack, packs.at[own], cs.at[count, 0], cr.at[count, 0], me["partner"]
        )
        self.across[count, 0].start()
        packs[own] = pack[...]
        for m in range(min(WINDOW, count)):
            start_along(m)
        load, store = [], []
        for n in range(len(ins)):
            load.append(pltpu.make_async_copy(ins[n], own_copy[n], ls.at[n, 0]))
            load[-1].start()
        for m in range(count):
            source, place = part(m, ins[weight(m)]), part(m, outs[weight(m)].at[own])
            self.across[m, 0] = remote(source, place, cs.at[m, 0], cr.at[m, 0], me["partner"])
            self.across[m, 0].start()
        for n in range(len(ins)):
            load[n].wait()
            store.append(pltpu.make_async_copy(own_copy[n], outs[n].at[own], ls.at[n, 1]))
            store[-1].start()
        for k in order:
            along[count, k].wait_recv()
            piece = packs.at[me["chip_from"][k] * 2 + me["core"]]
            self.across[count, k] = remote(
                piece, piece, cs.at[count, k], cr.at[count, k], me["partner"]
            )
            self.across[count, k].start()
        self.store = store
        yield
        for step in range(count + 2):
            m = step
            if m < count:
                for k in order:
                    along[m, k].wait_recv()
                    piece = part(m, block(m, k).at[me["quarter"]])
                    over_x[m, k] = remote(piece, piece, xs.at[m, k], xr.at[m, k], me["x"])
                    over_y[m, k] = remote(piece, piece, ys.at[m, k], yr.at[m, k], me["y"])
                    over_x[m, k].start()
                    over_y[m, k].start()
                if m + WINDOW < count:
                    start_along(m + WINDOW)
            m = step - 1
            if 0 <= m < count:
                for k in order:
                    if (m + k) % 2 == 0:
                        over_x[m, k].wait_recv()
                        q, device = me["qx"], me["y"]
                    else:
                        over_y[m, k].wait_recv()
                        q, device = me["qy"], me["x"]
                    piece = part(m, block(m, k).at[q])
                    diagonal[m, k] = remote(piece, piece, ds.at[m, k], dr.at[m, k], device)
                    diagonal[m, k].start()
            m = step - 2
            if 0 <= m < count:
                for k in order:
                    if (m + k) % 2 == 0:
                        over_y[m, k].wait_recv()
                    else:
                        over_x[m, k].wait_recv()
                    diagonal[m, k].wait_recv()
                    piece = part(m, block(m, k))
                    self.across[m, k] = remote(
                        piece, piece, cs.at[m, k], cr.at[m, k], me["partner"]
                    )
                    self.across[m, k].start()
            yield
        self.all_copies = (along, over_x, over_y, diagonal, self.across)

    def arrive(self, m):
        for k in range(self.chips):
            self.across[m, k].wait_recv()

    def finish(self, waited):
        for m in range(len(self.chunks)):
            if m not in waited:
                self.arrive(m)
        for copies in self.all_copies:
            for copy in copies.values():
                copy.wait_send()


def f32(value):
    return value.astype(jnp.float32)


def turn_rows(source, turned, chips, piece, is_turned):
    features = source.shape[0] if is_turned else source.shape[1]
    width = math.lcm(128, piece)
    for start in range(0, features, width):
        if is_turned:
            value = f32(source[start : start + width, :])
        else:
            value = f32(source[:, start : start + width]).T
        for i in range(width // piece):
            at = start // piece + i
            chip, core, quarter = at // 8, (at // 4) % 2, at % 4
            block = value[i * piece : (i + 1) * piece].astype(jnp.bfloat16)
            turned[core, quarter, chip * piece : (chip + 1) * piece, :] = block


class GradPlan:
    def __init__(self, lefts, turned, rights, chunks):
        self.chips = lax.axis_size("grp") // 2
        self.extras = lax.axis_size("rep") // 4
        self.lefts, self.turned, self.rights, self.chunks = lefts, turned, rights, chunks
        self.tokens = rights[0].shape[0]
        sizes = [x.shape[0] if flag else x.shape[1] for x, flag in zip(lefts, turned)]
        self.rows = [size // 8 for size in sizes]
        self.piece = [size // (8 * self.chips) for size in sizes]

    def operands(self):
        return [*self.lefts, *self.rights]

    def outs(self):
        return [
            jax.ShapeDtypeStruct((4, self.piece[a], width), jnp.bfloat16)
            for a, _, _, width in self.chunks
        ]

    def scratch(self):
        low, vmem, dma = jnp.bfloat16, pltpu.VMEM, pltpu.SemaphoreType.DMA
        lefts, rights, count = len(self.lefts), len(self.rights), len(self.chunks)
        work = [vmem((2, 4, rows, self.tokens), low) for rows in self.rows]
        work += [vmem((4, rows, self.tokens), low) for rows in self.rows]
        work += [vmem(right.shape, low) for right in self.rights]
        shapes = [(self.rows[a], self.piece[a], width) for a, _, _, width in self.chunks]
        work += [vmem((4, rows, width), low) for rows, _, width in shapes]
        work += [vmem((2, rows, width), low) for rows, _, width in shapes]
        work += [vmem((rows, width), low) for rows, _, width in shapes]
        work += [vmem((self.chips, piece, width), low) for _, piece, width in shapes]
        work += [vmem((self.chips - 1, piece, width), low) for _, piece, width in shapes]
        if self.extras > 1:
            work += [vmem((self.extras, piece, width), low) for _, piece, width in shapes]
        sems = [dma((lefts,))] * 2 + [dma((rights,))] * 2
        sems += [dma((count, 2)), dma((count, 2)), dma((count,)), dma((count,))]
        sems += [dma((count, self.chips))] * 2 + [dma((count, self.extras))] * 2
        sems += [dma((count, 3))] * 2
        return [*work, *sems]

    def steps(self, me, ins, outs, scratch, lag=2):
        chips, extras, count = self.chips, self.extras, len(self.chunks)
        lefts, rights = ins[: len(self.lefts)], ins[len(self.lefts) :]
        groups = []
        for size in (len(lefts), len(lefts), len(rights), *[count] * (6 if extras > 1 else 5)):
            groups.append(scratch[:size])
            scratch = scratch[size:]
        turned, turned_in, rights_in, parts, one, two, total, slots = groups[:8]
        extra_in = groups[8] if extras > 1 else ()
        la_s, la_r, ri_s, ri_r, s1, r1, s2, r2, zs, zr, es, er, gs, gr = scratch
        core = me["core"]
        reps, rep = lax.axis_size("rep"), lax.axis_index("rep")
        beyond = [{"rep": lax.rem(rep + 4 * e, reps)} for e in range(1, extras)]
        swap_left, swap_right = {}, {}
        for n in range(len(rights)):
            swap_right[n] = remote(rights[n], rights_in[n], ri_s.at[n], ri_r.at[n], me["partner"])
            swap_right[n].start()
        for n in range(len(lefts)):
            turn_rows(lefts[n], turned[n], chips, self.piece[n], self.turned[n])
            swap_left[n] = remote(
                turned[n].at[1 - core], turned_in[n], la_s.at[n], la_r.at[n], me["partner"]
            )
            if n > 0:
                swap_left[n - 1].start()
            yield
        swap_left[len(lefts) - 1].start()
        have = set()
        first, second, along, other, spread = {}, {}, {}, {}, {}

        def form(m):
            a, b, start, width = self.chunks[m]
            for key, copy in (("left", a), swap_left[a]), (("right", b), swap_right[b]):
                if key not in have:
                    have.add(key)
                    copy.wait_recv()
            at = slice(start, start + width)

            def quarter(q, _):
                value = dot_plain(turned[a][core, q], rights[b][:, at])
                value = value + dot_plain(turned_in[a][q], rights_in[b][:, at])
                parts[m][q] = value.astype(jnp.bfloat16)
                return 0

            lax.fori_loop(0, 4, quarter, 0)

        def send_first(m):
            device, mine = (me["x"], me["qx"]) if m % 2 == 0 else (me["y"], me["qy"])
            for i, q in ((1, me["qd"]), (0, mine)):
                first[m, i] = remote(
                    parts[m].at[q], one[m].at[i], s1.at[m, i], r1.at[m, i], device
                )
                first[m, i].start()

        def send_second(m):
            rows = self.rows[self.chunks[m][0]]
            device, q = (me["y"], me["qy"]) if m % 2 == 0 else (me["x"], me["qx"])
            first[m, 1].wait_recv()

            def add(j, _):
                at = pl.ds(pl.multiple_of(j * 64, 64), 64)
                value = f32(parts[m][q, at, :]) + f32(one[m][1, at, :])
                parts[m][q, at, :] = value.astype(jnp.bfloat16)
                return 0

            lax.fori_loop(0, rows // 64, add, 0)
            second[m] = remote(parts[m].at[q], two[m], s2.at[m], r2.at[m], device)
            second[m].start()

        def send_along(m):
            piece = self.piece[self.chunks[m][0]]
            first[m, 0].wait_recv()
            second[m].wait_recv()
            for j in range(chips):
                at = slice(j * piece, (j + 1) * piece)
                value = f32(parts[m][me["quarter"], at, :]) + f32(one[m][0, at, :]) + f32(two[m][at, :])
                total[m][j] = value.astype(jnp.bfloat16)
            for k in near_first(chips):
                along[m, k] = remote(
                    total[m].at[me["chip_to"][k]],
                    slots[m].at[k - 1],
                    zs.at[m, k],
                    zr.at[m, k],
                    me["along"][k],
                )
                along[m, k].start()

        def send_spread(m):
            value = f32(total[m][me["chip"]])
            for k in near_first(chips):
                along[m, k].wait_recv()
                value = value + f32(slots[m][k - 1])
            if extras > 1:
                extra_in[m][0] = value.astype(jnp.bfloat16)
                for e in range(1, extras):
                    other[m, e] = remote(
                        extra_in[m].at[0],
                        extra_in[m].at[e],
                        es.at[m, e],
                        er.at[m, e],
                        beyond[e - 1],
                    )
                    other[m, e].start()
                for e in range(1, extras):
                    other[m, e].wait_recv()
                    value = value + f32(extra_in[m][e])
            outs[m][me["quarter"]] = value.astype(jnp.bfloat16)
            piece = outs[m].at[me["quarter"]]
            for i, device in enumerate((me["x"], me["y"])):
                spread[m, i] = remote(piece, piece, gs.at[m, i], gr.at[m, i], device)
                spread[m, i].start()

        def send_diagonal(m):
            way = m % 2
            spread[m, way].wait_recv()
            q, device = (me["qx"], me["y"]) if way == 0 else (me["qy"], me["x"])
            piece = outs[m].at[q]
            spread[m, 2] = remote(piece, piece, gs.at[m, 2], gr.at[m, 2], device)
            spread[m, 2].start()

        stages = (send_second, send_along, send_spread, send_diagonal)
        for step in range(count + lag * len(stages)):
            if step < count:
                form(step)
                send_first(step)
            for n, stage in enumerate(stages):
                m = step - lag * (n + 1)
                if 0 <= m < count:
                    stage(m)
            yield
        for m in range(count):
            spread[m, 1 - m % 2].wait_recv()
            spread[m, 2].wait_recv()
        for copies in (swap_left, swap_right, first, second, along, other, spread):
            for copy in copies.values():
                copy.wait_send()
        yield


def small_steps(me, chips, extras, vec, out, stage, slots, sems, more):
    ss, sr, zs, zr = sems
    copies = []
    value = vec[...]
    hops = [me["x"], me["y"], me["partner"]]
    for i, device in enumerate(hops):
        stage[i] = value
        copies.append(remote(stage.at[i], slots.at[i], ss.at[i], sr.at[i], device))
        copies[-1].start()
        yield
        copies[-1].wait_recv()
        value = value + slots[i]
    if extras > 1:
        stage[3] = value
        for e in range(1, extras):
            at = 3 + chips + e
            copies.append(remote(stage.at[3], slots.at[at], ss.at[2 + e], sr.at[2 + e], more[e - 1]))
            copies[-1].start()
        yield
        for e in range(1, extras):
            copies[-e].wait_recv()
        for e in range(1, extras):
            value = value + slots[3 + chips + e]
    stage[4] = value
    along = []
    for k in near_first(chips):
        along.append(remote(stage.at[4], slots.at[3 + k], zs.at[k], zr.at[k], me["along"][k]))
        along[-1].start()
    yield
    for copy in along:
        copy.wait_recv()
    for k in range(1, chips):
        value = value + slots[3 + k]
    out[...] = value
    for copy in copies + along:
        copy.wait_send()
    yield


def run_out(steps):
    for _ in steps:
        pass


def tail_kernel(plan, *refs):
    cut = (len(plan.operands()), 1, len(plan.chunks), 1)
    groups = []
    for size in cut:
        groups.append(refs[:size])
        refs = refs[size:]
    (vec,), (total,) = groups[1], groups[3]
    stage, slots = refs[-6:-4]
    me = seat()
    rep, reps = lax.axis_index("rep"), lax.axis_size("rep")
    beyond = [{"rep": lax.rem(rep + 4 * e, reps)} for e in range(1, plan.extras)]
    greet(me, beyond)
    large = plan.steps(me, groups[0], groups[2], refs[:-6], lag=TAIL_LAG)
    small = small_steps(me, plan.chips, plan.extras, vec, total, stage, slots, refs[-4:], beyond)
    for _ in small:
        next(large, None)
    run_out(large)


def sum_gradients(plan, vec):
    dma = pltpu.SemaphoreType.DMA
    chips, extras = plan.chips, plan.extras
    small = [
        pltpu.VMEM((5, *vec.shape), vec.dtype),
        pltpu.VMEM((3 + chips + extras, *vec.shape), vec.dtype),
    ]
    small += [dma((2 + extras,)), dma((2 + extras,)), dma((chips,)), dma((chips,))]
    count = len(plan.chunks)
    *sums, total = pl.pallas_call(
        functools.partial(tail_kernel, plan),
        out_shape=[*plan.outs(), jax.ShapeDtypeStruct(vec.shape, vec.dtype)],
        in_specs=[pl.BlockSpec(memory_space=pltpu.VMEM)] * (len(plan.operands()) + 1),
        out_specs=[pl.BlockSpec(memory_space=pltpu.VMEM)] * (count + 1),
        scratch_shapes=[*plan.scratch(), *small],
        compiler_params=pltpu.CompilerParams(
            collective_id=1, has_side_effects=True, vmem_limit_bytes=VMEM_LIMIT
        ),
        name="sum_gradients",
    )(*plan.operands(), vec)
    return sums, total


def shard_rows(totals):
    wide = [total.reshape(-1, total.shape[-1]) for total in totals]
    return jnp.concatenate(wide, axis=1).astype(jnp.float32)


def column_chunks(left, right, columns, pieces):
    width = columns // pieces // 128 * 128
    starts = [i * width for i in range(pieces)] + [columns]
    return [(left, right, low, high - low) for low, high in zip(starts, starts[1:])]


def axis_seat():
    grp = lax.axis_index("grp")
    return lax.div(grp, 2), lax.rem(grp, 2)


def greet_group(extra=()):
    size, grp = lax.axis_size("grp"), lax.axis_index("grp")
    barrier = pltpu.get_barrier_semaphore()
    others = [{"grp": lax.rem(grp + k, size)} for k in range(1, size)] + list(extra)
    for device in others:
        pl.semaphore_signal(barrier, inc=1, device_id=device, device_id_type=MESH)
    pl.semaphore_wait(barrier, len(others))


def lanes(shape):
    return lax.broadcasted_iota(jnp.int32, shape, len(shape) - 1)


def pair_columns(columns, pair):
    rows = columns.shape[0]
    low = jnp.broadcast_to(columns[:, 2 * pair : 2 * pair + 1], (rows, 128))
    high = jnp.broadcast_to(columns[:, 2 * pair + 1 : 2 * pair + 2], (rows, 128))
    return jnp.where(lanes((rows, 128)) < 64, low, high)


def dot_rows(left, right):
    return lax.dot_general(
        left, right, (((1,), (1,)), ((), ())), preferred_element_type=jnp.float32
    )


def dot_plain(left, right):
    return jnp.dot(left, right, preferred_element_type=jnp.float32)


def align_heads(source, target, scale):
    for pair in range(HEADS // 2):
        both = source[:, pair * 128 : (pair + 1) * 128].astype(jnp.float32) * scale
        swapped = pltpu.roll(both, 64, 1)
        for odd in range(2):
            head = 2 * pair + odd
            group = head // (HEADS // KV_HEADS)
            value = both if odd == group else swapped
            keep = lanes(value.shape) // 64 == group
            target[head] = jnp.where(keep, value, 0.0).astype(jnp.bfloat16)


def slot_plan(reach):
    return [(0, 0)] + [(k, core) for k in range(1, reach + 1) for core in (1, 0)]


def slot_live(slot, chip, core, reach):
    back, side = slot
    if back == 0:
        return core == 1
    live = chip - back >= 0
    if back == reach and side == 0:
        live = jnp.logical_and(live, core == 0)
    return live


def same_document(key_column, query_row, causal):
    size = query_row.shape[-1]
    allowed = across(key_column, size) == query_row
    if causal:
        rows = lax.broadcasted_iota(jnp.int32, (size, size), 0)
        allowed = jnp.logical_and(allowed, rows <= lanes((size, size)))
    return jnp.where(allowed, 0.0, HIDDEN)


def across(column, width):
    return jnp.concatenate([column] * (width // 128), axis=1)


def forward_kernel(reach, gather, *refs):
    chips, many = gather.chips, len(gather.cut)
    groups = []
    for size in (6, many, 21, many, 41):
        groups.append(refs[:size])
        refs = refs[size:]
    (
        tokens_ref,
        pack,
        docs_ref,
        heads_ref,
        cosine_ref,
        sine_ref,
    ) = groups[0]
    shards = groups[1]
    (
        normed_ref,
        q_ref,
        gate_ref,
        ext_ref,
        act_ref,
        step_ref,
        dt_ref,
        run_ref,
        runt_ref,
        e_ref,
        wd_ref,
        car_ref,
        carried_ref,
        att_ref,
        attt_ref,
        inv_ref,
        mixed_ref,
        ent_ref,
        kvw_ref,
        segk_ref,
        packs,
    ) = groups[2]
    fulls = groups[3]
    (
        kv_ref,
        attention_w,
        mixer_w,
        rim_out,
        rim_in,
        seg_ext,
        same,
        taps,
        skip_lanes,
        qa,
        bias,
        vt,
        ot,
        total,
        xdt,
        xw,
        runb,
        gram,
        own_state,
        half_out,
        half_in,
        car_in,
        chip_out,
        chip_car,
        chip_in,
        chip_car_in,
        enter_out,
        acc,
        fetch_sem,
        rim_s,
        rim_r,
        ka_s,
        ka_r,
        kp_s,
        kp_r,
        ha_s,
        ha_r,
        ca_s,
        ca_r,
        en_s,
        en_r,
    ) = groups[4]
    travel = refs
    chip, core = axis_seat()
    grp = lax.axis_index("grp")
    span = tokens_ref.shape[0]
    inner = SSM_HEADS * SSM_HEAD
    half = inner // 2
    partner = {"grp": chip * 2 + 1 - core}

    def ahead(k):
        return {"grp": lax.rem(grp + 2 * k, 2 * chips)}

    me = seat()
    greet_group([me["x"], me["y"]])
    gathering = gather.steps(me, shards, pack, packs, fulls, travel)

    def tick():
        next(gathering, None)

    tick()
    for i in range(2 * (reach + 1)):
        segk_ref[i] = jnp.broadcast_to(docs_ref[i], (128, span)).T
    own_row = docs_ref[2 * reach + core]
    own_docs = segk_ref[2 * reach + core]
    seg_ext[8:, :] = own_docs
    seg_ext[0:8, :] = segk_ref[2 * reach + core - 1][span - 8 :]
    prior, tail = seg_ext[7:8, :], own_docs[span - 1 :]
    for j in range(CONV - 1):
        same[j] = jnp.where(seg_ext[5 + j : 5 + j + span, :] == own_docs, 1.0, 0.0)

    for k in range(chips):
        gather.across[len(gather.chunks), k].wait_recv()

    def whole_rows(width):
        total = width * 2 * chips
        rows = lax.broadcasted_iota(jnp.int32, (pack.shape[1], total), 0)
        value = jnp.zeros((8, total), jnp.float32)
        for i in range(2 * chips):
            here = jnp.logical_and(lanes(rows.shape) == rows + width * i, rows < width)
            value = value + dot_plain(packs[i], jnp.where(here, 1.0, 0.0).astype(jnp.bfloat16))
        return value

    taps[...] = whole_rows(taps.shape[1] // (2 * chips))
    gain = whole_rows(tokens_ref.shape[1] // (2 * chips))[5:6]

    def norm(i, _):
        at = pl.ds(pl.multiple_of(i * 64, 64), 64)
        value = f32(tokens_ref[at, :])
        scale = lax.rsqrt(jnp.mean(value * value, axis=-1, keepdims=True) + NORM_EPS)
        normed_ref[at, :] = (value * scale * gain).astype(jnp.bfloat16)
        return 0

    lax.fori_loop(0, span // 64, norm, 0)
    for pair in range(SSM_HEADS // 2):
        at = slice(pair * 128, (pair + 1) * 128)
        skip_lanes[:, at] = pair_columns(jnp.broadcast_to(heads_ref[2:3], (8, 128)), pair)

    for _ in range(3):
        tick()
    gather.arrive(0)
    waited = {0}
    fetch = pltpu.make_async_copy(fulls[0], attention_w, fetch_sem.at[0])
    gather.store[0].wait()
    fetch.start()
    tick()
    fetch.wait()
    width = tokens_ref.shape[1]
    low_half = lanes((span, 128)) % HEAD < HEAD // 2

    def turned(value):
        other = jnp.where(low_half, pltpu.roll(value, 128 - HEAD // 2, 1), pltpu.roll(value, HEAD // 2, 1))
        return value * cosine_ref[...] + other * sine_ref[...]

    for j in range(3):
        part = attention_w[:, :, :, j * 256 : (j + 1) * 256].reshape(width, 256)
        value = dot_plain(normed_ref[...], part)
        one, two = value[:, 0:128], value[:, 128:256]
        if j < 2:
            q_ref[:, j * 256 : j * 256 + 128] = turned(one).astype(jnp.bfloat16)
            q_ref[:, j * 256 + 128 : (j + 1) * 256] = turned(two).astype(jnp.bfloat16)
        else:
            kv_ref[:, 0:128] = turned(one).astype(jnp.bfloat16)
            kv_ref[:, 128:256] = two.astype(jnp.bfloat16)

    tick()
    for m in (1, 2):
        gather.arrive(m)
        waited.add(m)
    fetch = pltpu.make_async_copy(fulls[1], mixer_w, fetch_sem.at[1])
    gather.store[1].wait()
    fetch.start()
    fetch.wait()

    def project(at):
        return dot_plain(normed_ref[...], mixer_w[:, :, :, at].reshape(width, -1))

    conv_width = inner + 2 * STATE
    rest = inner + conv_width

    def conv_block(j, _):
        value = project(pl.ds(pl.multiple_of(inner + j * 256, 256), 256)).astype(jnp.bfloat16)
        at = pl.ds(pl.multiple_of(j * 256, 256), 256)
        ext_ref[8:, at] = f32(value)
        rim_out[:, at] = value[span - 16 :]
        return 0

    lax.fori_loop(0, conv_width // 256, conv_block, 0)
    step_ref[...] = jnp.zeros_like(step_ref)
    step_ref[:, 0:SSM_HEADS] = project(slice(rest, rest + SSM_HEADS))
    rim = remote(rim_out, rim_in, rim_s, rim_r, {"grp": lax.rem(grp + 1, 2 * chips)})
    pl.when(grp + 1 < 2 * chips)(rim.start)

    def gate_block(j, _):
        at = pl.ds(pl.multiple_of(j * 256, 256), 256)
        gate_ref[:, at] = project(at)
        return 0

    lax.fori_loop(0, inner // 256, gate_block, 0)

    raw = step_ref[...] + heads_ref[0:1]
    dt_ref[...] = jnp.maximum(raw, 0.0) + jnp.log1p(jnp.exp(-jnp.abs(raw)))
    before = lax.broadcasted_iota(jnp.int32, (span, span), 0) >= lanes((span, span))
    running = lax.dot_general(
        jnp.where(before, 1.0, 0.0), dt_ref[...] * -jnp.exp(heads_ref[1:2]), (((1,), (0,)), ((), ())),
        precision=HIGHEST, preferred_element_type=jnp.float32,
    )
    run_ref[...] = running
    turned_run = running.T
    for head in range(SSM_HEADS):
        runt_ref[head] = turned_run[head : head + 1]
    final = running[span - 1 :]
    e_ref[...] = jnp.where(own_docs == prior, jnp.exp(running), 0.0)
    wd_ref[...] = jnp.where(own_docs == tail, jnp.exp(final - running), 0.0)
    carried = jnp.where(tail == prior, jnp.exp(final), 0.0)
    carried_ref[...] = jnp.broadcast_to(carried, (8, 128))
    for pair in range(SSM_HEADS // 2):
        at = pair * 128 % half
        car_ref[pair * 128 // half, :, at : at + 128] = pair_columns(carried_ref, pair)

    def rim_none():
        ext_ref[0:8, :] = jnp.zeros((8, conv_width), jnp.float32)

    def rim_some():
        rim.wait_recv()
        ext_ref[0:8, :] = f32(rim_in[8:16, :])

    pl.when(grp == 0)(rim_none)
    pl.when(grp > 0)(rim_some)

    def convolve(j, _):
        at = pl.ds(pl.multiple_of(j * 256, 256), 256)
        value = jnp.broadcast_to(taps[CONV : CONV + 1, at], (span, 256))
        for tap in range(CONV):
            term = ext_ref[5 + tap : 5 + tap + span, at] * taps[tap : tap + 1, at]
            if tap < CONV - 1:
                term = jnp.where(across(same[tap], 256) > 0.0, term, 0.0)
            value = value + term
        act_ref[:, at] = value / (1.0 + jnp.exp(-value))
        return 0

    lax.fori_loop(0, conv_width // 256, convolve, 0)
    tick()
    own_kv = remote(kv_ref, kvw_ref.at[0, core], kp_s.at[0], kp_r.at[0], partner)
    own_kv.start()
    kv_along = {}
    for k in range(1, reach + 1):
        kv_along[k] = remote(kv_ref, kvw_ref.at[k, core], ka_s.at[k], ka_r.at[k], ahead(k))
        pl.when(chip + k < chips)(kv_along[k].start)
    kvw_ref[0, core] = kv_ref[...]

    weight = wd_ref[...] * dt_ref[...]
    for pair in range(SSM_HEADS // 2):
        at = slice(pair * 128, (pair + 1) * 128)
        x_pair = act_ref[:, at]
        xdt[:, at] = (x_pair * pair_columns(dt_ref, pair)).astype(jnp.bfloat16)
        xw[:, at] = (x_pair * pair_columns(weight, pair)).astype(jnp.bfloat16)
    in_map = act_ref[:, inner : inner + STATE]
    out_map = act_ref[:, inner + STATE :]
    out_low = out_map.astype(jnp.bfloat16)
    in_turned = in_map.T.astype(jnp.bfloat16)
    for i in range(2):
        own_state[i] = dot_plain(in_turned, xw[:, i * half : (i + 1) * half])
    half_out[...] = own_state[1 - core].astype(jnp.bfloat16)
    align_heads(q_ref, qa, HEAD**-0.5)
    ot[...] = jnp.zeros_like(ot)
    total[...] = jnp.zeros_like(total)
    half_car = remote(car_ref.at[1 - core], car_in, ha_s.at[0], ha_r.at[0], partner)
    half_state = remote(half_out, half_in, ha_s.at[1], ha_r.at[1], partner)
    half_car.start()
    half_state.start()

    def attend_slot(keys, values, key_docs, causal):
        bias[...] = same_document(key_docs, own_row, causal)
        vt[...] = values.astype(jnp.float32).T.astype(jnp.bfloat16)

        def per_head(head, _):
            group = lax.div(head, HEADS // KV_HEADS)
            scores = dot_rows(keys[...], qa[head]) + bias[...]
            weights = jnp.exp(scores)
            total[head] += jnp.sum(weights, axis=0, keepdims=True)
            rows = pl.ds(pl.multiple_of(group * HEAD, HEAD), HEAD)
            into = pl.ds(pl.multiple_of(head * HEAD, HEAD), HEAD)
            ot[into, :] += dot_plain(vt[rows, :], weights.astype(jnp.bfloat16))
            return 0

        lax.fori_loop(0, HEADS, per_head, 0)

    def attend_ref(ref, key_docs, causal):
        attend_slot(ref.at[:, 0:128], ref[:, 128:256], key_docs, causal)

    attend_ref(kv_ref, segk_ref[2 * reach + core], True)
    tick()

    half_car.wait_recv()
    half_state.wait_recv()
    mine, theirs = own_state[core], half_in[...].astype(jnp.float32)
    car_mine, car_theirs = car_ref[core], car_in[...]
    first = core == 0
    car_0 = jnp.where(first, car_mine, car_theirs)
    car_1 = jnp.where(first, car_theirs, car_mine)
    state_0 = jnp.where(first, mine, theirs)
    state_1 = jnp.where(first, theirs, mine)
    chip_out[...] = (state_1 + car_1[0:1] * state_0).astype(jnp.bfloat16)
    chip_car[...] = car_0 * car_1

    for head in range(SSM_HEADS):
        runb[head] = jnp.broadcast_to(run_ref[:, head : head + 1], (span, 128))
    gram[...] = lax.dot_general(
        out_map, in_map, (((1,), (1,)), ((), ())), precision=HIGHEST,
        preferred_element_type=jnp.float32,
    )
    state_along = {}
    for k in range(1, reach + 1):
        state_along[k] = (
            remote(chip_out, chip_in.at[k], ca_s.at[k, 0], ca_r.at[k, 0], ahead(k)),
            remote(chip_car, chip_car_in.at[k], ca_s.at[k, 1], ca_r.at[k, 1], ahead(k)),
        )
        for copy in state_along[k]:
            pl.when(chip + k < chips)(copy.start)

    kv_pass = {}
    for k in range(1, reach + 1):
        place = kvw_ref.at[k, core]
        kv_pass[k] = remote(place, place, kp_s.at[k], kp_r.at[k], partner)

        def hand_on(k=k):
            kv_along[k].wait_recv()
            kv_pass[k].start()

        pl.when(chip - k >= 0)(hand_on)

    rows = lax.broadcasted_iota(jnp.int32, (span, span), 0)
    allowed = jnp.logical_and(
        across(segk_ref[2 * reach + core], span) == own_row, rows >= lanes((span, span))
    )
    bias[...] = jnp.where(allowed, 0.0, HIDDEN)

    def intra(quad, _):
        at = pl.ds(pl.multiple_of(quad * 256, 256), 256)
        value = jnp.zeros((span, 256), jnp.float32)
        for i in range(4):
            head = quad * 4 + i
            column = runb[head]
            spread = jnp.concatenate([column] * (span // 128), axis=1) - runt_ref[head]
            mixing = (jnp.exp(spread + bias[...]) * gram[...]).astype(jnp.bfloat16)
            part = dot_plain(mixing, xdt[:, at])
            value = jnp.where(lanes((span, 256)) // 64 == i, part, value)
        mixed_ref[:, at] = value + skip_lanes[0:1, at] * act_ref[:, at]
        return 0

    lax.fori_loop(0, SSM_HEADS // 4, intra, 0)
    tick()

    own_kv.wait_recv()
    for index, slot in enumerate(slot_plan(reach)):
        back, side = slot
        if slot == (1, 1):
            acc[...] = jnp.zeros_like(acc)
            for k in range(reach, 0, -1):

                def take(k=k):
                    for copy in state_along[k]:
                        copy.wait_recv()
                    acc[...] = chip_in[k].astype(jnp.float32) + chip_car_in[k, 0:1] * acc[...]

                pl.when(chip - k >= 0)(take)
            enter_0, enter_1 = acc[...], state_0 + car_0[0:1] * acc[...]
            ent_ref[core] = jnp.where(first, enter_0, enter_1)
            enter_out[...] = jnp.where(first, enter_1, enter_0)
            for k in range(1, reach + 1):
                pl.when(chip - k >= 0)(kv_pass[k].wait_recv)

        def visit(back=back, side=side):
            ref = kvw_ref.at[back, side]
            attend_ref(ref, segk_ref[2 * (reach - back) + side], False)

        pl.when(slot_live(slot, chip, core, reach))(visit)
        tick()
        if slot == (1, 1):
            enter_pass = remote(enter_out, ent_ref.at[core], en_s, en_r, partner)
            enter_pass.start()

    for head in range(HEADS):
        inverse = 1.0 / total[head]
        inv_ref[head] = inverse
        into = slice(head * HEAD, (head + 1) * HEAD)
        ot[into, :] = ot[into, :] * inverse
    attt_ref[...] = ot[...].astype(jnp.bfloat16)
    for pair in range(HEADS // 2):
        at = slice(pair * 128, (pair + 1) * 128)
        att_ref[:, at] = ot[at, :].T.astype(jnp.bfloat16)

    enter_pass.wait_recv()
    for i in range(2):
        carried_in = dot_plain(out_low, ent_ref[i].astype(jnp.bfloat16))
        for j in range(SSM_HEADS // 4):
            pair = i * (SSM_HEADS // 4) + j
            at = slice(pair * 128, (pair + 1) * 128)
            part = carried_in[:, j * 128 : (j + 1) * 128]
            mixed_ref[:, at] += pair_columns(e_ref, pair) * part

    run_out(gathering)
    gather.finish(waited)
    for copy in gather.store[2:]:
        copy.wait()
    own_kv.wait_send()
    pl.when(grp + 1 < 2 * chips)(rim.wait_send)
    half_car.wait_send()
    half_state.wait_send()
    enter_pass.wait_send()
    for k in range(1, reach + 1):

        def sent(k=k):
            kv_along[k].wait_send()
            for copy in state_along[k]:
                copy.wait_send()

        pl.when(chip + k < chips)(sent)
        pl.when(chip - k >= 0)(kv_pass[k].wait_send)


def run_forward(reach, gather, tokens, docs, heads, cosine, sine):
    chips, group = gather.chips, gather.group
    span, width = tokens.shape
    inner = SSM_HEADS * SSM_HEAD
    half, conv_width = inner // 2, inner + 2 * STATE
    kv_width = 2 * KV_HEADS * HEAD
    f32, low = jnp.float32, jnp.bfloat16
    shape = jax.ShapeDtypeStruct
    dma = pltpu.SemaphoreType.DMA
    vmem = pltpu.VMEM
    column = shape((span, 128), f32)
    outs = [
        shape((span, width), low),
        shape((span, HEADS * HEAD), low),
        shape((span, inner), f32),
        shape((span + 8, conv_width), f32),
        shape((span, conv_width), f32),
        column,
        column,
        column,
        shape((SSM_HEADS, 1, span), f32),
        column,
        column,
        shape((2, 8, half), f32),
        shape((8, 128), f32),
        shape((span, HEADS * HEAD), low),
        shape((HEADS * HEAD, span), low),
        shape((HEADS, 1, span), f32),
        shape((span, inner), f32),
        shape((2, STATE, half), f32),
        shape((reach + 1, 2, span, kv_width), low),
        shape((2 * (reach + 1), span, 128), f32),
        shape((group, *gather.pack.shape), low),
    ]
    scratch = [
        vmem((span, kv_width), low),
        vmem((group, *gather.cut[0].shape), low),
        vmem((group, *gather.cut[1].shape), low),
        vmem((16, conv_width), low),
        vmem((16, conv_width), low),
        vmem((span + 8, 128), f32),
        vmem((CONV - 1, span, 128), f32),
        vmem((8, conv_width), f32),
        vmem((8, inner), f32),
        vmem((HEADS, span, 128), low),
        vmem((span, span), f32),
        vmem((128, span), low),
        vmem((HEADS * HEAD, span), f32),
        vmem((HEADS, 1, span), f32),
        vmem((span, inner), low),
        vmem((span, inner), low),
        vmem((SSM_HEADS, span, 128), f32),
        vmem((span, span), f32),
        vmem((2, STATE, half), f32),
        vmem((STATE, half), low),
        vmem((STATE, half), low),
        vmem((8, half), f32),
        vmem((STATE, half), low),
        vmem((8, half), f32),
        vmem((reach + 1, STATE, half), low),
        vmem((reach + 1, 8, half), f32),
        vmem((STATE, half), f32),
        vmem((STATE, half), f32),
        dma((2,)),
        dma,
        dma,
        dma((reach + 1,)),
        dma((reach + 1,)),
        dma((reach + 1,)),
        dma((reach + 1,)),
        dma((2,)),
        dma((2,)),
        dma((reach + 1, 2)),
        dma((reach + 1, 2)),
        dma,
        dma,
    ]
    vm, anywhere = pl.BlockSpec(memory_space=pltpu.VMEM), pl.BlockSpec(memory_space=pl.ANY)
    many = len(gather.cut)
    results = pl.pallas_call(
        functools.partial(forward_kernel, reach, gather),
        out_shape=[*outs, *gather.outs()],
        in_specs=[vm] * 6 + [anywhere] * many,
        out_specs=[vm] * len(outs) + [anywhere] * many,
        scratch_shapes=[*scratch, *gather.scratch()],
        compiler_params=pltpu.CompilerParams(
            collective_id=2, has_side_effects=True, vmem_limit_bytes=VMEM_LIMIT
        ),
        name="run_forward",
    )(tokens, gather.pack, docs, heads, cosine, sine, *gather.cut)
    full = [part.reshape(-1, part.shape[-1]) for part in results[len(outs) :]]
    return results[: len(outs)], full


def mix_backward_kernel(reach, plan, *refs):
    chips, extras = plan.chips, plan.extras
    many = len(plan.chunks)
    cut = [18, len(plan.operands()), 5, many, 44]
    groups = []
    for size in cut:
        groups.append(refs[:size])
        refs = refs[size:]
    (
        q_ref,
        kvw_ref,
        segc_ref,
        segr_ref,
        act_ref,
        dt_ref,
        run_ref,
        runt_ref,
        e_ref,
        wd_ref,
        car_ref,
        skip_ref,
        attt_ref,
        inv_ref,
        ent_ref,
        gout_ref,
        gmix_ref,
        rate_ref,
    ) = groups[0]
    (
        dq_ref,
        dkv_ref,
        dact_ref,
        ddt_ref,
        heads_ref,
    ) = groups[2]
    (
        qa,
        da,
        bias,
        kt,
        dqt,
        centre,
        dk,
        dv,
        part_out,
        part_in,
        sum_out,
        sum_in,
        xdt,
        xw,
        ge,
        runb,
        gramt,
        dgram,
        own_grad,
        half_out,
        half_in,
        car_in,
        chip_out,
        chip_car,
        chip_in,
        chip_car_in,
        later_out,
        later,
        acc,
        qrow,
        qcol,
        dxdt,
        sums,
        fold_ref,
        pp_s,
        pp_r,
        pa_s,
        pa_r,
        ha_s,
        ha_r,
        ca_s,
        ca_r,
        la_s,
        la_r,
    ) = groups[4]
    me = seat()
    rep, reps = lax.axis_index("rep"), lax.axis_size("rep")
    beyond = [{"rep": lax.rem(rep + 4 * e, reps)} for e in range(1, extras)]
    reduction = plan.steps(me, groups[1], groups[3], refs)
    chip, core = axis_seat()
    grp = lax.axis_index("grp")
    span = q_ref.shape[0]
    inner = SSM_HEADS * SSM_HEAD
    half = inner // 2
    low = jnp.bfloat16
    partner = {"grp": chip * 2 + 1 - core}
    first = core == 0

    def behind(k):
        return {"grp": lax.rem(grp - 2 * k + 2 * chips, 2 * chips)}

    greet_group([me["x"], me["y"], *beyond])
    next(reduction)
    in_map = act_ref[:, inner : inner + STATE]
    out_map = act_ref[:, inner + STATE :]
    in_low, out_low = in_map.astype(low), out_map.astype(low)
    weight = wd_ref[...] * dt_ref[...]
    for pair in range(SSM_HEADS // 2):
        at = slice(pair * 128, (pair + 1) * 128)
        x_pair = act_ref[:, at]
        ge[:, at] = (gmix_ref[:, at] * pair_columns(e_ref, pair)).astype(low)
        xdt[:, at] = (x_pair * pair_columns(dt_ref, pair)).astype(low)
        xw[:, at] = (x_pair * pair_columns(weight, pair)).astype(low)
    out_turned = out_map.T.astype(low)
    for i in range(2):
        own_grad[i] = dot_plain(out_turned, ge[:, i * half : (i + 1) * half])
    half_out[...] = own_grad[1 - core].astype(low)
    align_heads(q_ref, qa, HEAD**-0.5)
    align_heads(gout_ref, da, 1.0)
    half_car = remote(car_ref.at[1 - core], car_in, ha_s.at[0], ha_r.at[0], partner)
    half_grad = remote(half_out, half_in, ha_s.at[1], ha_r.at[1], partner)
    half_car.start()
    half_grad.start()

    next(reduction, None)
    for pair in range(HEADS // 2):
        at = slice(pair * 128, (pair + 1) * 128)
        product = gout_ref[:, at].astype(jnp.float32).T * attt_ref[at, :].astype(jnp.float32)
        for odd in range(2):
            rows = product[odd * HEAD : (odd + 1) * HEAD]
            centre[2 * pair + odd] = jnp.sum(rows, axis=0, keepdims=True)
    dqt[...] = jnp.zeros_like(dqt)

    def attend_back(ref, key_docs, causal):
        bias[...] = same_document(key_docs, segr_ref[...], causal)
        kt[...] = ref[:, 0:128].astype(jnp.float32).T.astype(low)
        dk[...] = jnp.zeros_like(dk)
        dv[...] = jnp.zeros_like(dv)

        def per_head(head, _):
            group = lax.div(head, HEADS // KV_HEADS)
            scores = dot_rows(ref[:, 0:128], qa[head]) + bias[...]
            probs = jnp.exp(scores) * inv_ref[head]
            grad_probs = dot_rows(ref[:, 128:256], da[head])
            grad_scores = (probs * (grad_probs - centre[head])).astype(low)
            dv[...] += dot_plain(probs.astype(low), da[head])
            dk[...] += dot_plain(grad_scores, qa[head])
            rows = pl.ds(pl.multiple_of(group * HEAD, HEAD), HEAD)
            into = pl.ds(pl.multiple_of(head * HEAD, HEAD), HEAD)
            dqt[into, :] += dot_plain(kt[rows, :], grad_scores)
            return 0

        lax.fori_loop(0, HEADS // 2, per_head, 0)
        lax.fori_loop(HEADS // 2, HEADS, per_head, 0)

    passed, sent_on = {}, {}

    def pass_slot(back, side):
        live = slot_live((back, side), chip, core, reach)

        def compute():
            attend_back(kvw_ref.at[back, side], segc_ref[2 * (reach - back) + side], False)
            part_out[back, side, :, 0:128] = dk[...].astype(low)
            part_out[back, side, :, 128:256] = dv[...].astype(low)

        pl.when(live)(compute)

    def start_part(back):
        for side in (0, 1):
            passed[back, side] = remote(
                part_out.at[back, side],
                part_in.at[back],
                pp_s.at[back],
                pp_r.at[back],
                partner,
            )
            live = slot_live((back, side), chip, core, reach)
            pl.when(jnp.logical_and(live, core != side))(passed[back, side].start)

    def send_sum(back):
        both = chip - back >= 0
        partner_has = jnp.logical_and(both, core == 1) if back == reach else both

        def add_partner():
            passed[back, 0].wait_recv()
            value = part_out[back, core].astype(jnp.float32) + part_in[back].astype(jnp.float32)
            sum_out[back] = value.astype(low)

        pl.when(partner_has)(add_partner)
        if back == reach:

            def alone():
                sum_out[back] = part_out[back, core]

            pl.when(jnp.logical_and(both, core == 0))(alone)

    def send_sum_start(back):
        sent_on[back] = remote(
            sum_out.at[back], sum_in.at[back], pa_s.at[back], pa_r.at[back], behind(back)
        )
        pl.when(chip - back >= 0)(sent_on[back].start)

    next(reduction, None)
    pass_slot(reach, 1)
    next(reduction, None)

    half_car.wait_recv()
    half_grad.wait_recv()
    mine, theirs = own_grad[core], half_in[...].astype(jnp.float32)
    car_mine, car_theirs = car_ref[core], car_in[...]
    car_0 = jnp.where(first, car_mine, car_theirs)
    car_1 = jnp.where(first, car_theirs, car_mine)
    grad_0 = jnp.where(first, mine, theirs)
    grad_1 = jnp.where(first, theirs, mine)
    chip_out[...] = (grad_0 + car_0[0:1] * grad_1).astype(low)
    chip_car[...] = car_0 * car_1
    pass_slot(reach, 0)
    next(reduction, None)
    state_along = {}
    for k in range(1, reach + 1):
        state_along[k] = (
            remote(chip_out, chip_in.at[k], ca_s.at[k, 0], ca_r.at[k, 0], behind(k)),
            remote(chip_car, chip_car_in.at[k], ca_s.at[k, 1], ca_r.at[k, 1], behind(k)),
        )
        for copy in state_along[k]:
            pl.when(chip - k >= 0)(copy.start)
    start_part(reach)
    for back in range(reach - 1, 0, -1):
        pass_slot(back, 1)
        next(reduction, None)
        send_sum(back + 1)
        pass_slot(back, 0)
        next(reduction, None)
        send_sum_start(back + 1)
        start_part(back)
    pass_slot(0, 0)
    next(reduction, None)
    start_part(0)
    send_sum(1)

    for head in range(SSM_HEADS):
        runb[head] = jnp.broadcast_to(run_ref[:, head : head + 1], (span, 128))
    send_sum_start(1)
    bias[...] = same_document(segc_ref[2 * reach + core], segr_ref[...], True)
    gramt[...] = lax.dot_general(
        in_map, out_map, (((1,), (1,)), ((), ())), precision=HIGHEST,
        preferred_element_type=jnp.float32,
    )
    dgram[...] = jnp.zeros_like(dgram)
    qcol[...] = jnp.zeros_like(qcol)
    qrow[...] = jnp.zeros_like(qrow)
    heads_of = lax.broadcasted_iota(jnp.int32, (inner, 128), 0) // SSM_HEAD
    fold_ref[...] = jnp.where(heads_of == lanes((inner, 128)), 1.0, 0.0).astype(low)

    def intra(quad, _):
        at = pl.ds(pl.multiple_of(quad * 256, 256), 256)
        grads = gmix_ref[:, at].astype(low)
        inputs = xdt[:, at]
        place = lanes((span, 256)) // 64
        value = jnp.zeros((span, 256), jnp.float32)
        for i in range(4):
            head = quad * 4 + i
            column = runb[head]
            spread = runt_ref[head] - jnp.concatenate([column] * (span // 128), axis=1)
            decay = jnp.exp(spread + bias[...])
            mixing = decay * gramt[...]
            alone = jnp.where(place == i, inputs, jnp.zeros_like(inputs))
            grad_mixing = dot_rows(alone, grads)
            dgram[...] += decay * grad_mixing
            product = mixing * grad_mixing
            qrow[pl.ds(head, 1), :] = jnp.sum(product, axis=0, keepdims=True)
            by_row = jnp.sum(product, axis=1, keepdims=True)
            qcol[...] = jnp.where(lanes((span, 128)) == head, by_row, qcol[...])
            part = dot_plain(mixing.astype(low), grads)
            value = jnp.where(place == i, part, value)
        dxdt[:, at] = value
        return 0

    for quad in range(SSM_HEADS // 4):
        lax.fori_loop(quad, quad + 1, intra, 0)
        next(reduction, None)

    acc[...] = jnp.zeros_like(acc)
    for k in range(reach, 0, -1):

        def take(k=k):
            for copy in state_along[k]:
                copy.wait_recv()
            acc[...] = chip_in[k].astype(jnp.float32) + chip_car_in[k, 0:1] * acc[...]

        pl.when(chip + k < chips)(take)
    later_1, later_0 = acc[...], grad_1 + car_1[0:1] * acc[...]
    later[core] = jnp.where(first, later_0, later_1)
    later_out[...] = jnp.where(first, later_1, later_0)

    attend_back(kvw_ref.at[0, core], segc_ref[2 * reach + core], True)
    next(reduction, None)
    later_pass = remote(later_out, later.at[core], la_s, la_r, partner)
    later_pass.start()
    for pair in range(HEADS // 2):
        at = slice(pair * 128, (pair + 1) * 128)
        dq_ref[:, at] = dqt[at, :].T * HEAD**-0.5

    dkv_ref[:, 0:128] = dk[...]
    dkv_ref[:, 128:256] = dv[...]

    def add_zero():
        passed[0, 0].wait_recv()
        dkv_ref[...] += part_in[0].astype(jnp.float32)

    pl.when(core == 0)(add_zero)
    for k in range(1, reach + 1):

        def add_ahead(k=k):
            sent_on[k].wait_recv()
            dkv_ref[...] += sum_in[k].astype(jnp.float32)

        pl.when(chip + k < chips)(add_ahead)

    grad_low = dgram[...].astype(low)
    grad_in = dot_plain(grad_low, out_low)
    grad_out = dot_plain(dgram[...].T.astype(low), in_low)
    later_pass.wait_recv()

    def fold(value, own):
        high = value.astype(low)
        rest = (value - high.astype(jnp.float32)).astype(low)
        return dot_plain(high, fold_ref[own, :]) + dot_plain(rest, fold_ref[own, :])

    carried = jnp.zeros((1, 128), jnp.float32)
    skip_sum = jnp.zeros((8, 128), jnp.float32)
    x_inside, x_part, g_reached = (jnp.zeros((span, 128), jnp.float32) for _ in range(3))
    for i in range(2):
        entering = ent_ref[i]
        grads = later[i]
        own = slice(i * half, (i + 1) * half)
        by_lane = jnp.sum(entering * grads, axis=0, keepdims=True)
        carried = carried + fold(jnp.broadcast_to(by_lane, (8, half)), own)[0:1]
        enter_low, later_low = entering.astype(low), grads.astype(low)
        grad_out = grad_out + dot_rows(ge[:, own], enter_low)
        grad_in = grad_in + dot_rows(xw[:, own], later_low)
        reached = dot_plain(out_low, enter_low)
        grad_xw = dot_plain(in_low, later_low)
        for j in range(SSM_HEADS // 4):
            pair = i * (SSM_HEADS // 4) + j
            at = slice(pair * 128, (pair + 1) * 128)
            here = slice(j * 128, (j + 1) * 128)
            x_pair, g_pair = act_ref[:, at], gmix_ref[:, at]
            part = grad_xw[:, here]
            inside = dxdt[:, at]
            dact_ref[:, at] = (
                skip_ref[:, at] * g_pair
                + pair_columns(dt_ref, pair) * inside
                + pair_columns(weight, pair) * part
            )
            sums[0, :, here] = x_pair * inside
            sums[1, :, here] = x_pair * part
            sums[2, :, here] = g_pair * reached[:, here]
            sums[3, :, here] = x_pair * g_pair
        x_inside, x_part, g_reached = (
            total + fold(sums[n], own) for n, total in enumerate((x_inside, x_part, g_reached))
        )
        by_lane = jnp.sum(sums[3], axis=0, keepdims=True)
        skip_sum = skip_sum + fold(jnp.broadcast_to(by_lane, (8, half)), own)
    dact_ref[:, inner : inner + STATE] = grad_in
    dact_ref[:, inner + STATE :] = grad_out

    w_part = weight * x_part
    drun = qrow[...].T - qcol[...] + e_ref[...] * g_reached - w_part
    last = jnp.sum(w_part, axis=0, keepdims=True) + rate_ref[1:2] * carried
    rows = lax.broadcasted_iota(jnp.int32, (span, 128), 0)
    drun = jnp.where(rows == span - 1, drun + last, drun)
    upper = lax.broadcasted_iota(jnp.int32, (span, span), 0) <= lanes((span, span))
    drate = lax.dot_general(
        jnp.where(upper, 1.0, 0.0), drun, (((1,), (0,)), ((), ())), precision=HIGHEST,
        preferred_element_type=jnp.float32,
    )
    rate = rate_ref[0:1]
    ddt_ref[...] = x_inside + wd_ref[...] * x_part + rate * drate
    heads_ref[...] = jnp.zeros_like(heads_ref)
    heads_ref[0:1] = jnp.sum(rate * dt_ref[...] * drate, axis=0, keepdims=True)
    heads_ref[1:2] = skip_sum[0:1]

    run_out(reduction)
    half_car.wait_send()
    half_grad.wait_send()
    later_pass.wait_send()
    for k in range(1, reach + 1):

        def sent(k=k):
            sent_on[k].wait_send()
            for copy in state_along[k]:
                copy.wait_send()

        pl.when(chip - k >= 0)(sent)
    for back in range(reach + 1):
        for side in (0, 1):
            if (back, side) in ((0, 1),):
                continue
            live = slot_live((back, side), chip, core, reach)
            pl.when(jnp.logical_and(live, core != side))(passed[back, side].wait_send)


def mix_backward(reach, operands, plan):
    sums = plan.outs()
    chips = lax.axis_size("grp") // 2
    span = operands[0].shape[0]
    inner = SSM_HEADS * SSM_HEAD
    half = inner // 2
    kv_width = 2 * KV_HEADS * HEAD
    f32, low = jnp.float32, jnp.bfloat16
    shape = jax.ShapeDtypeStruct
    dma = pltpu.SemaphoreType.DMA
    vmem = pltpu.VMEM
    outs = [
        shape((span, HEADS * HEAD), f32),
        shape((span, kv_width), f32),
        shape((span, inner + 2 * STATE), f32),
        shape((span, 128), f32),
        shape((8, 128), f32),
    ]
    scratch = [
        vmem((HEADS, span, 128), low),
        vmem((HEADS, span, 128), low),
        vmem((span, span), f32),
        vmem((128, span), low),
        vmem((HEADS * HEAD, span), f32),
        vmem((HEADS, 1, span), f32),
        vmem((span, 128), f32),
        vmem((span, 128), f32),
        vmem((reach + 1, 2, span, kv_width), low),
        vmem((reach + 1, span, kv_width), low),
        vmem((reach + 1, span, kv_width), low),
        vmem((reach + 1, span, kv_width), low),
        vmem((span, inner), low),
        vmem((span, inner), low),
        vmem((span, inner), low),
        vmem((SSM_HEADS, span, 128), f32),
        vmem((span, span), f32),
        vmem((span, span), f32),
        vmem((2, STATE, half), f32),
        vmem((STATE, half), low),
        vmem((STATE, half), low),
        vmem((8, half), f32),
        vmem((STATE, half), low),
        vmem((8, half), f32),
        vmem((reach + 1, STATE, half), low),
        vmem((reach + 1, 8, half), f32),
        vmem((STATE, half), f32),
        vmem((2, STATE, half), f32),
        vmem((STATE, half), f32),
        vmem((128, span), f32),
        vmem((span, 128), f32),
        vmem((span, inner), f32),
        vmem((4, span, half), f32),
        vmem((inner, 128), low),
        dma((reach + 1,)),
        dma((reach + 1,)),
        dma((reach + 1,)),
        dma((reach + 1,)),
        dma((2,)),
        dma((2,)),
        dma((reach + 1, 2)),
        dma((reach + 1, 2)),
        dma,
        dma,
    ]
    results = pl.pallas_call(
        functools.partial(mix_backward_kernel, reach, plan),
        out_shape=[*outs, *sums],
        in_specs=[pl.BlockSpec(memory_space=pltpu.VMEM)] * (len(operands) + len(plan.operands())),
        out_specs=[pl.BlockSpec(memory_space=pltpu.VMEM)] * (len(outs) + len(sums)),
        scratch_shapes=[*scratch, *plan.scratch()],
        compiler_params=pltpu.CompilerParams(
            collective_id=3, has_side_effects=True, vmem_limit_bytes=VMEM_LIMIT
        ),
        name="mix_backward",
    )(*operands, *plan.operands())
    return results[: len(outs)], results[len(outs) :]


def shards(
    tokens,
    segments,
    input_gain,
    attention_in,
    attention_out,
    mixer_in,
    filter_taps,
    filter_bias,
    step_bias,
    decay_log,
    skip_scale,
    mixer_gain,
    mixer_out,
    feed_gain,
    gate_up,
    down_proj,
    cotangent,
):
    seq_count, span_len, model_width = tokens.shape
    row_count = seq_count * span_len
    seq_len = segments.shape[1]
    group_devices = lax.axis_size("grp")
    position = lax.axis_index("grp") * span_len
    inner_width = SSM_HEADS * SSM_HEAD
    xbc_width = inner_width + 2 * STATE
    query_width = HEADS * HEAD
    kv_width = KV_HEADS * HEAD
    rim_rows = CONV - 1
    def padded(value):
        return jnp.pad(value, ((0, 0), (0, 256 - value.shape[1])))

    small = [filter_taps] + [p[None] for p in (filter_bias, input_gain, mixer_gain, feed_gain)]
    pack = jnp.concatenate([padded(part) for part in small])
    shares = [attention_in, mixer_in, gate_up, down_proj, mixer_out, attention_out]
    gather = Gather(
        shares,
        [
            column_chunks(n, n, share.shape[1], pieces)[i][1:]
            for n, (share, pieces) in enumerate(zip(shares, (1, 2, 2, 1, 1, 1)))
            for i in range(pieces)
        ],
        pack,
    )
    offsets = position + jnp.arange(span_len, dtype=jnp.int32)
    cosine_table, sine_table = rope_tables(offsets, HEAD)
    turner = partial(rotate, cosine_table=cosine_table, sine_table=sine_table)
    reach = min(seq_len // (4 * span_len), group_devices // 2 - 1)
    chip = lax.axis_index("grp") // 2
    docs = jnp.concatenate([jnp.full((2 * reach * span_len,), -1, jnp.int32), segments[0]])
    window = lax.dynamic_slice_in_dim(docs, 2 * chip * span_len, 2 * (reach + 1) * span_len)
    window = window.reshape(2 * (reach + 1), 1, span_len).astype(jnp.float32)
    own_docs = lax.dynamic_slice_in_dim(segments[0], position, span_len)
    heads_rows = jnp.stack([step_bias, decay_log, skip_scale])
    heads_rows = jnp.pad(heads_rows, ((0, 5), (0, 128 - SSM_HEADS)))
    results, full = run_forward(
        reach,
        gather,
        tokens[0],
        window,
        heads_rows,
        jnp.concatenate([cosine_table] * 4, axis=1),
        jnp.concatenate([-sine_table, sine_table] * 2, axis=1),
    )
    full_attn_in, full_mix_in, full_gate_up, full_down, full_mix_out, full_attn_out = full
    (
        normed_low,
        query_rows,
        gate_part,
        ext_rows,
        active,
        step_wide,
        steps,
        running,
        running_turned,
        enter_decay,
        tail_decay,
        carried_lanes,
        carried,
        attended,
        attended_turned,
        inverse_total,
        mixed,
        entering,
        kv_window,
        key_docs,
        packs,
    ) = results
    full_gain_in, full_mix_gain, full_feed_gain = (
        packs[:, 5 + i, : part.shape[0]].reshape(-1)
        for i, part in enumerate((input_gain, mixer_gain, feed_gain))
    )
    taps_wide = packs[:, : CONV + 1, : filter_bias.shape[0]].transpose(1, 0, 2)
    taps_wide = taps_wide.reshape(CONV + 1, -1).astype(jnp.float32)
    token_float = tokens.reshape(row_count, model_width).astype(jnp.float32)
    _, norm_back = jax.vjp(rms_scale, token_float, full_gain_in.astype(jnp.float32))
    query_raw = jnp.zeros((seq_count, span_len, HEADS, HEAD), jnp.float32)
    _, query_back = jax.vjp(turner, query_raw)
    _, key_back = jax.vjp(turner, query_raw[:, :, :KV_HEADS])
    back_attn_in, back_attn_out, back_mix_in = full_attn_in, full_attn_out, full_mix_in
    back_mix_out, back_gate_up, back_down = full_mix_out, full_gate_up, full_down
    padded_docs = jnp.concatenate(
        [jnp.full((seq_count, rim_rows), -1, jnp.int32), segments], axis=1
    )
    seg_ext = lax.dynamic_slice_in_dim(padded_docs, position, span_len + rim_rows, 1)
    _, prep_back = jax.vjp(
        partial(mixer_inputs, seg_ext=seg_ext),
        ext_rows[None, 8 - rim_rows :],
        step_wide[None, :, :SSM_HEADS],
        taps_wide[:CONV],
        taps_wide[CONV],
        step_bias,
    )
    gate_part, mixed = gate_part[None], mixed[None]
    rate_scale = -jnp.exp(decay_log)
    recurrence = (
        active,
        steps,
        running,
        running_turned,
        enter_decay,
        tail_decay,
        carried_lanes,
        jnp.repeat(skip_scale, SSM_HEAD)[None, :],
    )
    normed_mix, gate_back = jax.vjp(gated_norm, mixed, gate_part, full_mix_gain.astype(jnp.float32))
    normed_mix_low = normed_mix.reshape(row_count, inner_width).astype(jnp.bfloat16)
    hidden = (
        token_float
        + jnp.dot(attended, full_attn_out, preferred_element_type=jnp.float32)
        + jnp.dot(normed_mix_low, full_mix_out, preferred_element_type=jnp.float32)
    )
    normed_feed, feed_back = jax.vjp(rms_scale, hidden, full_feed_gain.astype(jnp.float32))
    normed_feed_low = normed_feed.astype(jnp.bfloat16)
    gate_vals = jnp.dot(normed_feed_low, full_gate_up, preferred_element_type=jnp.float32)
    activation, act_back = jax.vjp(swiglu, gate_vals[:, :FF], gate_vals[:, FF:])
    activation_low = activation.astype(jnp.bfloat16)
    out_rows = (
        hidden + jnp.dot(activation_low, full_down, preferred_element_type=jnp.float32)
    ).astype(jnp.bfloat16)
    grad_rows = cotangent.reshape(row_count, model_width)
    grad_act = jnp.dot(grad_rows, back_down.T, preferred_element_type=jnp.float32)
    grad_gate, grad_upper = act_back(grad_act)
    grad_gu = jnp.concatenate([grad_gate, grad_upper], axis=-1).astype(jnp.bfloat16)
    grad_feed_in = jnp.dot(grad_gu, back_gate_up.T, preferred_element_type=jnp.float32)
    grad_hidden_norm, grad_feed = feed_back(grad_feed_in)
    grad_hidden = grad_rows.astype(jnp.float32) + grad_hidden_norm
    grad_hidden_low = grad_hidden.astype(jnp.bfloat16)
    grad_attended = jnp.dot(
        grad_hidden_low, back_attn_out.T, preferred_element_type=jnp.float32
    ).astype(jnp.bfloat16)
    grad_normed_mix = jnp.dot(grad_hidden_low, back_mix_out.T, preferred_element_type=jnp.float32)
    grad_mixed, grad_gate_part, grad_mix_gain = gate_back(
        grad_normed_mix.reshape(seq_count, span_len, inner_width)
    )
    heads_scale = jnp.stack([rate_scale, carried[0, :SSM_HEADS]])
    heads_scale = jnp.pad(heads_scale, ((0, 6), (0, 128 - SSM_HEADS)))
    operands = (
        query_rows,
        kv_window,
        key_docs,
        own_docs[None, :].astype(jnp.float32),
        *recurrence,
        attended_turned,
        inverse_total,
        entering,
        grad_attended,
        grad_mixed.reshape(row_count, inner_width),
        heads_scale,
    )
    early = GradPlan(
        [normed_feed_low, activation_low, normed_mix_low, attended_turned],
        [False, False, False, True],
        [grad_gu, grad_rows, grad_hidden_low],
        [
            *column_chunks(0, 0, 2 * FF, 4),
            *column_chunks(1, 1, model_width, 2),
            *column_chunks(2, 2, model_width, 2),
            (3, 2, 0, model_width),
        ],
    )
    (grad_query, grad_kv_own, grad_active, grad_steps, grad_heads), early_sums = mix_backward(
        reach, operands, early
    )
    grad_query = grad_query.reshape(seq_count, span_len, HEADS, HEAD)
    grad_kv_own = grad_kv_own.reshape(seq_count, span_len, 2 * kv_width)
    grad_extended, grad_step_raw, grad_taps, grad_tap_bias, grad_step_bias = prep_back(
        (grad_active[None], grad_steps[None, :, :SSM_HEADS])
    )
    rim_back = shifted(grad_extended[:, :rim_rows], "grp", -1)
    grad_conv = grad_extended[:, rim_rows:] + jnp.pad(
        rim_back, ((0, 0), (span_len - rim_rows, 0), (0, 0))
    )
    grad_mix_proj = jnp.concatenate(
        [
            grad_gate_part.reshape(row_count, inner_width),
            grad_conv.reshape(row_count, xbc_width),
            grad_step_raw.reshape(row_count, SSM_HEADS),
        ],
        axis=-1,
    ).astype(jnp.bfloat16)
    grad_normed_m = jnp.dot(grad_mix_proj, back_mix_in.T, preferred_element_type=jnp.float32)
    (grad_query_raw,) = query_back(grad_query)
    (grad_key_raw,) = key_back(
        grad_kv_own[..., :kv_width].reshape(seq_count, span_len, KV_HEADS, HEAD)
    )
    grad_projected = jnp.concatenate(
        [
            grad_query_raw.reshape(row_count, query_width),
            grad_key_raw.reshape(row_count, kv_width),
            grad_kv_own[..., kv_width:].reshape(row_count, kv_width),
        ],
        axis=-1,
    ).astype(jnp.bfloat16)
    grad_normed_a = jnp.dot(grad_projected, back_attn_in.T, preferred_element_type=jnp.float32)
    grad_token_norm, grad_gain_in = norm_back(grad_normed_a + grad_normed_m)
    grad_token = grad_hidden + grad_token_norm
    heads = jnp.concatenate([grad_step_bias, grad_heads[0, :SSM_HEADS], grad_heads[1, :SSM_HEADS]])
    parts = [grad_gain_in, grad_taps.reshape(-1), grad_tap_bias, grad_mix_gain, grad_feed, heads]
    lengths = [part.shape[0] for part in parts]
    vec = jnp.concatenate(parts)
    vec = jnp.pad(vec, (0, -vec.shape[0] % 1024)).reshape(-1, 128)
    late = GradPlan(
        [normed_low],
        [False],
        [grad_mix_proj, grad_projected],
        [*column_chunks(0, 0, grad_mix_proj.shape[1], 5), (0, 1, 0, grad_projected.shape[1])],
    )
    late_sums, summed = sum_gradients(late, vec)
    summed = summed.reshape(-1)
    marks = [sum(lengths[:i]) for i in range(len(lengths) + 1)]
    sums = [summed[marks[i] : marks[i + 1]] for i in range(len(lengths))]
    index = lax.axis_index("grp")

    def own_part(value):
        size = value.shape[-1] // group_devices
        return lax.dynamic_slice_in_dim(value, index * size, size, value.ndim - 1)

    own_gate_up, own_down = shard_rows(early_sums[:4]), shard_rows(early_sums[4:6])
    own_mix_out, own_attn_out = shard_rows(early_sums[6:8]), shard_rows(early_sums[8:])
    own_mix_in, own_attn_in = shard_rows(late_sums[:-1]), shard_rows(late_sums[-1:])
    return (
        out_rows.reshape(seq_count, span_len, model_width),
        grad_token.reshape(seq_count, span_len, model_width),
        own_part(sums[0]),
        own_attn_in,
        own_attn_out,
        own_mix_in,
        own_part(sums[1].reshape(CONV, -1)),
        own_part(sums[2]),
        sums[5][:SSM_HEADS],
        sums[5][SSM_HEADS : 2 * SSM_HEADS],
        sums[5][2 * SSM_HEADS :],
        own_part(sums[3]),
        own_mix_out,
        own_part(sums[4]),
        own_gate_up,
        own_down,
    )


def solution(mesh):
    return jax.shard_map(
        shards,
        mesh=mesh,
        in_specs=(
            P("rep", "grp", None),
            P("rep", None),
            P("grp"),
            P("grp", None),
            P("grp", None),
            P("grp", None),
            P(None, "grp"),
            P("grp"),
            P(),
            P(),
            P(),
            P("grp"),
            P("grp", None),
            P("grp"),
            P("grp", None),
            P("grp", None),
            P("rep", "grp", None),
        ),
        out_specs=(
            P("rep", "grp", None),
            P("rep", "grp", None),
            P("grp"),
            P("grp", None),
            P("grp", None),
            P("grp", None),
            P(None, "grp"),
            P("grp"),
            P(),
            P(),
            P(),
            P("grp"),
            P("grp", None),
            P("grp"),
            P("grp", None),
            P("grp", None),
        ),
        check_vma=False,
    )
```

```python
import functools
import itertools
import math
from functools import partial

import jax
import jax.numpy as jnp
from jax import lax
from jax.experimental import pallas as pl
from jax.experimental.pallas import tpu as pltpu
from jax.sharding import PartitionSpec as P

HEADS = 8
KV_HEADS = 2
HEAD = 64
SSM_HEADS = 24
SSM_HEAD = 64
STATE = 128
CONV = 4
FF = 2048


NORM_EPS = 1e-05
ROPE_BASE = 100000000000.0
HIGHEST = lax.Precision.HIGHEST


def rms_scale(values, scales):
    return values * lax.rsqrt(jnp.mean(values * values, axis=-1, keepdims=True) + NORM_EPS) * scales


def rope_tables(positions, head_width):
    indices = jnp.arange(head_width // 2, dtype=jnp.float32)
    frequency = ROPE_BASE ** (-2.0 * indices / head_width)
    angles = positions.astype(jnp.float32)[:, None] * frequency[None, :]
    return (jnp.cos(angles), jnp.sin(angles))


def gated_norm(mixed, gate_part, scales):
    flat_mixed = mixed.reshape(gate_part.shape)
    return rms_scale(flat_mixed * jax.nn.silu(gate_part), scales)


def swiglu(gate_vals, up_vals):
    return jax.nn.silu(gate_vals) * up_vals


MESH = pl.DeviceIdType.MESH
HIDDEN = -1e30
VMEM_LIMIT = 67043328
TAIL_LAG = 2
WINDOW = 2
HANDED = 4
CONV_PIECES = 2


def seat():
    rep, grp = lax.axis_index("rep"), lax.axis_index("grp")
    chips = lax.axis_size("grp") // 2
    quarter = lax.rem(rep, 4)
    base = rep - quarter
    flip_x = quarter + 1 - 2 * lax.rem(quarter, 2)
    flip_y = lax.rem(quarter + 2, 4)
    chip, core = lax.div(grp, 2), lax.rem(grp, 2)
    return dict(
        quarter=quarter,
        qx=flip_x,
        qy=flip_y,
        qd=lax.rem(flip_x + 2, 4),
        chip=chip,
        core=core,
        x={"rep": base + flip_x},
        y={"rep": base + flip_y},
        partner={"grp": chip * 2 + 1 - core},
        along=[{"grp": lax.rem(chip + k, chips) * 2 + core} for k in range(chips)],
        chip_to=[lax.rem(chip + k, chips) for k in range(chips)],
        chip_from=[lax.rem(chip - k + chips, chips) for k in range(chips)],
    )


def remote(source, target, sent, arrived, device):
    return pltpu.make_async_remote_copy(
        src_ref=source,
        dst_ref=target,
        send_sem=sent,
        recv_sem=arrived,
        device_id=device,
        device_id_type=MESH,
    )


def greet(me, extra=()):
    barrier = pltpu.get_barrier_semaphore()
    others = [me["x"], me["y"], me["partner"], *me["along"][1:], *extra]
    for device in others:
        pl.semaphore_signal(barrier, inc=1, device_id=device, device_id_type=MESH)
    pl.semaphore_wait(barrier, len(others))


def near_first(chips):
    return sorted(range(1, chips), key=lambda k: min(k, chips - k))


class Gather:
    def __init__(self, shards, chunks, pack):
        self.group = lax.axis_size("grp")
        self.chips = self.group // 2
        self.cut = [s.reshape(4, s.shape[0] // 4, s.shape[1]) for s in shards]
        self.chunks = chunks
        self.pack = pack

    def outs(self):
        shape = jax.ShapeDtypeStruct
        return [shape((self.group, *part.shape), part.dtype) for part in self.cut]

    def scratch(self):
        dma = pltpu.SemaphoreType.DMA
        count = len(self.chunks) + 1
        own = [pltpu.VMEM(part.shape, part.dtype) for part in self.cut]
        return [*own, *[dma((count, self.chips))] * 10, dma((len(self.cut), 2))]

    def steps(self, me, ins, pack, packs, outs, scratch):
        chips, count = self.chips, len(self.chunks)
        own_copy = scratch[: len(ins)]
        zs, zr, xs, xr, ys, yr, ds, dr, cs, cr, ls = scratch[len(ins) :]
        own = me["chip"] * 2 + me["core"]
        order = near_first(chips)
        along, over_x, over_y, diagonal, self.across = {}, {}, {}, {}, {}

        def part(m, ref):
            n, start, width = self.chunks[m]
            return ref if width == outs[n].shape[-1] else ref.at[..., start : start + width]

        def weight(m):
            return self.chunks[m][0]

        def start_along(m):
            source = part(m, ins[weight(m)].at[me["quarter"]])
            place = part(m, outs[weight(m)].at[own, me["quarter"]])
            for k in order:
                along[m, k] = remote(source, place, zs.at[m, k], zr.at[m, k], me["along"][k])
                along[m, k].start()

        def block(m, k):
            return outs[weight(m)].at[me["chip_from"][k] * 2 + me["core"]]

        for k in order:
            along[count, k] = remote(
                pack, packs.at[own], zs.at[count, k], zr.at[count, k], me["along"][k]
            )
            along[count, k].start()
        self.across[count, 0] = remote(
            pack, packs.at[own], cs.at[count, 0], cr.at[count, 0], me["partner"]
        )
        self.across[count, 0].start()
        packs[own] = pack[...]
        for m in range(min(WINDOW, count)):
            start_along(m)
        load, store = [], []
        for n in range(len(ins)):
            load.append(pltpu.make_async_copy(ins[n], own_copy[n], ls.at[n, 0]))
            load[-1].start()
        for m in range(count):
            source, place = part(m, ins[weight(m)]), part(m, outs[weight(m)].at[own])
            self.across[m, 0] = remote(source, place, cs.at[m, 0], cr.at[m, 0], me["partner"])
            self.across[m, 0].start()
        for n in range(len(ins)):
            load[n].wait()
            store.append(pltpu.make_async_copy(own_copy[n], outs[n].at[own], ls.at[n, 1]))
            store[-1].start()
        for k in order:
            along[count, k].wait_recv()
            piece = packs.at[me["chip_from"][k] * 2 + me["core"]]
            self.across[count, k] = remote(
                piece, piece, cs.at[count, k], cr.at[count, k], me["partner"]
            )
            self.across[count, k].start()
        self.store = store
        yield
        for step in range(count + 2):
            m = step
            if m < count:
                for k in order:
                    along[m, k].wait_recv()
                    piece = part(m, block(m, k).at[me["quarter"]])
                    over_x[m, k] = remote(piece, piece, xs.at[m, k], xr.at[m, k], me["x"])
                    over_y[m, k] = remote(piece, piece, ys.at[m, k], yr.at[m, k], me["y"])
                    over_x[m, k].start()
                    over_y[m, k].start()
                if m + WINDOW < count:
                    start_along(m + WINDOW)
            m = step - 1
            if 0 <= m < count:
                for k in order:
                    if (m + k) % 2 == 0:
                        over_x[m, k].wait_recv()
                        q, device = me["qx"], me["y"]
                    else:
                        over_y[m, k].wait_recv()
                        q, device = me["qy"], me["x"]
                    piece = part(m, block(m, k).at[q])
                    diagonal[m, k] = remote(piece, piece, ds.at[m, k], dr.at[m, k], device)
                    diagonal[m, k].start()
            m = step - 2
            if 0 <= m < count:
                for k in order:
                    if (m + k) % 2 == 0:
                        over_y[m, k].wait_recv()
                    else:
                        over_x[m, k].wait_recv()
                    diagonal[m, k].wait_recv()
                    piece = part(m, block(m, k))
                    self.across[m, k] = remote(
                        piece, piece, cs.at[m, k], cr.at[m, k], me["partner"]
                    )
                    self.across[m, k].start()
            yield
        self.all_copies = (along, over_x, over_y, diagonal, self.across)

    def arrive(self, m):
        for k in range(self.chips):
            self.across[m, k].wait_recv()

    def finish(self, waited):
        for m in range(len(self.chunks)):
            if m not in waited:
                self.arrive(m)
        for copies in self.all_copies:
            for copy in copies.values():
                copy.wait_send()


def f32(value):
    return value.astype(jnp.float32)


def turn_rows(source, turned, chips, piece, is_turned):
    features = source.shape[0] if is_turned else source.shape[1]
    width = math.lcm(128, piece)
    for start in range(0, features, width):
        if is_turned:
            value = f32(source[start : start + width, :])
        else:
            value = f32(source[:, start : start + width]).T
        for i in range(width // piece):
            at = start // piece + i
            chip, core, quarter = at // 8, (at // 4) % 2, at % 4
            block = value[i * piece : (i + 1) * piece].astype(jnp.bfloat16)
            turned[core, quarter, chip * piece : (chip + 1) * piece, :] = block


class GradPlan:
    def __init__(self, lefts, turned, rights, chunks, later=(), handed=0, received=()):
        self.handed, self.received = handed, list(received)
        self.later, self.swap_right = later, {}
        self.chips = lax.axis_size("grp") // 2
        self.extras = lax.axis_size("rep") // 4
        self.lefts, self.turned, self.rights, self.chunks = lefts, turned, rights, chunks
        self.tokens = rights[0].shape[0]
        sizes = [x.shape[0] if flag else x.shape[1] for x, flag in zip(lefts, turned)]
        self.rows = [size // 8 for size in sizes]
        self.piece = [size // (8 * self.chips) for size in sizes]

    def operands(self):
        rights = [r for n, r in enumerate(self.rights) if n not in self.later]
        return [*self.lefts, *rights, *self.received]

    def outs(self):
        whole = len(self.chunks) - self.handed
        shapes = [
            (4 if m < whole else self.chips, self.piece[a], width)
            for m, (a, _, _, width) in enumerate(self.chunks)
        ]
        shapes += [(4, *total.shape[1:]) for total in self.received]
        return [jax.ShapeDtypeStruct(shape, jnp.bfloat16) for shape in shapes]

    def scratch(self):
        low, vmem, dma = jnp.bfloat16, pltpu.VMEM, pltpu.SemaphoreType.DMA
        lefts, rights, count = len(self.lefts), len(self.rights), len(self.chunks)
        work = [vmem((2, 4, rows, self.tokens), low) for rows in self.rows]
        work += [vmem((4, rows, self.tokens), low) for rows in self.rows]
        work += [vmem(right.shape, low) for right in self.rights]
        shapes = [(self.rows[a], self.piece[a], width) for a, _, _, width in self.chunks]
        work += [vmem((4, rows, width), low) for rows, _, width in shapes]
        work += [vmem((2, rows, width), low) for rows, _, width in shapes]
        work += [vmem((rows, width), low) for rows, _, width in shapes]
        work += [vmem((self.chips, piece, width), low) for _, piece, width in shapes]
        ends = [shape[1:] for shape in shapes] + [total.shape[1:] for total in self.received]
        count = len(ends)
        work += [vmem((self.chips - 1, *end), low) for end in ends]
        if self.extras > 1:
            work += [vmem((self.extras, *end), low) for end in ends]
        sems = [dma((lefts,))] * 2 + [dma((rights,))] * 2
        sems += [dma((count, 2)), dma((count, 2)), dma((count,)), dma((count,))]
        sems += [dma((count, self.chips))] * 2 + [dma((count, self.extras))] * 2
        sems += [dma((count, 3))] * 2
        return [*work, *sems]

    def steps(self, me, ins, outs, scratch, lag=2):
        chips, extras, count = self.chips, self.extras, len(self.chunks)
        whole, ends = count - self.handed, count + len(self.received)
        lefts, rights = ins[: len(self.lefts)], ins[len(self.lefts) :]
        rights, received = rights[: len(self.rights)], rights[len(self.rights) :]
        groups = []
        sizes = [len(lefts), len(lefts), len(rights), *[count] * 4, ends]
        for size in sizes + ([ends] if extras > 1 else []):
            groups.append(scratch[:size])
            scratch = scratch[size:]
        turned, turned_in, rights_in, parts, one, two, total, slots = groups[:8]
        extra_in = groups[8] if extras > 1 else ()
        la_s, la_r, ri_s, ri_r, s1, r1, s2, r2, zs, zr, es, er, gs, gr = scratch
        total = [*total, *received]
        core = me["core"]
        reps, rep = lax.axis_size("rep"), lax.axis_index("rep")
        beyond = [{"rep": lax.rem(rep + 4 * e, reps)} for e in range(1, extras)]
        swap_left, swap_right = {}, self.swap_right
        for n in range(len(rights)):
            swap_right[n] = remote(rights[n], rights_in[n], ri_s.at[n], ri_r.at[n], me["partner"])
            if n not in self.later and n == 0:
                swap_right[n].start()
        for n in range(len(lefts)):
            turn_rows(lefts[n], turned[n], chips, self.piece[n], self.turned[n])
            swap_left[n] = remote(
                turned[n].at[1 - core], turned_in[n], la_s.at[n], la_r.at[n], me["partner"]
            )
            if n == 0:
                swap_left[n].start()
            yield
        waiting = [swap_right[n] for n in range(1, len(rights)) if n not in self.later]
        waiting = [copy for pair in itertools.zip_longest([swap_left[n] for n in range(1, len(lefts))], waiting) for copy in pair if copy is not None]
        have = set()
        first, second, along, other, spread = {}, {}, {}, {}, {}

        def form(m):
            a, b, start, width = self.chunks[m]
            for key, copy in (("left", a), swap_left[a]), (("right", b), swap_right[b]):
                if key not in have:
                    have.add(key)
                    copy.wait_recv()
            at = slice(start, start + width)

            rows = 4 * self.rows[a]
            value = dot_plain(turned[a][core].reshape(rows, self.tokens), rights[b][:, at])
            other = turned_in[a][...].reshape(rows, self.tokens)
            value = value + dot_plain(other, rights_in[b][:, at])
            parts[m][...] = value.astype(jnp.bfloat16).reshape(parts[m].shape)

        def send_first(m):
            device, mine = (me["x"], me["qx"]) if m % 2 == 0 else (me["y"], me["qy"])
            for i, q in ((1, me["qd"]), (0, mine)):
                first[m, i] = remote(
                    parts[m].at[q], one[m].at[i], s1.at[m, i], r1.at[m, i], device
                )
                first[m, i].start()

        def send_second(m):
            rows = self.rows[self.chunks[m][0]]
            device, q = (me["y"], me["qy"]) if m % 2 == 0 else (me["x"], me["qx"])
            first[m, 1].wait_recv()

            def add(j, _):
                at = pl.ds(pl.multiple_of(j * 64, 64), 64)
                value = f32(parts[m][q, at, :]) + f32(one[m][1, at, :])
                parts[m][q, at, :] = value.astype(jnp.bfloat16)
                return 0

            lax.fori_loop(0, rows // 64, add, 0)
            second[m] = remote(parts[m].at[q], two[m], s2.at[m], r2.at[m], device)
            second[m].start()

        def send_along(m):
            piece = self.piece[self.chunks[m][0]]
            first[m, 0].wait_recv()
            second[m].wait_recv()
            for j in range(chips):
                at = slice(j * piece, (j + 1) * piece)
                value = f32(parts[m][me["quarter"], at, :]) + f32(one[m][0, at, :]) + f32(two[m][at, :])
                (total if m < whole else outs)[m][j] = value.astype(jnp.bfloat16)
            if m < whole:
                pass_along(m)

        def pass_along(m):
            for k in near_first(chips):
                along[m, k] = remote(
                    total[m].at[me["chip_to"][k]],
                    slots[m].at[k - 1],
                    zs.at[m, k],
                    zr.at[m, k],
                    me["along"][k],
                )
                along[m, k].start()

        def send_spread(m):
            value = f32(total[m][me["chip"]])
            for k in near_first(chips):
                along[m, k].wait_recv()
                value = value + f32(slots[m][k - 1])
            if extras > 1:
                extra_in[m][0] = value.astype(jnp.bfloat16)
                for e in range(1, extras):
                    other[m, e] = remote(
                        extra_in[m].at[0],
                        extra_in[m].at[e],
                        es.at[m, e],
                        er.at[m, e],
                        beyond[e - 1],
                    )
                    other[m, e].start()
                for e in range(1, extras):
                    other[m, e].wait_recv()
                    value = value + f32(extra_in[m][e])
            outs[m][me["quarter"]] = value.astype(jnp.bfloat16)
            piece = outs[m].at[me["quarter"]]
            for i, device in enumerate((me["x"], me["y"])):
                spread[m, i] = remote(piece, piece, gs.at[m, i], gr.at[m, i], device)
                spread[m, i].start()

        def send_diagonal(m):
            way = m % 2
            spread[m, way].wait_recv()
            q, device = (me["qx"], me["y"]) if way == 0 else (me["qy"], me["x"])
            piece = outs[m].at[q]
            spread[m, 2] = remote(piece, piece, gs.at[m, 2], gr.at[m, 2], device)
            spread[m, 2].start()

        for m in range(count, ends):
            pass_along(m)
        stages = (send_second, send_along, send_spread, send_diagonal)
        spans = (count, count, whole, whole)
        last = max([lag * (n + 1) + span for n, span in enumerate(spans)])
        for step in range(max(last, len(received) + 2 * lag)):
            if step < count:
                form(step)
                send_first(step)
            for _ in range(2):
                if waiting:
                    waiting.pop(0).start()
            for n, stage in enumerate(stages):
                m = step - lag * (n + 1)
                if 0 <= m < spans[n]:
                    stage(m)
                m = count + step - lag * (n - 1)
                if n >= 2 and count <= m < ends:
                    stage(m)
            yield
        for m in [*range(whole), *range(count, ends)]:
            spread[m, 1 - m % 2].wait_recv()
            spread[m, 2].wait_recv()
        for copies in (swap_left, swap_right, first, second, along, other, spread):
            for copy in copies.values():
                copy.wait_send()
        yield


def small_steps(me, chips, extras, vec, out, stage, slots, sems, more):
    ss, sr, zs, zr = sems
    copies = []
    value = vec[...]
    hops = [me["x"], me["y"], me["partner"]]
    for i, device in enumerate(hops):
        stage[i] = value
        copies.append(remote(stage.at[i], slots.at[i], ss.at[i], sr.at[i], device))
        copies[-1].start()
        yield
        copies[-1].wait_recv()
        value = value + slots[i]
    if extras > 1:
        stage[3] = value
        for e in range(1, extras):
            at = 3 + chips + e
            copies.append(remote(stage.at[3], slots.at[at], ss.at[2 + e], sr.at[2 + e], more[e - 1]))
            copies[-1].start()
        yield
        for e in range(1, extras):
            copies[-e].wait_recv()
        for e in range(1, extras):
            value = value + slots[3 + chips + e]
    stage[4] = value
    along = []
    for k in near_first(chips):
        along.append(remote(stage.at[4], slots.at[3 + k], zs.at[k], zr.at[k], me["along"][k]))
        along[-1].start()
    yield
    for copy in along:
        copy.wait_recv()
    for k in range(1, chips):
        value = value + slots[3 + k]
    out[...] = value
    for copy in copies + along:
        copy.wait_send()
    yield


def run_out(steps):
    for _ in steps:
        pass


def tail_kernel(plan, early, joins, *refs):
    groups = []
    kept = len(plan.outs())
    for size in (len(plan.operands()), 19 + len(early), 2 + len(joins), 13 + kept):
        groups.append(refs[:size])
        refs = refs[size:]
    normed_ref, dz_ref, *received = groups[0]
    (
        dact_ref,
        ddt_ref,
        dq_ref,
        dkv_ref,
        ext_ref,
        step_ref,
        heads_ref,
        taps_ref,
        same_ref,
        cosine_ref,
        sine_ref,
        tokens_ref,
        gain_ref,
        hidden_ref,
        early_heads,
        feed_gain_ref,
        mixer_gain_ref,
        mixer_w,
        attention_w,
    ) = groups[1][len(early) :]
    token_grad_ref, total_ref, *joined = groups[2]
    (
        dconv,
        dproj,
        padded,
        last_rows,
        rim_out,
        rim_in,
        mixer_rows,
        attention_rows,
        dnormed,
        vec,
        rim_s,
        rim_r,
        fetch_sem,
        *sums,
    ) = groups[3]
    stage, slots, small_sems = refs[-6], refs[-5], refs[-4:]
    me = seat()
    rep, reps = lax.axis_index("rep"), lax.axis_size("rep")
    grp, size = lax.axis_index("grp"), lax.axis_size("grp")
    span, conv_width = dact_ref.shape
    width = tokens_ref.shape[1]
    inner = dz_ref.shape[1]
    beyond = [{"rep": lax.rem(rep + 4 * e, reps)} for e in range(1, plan.extras)]
    greet(me, [*beyond, {"grp": lax.rem(grp + 1, size)}, {"grp": lax.rem(grp + size - 1, size)}])
    large = plan.steps(me, [normed_ref, dz_ref, dconv, dproj, *received], sums, refs[:-6], lag=TAIL_LAG)
    next(large)

    blocks = width // 256
    fetched = (
        pltpu.make_async_copy(mixer_w, mixer_rows, fetch_sem.at[0]),
        pltpu.make_async_copy(attention_w, attention_rows, fetch_sem.at[1]),
    )
    for copy in fetched:
        copy.start()

    low_half = lanes((span, 128)) % HEAD < HEAD // 2

    def turned_back(value):
        other = jnp.where(low_half, pltpu.roll(value, 128 - HEAD // 2, 1), pltpu.roll(value, HEAD // 2, 1))
        return value * cosine_ref[...] - other * sine_ref[...]

    queries = dq_ref.shape[1]
    for start in range(0, queries, 128):
        at = slice(start, start + 128)
        dproj[:, at] = turned_back(dq_ref[:, at]).astype(jnp.bfloat16)
    dproj[:, queries : queries + 128] = turned_back(dkv_ref[:, 0:128]).astype(jnp.bfloat16)
    dproj[:, queries + 128 :] = dkv_ref[:, 128:].astype(jnp.bfloat16)
    next(large)
    plan.swap_right[2].start()

    vec[...] = jnp.zeros_like(vec)
    padded[...] = jnp.zeros_like(padded)
    step_slope = 1.0 / (1.0 + jnp.exp(-(step_ref[...] + heads_ref[0:1])))
    dstep = ddt_ref[...] * step_slope
    dconv[:, conv_width:] = dstep[:, 0:SSM_HEADS].astype(jnp.bfloat16)

    def convolve_back(j, _):
        at = pl.ds(pl.multiple_of(j * 256, 256), 256)
        value = jnp.broadcast_to(taps_ref[CONV : CONV + 1, at], (span, 256))
        inside = [across(same_ref[tap], 256) > 0.0 for tap in range(CONV - 1)]
        for tap in range(CONV):
            term = ext_ref[5 + tap : 5 + tap + span, at] * taps_ref[tap : tap + 1, at]
            value = value + (jnp.where(inside[tap], term, 0.0) if tap < CONV - 1 else term)
        gate = 1.0 / (1.0 + jnp.exp(-value))
        grad = dact_ref[:, at] * gate * (1.0 + value * (1.0 - gate))
        vec[CONV : CONV + 1, at] = jnp.sum(grad, axis=0, keepdims=True)
        for tap in range(CONV):
            kept = jnp.where(inside[tap], grad, 0.0) if tap < CONV - 1 else grad
            product = kept * ext_ref[5 + tap : 5 + tap + span, at]
            vec[tap : tap + 1, at] = jnp.sum(product, axis=0, keepdims=True)
            padded[tap, 8 : 8 + span, :] = kept * taps_ref[tap : tap + 1, at]
        value = jnp.zeros((span, 256), jnp.float32)
        edge = jnp.zeros((8, 256), jnp.float32)
        for tap in range(CONV):
            back = CONV - 1 - tap
            value = value + padded[tap, 8 + back : 8 + back + span, :]
            edge = edge + padded[tap, back : back + 8, :]
        rim_out[:, at] = edge
        dconv[:, at] = value.astype(jnp.bfloat16)
        last_rows[:, at] = value[span - 16 :]
        return 0

    for j in range(conv_width // 256):
        lax.fori_loop(j, j + 1, convolve_back, 0)
        if j % 3 == 2:
            next(large)
    rim = remote(rim_out, rim_in, rim_s, rim_r, {"grp": lax.rem(grp + size - 1, size)})
    pl.when(grp > 0)(rim.start)

    for copy in fetched:
        copy.wait()
    for i in range(blocks):
        at = slice(i * 256, (i + 1) * 256)
        value = dot_rows(dz_ref[...], mixer_rows[at, 0:inner])
        dnormed[:, at] = value + dot_rows(dproj[...], attention_rows[at, :])

    def add_rim():
        rim.wait_recv()
        dconv[span - 16 : span - 8, 0:conv_width] = last_rows[0:8, :].astype(jnp.bfloat16)
        last = last_rows[8:16, :] + rim_in[...]
        dconv[span - 8 :, 0:conv_width] = last.astype(jnp.bfloat16)

    pl.when(grp + 1 < size)(add_rim)
    plan.swap_right[1].start()
    for i in range(blocks):
        at = slice(i * 256, (i + 1) * 256)
        value = dot_rows(dconv[:, 0:conv_width], mixer_rows[at, inner : inner + conv_width])
        dnormed[:, at] += value + dot_rows(dconv[:, conv_width:], mixer_rows[at, inner + conv_width :])
        if i == blocks // 2:
            for _ in range(len(plan.chunks) - 3):
                next(large, None)

    def norm_back(i, gain_grad):
        at = pl.ds(pl.multiple_of(i * 64, 64), 64)
        value = f32(tokens_ref[at, :])
        scale = lax.rsqrt(jnp.mean(value * value, axis=-1, keepdims=True) + NORM_EPS)
        unit = value * scale
        grad = dnormed[at, :]
        inner_grad = grad * gain_ref[0:1]
        mean = jnp.mean(inner_grad * unit, axis=-1, keepdims=True)
        token_grad_ref[at, :] = hidden_ref[at, :] + scale * (inner_grad - unit * mean)
        return gain_grad + jnp.sum(grad * unit, axis=0, keepdims=True)

    gain_grad = lax.fori_loop(0, span // 64, norm_back, jnp.zeros((1, width), jnp.float32))
    vec[5:6, 0:inner] = mixer_gain_ref[...]
    vec[6:7, 0:width] = feed_gain_ref[...]
    vec[7:8, 0:width] = gain_grad
    vec[7:8, width : width + 128] = jnp.sum(dstep, axis=0, keepdims=True)
    for i in range(2):
        vec[7:8, width + 128 * (i + 1) : width + 128 * (i + 2)] = early_heads[i : i + 1]
    next(large, None)
    small = small_steps(me, plan.chips, plan.extras, vec, total_ref, stage, slots, small_sems, beyond)
    for _ in small:
        next(large, None)
    pieces = [*groups[1][: len(early)], *sums]

    def join(wanted):
        for target, parts in zip(joined, joins):
            start = 0
            for part in parts:
                source = pieces[part]
                rows, columns = source.shape[1:]
                if part in wanted:
                    for q in range(4):
                        at = (slice(q * rows, (q + 1) * rows), slice(start, start + columns))
                        target[at] = f32(source[q])
                start += columns

    join(range(len(early)))
    run_out(large)
    join(range(len(early), len(pieces)))
    pl.when(grp > 0)(rim.wait_send)


def run_tail(plan, early, joins, *operands):
    dma, vmem = pltpu.SemaphoreType.DMA, pltpu.VMEM
    chips, extras = plan.chips, plan.extras
    f32, low = jnp.float32, jnp.bfloat16
    span, conv_width = operands[0].shape
    width = operands[11].shape[1]
    mixer_w, attention_w = operands[-2:]
    vec = (8, conv_width)
    scratch = [
        vmem((span, conv_width + SSM_HEADS), low),
        vmem((span, attention_w.shape[1]), low),
        vmem((CONV, span + 16, 256), f32),
        vmem((16, conv_width), f32),
        vmem((8, conv_width), f32),
        vmem((8, conv_width), f32),
        vmem(mixer_w.shape, low),
        vmem(attention_w.shape, low),
        vmem((span, width), f32),
        vmem(vec, f32),
        dma,
        dma,
        dma((2,)),
        *[vmem(out.shape, out.dtype) for out in plan.outs()],
    ]
    pieces = [*early, *plan.outs()]
    full = []
    for parts in joins:
        rows = 4 * pieces[parts[0]].shape[1]
        full.append(jax.ShapeDtypeStruct((rows, sum(pieces[p].shape[2] for p in parts)), f32))
    small = [vmem((5, *vec), f32), vmem((3 + chips + extras, *vec), f32)]
    small += [dma((2 + extras,)), dma((2 + extras,)), dma((chips,)), dma((chips,))]
    vm, anywhere = pl.BlockSpec(memory_space=pltpu.VMEM), pl.BlockSpec(memory_space=pl.ANY)
    token_grad, total, *joined = pl.pallas_call(
        functools.partial(tail_kernel, plan, early, joins),
        out_shape=[
            jax.ShapeDtypeStruct((span, width), f32),
            jax.ShapeDtypeStruct(vec, f32),
            *full,
        ],
        in_specs=[vm] * (len(plan.operands()) + len(early) + 17) + [anywhere] * 2,
        out_specs=[vm] * (2 + len(full)),
        scratch_shapes=[*scratch, *plan.scratch(), *small],
        compiler_params=pltpu.CompilerParams(
            collective_id=1, has_side_effects=True, vmem_limit_bytes=VMEM_LIMIT
        ),
        name="run_tail",
    )(*plan.operands(), *early, *operands)
    return token_grad, total, joined


def column_chunks(left, right, columns, pieces):
    width = columns // pieces // 128 * 128
    starts = [i * width for i in range(pieces)] + [columns]
    return [(left, right, low, high - low) for low, high in zip(starts, starts[1:])]


def axis_seat():
    grp = lax.axis_index("grp")
    return lax.div(grp, 2), lax.rem(grp, 2)


def greet_group(extra=()):
    size, grp = lax.axis_size("grp"), lax.axis_index("grp")
    barrier = pltpu.get_barrier_semaphore()
    others = [{"grp": lax.rem(grp + k, size)} for k in range(1, size)] + list(extra)
    for device in others:
        pl.semaphore_signal(barrier, inc=1, device_id=device, device_id_type=MESH)
    pl.semaphore_wait(barrier, len(others))


def lanes(shape):
    return lax.broadcasted_iota(jnp.int32, shape, len(shape) - 1)


def pair_columns(columns, pair):
    rows = columns.shape[0]
    low = jnp.broadcast_to(columns[:, 2 * pair : 2 * pair + 1], (rows, 128))
    high = jnp.broadcast_to(columns[:, 2 * pair + 1 : 2 * pair + 2], (rows, 128))
    return jnp.where(lanes((rows, 128)) < 64, low, high)


def dot_rows(left, right):
    return lax.dot_general(
        left, right, (((1,), (1,)), ((), ())), preferred_element_type=jnp.float32
    )


def dot_plain(left, right):
    return jnp.dot(left, right, preferred_element_type=jnp.float32)


def align_heads(source, target, scale):
    for pair in range(HEADS // 2):
        both = source[:, pair * 128 : (pair + 1) * 128].astype(jnp.float32) * scale
        swapped = pltpu.roll(both, 64, 1)
        for odd in range(2):
            head = 2 * pair + odd
            group = head // (HEADS // KV_HEADS)
            value = both if odd == group else swapped
            keep = lanes(value.shape) // 64 == group
            target[head] = jnp.where(keep, value, 0.0).astype(jnp.bfloat16)


def slot_plan(reach):
    return [(0, 0)] + [(k, core) for k in range(1, reach + 1) for core in (1, 0)]


def slot_live(slot, chip, core, reach):
    back, side = slot
    if back == 0:
        return core == 1
    live = chip - back >= 0
    if back == reach and side == 0:
        live = jnp.logical_and(live, core == 0)
    return live


def same_document(key_column, query_row, causal):
    size = query_row.shape[-1]
    allowed = across(key_column, size) == query_row
    if causal:
        rows = lax.broadcasted_iota(jnp.int32, (size, size), 0)
        allowed = jnp.logical_and(allowed, rows <= lanes((size, size)))
    return jnp.where(allowed, 0.0, HIDDEN)


def across(column, width):
    return jnp.concatenate([column] * (width // 128), axis=1)


def forward_kernel(reach, gather, *refs):
    chips, many = gather.chips, len(gather.cut)
    groups = []
    for size in (6, many, 24, many, 39):
        groups.append(refs[:size])
        refs = refs[size:]
    (
        tokens_ref,
        pack,
        docs_ref,
        heads_ref,
        cosine_ref,
        sine_ref,
    ) = groups[0]
    shards = groups[1]
    (
        normed_ref,
        q_ref,
        gate_ref,
        ext_ref,
        act_ref,
        step_ref,
        dt_ref,
        run_ref,
        runt_ref,
        e_ref,
        wd_ref,
        car_ref,
        carried_ref,
        att_ref,
        attt_ref,
        inv_ref,
        mixed_ref,
        ent_ref,
        kvw_ref,
        segk_ref,
        packs,
        same,
        taps,
        gain_ref,
    ) = groups[2]
    fulls = groups[3]
    (
        kv_ref,
        attention_w,
        mixer_w,
        rim_out,
        rim_in,
        seg_ext,
        skip_lanes,
        qa,
        bias,
        vt,
        ot,
        total,
        xdt,
        xw,
        runb,
        gram,
        own_state,
        half_out,
        half_in,
        car_in,
        chip_out,
        chip_car,
        chip_in,
        chip_car_in,
        enter_out,
        acc,
        fetch_sem,
        rim_s,
        rim_r,
        ka_s,
        ka_r,
        kp_s,
        kp_r,
        ha_s,
        ha_r,
        ca_s,
        ca_r,
        en_s,
        en_r,
    ) = groups[4]
    travel = refs
    chip, core = axis_seat()
    grp = lax.axis_index("grp")
    span = tokens_ref.shape[0]
    inner = SSM_HEADS * SSM_HEAD
    half = inner // 2
    partner = {"grp": chip * 2 + 1 - core}

    def ahead(k):
        return {"grp": lax.rem(grp + 2 * k, 2 * chips)}

    me = seat()
    greet_group([me["x"], me["y"]])
    gathering = gather.steps(me, shards, pack, packs, fulls, travel)

    def tick():
        next(gathering, None)

    tick()
    for i in range(2 * (reach + 1)):
        segk_ref[i] = jnp.broadcast_to(docs_ref[i], (128, span)).T
    own_row = docs_ref[2 * reach + core]
    own_docs = segk_ref[2 * reach + core]
    seg_ext[8:, :] = own_docs
    seg_ext[0:8, :] = segk_ref[2 * reach + core - 1][span - 8 :]
    prior, tail = seg_ext[7:8, :], own_docs[span - 1 :]
    for j in range(CONV - 1):
        same[j] = jnp.where(seg_ext[5 + j : 5 + j + span, :] == own_docs, 1.0, 0.0)

    for k in range(chips):
        gather.across[len(gather.chunks), k].wait_recv()

    def whole_rows(width):
        total = width * 2 * chips
        rows = lax.broadcasted_iota(jnp.int32, (pack.shape[1], total), 0)
        value = jnp.zeros((8, total), jnp.float32)
        for i in range(2 * chips):
            here = jnp.logical_and(lanes(rows.shape) == rows + width * i, rows < width)
            value = value + dot_plain(packs[i], jnp.where(here, 1.0, 0.0).astype(jnp.bfloat16))
        return value

    taps[...] = whole_rows(taps.shape[1] // (2 * chips))
    gain = whole_rows(tokens_ref.shape[1] // (2 * chips))[5:6]
    gain_ref[...] = jnp.broadcast_to(gain, gain_ref.shape)

    def norm(i, _):
        at = pl.ds(pl.multiple_of(i * 64, 64), 64)
        value = f32(tokens_ref[at, :])
        scale = lax.rsqrt(jnp.mean(value * value, axis=-1, keepdims=True) + NORM_EPS)
        normed_ref[at, :] = (value * scale * gain).astype(jnp.bfloat16)
        return 0

    lax.fori_loop(0, span // 64, norm, 0)
    for pair in range(SSM_HEADS // 2):
        at = slice(pair * 128, (pair + 1) * 128)
        skip_lanes[:, at] = pair_columns(jnp.broadcast_to(heads_ref[2:3], (8, 128)), pair)

    for _ in range(3):
        tick()
    gather.arrive(0)
    mixer_chunks = [m for m, chunk in enumerate(gather.chunks) if chunk[0] == 1]
    waited = {0}
    fetch = pltpu.make_async_copy(fulls[0], attention_w, fetch_sem.at[0])
    gather.store[0].wait()
    fetch.start()
    tick()
    fetch.wait()
    width = tokens_ref.shape[1]
    low_half = lanes((span, 128)) % HEAD < HEAD // 2

    def turned(value):
        other = jnp.where(low_half, pltpu.roll(value, 128 - HEAD // 2, 1), pltpu.roll(value, HEAD // 2, 1))
        return value * cosine_ref[...] + other * sine_ref[...]

    for j in range(3):
        part = attention_w[:, :, :, j * 256 : (j + 1) * 256].reshape(width, 256)
        value = dot_plain(normed_ref[...], part)
        one, two = value[:, 0:128], value[:, 128:256]
        if j < 2:
            q_ref[:, j * 256 : j * 256 + 128] = turned(one).astype(jnp.bfloat16)
            q_ref[:, j * 256 + 128 : (j + 1) * 256] = turned(two).astype(jnp.bfloat16)
        else:
            kv_ref[:, 0:128] = turned(one).astype(jnp.bfloat16)
            kv_ref[:, 128:256] = two.astype(jnp.bfloat16)

    for _ in mixer_chunks[1:]:
        tick()
    for m in mixer_chunks:
        gather.arrive(m)
        waited.add(m)
    fetch = pltpu.make_async_copy(fulls[1], mixer_w, fetch_sem.at[1])
    gather.store[1].wait()
    fetch.start()
    fetch.wait()

    def project(at):
        return dot_plain(normed_ref[...], mixer_w[:, :, :, at].reshape(width, -1))

    conv_width = inner + 2 * STATE
    rest = inner + conv_width

    def conv_block(j, _):
        value = project(pl.ds(pl.multiple_of(inner + j * 256, 256), 256)).astype(jnp.bfloat16)
        at = pl.ds(pl.multiple_of(j * 256, 256), 256)
        ext_ref[8:, at] = f32(value)
        rim_out[:, at] = value[span - 16 :]
        return 0

    lax.fori_loop(0, conv_width // 256, conv_block, 0)
    tick()
    step_ref[...] = jnp.zeros_like(step_ref)
    step_ref[:, 0:SSM_HEADS] = project(slice(rest, rest + SSM_HEADS))
    rim = remote(rim_out, rim_in, rim_s, rim_r, {"grp": lax.rem(grp + 1, 2 * chips)})
    pl.when(grp + 1 < 2 * chips)(rim.start)

    def gate_block(j, _):
        at = pl.ds(pl.multiple_of(j * 256, 256), 256)
        gate_ref[:, at] = project(at)
        return 0

    lax.fori_loop(0, inner // 256, gate_block, 0)
    tick()

    raw = step_ref[...] + heads_ref[0:1]
    dt_ref[...] = jnp.maximum(raw, 0.0) + jnp.log1p(jnp.exp(-jnp.abs(raw)))
    before = lax.broadcasted_iota(jnp.int32, (span, span), 0) >= lanes((span, span))
    running = lax.dot_general(
        jnp.where(before, 1.0, 0.0), dt_ref[...] * -jnp.exp(heads_ref[1:2]), (((1,), (0,)), ((), ())),
        precision=HIGHEST, preferred_element_type=jnp.float32,
    )
    run_ref[...] = running
    turned_run = running.T
    for head in range(SSM_HEADS):
        runt_ref[head] = turned_run[head : head + 1]
    final = running[span - 1 :]
    e_ref[...] = jnp.where(own_docs == prior, jnp.exp(running), 0.0)
    wd_ref[...] = jnp.where(own_docs == tail, jnp.exp(final - running), 0.0)
    carried = jnp.where(tail == prior, jnp.exp(final), 0.0)
    carried_ref[...] = jnp.broadcast_to(carried, (8, 128))
    for pair in range(SSM_HEADS // 2):
        at = pair * 128 % half
        car_ref[pair * 128 // half, :, at : at + 128] = pair_columns(carried_ref, pair)

    def rim_none():
        ext_ref[0:8, :] = jnp.zeros((8, conv_width), jnp.float32)

    def rim_some():
        rim.wait_recv()
        ext_ref[0:8, :] = f32(rim_in[8:16, :])

    pl.when(grp == 0)(rim_none)
    pl.when(grp > 0)(rim_some)

    def convolve(j, _):
        at = pl.ds(pl.multiple_of(j * 256, 256), 256)
        value = jnp.broadcast_to(taps[CONV : CONV + 1, at], (span, 256))
        for tap in range(CONV):
            term = ext_ref[5 + tap : 5 + tap + span, at] * taps[tap : tap + 1, at]
            if tap < CONV - 1:
                term = jnp.where(across(same[tap], 256) > 0.0, term, 0.0)
            value = value + term
        act_ref[:, at] = value / (1.0 + jnp.exp(-value))
        return 0

    lax.fori_loop(0, conv_width // 256, convolve, 0)
    tick()
    own_kv = remote(kv_ref, kvw_ref.at[0, core], kp_s.at[0], kp_r.at[0], partner)
    own_kv.start()
    kv_along = {}
    for k in range(1, reach + 1):
        kv_along[k] = remote(kv_ref, kvw_ref.at[k, core], ka_s.at[k], ka_r.at[k], ahead(k))
        pl.when(chip + k < chips)(kv_along[k].start)
    kvw_ref[0, core] = kv_ref[...]

    weight = wd_ref[...] * dt_ref[...]
    for pair in range(SSM_HEADS // 2):
        at = slice(pair * 128, (pair + 1) * 128)
        x_pair = act_ref[:, at]
        xdt[:, at] = (x_pair * pair_columns(dt_ref, pair)).astype(jnp.bfloat16)
        xw[:, at] = (x_pair * pair_columns(weight, pair)).astype(jnp.bfloat16)
    in_map = act_ref[:, inner : inner + STATE]
    out_map = act_ref[:, inner + STATE :]
    out_low = out_map.astype(jnp.bfloat16)
    in_turned = in_map.T.astype(jnp.bfloat16)
    for i in range(2):
        own_state[i] = dot_plain(in_turned, xw[:, i * half : (i + 1) * half])
    half_out[...] = own_state[1 - core].astype(jnp.bfloat16)
    align_heads(q_ref, qa, HEAD**-0.5)
    ot[...] = jnp.zeros_like(ot)
    total[...] = jnp.zeros_like(total)
    half_car = remote(car_ref.at[1 - core], car_in, ha_s.at[0], ha_r.at[0], partner)
    half_state = remote(half_out, half_in, ha_s.at[1], ha_r.at[1], partner)
    half_car.start()
    half_state.start()

    def attend_slot(keys, values, key_docs, causal):
        bias[...] = same_document(key_docs, own_row, causal)
        vt[...] = values.astype(jnp.float32).T.astype(jnp.bfloat16)

        def per_head(head, _):
            group = lax.div(head, HEADS // KV_HEADS)
            scores = dot_rows(keys[...], qa[head]) + bias[...]
            weights = jnp.exp(scores)
            total[head] += jnp.sum(weights, axis=0, keepdims=True)
            rows = pl.ds(pl.multiple_of(group * HEAD, HEAD), HEAD)
            into = pl.ds(pl.multiple_of(head * HEAD, HEAD), HEAD)
            ot[into, :] += dot_plain(vt[rows, :], weights.astype(jnp.bfloat16))
            return 0

        lax.fori_loop(0, HEADS, per_head, 0)

    def attend_ref(ref, key_docs, causal):
        attend_slot(ref.at[:, 0:128], ref[:, 128:256], key_docs, causal)

    attend_ref(kv_ref, segk_ref[2 * reach + core], True)
    tick()

    half_car.wait_recv()
    half_state.wait_recv()
    mine, theirs = own_state[core], half_in[...].astype(jnp.float32)
    car_mine, car_theirs = car_ref[core], car_in[...]
    first = core == 0
    car_0 = jnp.where(first, car_mine, car_theirs)
    car_1 = jnp.where(first, car_theirs, car_mine)
    state_0 = jnp.where(first, mine, theirs)
    state_1 = jnp.where(first, theirs, mine)
    chip_out[...] = (state_1 + car_1[0:1] * state_0).astype(jnp.bfloat16)
    chip_car[...] = car_0 * car_1

    for head in range(SSM_HEADS):
        runb[head] = jnp.broadcast_to(run_ref[:, head : head + 1], (span, 128))
    gram[...] = lax.dot_general(
        out_map, in_map, (((1,), (1,)), ((), ())), precision=HIGHEST,
        preferred_element_type=jnp.float32,
    )
    state_along = {}
    for k in range(1, reach + 1):
        state_along[k] = (
            remote(chip_out, chip_in.at[k], ca_s.at[k, 0], ca_r.at[k, 0], ahead(k)),
            remote(chip_car, chip_car_in.at[k], ca_s.at[k, 1], ca_r.at[k, 1], ahead(k)),
        )
        for copy in state_along[k]:
            pl.when(chip + k < chips)(copy.start)

    kv_pass = {}
    for k in range(1, reach + 1):
        place = kvw_ref.at[k, core]
        kv_pass[k] = remote(place, place, kp_s.at[k], kp_r.at[k], partner)

        def hand_on(k=k):
            kv_along[k].wait_recv()
            kv_pass[k].start()

        pl.when(chip - k >= 0)(hand_on)

    rows = lax.broadcasted_iota(jnp.int32, (span, span), 0)
    allowed = jnp.logical_and(
        across(segk_ref[2 * reach + core], span) == own_row, rows >= lanes((span, span))
    )
    bias[...] = jnp.where(allowed, 0.0, HIDDEN)

    def intra(quad, _):
        at = pl.ds(pl.multiple_of(quad * 256, 256), 256)
        value = jnp.zeros((span, 256), jnp.float32)
        for i in range(4):
            head = quad * 4 + i
            column = runb[head]
            spread = jnp.concatenate([column] * (span // 128), axis=1) - runt_ref[head]
            mixing = (jnp.exp(spread + bias[...]) * gram[...]).astype(jnp.bfloat16)
            part = dot_plain(mixing, xdt[:, at])
            value = jnp.where(lanes((span, 256)) // 64 == i, part, value)
        mixed_ref[:, at] = value + skip_lanes[0:1, at] * act_ref[:, at]
        return 0

    lax.fori_loop(0, SSM_HEADS // 4, intra, 0)
    tick()

    own_kv.wait_recv()
    for index, slot in enumerate(slot_plan(reach)):
        back, side = slot
        if slot == (1, 1):
            acc[...] = jnp.zeros_like(acc)
            for k in range(reach, 0, -1):

                def take(k=k):
                    for copy in state_along[k]:
                        copy.wait_recv()
                    acc[...] = chip_in[k].astype(jnp.float32) + chip_car_in[k, 0:1] * acc[...]

                pl.when(chip - k >= 0)(take)
            enter_0, enter_1 = acc[...], state_0 + car_0[0:1] * acc[...]
            ent_ref[core] = jnp.where(first, enter_0, enter_1)
            enter_out[...] = jnp.where(first, enter_1, enter_0)
            for k in range(1, reach + 1):
                pl.when(chip - k >= 0)(kv_pass[k].wait_recv)

        def visit(back=back, side=side):
            ref = kvw_ref.at[back, side]
            attend_ref(ref, segk_ref[2 * (reach - back) + side], False)

        pl.when(slot_live(slot, chip, core, reach))(visit)
        tick()
        if slot == (1, 1):
            enter_pass = remote(enter_out, ent_ref.at[core], en_s, en_r, partner)
            enter_pass.start()

    for head in range(HEADS):
        inverse = 1.0 / total[head]
        inv_ref[head] = inverse
        into = slice(head * HEAD, (head + 1) * HEAD)
        ot[into, :] = ot[into, :] * inverse
    attt_ref[...] = ot[...].astype(jnp.bfloat16)
    for pair in range(HEADS // 2):
        at = slice(pair * 128, (pair + 1) * 128)
        att_ref[:, at] = ot[at, :].T.astype(jnp.bfloat16)

    enter_pass.wait_recv()
    for i in range(2):
        carried_in = dot_plain(out_low, ent_ref[i].astype(jnp.bfloat16))
        for j in range(SSM_HEADS // 4):
            pair = i * (SSM_HEADS // 4) + j
            at = slice(pair * 128, (pair + 1) * 128)
            part = carried_in[:, j * 128 : (j + 1) * 128]
            mixed_ref[:, at] += pair_columns(e_ref, pair) * part

    run_out(gathering)
    gather.finish(waited)
    for copy in gather.store[2:]:
        copy.wait()
    own_kv.wait_send()
    pl.when(grp + 1 < 2 * chips)(rim.wait_send)
    half_car.wait_send()
    half_state.wait_send()
    enter_pass.wait_send()
    for k in range(1, reach + 1):

        def sent(k=k):
            kv_along[k].wait_send()
            for copy in state_along[k]:
                copy.wait_send()

        pl.when(chip + k < chips)(sent)
        pl.when(chip - k >= 0)(kv_pass[k].wait_send)


def run_forward(reach, gather, tokens, docs, heads, cosine, sine):
    chips, group = gather.chips, gather.group
    span, width = tokens.shape
    inner = SSM_HEADS * SSM_HEAD
    half, conv_width = inner // 2, inner + 2 * STATE
    kv_width = 2 * KV_HEADS * HEAD
    f32, low = jnp.float32, jnp.bfloat16
    shape = jax.ShapeDtypeStruct
    dma = pltpu.SemaphoreType.DMA
    vmem = pltpu.VMEM
    column = shape((span, 128), f32)
    outs = [
        shape((span, width), low),
        shape((span, HEADS * HEAD), low),
        shape((span, inner), f32),
        shape((span + 8, conv_width), f32),
        shape((span, conv_width), f32),
        column,
        column,
        column,
        shape((SSM_HEADS, 1, span), f32),
        column,
        column,
        shape((2, 8, half), f32),
        shape((8, 128), f32),
        shape((span, HEADS * HEAD), low),
        shape((HEADS * HEAD, span), low),
        shape((HEADS, 1, span), f32),
        shape((span, inner), f32),
        shape((2, STATE, half), f32),
        shape((reach + 1, 2, span, kv_width), low),
        shape((2 * (reach + 1), span, 128), f32),
        shape((group, *gather.pack.shape), low),
        shape((CONV - 1, span, 128), f32),
        shape((8, conv_width), f32),
        shape((8, width), f32),
    ]
    scratch = [
        vmem((span, kv_width), low),
        vmem((group, *gather.cut[0].shape), low),
        vmem((group, *gather.cut[1].shape), low),
        vmem((16, conv_width), low),
        vmem((16, conv_width), low),
        vmem((span + 8, 128), f32),
        vmem((8, inner), f32),
        vmem((HEADS, span, 128), low),
        vmem((span, span), f32),
        vmem((128, span), low),
        vmem((HEADS * HEAD, span), f32),
        vmem((HEADS, 1, span), f32),
        vmem((span, inner), low),
        vmem((span, inner), low),
        vmem((SSM_HEADS, span, 128), f32),
        vmem((span, span), f32),
        vmem((2, STATE, half), f32),
        vmem((STATE, half), low),
        vmem((STATE, half), low),
        vmem((8, half), f32),
        vmem((STATE, half), low),
        vmem((8, half), f32),
        vmem((reach + 1, STATE, half), low),
        vmem((reach + 1, 8, half), f32),
        vmem((STATE, half), f32),
        vmem((STATE, half), f32),
        dma((2,)),
        dma,
        dma,
        dma((reach + 1,)),
        dma((reach + 1,)),
        dma((reach + 1,)),
        dma((reach + 1,)),
        dma((2,)),
        dma((2,)),
        dma((reach + 1, 2)),
        dma((reach + 1, 2)),
        dma,
        dma,
    ]
    vm, anywhere = pl.BlockSpec(memory_space=pltpu.VMEM), pl.BlockSpec(memory_space=pl.ANY)
    many = len(gather.cut)
    results = pl.pallas_call(
        functools.partial(forward_kernel, reach, gather),
        out_shape=[*outs, *gather.outs()],
        in_specs=[vm] * 6 + [anywhere] * many,
        out_specs=[vm] * len(outs) + [anywhere] * many,
        scratch_shapes=[*scratch, *gather.scratch()],
        compiler_params=pltpu.CompilerParams(
            collective_id=2, has_side_effects=True, vmem_limit_bytes=VMEM_LIMIT
        ),
        name="run_forward",
    )(tokens, gather.pack, docs, heads, cosine, sine, *gather.cut)
    full = [part.reshape(-1, part.shape[-1]) for part in results[len(outs) :]]
    return results[: len(outs)], full


def mix_backward_kernel(reach, plan, *refs):
    chips, extras = plan.chips, plan.extras
    many = len(plan.chunks)
    cut = [18, len(plan.operands()), 5, many, 44]
    groups = []
    for size in cut:
        groups.append(refs[:size])
        refs = refs[size:]
    (
        q_ref,
        kvw_ref,
        segc_ref,
        segr_ref,
        act_ref,
        dt_ref,
        run_ref,
        runt_ref,
        e_ref,
        wd_ref,
        car_ref,
        skip_ref,
        attt_ref,
        inv_ref,
        ent_ref,
        gout_ref,
        gmix_ref,
        rate_ref,
    ) = groups[0]
    (
        dq_ref,
        dkv_ref,
        dact_ref,
        ddt_ref,
        heads_ref,
    ) = groups[2]
    (
        qa,
        da,
        bias,
        kt,
        dqt,
        centre,
        dk,
        dv,
        part_out,
        part_in,
        sum_out,
        sum_in,
        xdt,
        xw,
        ge,
        runb,
        gramt,
        dgram,
        own_grad,
        half_out,
        half_in,
        car_in,
        chip_out,
        chip_car,
        chip_in,
        chip_car_in,
        later_out,
        later,
        acc,
        qrow,
        qcol,
        dxdt,
        sums,
        fold_ref,
        pp_s,
        pp_r,
        pa_s,
        pa_r,
        ha_s,
        ha_r,
        ca_s,
        ca_r,
        la_s,
        la_r,
    ) = groups[4]
    me = seat()
    rep, reps = lax.axis_index("rep"), lax.axis_size("rep")
    beyond = [{"rep": lax.rem(rep + 4 * e, reps)} for e in range(1, extras)]
    reduction = plan.steps(me, groups[1], groups[3], refs)
    chip, core = axis_seat()
    grp = lax.axis_index("grp")
    span = q_ref.shape[0]
    inner = SSM_HEADS * SSM_HEAD
    half = inner // 2
    low = jnp.bfloat16
    partner = {"grp": chip * 2 + 1 - core}
    first = core == 0

    def behind(k):
        return {"grp": lax.rem(grp - 2 * k + 2 * chips, 2 * chips)}

    greet_group([me["x"], me["y"], *beyond])
    for _ in plan.lefts:
        next(reduction)
    in_map = act_ref[:, inner : inner + STATE]
    out_map = act_ref[:, inner + STATE :]
    in_low, out_low = in_map.astype(low), out_map.astype(low)
    weight = wd_ref[...] * dt_ref[...]
    for pair in range(SSM_HEADS // 2):
        at = slice(pair * 128, (pair + 1) * 128)
        x_pair = act_ref[:, at]
        ge[:, at] = (gmix_ref[:, at] * pair_columns(e_ref, pair)).astype(low)
        xdt[:, at] = (x_pair * pair_columns(dt_ref, pair)).astype(low)
        xw[:, at] = (x_pair * pair_columns(weight, pair)).astype(low)
    out_turned = out_map.T.astype(low)
    for i in range(2):
        own_grad[i] = dot_plain(out_turned, ge[:, i * half : (i + 1) * half])
    half_out[...] = own_grad[1 - core].astype(low)
    align_heads(q_ref, qa, HEAD**-0.5)
    align_heads(gout_ref, da, 1.0)
    half_car = remote(car_ref.at[1 - core], car_in, ha_s.at[0], ha_r.at[0], partner)
    half_grad = remote(half_out, half_in, ha_s.at[1], ha_r.at[1], partner)
    half_car.start()
    half_grad.start()

    next(reduction, None)
    next(reduction, None)
    for pair in range(HEADS // 2):
        at = slice(pair * 128, (pair + 1) * 128)
        product = gout_ref[:, at].astype(jnp.float32).T * attt_ref[at, :].astype(jnp.float32)
        for odd in range(2):
            rows = product[odd * HEAD : (odd + 1) * HEAD]
            centre[2 * pair + odd] = jnp.sum(rows, axis=0, keepdims=True)
    dqt[...] = jnp.zeros_like(dqt)

    def attend_back(ref, key_docs, causal):
        bias[...] = same_document(key_docs, segr_ref[...], causal)
        kt[...] = ref[:, 0:128].astype(jnp.float32).T.astype(low)
        dk[...] = jnp.zeros_like(dk)
        dv[...] = jnp.zeros_like(dv)

        def per_head(head, _):
            group = lax.div(head, HEADS // KV_HEADS)
            scores = dot_rows(ref[:, 0:128], qa[head]) + bias[...]
            probs = jnp.exp(scores) * inv_ref[head]
            grad_probs = dot_rows(ref[:, 128:256], da[head])
            grad_scores = (probs * (grad_probs - centre[head])).astype(low)
            dv[...] += dot_plain(probs.astype(low), da[head])
            dk[...] += dot_plain(grad_scores, qa[head])
            rows = pl.ds(pl.multiple_of(group * HEAD, HEAD), HEAD)
            into = pl.ds(pl.multiple_of(head * HEAD, HEAD), HEAD)
            dqt[into, :] += dot_plain(kt[rows, :], grad_scores)
            return 0

        lax.fori_loop(0, HEADS // 2, per_head, 0)
        lax.fori_loop(HEADS // 2, HEADS, per_head, 0)

    passed, sent_on = {}, {}

    def pass_slot(back, side):
        live = slot_live((back, side), chip, core, reach)

        def compute():
            attend_back(kvw_ref.at[back, side], segc_ref[2 * (reach - back) + side], False)
            part_out[back, side, :, 0:128] = dk[...].astype(low)
            part_out[back, side, :, 128:256] = dv[...].astype(low)

        pl.when(live)(compute)

    def start_part(back):
        for side in (0, 1):
            passed[back, side] = remote(
                part_out.at[back, side],
                part_in.at[back],
                pp_s.at[back],
                pp_r.at[back],
                partner,
            )
            live = slot_live((back, side), chip, core, reach)
            pl.when(jnp.logical_and(live, core != side))(passed[back, side].start)

    def send_sum(back):
        both = chip - back >= 0
        partner_has = jnp.logical_and(both, core == 1) if back == reach else both

        def add_partner():
            passed[back, 0].wait_recv()
            value = part_out[back, core].astype(jnp.float32) + part_in[back].astype(jnp.float32)
            sum_out[back] = value.astype(low)

        pl.when(partner_has)(add_partner)
        if back == reach:

            def alone():
                sum_out[back] = part_out[back, core]

            pl.when(jnp.logical_and(both, core == 0))(alone)

    def send_sum_start(back):
        sent_on[back] = remote(
            sum_out.at[back], sum_in.at[back], pa_s.at[back], pa_r.at[back], behind(back)
        )
        pl.when(chip - back >= 0)(sent_on[back].start)

    next(reduction, None)
    pass_slot(reach, 1)
    next(reduction, None)

    half_car.wait_recv()
    half_grad.wait_recv()
    mine, theirs = own_grad[core], half_in[...].astype(jnp.float32)
    car_mine, car_theirs = car_ref[core], car_in[...]
    car_0 = jnp.where(first, car_mine, car_theirs)
    car_1 = jnp.where(first, car_theirs, car_mine)
    grad_0 = jnp.where(first, mine, theirs)
    grad_1 = jnp.where(first, theirs, mine)
    chip_out[...] = (grad_0 + car_0[0:1] * grad_1).astype(low)
    chip_car[...] = car_0 * car_1
    pass_slot(reach, 0)
    next(reduction, None)
    state_along = {}
    for k in range(1, reach + 1):
        state_along[k] = (
            remote(chip_out, chip_in.at[k], ca_s.at[k, 0], ca_r.at[k, 0], behind(k)),
            remote(chip_car, chip_car_in.at[k], ca_s.at[k, 1], ca_r.at[k, 1], behind(k)),
        )
        for copy in state_along[k]:
            pl.when(chip - k >= 0)(copy.start)
    start_part(reach)
    for back in range(reach - 1, 0, -1):
        pass_slot(back, 1)
        next(reduction, None)
        send_sum(back + 1)
        pass_slot(back, 0)
        next(reduction, None)
        send_sum_start(back + 1)
        start_part(back)
    pass_slot(0, 0)
    next(reduction, None)
    start_part(0)
    send_sum(1)

    for head in range(SSM_HEADS):
        runb[head] = jnp.broadcast_to(run_ref[:, head : head + 1], (span, 128))
    send_sum_start(1)
    bias[...] = same_document(segc_ref[2 * reach + core], segr_ref[...], True)
    gramt[...] = lax.dot_general(
        in_map, out_map, (((1,), (1,)), ((), ())), precision=HIGHEST,
        preferred_element_type=jnp.float32,
    )
    dgram[...] = jnp.zeros_like(dgram)
    qcol[...] = jnp.zeros_like(qcol)
    qrow[...] = jnp.zeros_like(qrow)
    heads_of = lax.broadcasted_iota(jnp.int32, (inner, 128), 0) // SSM_HEAD
    fold_ref[...] = jnp.where(heads_of == lanes((inner, 128)), 1.0, 0.0).astype(low)

    def intra(quad, _):
        at = pl.ds(pl.multiple_of(quad * 256, 256), 256)
        grads = gmix_ref[:, at].astype(low)
        inputs = xdt[:, at]
        place = lanes((span, 256)) // 64
        value = jnp.zeros((span, 256), jnp.float32)
        for i in range(4):
            head = quad * 4 + i
            column = runb[head]
            spread = runt_ref[head] - jnp.concatenate([column] * (span // 128), axis=1)
            decay = jnp.exp(spread + bias[...])
            mixing = decay * gramt[...]
            alone = jnp.where(place == i, inputs, jnp.zeros_like(inputs))
            grad_mixing = dot_rows(alone, grads)
            dgram[...] += decay * grad_mixing
            product = mixing * grad_mixing
            qrow[pl.ds(head, 1), :] = jnp.sum(product, axis=0, keepdims=True)
            by_row = jnp.sum(product, axis=1, keepdims=True)
            qcol[...] = jnp.where(lanes((span, 128)) == head, by_row, qcol[...])
            part = dot_plain(mixing.astype(low), grads)
            value = jnp.where(place == i, part, value)
        dxdt[:, at] = value
        return 0

    for quad in range(SSM_HEADS // 4):
        lax.fori_loop(quad, quad + 1, intra, 0)
        next(reduction, None)

    acc[...] = jnp.zeros_like(acc)
    for k in range(reach, 0, -1):

        def take(k=k):
            for copy in state_along[k]:
                copy.wait_recv()
            acc[...] = chip_in[k].astype(jnp.float32) + chip_car_in[k, 0:1] * acc[...]

        pl.when(chip + k < chips)(take)
    later_1, later_0 = acc[...], grad_1 + car_1[0:1] * acc[...]
    later[core] = jnp.where(first, later_0, later_1)
    later_out[...] = jnp.where(first, later_1, later_0)

    attend_back(kvw_ref.at[0, core], segc_ref[2 * reach + core], True)
    next(reduction, None)
    later_pass = remote(later_out, later.at[core], la_s, la_r, partner)
    later_pass.start()
    for pair in range(HEADS // 2):
        at = slice(pair * 128, (pair + 1) * 128)
        dq_ref[:, at] = dqt[at, :].T * HEAD**-0.5

    dkv_ref[:, 0:128] = dk[...]
    dkv_ref[:, 128:256] = dv[...]

    def add_zero():
        passed[0, 0].wait_recv()
        dkv_ref[...] += part_in[0].astype(jnp.float32)

    pl.when(core == 0)(add_zero)
    for k in range(1, reach + 1):

        def add_ahead(k=k):
            sent_on[k].wait_recv()
            dkv_ref[...] += sum_in[k].astype(jnp.float32)

        pl.when(chip + k < chips)(add_ahead)

    grad_low = dgram[...].astype(low)
    grad_in = dot_plain(grad_low, out_low)
    grad_out = dot_plain(dgram[...].T.astype(low), in_low)
    later_pass.wait_recv()

    def fold(value, own):
        high = value.astype(low)
        rest = (value - high.astype(jnp.float32)).astype(low)
        return dot_plain(high, fold_ref[own, :]) + dot_plain(rest, fold_ref[own, :])

    carried = jnp.zeros((1, 128), jnp.float32)
    skip_sum = jnp.zeros((8, 128), jnp.float32)
    x_inside, x_part, g_reached = (jnp.zeros((span, 128), jnp.float32) for _ in range(3))
    for i in range(2):
        entering = ent_ref[i]
        grads = later[i]
        own = slice(i * half, (i + 1) * half)
        by_lane = jnp.sum(entering * grads, axis=0, keepdims=True)
        carried = carried + fold(jnp.broadcast_to(by_lane, (8, half)), own)[0:1]
        enter_low, later_low = entering.astype(low), grads.astype(low)
        grad_out = grad_out + dot_rows(ge[:, own], enter_low)
        grad_in = grad_in + dot_rows(xw[:, own], later_low)
        reached = dot_plain(out_low, enter_low)
        grad_xw = dot_plain(in_low, later_low)
        for j in range(SSM_HEADS // 4):
            pair = i * (SSM_HEADS // 4) + j
            at = slice(pair * 128, (pair + 1) * 128)
            here = slice(j * 128, (j + 1) * 128)
            x_pair, g_pair = act_ref[:, at], gmix_ref[:, at]
            part = grad_xw[:, here]
            inside = dxdt[:, at]
            dact_ref[:, at] = (
                skip_ref[:, at] * g_pair
                + pair_columns(dt_ref, pair) * inside
                + pair_columns(weight, pair) * part
            )
            sums[0, :, here] = x_pair * inside
            sums[1, :, here] = x_pair * part
            sums[2, :, here] = g_pair * reached[:, here]
            sums[3, :, here] = x_pair * g_pair
        x_inside, x_part, g_reached = (
            total + fold(sums[n], own) for n, total in enumerate((x_inside, x_part, g_reached))
        )
        by_lane = jnp.sum(sums[3], axis=0, keepdims=True)
        skip_sum = skip_sum + fold(jnp.broadcast_to(by_lane, (8, half)), own)
    dact_ref[:, inner : inner + STATE] = grad_in
    dact_ref[:, inner + STATE :] = grad_out

    w_part = weight * x_part
    drun = qrow[...].T - qcol[...] + e_ref[...] * g_reached - w_part
    last = jnp.sum(w_part, axis=0, keepdims=True) + rate_ref[1:2] * carried
    rows = lax.broadcasted_iota(jnp.int32, (span, 128), 0)
    drun = jnp.where(rows == span - 1, drun + last, drun)
    upper = lax.broadcasted_iota(jnp.int32, (span, span), 0) <= lanes((span, span))
    drate = lax.dot_general(
        jnp.where(upper, 1.0, 0.0), drun, (((1,), (0,)), ((), ())), precision=HIGHEST,
        preferred_element_type=jnp.float32,
    )
    rate = rate_ref[0:1]
    ddt_ref[...] = x_inside + wd_ref[...] * x_part + rate * drate
    heads_ref[...] = jnp.zeros_like(heads_ref)
    heads_ref[0:1] = jnp.sum(rate * dt_ref[...] * drate, axis=0, keepdims=True)
    heads_ref[1:2] = skip_sum[0:1]

    run_out(reduction)
    half_car.wait_send()
    half_grad.wait_send()
    later_pass.wait_send()
    for k in range(1, reach + 1):

        def sent(k=k):
            sent_on[k].wait_send()
            for copy in state_along[k]:
                copy.wait_send()

        pl.when(chip - k >= 0)(sent)
    for back in range(reach + 1):
        for side in (0, 1):
            if (back, side) in ((0, 1),):
                continue
            live = slot_live((back, side), chip, core, reach)
            pl.when(jnp.logical_and(live, core != side))(passed[back, side].wait_send)


def mix_backward(reach, operands, plan):
    sums = plan.outs()
    chips = lax.axis_size("grp") // 2
    span = operands[0].shape[0]
    inner = SSM_HEADS * SSM_HEAD
    half = inner // 2
    kv_width = 2 * KV_HEADS * HEAD
    f32, low = jnp.float32, jnp.bfloat16
    shape = jax.ShapeDtypeStruct
    dma = pltpu.SemaphoreType.DMA
    vmem = pltpu.VMEM
    outs = [
        shape((span, HEADS * HEAD), f32),
        shape((span, kv_width), f32),
        shape((span, inner + 2 * STATE), f32),
        shape((span, 128), f32),
        shape((8, 128), f32),
    ]
    scratch = [
        vmem((HEADS, span, 128), low),
        vmem((HEADS, span, 128), low),
        vmem((span, span), f32),
        vmem((128, span), low),
        vmem((HEADS * HEAD, span), f32),
        vmem((HEADS, 1, span), f32),
        vmem((span, 128), f32),
        vmem((span, 128), f32),
        vmem((reach + 1, 2, span, kv_width), low),
        vmem((reach + 1, span, kv_width), low),
        vmem((reach + 1, span, kv_width), low),
        vmem((reach + 1, span, kv_width), low),
        vmem((span, inner), low),
        vmem((span, inner), low),
        vmem((span, inner), low),
        vmem((SSM_HEADS, span, 128), f32),
        vmem((span, span), f32),
        vmem((span, span), f32),
        vmem((2, STATE, half), f32),
        vmem((STATE, half), low),
        vmem((STATE, half), low),
        vmem((8, half), f32),
        vmem((STATE, half), low),
        vmem((8, half), f32),
        vmem((reach + 1, STATE, half), low),
        vmem((reach + 1, 8, half), f32),
        vmem((STATE, half), f32),
        vmem((2, STATE, half), f32),
        vmem((STATE, half), f32),
        vmem((128, span), f32),
        vmem((span, 128), f32),
        vmem((span, inner), f32),
        vmem((4, span, half), f32),
        vmem((inner, 128), low),
        dma((reach + 1,)),
        dma((reach + 1,)),
        dma((reach + 1,)),
        dma((reach + 1,)),
        dma((2,)),
        dma((2,)),
        dma((reach + 1, 2)),
        dma((reach + 1, 2)),
        dma,
        dma,
    ]
    results = pl.pallas_call(
        functools.partial(mix_backward_kernel, reach, plan),
        out_shape=[*outs, *sums],
        in_specs=[pl.BlockSpec(memory_space=pltpu.VMEM)] * (len(operands) + len(plan.operands())),
        out_specs=[pl.BlockSpec(memory_space=pltpu.VMEM)] * (len(outs) + len(sums)),
        scratch_shapes=[*scratch, *plan.scratch()],
        compiler_params=pltpu.CompilerParams(
            collective_id=3, has_side_effects=True, vmem_limit_bytes=VMEM_LIMIT
        ),
        name="mix_backward",
    )(*operands, *plan.operands())
    return results[: len(outs)], results[len(outs) :]


def shards(
    tokens,
    segments,
    input_gain,
    attention_in,
    attention_out,
    mixer_in,
    filter_taps,
    filter_bias,
    step_bias,
    decay_log,
    skip_scale,
    mixer_gain,
    mixer_out,
    feed_gain,
    gate_up,
    down_proj,
    cotangent,
):
    seq_count, span_len, model_width = tokens.shape
    row_count = seq_count * span_len
    seq_len = segments.shape[1]
    group_devices = lax.axis_size("grp")
    position = lax.axis_index("grp") * span_len
    inner_width = SSM_HEADS * SSM_HEAD
    xbc_width = inner_width + 2 * STATE
    query_width = HEADS * HEAD
    kv_width = KV_HEADS * HEAD
    rim_rows = CONV - 1
    def padded(value):
        return jnp.pad(value, ((0, 0), (0, 256 - value.shape[1])))

    small = [filter_taps] + [p[None] for p in (filter_bias, input_gain, mixer_gain, feed_gain)]
    pack = jnp.concatenate([padded(part) for part in small])
    shares = [attention_in, mixer_in, gate_up, down_proj, mixer_out, attention_out]
    gather = Gather(
        shares,
        [
            column_chunks(n, n, share.shape[1], pieces)[i][1:]
            for n, (share, pieces) in enumerate(zip(shares, (1, 4, 4, 2, 2, 1)))
            for i in range(pieces)
        ],
        pack,
    )
    offsets = position + jnp.arange(span_len, dtype=jnp.int32)
    cosine_table, sine_table = rope_tables(offsets, HEAD)
    cosine = jnp.concatenate([cosine_table] * 4, axis=1)
    sine = jnp.concatenate([-sine_table, sine_table] * 2, axis=1)
    reach = min(seq_len // (4 * span_len), group_devices // 2 - 1)
    chip = lax.axis_index("grp") // 2
    docs = jnp.concatenate([jnp.full((2 * reach * span_len,), -1, jnp.int32), segments[0]])
    window = lax.dynamic_slice_in_dim(docs, 2 * chip * span_len, 2 * (reach + 1) * span_len)
    window = window.reshape(2 * (reach + 1), 1, span_len).astype(jnp.float32)
    own_docs = lax.dynamic_slice_in_dim(segments[0], position, span_len)
    heads_rows = jnp.stack([step_bias, decay_log, skip_scale])
    heads_rows = jnp.pad(heads_rows, ((0, 5), (0, 128 - SSM_HEADS)))
    results, full = run_forward(
        reach,
        gather,
        tokens[0],
        window,
        heads_rows,
        cosine,
        sine,
    )
    full_attn_in, full_mix_in, full_gate_up, full_down, full_mix_out, full_attn_out = full
    (
        normed_low,
        query_rows,
        gate_part,
        ext_rows,
        active,
        step_wide,
        steps,
        running,
        running_turned,
        enter_decay,
        tail_decay,
        carried_lanes,
        carried,
        attended,
        attended_turned,
        inverse_total,
        mixed,
        entering,
        kv_window,
        key_docs,
        packs,
        same_docs,
        taps_wide,
        gain_in,
    ) = results
    full_mix_gain, full_feed_gain = (
        packs[:, 6 + i, : part.shape[0]].reshape(-1) for i, part in enumerate((mixer_gain, feed_gain))
    )
    token_float = tokens.reshape(row_count, model_width).astype(jnp.float32)
    back_attn_in, back_attn_out, back_mix_in = full_attn_in, full_attn_out, full_mix_in
    back_mix_out, back_gate_up, back_down = full_mix_out, full_gate_up, full_down
    gate_part, mixed = gate_part[None], mixed[None]
    rate_scale = -jnp.exp(decay_log)
    recurrence = (
        active,
        steps,
        running,
        running_turned,
        enter_decay,
        tail_decay,
        carried_lanes,
        jnp.repeat(skip_scale, SSM_HEAD)[None, :],
    )
    normed_mix, gate_back = jax.vjp(gated_norm, mixed, gate_part, full_mix_gain.astype(jnp.float32))
    normed_mix_low = normed_mix.reshape(row_count, inner_width).astype(jnp.bfloat16)
    hidden = (
        token_float
        + jnp.dot(attended, full_attn_out, preferred_element_type=jnp.float32)
        + jnp.dot(normed_mix_low, full_mix_out, preferred_element_type=jnp.float32)
    )
    normed_feed, feed_back = jax.vjp(rms_scale, hidden, full_feed_gain.astype(jnp.float32))
    normed_feed_low = normed_feed.astype(jnp.bfloat16)
    gate_vals = jnp.dot(normed_feed_low, full_gate_up, preferred_element_type=jnp.float32)
    activation, act_back = jax.vjp(swiglu, gate_vals[:, :FF], gate_vals[:, FF:])
    activation_low = activation.astype(jnp.bfloat16)
    out_rows = (
        hidden + jnp.dot(activation_low, full_down, preferred_element_type=jnp.float32)
    ).astype(jnp.bfloat16)
    grad_rows = cotangent.reshape(row_count, model_width)
    grad_act = jnp.dot(grad_rows, back_down.T, preferred_element_type=jnp.float32)
    grad_gate, grad_upper = act_back(grad_act)
    grad_gu = jnp.concatenate([grad_gate, grad_upper], axis=-1).astype(jnp.bfloat16)
    grad_feed_in = jnp.dot(grad_gu, back_gate_up.T, preferred_element_type=jnp.float32)
    grad_hidden_norm, grad_feed = feed_back(grad_feed_in)
    grad_hidden = grad_rows.astype(jnp.float32) + grad_hidden_norm
    grad_hidden_low = grad_hidden.astype(jnp.bfloat16)
    grad_attended = jnp.dot(
        grad_hidden_low, back_attn_out.T, preferred_element_type=jnp.float32
    ).astype(jnp.bfloat16)
    grad_normed_mix = jnp.dot(grad_hidden_low, back_mix_out.T, preferred_element_type=jnp.float32)
    grad_mixed, grad_gate_part, grad_mix_gain = gate_back(
        grad_normed_mix.reshape(seq_count, span_len, inner_width)
    )
    heads_scale = jnp.stack([rate_scale, carried[0, :SSM_HEADS]])
    heads_scale = jnp.pad(heads_scale, ((0, 6), (0, 128 - SSM_HEADS)))
    operands = (
        query_rows,
        kv_window,
        key_docs,
        own_docs[None, :].astype(jnp.float32),
        *recurrence,
        attended_turned,
        inverse_total,
        entering,
        grad_attended,
        grad_mixed.reshape(row_count, inner_width),
        heads_scale,
    )
    early = GradPlan(
        [normed_feed_low, activation_low, normed_mix_low, attended_turned],
        [False, False, False, True],
        [grad_gu, grad_rows, grad_hidden_low],
        [
            *column_chunks(0, 0, 2 * FF, 4),
            *column_chunks(1, 1, model_width, 2),
            *column_chunks(2, 2, model_width, 2),
            (3, 2, 0, model_width),
        ],
        handed=HANDED,
    )
    (grad_query, grad_kv_own, grad_active, grad_steps, grad_heads), early_sums = mix_backward(
        reach, operands, early
    )
    late = GradPlan(
        [normed_low],
        [False],
        [
            grad_gate_part.reshape(row_count, inner_width).astype(jnp.bfloat16),
            jax.ShapeDtypeStruct((row_count, xbc_width + SSM_HEADS), jnp.bfloat16),
            jax.ShapeDtypeStruct((row_count, attention_in.shape[1]), jnp.bfloat16),
        ],
        [
            *column_chunks(0, 0, inner_width, 2),
            (0, 2, 0, attention_in.shape[1]),
            *column_chunks(0, 1, xbc_width + SSM_HEADS, CONV_PIECES),
        ],
        later=(1, 2),
        received=early_sums[len(early_sums) - HANDED :],
    )
    done, own = len(early_sums) - HANDED, 3 + CONV_PIECES
    place = [*range(done), *range(done + own, done + own + HANDED)]
    joins = (
        place[:4],
        place[4:6],
        place[6:8],
        place[8:],
        [done, done + 1, *range(done + 3, done + own)],
        [done + 2],
    )
    grad_token, summed, joined = run_tail(
        late,
        early_sums[:done],
        joins,
        grad_active,
        grad_steps,
        grad_query,
        grad_kv_own,
        ext_rows,
        step_wide,
        heads_rows,
        taps_wide,
        same_docs,
        cosine,
        sine,
        tokens[0],
        gain_in,
        grad_hidden,
        grad_heads,
        grad_feed[None],
        grad_mix_gain[None],
        full_mix_in,
        full_attn_in,
    )
    index = lax.axis_index("grp")

    def own_part(value):
        size = value.shape[-1] // group_devices
        return lax.dynamic_slice_in_dim(value, index * size, size, value.ndim - 1)

    own_gate_up, own_down, own_mix_out, own_attn_out, own_mix_in, own_attn_in = joined
    return (
        out_rows.reshape(seq_count, span_len, model_width),
        grad_token.reshape(seq_count, span_len, model_width),
        own_part(summed[7, :model_width]),
        own_attn_in,
        own_attn_out,
        own_mix_in,
        own_part(summed[:CONV]),
        own_part(summed[CONV]),
        *(summed[7, model_width + 128 * i :][:SSM_HEADS] for i in range(3)),
        own_part(summed[5, :inner_width]),
        own_mix_out,
        own_part(summed[6, :model_width]),
        own_gate_up,
        own_down,
    )


def solution(mesh):
    return jax.shard_map(
        shards,
        mesh=mesh,
        in_specs=(
            P("rep", "grp", None),
            P("rep", None),
            P("grp"),
            P("grp", None),
            P("grp", None),
            P("grp", None),
            P(None, "grp"),
            P("grp"),
            P(),
            P(),
            P(),
            P("grp"),
            P("grp", None),
            P("grp"),
            P("grp", None),
            P("grp", None),
            P("rep", "grp", None),
        ),
        out_specs=(
            P("rep", "grp", None),
            P("rep", "grp", None),
            P("grp"),
            P("grp", None),
            P("grp", None),
            P("grp", None),
            P(None, "grp"),
            P("grp"),
            P(),
            P(),
            P(),
            P("grp"),
            P("grp", None),
            P("grp"),
            P("grp", None),
            P("grp", None),
        ),
        check_vma=False,
    )
```

```python
import functools
import itertools
import math
from functools import partial

import jax
import jax.numpy as jnp
from jax import lax
from jax.experimental import pallas as pl
from jax.experimental.pallas import tpu as pltpu
from jax.sharding import PartitionSpec as P

HEADS = 8
KV_HEADS = 2
HEAD = 64
SSM_HEADS = 24
SSM_HEAD = 64
STATE = 128
CONV = 4
FF = 2048


NORM_EPS = 1e-05
ROPE_BASE = 100000000000.0
HIGHEST = lax.Precision.HIGHEST


def rms_scale(values, scales):
    return values * lax.rsqrt(jnp.mean(values * values, axis=-1, keepdims=True) + NORM_EPS) * scales


def rope_tables(positions, head_width):
    indices = jnp.arange(head_width // 2, dtype=jnp.float32)
    frequency = ROPE_BASE ** (-2.0 * indices / head_width)
    angles = positions.astype(jnp.float32)[:, None] * frequency[None, :]
    return (jnp.cos(angles), jnp.sin(angles))


def gated_norm(mixed, gate_part, scales):
    flat_mixed = mixed.reshape(gate_part.shape)
    return rms_scale(flat_mixed * jax.nn.silu(gate_part), scales)


def swiglu(gate_vals, up_vals):
    return jax.nn.silu(gate_vals) * up_vals


MESH = pl.DeviceIdType.MESH
HIDDEN = -1e30
VMEM_LIMIT = 67043328
TAIL_LAG = 1
WINDOW = 2
HANDED = 4
CONV_PIECES = 2
LAST_TICKS = (2, 5)


def seat():
    rep, grp = lax.axis_index("rep"), lax.axis_index("grp")
    chips = lax.axis_size("grp") // 2
    quarter = lax.rem(rep, 4)
    base = rep - quarter
    flip_x = quarter + 1 - 2 * lax.rem(quarter, 2)
    flip_y = lax.rem(quarter + 2, 4)
    chip, core = lax.div(grp, 2), lax.rem(grp, 2)
    return dict(
        quarter=quarter,
        qx=flip_x,
        qy=flip_y,
        qd=lax.rem(flip_x + 2, 4),
        chip=chip,
        core=core,
        x={"rep": base + flip_x},
        y={"rep": base + flip_y},
        partner={"grp": chip * 2 + 1 - core},
        along=[{"grp": lax.rem(chip + k, chips) * 2 + core} for k in range(chips)],
        chip_to=[lax.rem(chip + k, chips) for k in range(chips)],
        chip_from=[lax.rem(chip - k + chips, chips) for k in range(chips)],
    )


def remote(source, target, sent, arrived, device):
    return pltpu.make_async_remote_copy(
        src_ref=source,
        dst_ref=target,
        send_sem=sent,
        recv_sem=arrived,
        device_id=device,
        device_id_type=MESH,
    )


def greet(me, extra=()):
    barrier = pltpu.get_barrier_semaphore()
    others = [me["x"], me["y"], me["partner"], *me["along"][1:], *extra]
    for device in others:
        pl.semaphore_signal(barrier, inc=1, device_id=device, device_id_type=MESH)
    pl.semaphore_wait(barrier, len(others))


def near_first(chips):
    return sorted(range(1, chips), key=lambda k: min(k, chips - k))


class Gather:
    def __init__(self, shards, chunks, pack):
        self.group = lax.axis_size("grp")
        self.chips = self.group // 2
        self.cut = [s.reshape(4, s.shape[0] // 4, s.shape[1]) for s in shards]
        self.chunks = chunks
        self.pack = pack

    def outs(self):
        shape = jax.ShapeDtypeStruct
        return [shape((self.group, *part.shape), part.dtype) for part in self.cut]

    def scratch(self):
        dma = pltpu.SemaphoreType.DMA
        count = len(self.chunks) + 1
        own = [pltpu.VMEM(part.shape, part.dtype) for part in self.cut]
        return [*own, *[dma((count, self.chips))] * 10, dma((len(self.cut), 2))]

    def steps(self, me, ins, pack, packs, outs, scratch):
        chips, count = self.chips, len(self.chunks)
        own_copy = scratch[: len(ins)]
        zs, zr, xs, xr, ys, yr, ds, dr, cs, cr, ls = scratch[len(ins) :]
        own = me["chip"] * 2 + me["core"]
        order = near_first(chips)
        along, over_x, over_y, diagonal, self.across = {}, {}, {}, {}, {}

        def part(m, ref):
            n, start, width = self.chunks[m]
            return ref if width == outs[n].shape[-1] else ref.at[..., start : start + width]

        def weight(m):
            return self.chunks[m][0]

        def start_along(m):
            source = part(m, ins[weight(m)].at[me["quarter"]])
            place = part(m, outs[weight(m)].at[own, me["quarter"]])
            for k in order:
                along[m, k] = remote(source, place, zs.at[m, k], zr.at[m, k], me["along"][k])
                along[m, k].start()

        def block(m, k):
            return outs[weight(m)].at[me["chip_from"][k] * 2 + me["core"]]

        for k in order:
            along[count, k] = remote(
                pack, packs.at[own], zs.at[count, k], zr.at[count, k], me["along"][k]
            )
            along[count, k].start()
        self.across[count, 0] = remote(
            pack, packs.at[own], cs.at[count, 0], cr.at[count, 0], me["partner"]
        )
        self.across[count, 0].start()
        packs[own] = pack[...]
        for m in range(min(WINDOW, count)):
            start_along(m)
        load, store = [], []
        for n in range(len(ins)):
            load.append(pltpu.make_async_copy(ins[n], own_copy[n], ls.at[n, 0]))
            load[-1].start()
        for m in range(count):
            source, place = part(m, ins[weight(m)]), part(m, outs[weight(m)].at[own])
            self.across[m, 0] = remote(source, place, cs.at[m, 0], cr.at[m, 0], me["partner"])
            self.across[m, 0].start()
        for n in range(len(ins)):
            load[n].wait()
            store.append(pltpu.make_async_copy(own_copy[n], outs[n].at[own], ls.at[n, 1]))
            store[-1].start()
        for k in order:
            along[count, k].wait_recv()
            piece = packs.at[me["chip_from"][k] * 2 + me["core"]]
            self.across[count, k] = remote(
                piece, piece, cs.at[count, k], cr.at[count, k], me["partner"]
            )
            self.across[count, k].start()
        self.store = store
        yield
        for step in range(count + 2):
            m = step
            if m < count:
                for k in order:
                    along[m, k].wait_recv()
                    piece = part(m, block(m, k).at[me["quarter"]])
                    over_x[m, k] = remote(piece, piece, xs.at[m, k], xr.at[m, k], me["x"])
                    over_y[m, k] = remote(piece, piece, ys.at[m, k], yr.at[m, k], me["y"])
                    over_x[m, k].start()
                    over_y[m, k].start()
                if m + WINDOW < count:
                    start_along(m + WINDOW)
            m = step - 1
            if 0 <= m < count:
                for k in order:
                    if (m + k) % 2 == 0:
                        over_x[m, k].wait_recv()
                        q, device = me["qx"], me["y"]
                    else:
                        over_y[m, k].wait_recv()
                        q, device = me["qy"], me["x"]
                    piece = part(m, block(m, k).at[q])
                    diagonal[m, k] = remote(piece, piece, ds.at[m, k], dr.at[m, k], device)
                    diagonal[m, k].start()
            m = step - 2
            if 0 <= m < count:
                for k in order:
                    if (m + k) % 2 == 0:
                        over_y[m, k].wait_recv()
                    else:
                        over_x[m, k].wait_recv()
                    diagonal[m, k].wait_recv()
                    piece = part(m, block(m, k))
                    self.across[m, k] = remote(
                        piece, piece, cs.at[m, k], cr.at[m, k], me["partner"]
                    )
                    self.across[m, k].start()
            yield
        self.all_copies = (along, over_x, over_y, diagonal, self.across)

    def arrive(self, m):
        for k in range(self.chips):
            self.across[m, k].wait_recv()

    def finish(self, waited):
        for m in range(len(self.chunks)):
            if m not in waited:
                self.arrive(m)
        for copies in self.all_copies:
            for copy in copies.values():
                copy.wait_send()


def f32(value):
    return value.astype(jnp.float32)


def turn_rows(source, turned, chips, piece, is_turned):
    features = source.shape[0] if is_turned else source.shape[1]
    width = math.lcm(128, piece)
    for start in range(0, features, width):
        if is_turned:
            value = f32(source[start : start + width, :])
        else:
            value = f32(source[:, start : start + width]).T
        for i in range(width // piece):
            at = start // piece + i
            chip, core, quarter = at // 8, (at // 4) % 2, at % 4
            block = value[i * piece : (i + 1) * piece].astype(jnp.bfloat16)
            turned[core, quarter, chip * piece : (chip + 1) * piece, :] = block


class GradPlan:
    def __init__(self, lefts, turned, rights, chunks, later=(), handed=0, received=()):
        self.handed, self.received = handed, list(received)
        self.later, self.swap_right = later, {}
        self.chips = lax.axis_size("grp") // 2
        self.extras = lax.axis_size("rep") // 4
        self.lefts, self.turned, self.rights, self.chunks = lefts, turned, rights, chunks
        self.tokens = rights[0].shape[0]
        sizes = [x.shape[0] if flag else x.shape[1] for x, flag in zip(lefts, turned)]
        self.rows = [size // 8 for size in sizes]
        self.piece = [size // (8 * self.chips) for size in sizes]

    def operands(self):
        rights = [r for n, r in enumerate(self.rights) if n not in self.later]
        return [*self.lefts, *rights, *self.received]

    def outs(self):
        whole = len(self.chunks) - self.handed
        shapes = [
            (4 if m < whole else self.chips, self.piece[a], width)
            for m, (a, _, _, width) in enumerate(self.chunks)
        ]
        shapes += [(4, *total.shape[1:]) for total in self.received]
        return [jax.ShapeDtypeStruct(shape, jnp.bfloat16) for shape in shapes]

    def scratch(self):
        low, vmem, dma = jnp.bfloat16, pltpu.VMEM, pltpu.SemaphoreType.DMA
        lefts, rights, count = len(self.lefts), len(self.rights), len(self.chunks)
        work = [vmem((2, 4, rows, self.tokens), low) for rows in self.rows]
        work += [vmem((4, rows, self.tokens), low) for rows in self.rows]
        work += [vmem(right.shape, low) for right in self.rights]
        shapes = [(self.rows[a], self.piece[a], width) for a, _, _, width in self.chunks]
        work += [vmem((4, rows, width), low) for rows, _, width in shapes]
        work += [vmem((2, rows, width), low) for rows, _, width in shapes]
        work += [vmem((rows, width), low) for rows, _, width in shapes]
        work += [vmem((self.chips, piece, width), low) for _, piece, width in shapes]
        ends = [shape[1:] for shape in shapes] + [total.shape[1:] for total in self.received]
        count = len(ends)
        work += [vmem((self.chips - 1, *end), low) for end in ends]
        if self.extras > 1:
            work += [vmem((self.extras, *end), low) for end in ends]
        sems = [dma((lefts,))] * 2 + [dma((rights,))] * 2
        sems += [dma((count, 2)), dma((count, 2)), dma((count,)), dma((count,))]
        sems += [dma((count, self.chips))] * 2 + [dma((count, self.extras))] * 2
        sems += [dma((count, 3))] * 2
        return [*work, *sems]

    def steps(self, me, ins, outs, scratch, lag=2):
        chips, extras, count = self.chips, self.extras, len(self.chunks)
        whole, ends = count - self.handed, count + len(self.received)
        lefts, rights = ins[: len(self.lefts)], ins[len(self.lefts) :]
        rights, received = rights[: len(self.rights)], rights[len(self.rights) :]
        groups = []
        sizes = [len(lefts), len(lefts), len(rights), *[count] * 4, ends]
        for size in sizes + ([ends] if extras > 1 else []):
            groups.append(scratch[:size])
            scratch = scratch[size:]
        turned, turned_in, rights_in, parts, one, two, total, slots = groups[:8]
        extra_in = groups[8] if extras > 1 else ()
        la_s, la_r, ri_s, ri_r, s1, r1, s2, r2, zs, zr, es, er, gs, gr = scratch
        total = [*total, *received]
        core = me["core"]
        reps, rep = lax.axis_size("rep"), lax.axis_index("rep")
        beyond = [{"rep": lax.rem(rep + 4 * e, reps)} for e in range(1, extras)]
        swap_left, swap_right = {}, self.swap_right
        for n in range(len(rights)):
            swap_right[n] = remote(rights[n], rights_in[n], ri_s.at[n], ri_r.at[n], me["partner"])
            if n not in self.later and n == 0:
                swap_right[n].start()
        for n in range(len(lefts)):
            turn_rows(lefts[n], turned[n], chips, self.piece[n], self.turned[n])
            swap_left[n] = remote(
                turned[n].at[1 - core], turned_in[n], la_s.at[n], la_r.at[n], me["partner"]
            )
            if n == 0:
                swap_left[n].start()
            yield
        waiting = [swap_right[n] for n in range(1, len(rights)) if n not in self.later]
        waiting = [copy for pair in itertools.zip_longest([swap_left[n] for n in range(1, len(lefts))], waiting) for copy in pair if copy is not None]
        have = set()
        first, second, along, other, spread = {}, {}, {}, {}, {}

        def form(m):
            a, b, start, width = self.chunks[m]
            for key, copy in (("left", a), swap_left[a]), (("right", b), swap_right[b]):
                if key not in have:
                    have.add(key)
                    copy.wait_recv()
            at = slice(start, start + width)

            def quarter(q, _):
                value = dot_plain(turned[a][core, q], rights[b][:, at])
                value = value + dot_plain(turned_in[a][q], rights_in[b][:, at])
                parts[m][q] = value.astype(jnp.bfloat16)
                return 0

            lax.fori_loop(0, 4, quarter, 0)

        def send_first(m, i):
            device, mine = (me["x"], me["qx"]) if m % 2 == 0 else (me["y"], me["qy"])
            q = me["qd"] if i == 1 else mine
            first[m, i] = remote(parts[m].at[q], one[m].at[i], s1.at[m, i], r1.at[m, i], device)
            first[m, i].start()

        def send_second(m):
            rows = self.rows[self.chunks[m][0]]
            device, q = (me["y"], me["qy"]) if m % 2 == 0 else (me["x"], me["qx"])
            first[m, 1].wait_recv()

            def add(j, _):
                at = pl.ds(pl.multiple_of(j * 64, 64), 64)
                value = f32(parts[m][q, at, :]) + f32(one[m][1, at, :])
                parts[m][q, at, :] = value.astype(jnp.bfloat16)
                return 0

            lax.fori_loop(0, rows // 64, add, 0)
            second[m] = remote(parts[m].at[q], two[m], s2.at[m], r2.at[m], device)
            second[m].start()

        def send_along(m):
            piece = self.piece[self.chunks[m][0]]
            first[m, 0].wait_recv()
            second[m].wait_recv()
            for j in range(chips):
                at = slice(j * piece, (j + 1) * piece)
                value = f32(parts[m][me["quarter"], at, :]) + f32(one[m][0, at, :]) + f32(two[m][at, :])
                (total if m < whole else outs)[m][j] = value.astype(jnp.bfloat16)
            if m < whole:
                pass_along(m)

        def pass_along(m):
            for k in near_first(chips):
                along[m, k] = remote(
                    total[m].at[me["chip_to"][k]],
                    slots[m].at[k - 1],
                    zs.at[m, k],
                    zr.at[m, k],
                    me["along"][k],
                )
                along[m, k].start()

        def send_spread(m):
            value = f32(total[m][me["chip"]])
            for k in near_first(chips):
                along[m, k].wait_recv()
                value = value + f32(slots[m][k - 1])
            if extras > 1:
                extra_in[m][0] = value.astype(jnp.bfloat16)
                for e in range(1, extras):
                    other[m, e] = remote(
                        extra_in[m].at[0],
                        extra_in[m].at[e],
                        es.at[m, e],
                        er.at[m, e],
                        beyond[e - 1],
                    )
                    other[m, e].start()
                for e in range(1, extras):
                    other[m, e].wait_recv()
                    value = value + f32(extra_in[m][e])
            outs[m][me["quarter"]] = value.astype(jnp.bfloat16)
            piece = outs[m].at[me["quarter"]]
            for i, device in enumerate((me["x"], me["y"])):
                spread[m, i] = remote(piece, piece, gs.at[m, i], gr.at[m, i], device)
                spread[m, i].start()

        def send_diagonal(m):
            way = m % 2
            spread[m, way].wait_recv()
            q, device = (me["qx"], me["y"]) if way == 0 else (me["qy"], me["x"])
            piece = outs[m].at[q]
            spread[m, 2] = remote(piece, piece, gs.at[m, 2], gr.at[m, 2], device)
            spread[m, 2].start()

        for m in range(count, ends):
            pass_along(m)
        stages = (send_second, send_along, send_spread, send_diagonal)
        spans = (count, count, whole, whole)
        last = max([lag * (n + 1) + span for n, span in enumerate(spans)])
        for step in range(max(last, len(received) + 2 * lag)):
            if step < count:
                form(step)
                send_first(step, 1)
            if 1 <= step <= count:
                send_first(step - 1, 0)
            for _ in range(2):
                if waiting:
                    waiting.pop(0).start()
            for n, stage in enumerate(stages):
                m = step - lag * (n + 1)
                if 0 <= m < spans[n]:
                    stage(m)
                m = count + step - lag * (n - 1)
                if n >= 2 and count <= m < ends:
                    stage(m)
            yield
        for m in [*range(whole), *range(count, ends)]:
            spread[m, 1 - m % 2].wait_recv()
            spread[m, 2].wait_recv()
        for copies in (swap_left, swap_right, first, second, along, other, spread):
            for copy in copies.values():
                copy.wait_send()
        yield


def small_steps(me, chips, extras, vec, out, stage, slots, sems, more):
    ss, sr, zs, zr = sems
    copies = []
    value = vec[...]
    hops = [me["x"], me["y"], me["partner"]]
    for i, device in enumerate(hops):
        stage[i] = value
        copies.append(remote(stage.at[i], slots.at[i], ss.at[i], sr.at[i], device))
        copies[-1].start()
        yield
        copies[-1].wait_recv()
        value = value + slots[i]
    if extras > 1:
        stage[3] = value
        for e in range(1, extras):
            at = 3 + chips + e
            copies.append(remote(stage.at[3], slots.at[at], ss.at[2 + e], sr.at[2 + e], more[e - 1]))
            copies[-1].start()
        yield
        for e in range(1, extras):
            copies[-e].wait_recv()
        for e in range(1, extras):
            value = value + slots[3 + chips + e]
    stage[4] = value
    along = []
    for k in near_first(chips):
        along.append(remote(stage.at[4], slots.at[3 + k], zs.at[k], zr.at[k], me["along"][k]))
        along[-1].start()
    yield
    for copy in along:
        copy.wait_recv()
    for k in range(1, chips):
        value = value + slots[3 + k]
    out[...] = value
    for copy in copies + along:
        copy.wait_send()
    yield


def run_out(steps):
    for _ in steps:
        pass


def tail_kernel(plan, early, joins, *refs):
    groups = []
    kept = len(plan.outs())
    for size in (len(plan.operands()), 13 + len(early), 2 + len(joins), 6 + kept):
        groups.append(refs[:size])
        refs = refs[size:]
    normed_ref, dz_ref, dconv, *received = groups[0]
    (
        conv_sums,
        dq_ref,
        dkv_ref,
        cosine_ref,
        sine_ref,
        tokens_ref,
        gain_ref,
        hidden_ref,
        early_heads,
        feed_gain_ref,
        mixer_gain_ref,
        mixer_w,
        attention_w,
    ) = groups[1][len(early) :]
    token_grad_ref, total_ref, *joined = groups[2]
    (
        dproj,
        mixer_rows,
        attention_rows,
        dnormed,
        vec,
        fetch_sem,
        *sums,
    ) = groups[3]
    stage, slots, small_sems = refs[-6], refs[-5], refs[-4:]
    me = seat()
    rep, reps = lax.axis_index("rep"), lax.axis_size("rep")
    span, conv_width = dz_ref.shape[0], conv_sums.shape[1]
    width = tokens_ref.shape[1]
    inner = dz_ref.shape[1]
    beyond = [{"rep": lax.rem(rep + 4 * e, reps)} for e in range(1, plan.extras)]
    greet(me, beyond)
    large = plan.steps(me, [normed_ref, dz_ref, dconv, dproj, *received], sums, refs[:-6], lag=TAIL_LAG)
    next(large)

    blocks = width // 256
    fetched = (
        pltpu.make_async_copy(mixer_w, mixer_rows, fetch_sem.at[0]),
        pltpu.make_async_copy(attention_w, attention_rows, fetch_sem.at[1]),
    )
    for copy in fetched:
        copy.start()

    low_half = lanes((span, 128)) % HEAD < HEAD // 2

    def turned_back(value):
        other = jnp.where(low_half, pltpu.roll(value, 128 - HEAD // 2, 1), pltpu.roll(value, HEAD // 2, 1))
        return value * cosine_ref[...] - other * sine_ref[...]

    queries = dq_ref.shape[1]
    for start in range(0, queries, 128):
        at = slice(start, start + 128)
        dproj[:, at] = turned_back(dq_ref[:, at]).astype(jnp.bfloat16)
    dproj[:, queries : queries + 128] = turned_back(dkv_ref[:, 0:128]).astype(jnp.bfloat16)
    dproj[:, queries + 128 :] = dkv_ref[:, 128:].astype(jnp.bfloat16)
    next(large)
    plan.swap_right[2].start()
    next(large)

    for copy in fetched:
        copy.wait()
    for i in range(blocks):
        at = slice(i * 256, (i + 1) * 256)
        value = dot_rows(dz_ref[...], mixer_rows[at, 0:inner])
        value = value + dot_rows(dconv[:, 0:conv_width], mixer_rows[at, inner : inner + conv_width])
        value = value + dot_rows(dconv[:, conv_width:], mixer_rows[at, inner + conv_width :])
        dnormed[:, at] = value + dot_rows(dproj[...], attention_rows[at, :])
        if i % 2 == 1:
            next(large, None)

    def norm_back(i, gain_grad):
        at = pl.ds(pl.multiple_of(i * 64, 64), 64)
        value = f32(tokens_ref[at, :])
        scale = lax.rsqrt(jnp.mean(value * value, axis=-1, keepdims=True) + NORM_EPS)
        unit = value * scale
        grad = dnormed[at, :]
        inner_grad = grad * gain_ref[0:1]
        mean = jnp.mean(inner_grad * unit, axis=-1, keepdims=True)
        token_grad_ref[at, :] = hidden_ref[at, :] + scale * (inner_grad - unit * mean)
        return gain_grad + jnp.sum(grad * unit, axis=0, keepdims=True)

    gain_grad = lax.fori_loop(0, span // 64, norm_back, jnp.zeros((1, width), jnp.float32))
    vec[...] = conv_sums[...]
    vec[5:6, 0:inner] = mixer_gain_ref[...]
    vec[6:7, 0:width] = feed_gain_ref[...]
    vec[7:8, 0:width] = gain_grad
    for i, row in enumerate((2, 0, 1)):
        vec[7:8, width + 128 * i : width + 128 * (i + 1)] = early_heads[row : row + 1]
    next(large, None)
    small = small_steps(me, plan.chips, plan.extras, vec, total_ref, stage, slots, small_sems, beyond)
    for _ in small:
        next(large, None)
    pieces = [*groups[1][: len(early)], *sums]

    def join(wanted):
        for target, parts in zip(joined, joins):
            start = 0
            for part in parts:
                source = pieces[part]
                rows, columns = source.shape[1:]
                if part in wanted:
                    for q in range(4):
                        at = (slice(q * rows, (q + 1) * rows), slice(start, start + columns))
                        target[at] = f32(source[q])
                start += columns

    join(range(len(early)))
    run_out(large)
    join(range(len(early), len(pieces)))


def run_tail(plan, early, joins, *operands):
    dma, vmem = pltpu.SemaphoreType.DMA, pltpu.VMEM
    chips, extras = plan.chips, plan.extras
    f32, low = jnp.float32, jnp.bfloat16
    conv_width, span = operands[0].shape[1], operands[1].shape[0]
    width = operands[5].shape[1]
    mixer_w, attention_w = operands[-2:]
    vec = (8, conv_width)
    scratch = [
        vmem((span, attention_w.shape[1]), low),
        vmem(mixer_w.shape, low),
        vmem(attention_w.shape, low),
        vmem((span, width), f32),
        vmem(vec, f32),
        dma((2,)),
        *[vmem(out.shape, out.dtype) for out in plan.outs()],
    ]
    pieces = [*early, *plan.outs()]
    full = []
    for parts in joins:
        rows = 4 * pieces[parts[0]].shape[1]
        full.append(jax.ShapeDtypeStruct((rows, sum(pieces[p].shape[2] for p in parts)), f32))
    small = [vmem((5, *vec), f32), vmem((3 + chips + extras, *vec), f32)]
    small += [dma((2 + extras,)), dma((2 + extras,)), dma((chips,)), dma((chips,))]
    vm, anywhere = pl.BlockSpec(memory_space=pltpu.VMEM), pl.BlockSpec(memory_space=pl.ANY)
    token_grad, total, *joined = pl.pallas_call(
        functools.partial(tail_kernel, plan, early, joins),
        out_shape=[
            jax.ShapeDtypeStruct((span, width), f32),
            jax.ShapeDtypeStruct(vec, f32),
            *full,
        ],
        in_specs=[vm] * (len(plan.operands()) + len(early) + 11) + [anywhere] * 2,
        out_specs=[vm] * (2 + len(full)),
        scratch_shapes=[*scratch, *plan.scratch(), *small],
        compiler_params=pltpu.CompilerParams(
            collective_id=1, has_side_effects=True, vmem_limit_bytes=VMEM_LIMIT
        ),
        name="run_tail",
    )(*plan.operands(), *early, *operands)
    return token_grad, total, joined


def column_chunks(left, right, columns, pieces):
    width = columns // pieces // 128 * 128
    starts = [i * width for i in range(pieces)] + [columns]
    return [(left, right, low, high - low) for low, high in zip(starts, starts[1:])]


def axis_seat():
    grp = lax.axis_index("grp")
    return lax.div(grp, 2), lax.rem(grp, 2)


def greet_group(extra=()):
    size, grp = lax.axis_size("grp"), lax.axis_index("grp")
    barrier = pltpu.get_barrier_semaphore()
    others = [{"grp": lax.rem(grp + k, size)} for k in range(1, size)] + list(extra)
    for device in others:
        pl.semaphore_signal(barrier, inc=1, device_id=device, device_id_type=MESH)
    pl.semaphore_wait(barrier, len(others))


def lanes(shape):
    return lax.broadcasted_iota(jnp.int32, shape, len(shape) - 1)


def pair_columns(columns, pair):
    rows = columns.shape[0]
    low = jnp.broadcast_to(columns[:, 2 * pair : 2 * pair + 1], (rows, 128))
    high = jnp.broadcast_to(columns[:, 2 * pair + 1 : 2 * pair + 2], (rows, 128))
    return jnp.where(lanes((rows, 128)) < 64, low, high)


def dot_rows(left, right):
    return lax.dot_general(
        left, right, (((1,), (1,)), ((), ())), preferred_element_type=jnp.float32
    )


def dot_plain(left, right):
    return jnp.dot(left, right, preferred_element_type=jnp.float32)


def align_heads(source, target, scale):
    for pair in range(HEADS // 2):
        both = source[:, pair * 128 : (pair + 1) * 128].astype(jnp.float32) * scale
        swapped = pltpu.roll(both, 64, 1)
        for odd in range(2):
            head = 2 * pair + odd
            group = head // (HEADS // KV_HEADS)
            value = both if odd == group else swapped
            keep = lanes(value.shape) // 64 == group
            target[head] = jnp.where(keep, value, 0.0).astype(jnp.bfloat16)


def slot_plan(reach):
    return [(0, 0)] + [(k, core) for k in range(1, reach + 1) for core in (1, 0)]


def slot_live(slot, chip, core, reach):
    back, side = slot
    if back == 0:
        return core == 1
    live = chip - back >= 0
    if back == reach and side == 0:
        live = jnp.logical_and(live, core == 0)
    return live


def same_document(key_column, query_row, causal):
    size = query_row.shape[-1]
    allowed = across(key_column, size) == query_row
    if causal:
        rows = lax.broadcasted_iota(jnp.int32, (size, size), 0)
        allowed = jnp.logical_and(allowed, rows <= lanes((size, size)))
    return jnp.where(allowed, 0.0, HIDDEN)


def across(column, width):
    return jnp.concatenate([column] * (width // 128), axis=1)


def forward_kernel(reach, gather, *refs):
    chips, many = gather.chips, len(gather.cut)
    groups = []
    for size in (6, many, 24, many, 39):
        groups.append(refs[:size])
        refs = refs[size:]
    (
        tokens_ref,
        pack,
        docs_ref,
        heads_ref,
        cosine_ref,
        sine_ref,
    ) = groups[0]
    shards = groups[1]
    (
        normed_ref,
        q_ref,
        gate_ref,
        ext_ref,
        act_ref,
        step_ref,
        dt_ref,
        run_ref,
        runt_ref,
        e_ref,
        wd_ref,
        car_ref,
        carried_ref,
        att_ref,
        attt_ref,
        inv_ref,
        mixed_ref,
        ent_ref,
        kvw_ref,
        segk_ref,
        packs,
        same,
        taps,
        gain_ref,
    ) = groups[2]
    fulls = groups[3]
    (
        kv_ref,
        attention_w,
        mixer_w,
        rim_out,
        rim_in,
        seg_ext,
        skip_lanes,
        qa,
        bias,
        vt,
        ot,
        total,
        xdt,
        xw,
        runb,
        gram,
        own_state,
        half_out,
        half_in,
        car_in,
        chip_out,
        chip_car,
        chip_in,
        chip_car_in,
        enter_out,
        acc,
        fetch_sem,
        rim_s,
        rim_r,
        ka_s,
        ka_r,
        kp_s,
        kp_r,
        ha_s,
        ha_r,
        ca_s,
        ca_r,
        en_s,
        en_r,
    ) = groups[4]
    travel = refs
    chip, core = axis_seat()
    grp = lax.axis_index("grp")
    span = tokens_ref.shape[0]
    inner = SSM_HEADS * SSM_HEAD
    half = inner // 2
    partner = {"grp": chip * 2 + 1 - core}

    def ahead(k):
        return {"grp": lax.rem(grp + 2 * k, 2 * chips)}

    me = seat()
    greet_group([me["x"], me["y"]])
    gathering = gather.steps(me, shards, pack, packs, fulls, travel)

    def tick():
        next(gathering, None)

    tick()
    for i in range(2 * (reach + 1)):
        segk_ref[i] = jnp.broadcast_to(docs_ref[i], (128, span)).T
    own_row = docs_ref[2 * reach + core]
    own_docs = segk_ref[2 * reach + core]
    seg_ext[8:, :] = own_docs
    seg_ext[0:8, :] = segk_ref[2 * reach + core - 1][span - 8 :]
    prior, tail = seg_ext[7:8, :], own_docs[span - 1 :]
    for j in range(CONV - 1):
        same[j] = jnp.where(seg_ext[5 + j : 5 + j + span, :] == own_docs, 1.0, 0.0)

    for k in range(chips):
        gather.across[len(gather.chunks), k].wait_recv()

    def whole_rows(width):
        total = width * 2 * chips
        rows = lax.broadcasted_iota(jnp.int32, (pack.shape[1], total), 0)
        value = jnp.zeros((8, total), jnp.float32)
        for i in range(2 * chips):
            here = jnp.logical_and(lanes(rows.shape) == rows + width * i, rows < width)
            value = value + dot_plain(packs[i], jnp.where(here, 1.0, 0.0).astype(jnp.bfloat16))
        return value

    taps[...] = whole_rows(taps.shape[1] // (2 * chips))
    gain = whole_rows(tokens_ref.shape[1] // (2 * chips))[5:6]
    gain_ref[...] = jnp.broadcast_to(gain, gain_ref.shape)

    def norm(i, _):
        at = pl.ds(pl.multiple_of(i * 64, 64), 64)
        value = f32(tokens_ref[at, :])
        scale = lax.rsqrt(jnp.mean(value * value, axis=-1, keepdims=True) + NORM_EPS)
        normed_ref[at, :] = (value * scale * gain).astype(jnp.bfloat16)
        return 0

    lax.fori_loop(0, span // 64, norm, 0)
    for pair in range(SSM_HEADS // 2):
        at = slice(pair * 128, (pair + 1) * 128)
        skip_lanes[:, at] = pair_columns(jnp.broadcast_to(heads_ref[2:3], (8, 128)), pair)

    for _ in range(3):
        tick()
    gather.arrive(0)
    mixer_chunks = [m for m, chunk in enumerate(gather.chunks) if chunk[0] == 1]
    waited = {0}
    fetch = pltpu.make_async_copy(fulls[0], attention_w, fetch_sem.at[0])
    gather.store[0].wait()
    fetch.start()
    tick()
    fetch.wait()
    width = tokens_ref.shape[1]
    low_half = lanes((span, 128)) % HEAD < HEAD // 2

    def turned(value):
        other = jnp.where(low_half, pltpu.roll(value, 128 - HEAD // 2, 1), pltpu.roll(value, HEAD // 2, 1))
        return value * cosine_ref[...] + other * sine_ref[...]

    for j in range(3):
        part = attention_w[:, :, :, j * 256 : (j + 1) * 256].reshape(width, 256)
        value = dot_plain(normed_ref[...], part)
        one, two = value[:, 0:128], value[:, 128:256]
        if j < 2:
            q_ref[:, j * 256 : j * 256 + 128] = turned(one).astype(jnp.bfloat16)
            q_ref[:, j * 256 + 128 : (j + 1) * 256] = turned(two).astype(jnp.bfloat16)
        else:
            kv_ref[:, 0:128] = turned(one).astype(jnp.bfloat16)
            kv_ref[:, 128:256] = two.astype(jnp.bfloat16)

    for _ in mixer_chunks[1:]:
        tick()
    for m in mixer_chunks:
        gather.arrive(m)
        waited.add(m)
    fetch = pltpu.make_async_copy(fulls[1], mixer_w, fetch_sem.at[1])
    gather.store[1].wait()
    fetch.start()
    fetch.wait()

    def project(at):
        return dot_plain(normed_ref[...], mixer_w[:, :, :, at].reshape(width, -1))

    conv_width = inner + 2 * STATE
    rest = inner + conv_width

    def conv_block(j, _):
        value = project(pl.ds(pl.multiple_of(inner + j * 256, 256), 256)).astype(jnp.bfloat16)
        at = pl.ds(pl.multiple_of(j * 256, 256), 256)
        ext_ref[8:, at] = f32(value)
        rim_out[:, at] = value[span - 16 :]
        return 0

    lax.fori_loop(0, conv_width // 256, conv_block, 0)
    tick()
    step_ref[...] = jnp.zeros_like(step_ref)
    step_ref[:, 0:SSM_HEADS] = project(slice(rest, rest + SSM_HEADS))
    rim = remote(rim_out, rim_in, rim_s, rim_r, {"grp": lax.rem(grp + 1, 2 * chips)})
    pl.when(grp + 1 < 2 * chips)(rim.start)

    def gate_block(j, _):
        at = pl.ds(pl.multiple_of(j * 256, 256), 256)
        gate_ref[:, at] = project(at)
        return 0

    lax.fori_loop(0, inner // 256, gate_block, 0)
    tick()

    raw = step_ref[...] + heads_ref[0:1]
    dt_ref[...] = jnp.maximum(raw, 0.0) + jnp.log1p(jnp.exp(-jnp.abs(raw)))
    before = lax.broadcasted_iota(jnp.int32, (span, span), 0) >= lanes((span, span))
    running = lax.dot_general(
        jnp.where(before, 1.0, 0.0), dt_ref[...] * -jnp.exp(heads_ref[1:2]), (((1,), (0,)), ((), ())),
        precision=HIGHEST, preferred_element_type=jnp.float32,
    )
    run_ref[...] = running
    turned_run = running.T
    for head in range(SSM_HEADS):
        runt_ref[head] = turned_run[head : head + 1]
    final = running[span - 1 :]
    e_ref[...] = jnp.where(own_docs == prior, jnp.exp(running), 0.0)
    wd_ref[...] = jnp.where(own_docs == tail, jnp.exp(final - running), 0.0)
    carried = jnp.where(tail == prior, jnp.exp(final), 0.0)
    carried_ref[...] = jnp.broadcast_to(carried, (8, 128))
    for pair in range(SSM_HEADS // 2):
        at = pair * 128 % half
        car_ref[pair * 128 // half, :, at : at + 128] = pair_columns(carried_ref, pair)

    def rim_none():
        ext_ref[0:8, :] = jnp.zeros((8, conv_width), jnp.float32)

    def rim_some():
        rim.wait_recv()
        ext_ref[0:8, :] = f32(rim_in[8:16, :])

    pl.when(grp == 0)(rim_none)
    pl.when(grp > 0)(rim_some)

    def convolve(j, _):
        at = pl.ds(pl.multiple_of(j * 256, 256), 256)
        value = jnp.broadcast_to(taps[CONV : CONV + 1, at], (span, 256))
        for tap in range(CONV):
            term = ext_ref[5 + tap : 5 + tap + span, at] * taps[tap : tap + 1, at]
            if tap < CONV - 1:
                term = jnp.where(across(same[tap], 256) > 0.0, term, 0.0)
            value = value + term
        act_ref[:, at] = value / (1.0 + jnp.exp(-value))
        return 0

    lax.fori_loop(0, conv_width // 256, convolve, 0)
    tick()
    own_kv = remote(kv_ref, kvw_ref.at[0, core], kp_s.at[0], kp_r.at[0], partner)
    own_kv.start()
    kv_along = {}
    for k in range(1, reach + 1):
        kv_along[k] = remote(kv_ref, kvw_ref.at[k, core], ka_s.at[k], ka_r.at[k], ahead(k))
        pl.when(chip + k < chips)(kv_along[k].start)
    kvw_ref[0, core] = kv_ref[...]

    weight = wd_ref[...] * dt_ref[...]
    for pair in range(SSM_HEADS // 2):
        at = slice(pair * 128, (pair + 1) * 128)
        x_pair = act_ref[:, at]
        xdt[:, at] = (x_pair * pair_columns(dt_ref, pair)).astype(jnp.bfloat16)
        xw[:, at] = (x_pair * pair_columns(weight, pair)).astype(jnp.bfloat16)
    in_map = act_ref[:, inner : inner + STATE]
    out_map = act_ref[:, inner + STATE :]
    out_low = out_map.astype(jnp.bfloat16)
    in_turned = in_map.T.astype(jnp.bfloat16)
    for i in range(2):
        own_state[i] = dot_plain(in_turned, xw[:, i * half : (i + 1) * half])
    half_out[...] = own_state[1 - core].astype(jnp.bfloat16)
    align_heads(q_ref, qa, HEAD**-0.5)
    ot[...] = jnp.zeros_like(ot)
    total[...] = jnp.zeros_like(total)
    half_car = remote(car_ref.at[1 - core], car_in, ha_s.at[0], ha_r.at[0], partner)
    half_state = remote(half_out, half_in, ha_s.at[1], ha_r.at[1], partner)
    half_car.start()
    half_state.start()

    def attend_slot(keys, values, key_docs, causal):
        bias[...] = same_document(key_docs, own_row, causal)
        vt[...] = values.astype(jnp.float32).T.astype(jnp.bfloat16)

        def per_head(head, _):
            group = lax.div(head, HEADS // KV_HEADS)
            scores = dot_rows(keys[...], qa[head]) + bias[...]
            weights = jnp.exp(scores)
            total[head] += jnp.sum(weights, axis=0, keepdims=True)
            rows = pl.ds(pl.multiple_of(group * HEAD, HEAD), HEAD)
            into = pl.ds(pl.multiple_of(head * HEAD, HEAD), HEAD)
            ot[into, :] += dot_plain(vt[rows, :], weights.astype(jnp.bfloat16))
            return 0

        lax.fori_loop(0, HEADS, per_head, 0)

    def attend_ref(ref, key_docs, causal):
        attend_slot(ref.at[:, 0:128], ref[:, 128:256], key_docs, causal)

    attend_ref(kv_ref, segk_ref[2 * reach + core], True)
    tick()

    half_car.wait_recv()
    half_state.wait_recv()
    mine, theirs = own_state[core], half_in[...].astype(jnp.float32)
    car_mine, car_theirs = car_ref[core], car_in[...]
    first = core == 0
    car_0 = jnp.where(first, car_mine, car_theirs)
    car_1 = jnp.where(first, car_theirs, car_mine)
    state_0 = jnp.where(first, mine, theirs)
    state_1 = jnp.where(first, theirs, mine)
    chip_out[...] = (state_1 + car_1[0:1] * state_0).astype(jnp.bfloat16)
    chip_car[...] = car_0 * car_1

    for head in range(SSM_HEADS):
        runb[head] = jnp.broadcast_to(run_ref[:, head : head + 1], (span, 128))
    gram[...] = lax.dot_general(
        out_map, in_map, (((1,), (1,)), ((), ())), precision=HIGHEST,
        preferred_element_type=jnp.float32,
    )
    state_along = {}
    for k in range(1, reach + 1):
        state_along[k] = (
            remote(chip_out, chip_in.at[k], ca_s.at[k, 0], ca_r.at[k, 0], ahead(k)),
            remote(chip_car, chip_car_in.at[k], ca_s.at[k, 1], ca_r.at[k, 1], ahead(k)),
        )
        for copy in state_along[k]:
            pl.when(chip + k < chips)(copy.start)

    kv_pass = {}
    for k in range(1, reach + 1):
        place = kvw_ref.at[k, core]
        kv_pass[k] = remote(place, place, kp_s.at[k], kp_r.at[k], partner)

        def hand_on(k=k):
            kv_along[k].wait_recv()
            kv_pass[k].start()

        pl.when(chip - k >= 0)(hand_on)

    rows = lax.broadcasted_iota(jnp.int32, (span, span), 0)
    allowed = jnp.logical_and(
        across(segk_ref[2 * reach + core], span) == own_row, rows >= lanes((span, span))
    )
    bias[...] = jnp.where(allowed, 0.0, HIDDEN)

    def intra(quad, _):
        at = pl.ds(pl.multiple_of(quad * 256, 256), 256)
        value = jnp.zeros((span, 256), jnp.float32)
        for i in range(4):
            head = quad * 4 + i
            column = runb[head]
            spread = jnp.concatenate([column] * (span // 128), axis=1) - runt_ref[head]
            mixing = (jnp.exp(spread + bias[...]) * gram[...]).astype(jnp.bfloat16)
            part = dot_plain(mixing, xdt[:, at])
            value = jnp.where(lanes((span, 256)) // 64 == i, part, value)
        mixed_ref[:, at] = value + skip_lanes[0:1, at] * act_ref[:, at]
        return 0

    lax.fori_loop(0, SSM_HEADS // 4, intra, 0)
    tick()

    own_kv.wait_recv()
    for index, slot in enumerate(slot_plan(reach)):
        back, side = slot
        if slot == (1, 1):
            acc[...] = jnp.zeros_like(acc)
            for k in range(reach, 0, -1):

                def take(k=k):
                    for copy in state_along[k]:
                        copy.wait_recv()
                    acc[...] = chip_in[k].astype(jnp.float32) + chip_car_in[k, 0:1] * acc[...]

                pl.when(chip - k >= 0)(take)
            enter_0, enter_1 = acc[...], state_0 + car_0[0:1] * acc[...]
            ent_ref[core] = jnp.where(first, enter_0, enter_1)
            enter_out[...] = jnp.where(first, enter_1, enter_0)
            for k in range(1, reach + 1):
                pl.when(chip - k >= 0)(kv_pass[k].wait_recv)

        def visit(back=back, side=side):
            ref = kvw_ref.at[back, side]
            attend_ref(ref, segk_ref[2 * (reach - back) + side], False)

        pl.when(slot_live(slot, chip, core, reach))(visit)
        tick()
        if slot == (1, 1):
            enter_pass = remote(enter_out, ent_ref.at[core], en_s, en_r, partner)
            enter_pass.start()

    for head in range(HEADS):
        inverse = 1.0 / total[head]
        inv_ref[head] = inverse
        into = slice(head * HEAD, (head + 1) * HEAD)
        ot[into, :] = ot[into, :] * inverse
    attt_ref[...] = ot[...].astype(jnp.bfloat16)
    for pair in range(HEADS // 2):
        at = slice(pair * 128, (pair + 1) * 128)
        att_ref[:, at] = ot[at, :].T.astype(jnp.bfloat16)

    enter_pass.wait_recv()
    for i in range(2):
        carried_in = dot_plain(out_low, ent_ref[i].astype(jnp.bfloat16))
        for j in range(SSM_HEADS // 4):
            pair = i * (SSM_HEADS // 4) + j
            at = slice(pair * 128, (pair + 1) * 128)
            part = carried_in[:, j * 128 : (j + 1) * 128]
            mixed_ref[:, at] += pair_columns(e_ref, pair) * part

    run_out(gathering)
    gather.finish(waited)
    for copy in gather.store[2:]:
        copy.wait()
    own_kv.wait_send()
    pl.when(grp + 1 < 2 * chips)(rim.wait_send)
    half_car.wait_send()
    half_state.wait_send()
    enter_pass.wait_send()
    for k in range(1, reach + 1):

        def sent(k=k):
            kv_along[k].wait_send()
            for copy in state_along[k]:
                copy.wait_send()

        pl.when(chip + k < chips)(sent)
        pl.when(chip - k >= 0)(kv_pass[k].wait_send)


def run_forward(reach, gather, tokens, docs, heads, cosine, sine):
    chips, group = gather.chips, gather.group
    span, width = tokens.shape
    inner = SSM_HEADS * SSM_HEAD
    half, conv_width = inner // 2, inner + 2 * STATE
    kv_width = 2 * KV_HEADS * HEAD
    f32, low = jnp.float32, jnp.bfloat16
    shape = jax.ShapeDtypeStruct
    dma = pltpu.SemaphoreType.DMA
    vmem = pltpu.VMEM
    column = shape((span, 128), f32)
    outs = [
        shape((span, width), low),
        shape((span, HEADS * HEAD), low),
        shape((span, inner), f32),
        shape((span + 8, conv_width), f32),
        shape((span, conv_width), f32),
        column,
        column,
        column,
        shape((SSM_HEADS, 1, span), f32),
        column,
        column,
        shape((2, 8, half), f32),
        shape((8, 128), f32),
        shape((span, HEADS * HEAD), low),
        shape((HEADS * HEAD, span), low),
        shape((HEADS, 1, span), f32),
        shape((span, inner), f32),
        shape((2, STATE, half), f32),
        shape((reach + 1, 2, span, kv_width), low),
        shape((2 * (reach + 1), span, 128), f32),
        shape((group, *gather.pack.shape), low),
        shape((CONV - 1, span, 128), f32),
        shape((8, conv_width), f32),
        shape((8, width), f32),
    ]
    scratch = [
        vmem((span, kv_width), low),
        vmem((group, *gather.cut[0].shape), low),
        vmem((group, *gather.cut[1].shape), low),
        vmem((16, conv_width), low),
        vmem((16, conv_width), low),
        vmem((span + 8, 128), f32),
        vmem((8, inner), f32),
        vmem((HEADS, span, 128), low),
        vmem((span, span), f32),
        vmem((128, span), low),
        vmem((HEADS * HEAD, span), f32),
        vmem((HEADS, 1, span), f32),
        vmem((span, inner), low),
        vmem((span, inner), low),
        vmem((SSM_HEADS, span, 128), f32),
        vmem((span, span), f32),
        vmem((2, STATE, half), f32),
        vmem((STATE, half), low),
        vmem((STATE, half), low),
        vmem((8, half), f32),
        vmem((STATE, half), low),
        vmem((8, half), f32),
        vmem((reach + 1, STATE, half), low),
        vmem((reach + 1, 8, half), f32),
        vmem((STATE, half), f32),
        vmem((STATE, half), f32),
        dma((2,)),
        dma,
        dma,
        dma((reach + 1,)),
        dma((reach + 1,)),
        dma((reach + 1,)),
        dma((reach + 1,)),
        dma((2,)),
        dma((2,)),
        dma((reach + 1, 2)),
        dma((reach + 1, 2)),
        dma,
        dma,
    ]
    vm, anywhere = pl.BlockSpec(memory_space=pltpu.VMEM), pl.BlockSpec(memory_space=pl.ANY)
    many = len(gather.cut)
    results = pl.pallas_call(
        functools.partial(forward_kernel, reach, gather),
        out_shape=[*outs, *gather.outs()],
        in_specs=[vm] * 6 + [anywhere] * many,
        out_specs=[vm] * len(outs) + [anywhere] * many,
        scratch_shapes=[*scratch, *gather.scratch()],
        compiler_params=pltpu.CompilerParams(
            collective_id=2, has_side_effects=True, vmem_limit_bytes=VMEM_LIMIT
        ),
        name="run_forward",
    )(tokens, gather.pack, docs, heads, cosine, sine, *gather.cut)
    full = [part.reshape(-1, part.shape[-1]) for part in results[len(outs) :]]
    return results[: len(outs)], full


def mix_backward_kernel(reach, plan, *refs):
    chips, extras = plan.chips, plan.extras
    many = len(plan.chunks)
    cut = [23, len(plan.operands()), 5, many, 50]
    groups = []
    for size in cut:
        groups.append(refs[:size])
        refs = refs[size:]
    (
        q_ref,
        kvw_ref,
        segc_ref,
        segr_ref,
        act_ref,
        dt_ref,
        run_ref,
        runt_ref,
        e_ref,
        wd_ref,
        car_ref,
        skip_ref,
        attt_ref,
        inv_ref,
        ent_ref,
        gout_ref,
        gmix_ref,
        rate_ref,
        ext_ref,
        step_ref,
        rows_ref,
        taps_ref,
        same_ref,
    ) = groups[0]
    (
        dq_ref,
        dkv_ref,
        dconv,
        conv_sums,
        heads_ref,
    ) = groups[2]
    (
        qa,
        da,
        bias,
        kt,
        dqt,
        centre,
        dk,
        dv,
        part_out,
        part_in,
        sum_out,
        sum_in,
        xdt,
        xw,
        ge,
        gramt,
        dgram,
        own_grad,
        half_out,
        half_in,
        car_in,
        chip_out,
        chip_car,
        chip_in,
        chip_car_in,
        later_out,
        later,
        acc,
        qrow,
        qcol,
        dxdt,
        sums,
        fold_ref,
        skip_row,
        padded,
        last_rows,
        rim_out,
        rim_in,
        rim_s,
        rim_r,
        pp_s,
        pp_r,
        pa_s,
        pa_r,
        ha_s,
        ha_r,
        ca_s,
        ca_r,
        la_s,
        la_r,
    ) = groups[4]
    me = seat()
    rep, reps = lax.axis_index("rep"), lax.axis_size("rep")
    beyond = [{"rep": lax.rem(rep + 4 * e, reps)} for e in range(1, extras)]
    reduction = plan.steps(me, groups[1], groups[3], refs)
    chip, core = axis_seat()
    grp = lax.axis_index("grp")
    span = q_ref.shape[0]
    inner = SSM_HEADS * SSM_HEAD
    half = inner // 2
    low = jnp.bfloat16
    partner = {"grp": chip * 2 + 1 - core}
    first = core == 0

    def behind(k):
        return {"grp": lax.rem(grp - 2 * k + 2 * chips, 2 * chips)}

    greet_group([me["x"], me["y"], *beyond])
    for _ in plan.lefts:
        next(reduction)
    in_map = act_ref[:, inner : inner + STATE]
    out_map = act_ref[:, inner + STATE :]
    in_low, out_low = in_map.astype(low), out_map.astype(low)
    weight = wd_ref[...] * dt_ref[...]
    for pair in range(SSM_HEADS // 2):
        at = slice(pair * 128, (pair + 1) * 128)
        x_pair = act_ref[:, at]
        ge[:, at] = (gmix_ref[:, at] * pair_columns(e_ref, pair)).astype(low)
        xdt[:, at] = (x_pair * pair_columns(dt_ref, pair)).astype(low)
        xw[:, at] = (x_pair * pair_columns(weight, pair)).astype(low)
    out_turned = out_map.T.astype(low)
    for i in range(2):
        own_grad[i] = dot_plain(out_turned, ge[:, i * half : (i + 1) * half])
    half_out[...] = own_grad[1 - core].astype(low)
    align_heads(q_ref, qa, HEAD**-0.5)
    align_heads(gout_ref, da, 1.0)
    half_car = remote(car_ref.at[1 - core], car_in, ha_s.at[0], ha_r.at[0], partner)
    half_grad = remote(half_out, half_in, ha_s.at[1], ha_r.at[1], partner)
    half_car.start()
    half_grad.start()

    next(reduction, None)
    next(reduction, None)
    for pair in range(HEADS // 2):
        at = slice(pair * 128, (pair + 1) * 128)
        product = gout_ref[:, at].astype(jnp.float32).T * attt_ref[at, :].astype(jnp.float32)
        for odd in range(2):
            rows = product[odd * HEAD : (odd + 1) * HEAD]
            centre[2 * pair + odd] = jnp.sum(rows, axis=0, keepdims=True)
    dqt[...] = jnp.zeros_like(dqt)

    def attend_back(ref, key_docs, causal):
        bias[...] = same_document(key_docs, segr_ref[...], causal)
        kt[...] = ref[:, 0:128].astype(jnp.float32).T.astype(low)
        dk[...] = jnp.zeros_like(dk)
        dv[...] = jnp.zeros_like(dv)

        def per_head(head, _):
            group = lax.div(head, HEADS // KV_HEADS)
            scores = dot_rows(ref[:, 0:128], qa[head]) + bias[...]
            probs = jnp.exp(scores) * inv_ref[head]
            grad_probs = dot_rows(ref[:, 128:256], da[head])
            grad_scores = (probs * (grad_probs - centre[head])).astype(low)
            dv[...] += dot_plain(probs.astype(low), da[head])
            dk[...] += dot_plain(grad_scores, qa[head])
            rows = pl.ds(pl.multiple_of(group * HEAD, HEAD), HEAD)
            into = pl.ds(pl.multiple_of(head * HEAD, HEAD), HEAD)
            dqt[into, :] += dot_plain(kt[rows, :], grad_scores)
            return 0

        lax.fori_loop(0, HEADS, per_head, 0)

    passed, sent_on = {}, {}

    def pass_slot(back, side):
        live = slot_live((back, side), chip, core, reach)

        def compute():
            attend_back(kvw_ref.at[back, side], segc_ref[2 * (reach - back) + side], False)
            part_out[back, side, :, 0:128] = dk[...].astype(low)
            part_out[back, side, :, 128:256] = dv[...].astype(low)

        pl.when(live)(compute)

    def start_part(back):
        for side in (0, 1):
            passed[back, side] = remote(
                part_out.at[back, side],
                part_in.at[back],
                pp_s.at[back],
                pp_r.at[back],
                partner,
            )
            live = slot_live((back, side), chip, core, reach)
            pl.when(jnp.logical_and(live, core != side))(passed[back, side].start)

    def send_sum(back):
        both = chip - back >= 0
        partner_has = jnp.logical_and(both, core == 1) if back == reach else both

        def add_partner():
            passed[back, 0].wait_recv()
            value = part_out[back, core].astype(jnp.float32) + part_in[back].astype(jnp.float32)
            sum_out[back] = value.astype(low)

        pl.when(partner_has)(add_partner)
        if back == reach:

            def alone():
                sum_out[back] = part_out[back, core]

            pl.when(jnp.logical_and(both, core == 0))(alone)

    def send_sum_start(back):
        sent_on[back] = remote(
            sum_out.at[back], sum_in.at[back], pa_s.at[back], pa_r.at[back], behind(back)
        )
        pl.when(chip - back >= 0)(sent_on[back].start)

    next(reduction, None)
    pass_slot(reach, 1)
    next(reduction, None)

    half_car.wait_recv()
    half_grad.wait_recv()
    mine, theirs = own_grad[core], half_in[...].astype(jnp.float32)
    car_mine, car_theirs = car_ref[core], car_in[...]
    car_0 = jnp.where(first, car_mine, car_theirs)
    car_1 = jnp.where(first, car_theirs, car_mine)
    grad_0 = jnp.where(first, mine, theirs)
    grad_1 = jnp.where(first, theirs, mine)
    chip_out[...] = (grad_0 + car_0[0:1] * grad_1).astype(low)
    chip_car[...] = car_0 * car_1
    pass_slot(reach, 0)
    next(reduction, None)
    state_along = {}
    for k in range(1, reach + 1):
        state_along[k] = (
            remote(chip_out, chip_in.at[k], ca_s.at[k, 0], ca_r.at[k, 0], behind(k)),
            remote(chip_car, chip_car_in.at[k], ca_s.at[k, 1], ca_r.at[k, 1], behind(k)),
        )
        for copy in state_along[k]:
            pl.when(chip - k >= 0)(copy.start)
    start_part(reach)
    for back in range(reach - 1, 0, -1):
        pass_slot(back, 1)
        next(reduction, None)
        send_sum(back + 1)
        pass_slot(back, 0)
        next(reduction, None)
        send_sum_start(back + 1)
        start_part(back)
    pass_slot(0, 0)
    next(reduction, None)
    start_part(0)
    send_sum(1)

    send_sum_start(1)
    bias[...] = same_document(segc_ref[2 * reach + core], segr_ref[...], True)
    gramt[...] = lax.dot_general(
        in_map, out_map, (((1,), (1,)), ((), ())), precision=HIGHEST,
        preferred_element_type=jnp.float32,
    )
    dgram[...] = jnp.zeros_like(dgram)
    qcol[...] = jnp.zeros_like(qcol)
    qrow[...] = jnp.zeros_like(qrow)
    heads_of = lax.broadcasted_iota(jnp.int32, (inner, 128), 0) // SSM_HEAD
    fold_ref[...] = jnp.where(heads_of == lanes((inner, 128)), 1.0, 0.0).astype(low)

    def intra(quad, _):
        at = pl.ds(pl.multiple_of(quad * 256, 256), 256)
        grads = gmix_ref[:, at].astype(low)
        inputs = xdt[:, at]
        place = lanes((span, 256)) // 64
        value = jnp.zeros((span, 256), jnp.float32)
        for i in range(4):
            head = quad * 4 + i
            column = jnp.broadcast_to(runt_ref[head], (128, span)).T
            spread = runt_ref[head] - across(column, span)
            decay = jnp.exp(spread + bias[...])
            mixing = decay * gramt[...]
            alone = jnp.where(place == i, inputs, jnp.zeros_like(inputs))
            grad_mixing = dot_rows(alone, grads)
            dgram[...] += decay * grad_mixing
            product = mixing * grad_mixing
            qrow[pl.ds(head, 1), :] = jnp.sum(product, axis=0, keepdims=True)
            by_row = jnp.sum(product, axis=1, keepdims=True)
            qcol[...] = jnp.where(lanes((span, 128)) == head, by_row, qcol[...])
            part = dot_plain(mixing.astype(low), grads)
            value = jnp.where(place == i, part, value)
        dxdt[:, at] = value
        return 0

    quads = SSM_HEADS // 4
    for low_quad, high_quad in ((0, quads // 2), (quads // 2, quads)):
        lax.fori_loop(low_quad, high_quad, intra, 0)
        next(reduction, None)

    acc[...] = jnp.zeros_like(acc)
    for k in range(reach, 0, -1):

        def take(k=k):
            for copy in state_along[k]:
                copy.wait_recv()
            acc[...] = chip_in[k].astype(jnp.float32) + chip_car_in[k, 0:1] * acc[...]

        pl.when(chip + k < chips)(take)
    later_1, later_0 = acc[...], grad_1 + car_1[0:1] * acc[...]
    later[core] = jnp.where(first, later_0, later_1)
    later_out[...] = jnp.where(first, later_1, later_0)

    attend_back(kvw_ref.at[0, core], segc_ref[2 * reach + core], True)
    next(reduction, None)
    later_pass = remote(later_out, later.at[core], la_s, la_r, partner)
    later_pass.start()
    for pair in range(HEADS // 2):
        at = slice(pair * 128, (pair + 1) * 128)
        dq_ref[:, at] = dqt[at, :].T * HEAD**-0.5

    dkv_ref[:, 0:128] = dk[...]
    dkv_ref[:, 128:256] = dv[...]

    def add_zero():
        passed[0, 0].wait_recv()
        dkv_ref[...] += part_in[0].astype(jnp.float32)

    pl.when(core == 0)(add_zero)
    for k in range(1, reach + 1):

        def add_ahead(k=k):
            sent_on[k].wait_recv()
            dkv_ref[...] += sum_in[k].astype(jnp.float32)

        pl.when(chip + k < chips)(add_ahead)

    grad_low = dgram[...].astype(low)
    grad_in = dot_plain(grad_low, out_low)
    grad_out = dot_plain(dgram[...].T.astype(low), in_low)
    later_pass.wait_recv()

    def fold(value, own):
        high = value.astype(low)
        rest = (value - high.astype(jnp.float32)).astype(low)
        return dot_plain(high, fold_ref[own, :]) + dot_plain(rest, fold_ref[own, :])

    carried = jnp.zeros((1, 128), jnp.float32)
    skip_sum = jnp.zeros((8, 128), jnp.float32)
    x_inside, x_part, g_reached = (jnp.zeros((span, 128), jnp.float32) for _ in range(3))
    for block in range(inner // 256):
        i, start = block * 256 // half, block * 256 % half
        own, wide = slice(block * 256, (block + 1) * 256), slice(start, start + 256)
        entering, grads = ent_ref[i, :, wide], later[i, :, wide]
        by_lane = jnp.sum(entering * grads, axis=0, keepdims=True)
        carried = carried + fold(jnp.broadcast_to(by_lane, (8, 256)), own)[0:1]
        enter_low, later_low = entering.astype(low), grads.astype(low)
        grad_out = grad_out + dot_rows(ge[:, own], enter_low)
        grad_in = grad_in + dot_rows(xw[:, own], later_low)
        reached = dot_plain(out_low, enter_low)
        grad_xw = dot_plain(in_low, later_low)
        for j in range(2):
            pair = block * 2 + j
            at = slice(pair * 128, (pair + 1) * 128)
            here = slice(j * 128, (j + 1) * 128)
            x_pair, g_pair = act_ref[:, at], gmix_ref[:, at]
            part = grad_xw[:, here]
            inside = dxdt[:, at]
            dxdt[:, at] = (
                skip_ref[:, at] * g_pair
                + pair_columns(dt_ref, pair) * inside
                + pair_columns(weight, pair) * part
            )
            sums[0, :, here] = x_pair * inside
            sums[1, :, here] = x_pair * part
            sums[2, :, here] = g_pair * reached[:, here]
            skip_row[0:1, here] = jnp.sum(x_pair * g_pair, axis=0, keepdims=True)
        x_inside, x_part, g_reached = (
            total + fold(sums[n], own) for n, total in enumerate((x_inside, x_part, g_reached))
        )
        skip_sum = skip_sum + fold(jnp.broadcast_to(skip_row[0:1], (8, 256)), own)
        if block in LAST_TICKS:
            next(reduction, None)
    dxdt[:, inner : inner + STATE] = grad_in
    dxdt[:, inner + STATE :] = grad_out

    w_part = weight * x_part
    drun = qrow[...].T - qcol[...] + e_ref[...] * g_reached - w_part
    last = jnp.sum(w_part, axis=0, keepdims=True) + rate_ref[1:2] * carried
    rows = lax.broadcasted_iota(jnp.int32, (span, 128), 0)
    drun = jnp.where(rows == span - 1, drun + last, drun)
    upper = lax.broadcasted_iota(jnp.int32, (span, span), 0) <= lanes((span, span))
    drate = lax.dot_general(
        jnp.where(upper, 1.0, 0.0), drun, (((1,), (0,)), ((), ())), precision=HIGHEST,
        preferred_element_type=jnp.float32,
    )
    rate = rate_ref[0:1]
    dstep = x_inside + wd_ref[...] * x_part + rate * drate
    dstep = dstep / (1.0 + jnp.exp(-(step_ref[...] + rows_ref[0:1])))
    heads_ref[...] = jnp.zeros_like(heads_ref)
    heads_ref[0:1] = jnp.sum(rate * dt_ref[...] * drate, axis=0, keepdims=True)
    heads_ref[1:2] = skip_sum[0:1]
    heads_ref[2:3] = jnp.sum(dstep, axis=0, keepdims=True)

    conv_width = inner + 2 * STATE
    conv_sums[...] = jnp.zeros_like(conv_sums)
    padded[...] = jnp.zeros_like(padded)
    dconv[:, conv_width:] = dstep[:, 0:SSM_HEADS].astype(low)

    def convolve_back(j, _):
        at = pl.ds(pl.multiple_of(j * 128, 128), 128)
        value = jnp.broadcast_to(taps_ref[CONV : CONV + 1, at], (span, 128))
        inside = [same_ref[tap] > 0.0 for tap in range(CONV - 1)]
        for tap in range(CONV):
            term = ext_ref[5 + tap : 5 + tap + span, at] * taps_ref[tap : tap + 1, at]
            value = value + (jnp.where(inside[tap], term, 0.0) if tap < CONV - 1 else term)
        gate = 1.0 / (1.0 + jnp.exp(-value))
        grad = dxdt[:, at] * gate * (1.0 + value * (1.0 - gate))
        conv_sums[CONV : CONV + 1, at] = jnp.sum(grad, axis=0, keepdims=True)
        for tap in range(CONV):
            kept = jnp.where(inside[tap], grad, 0.0) if tap < CONV - 1 else grad
            product = kept * ext_ref[5 + tap : 5 + tap + span, at]
            conv_sums[tap : tap + 1, at] = jnp.sum(product, axis=0, keepdims=True)
            padded[tap, 8 : 8 + span, :] = kept * taps_ref[tap : tap + 1, at]
        value = jnp.zeros((span, 128), jnp.float32)
        edge = jnp.zeros((8, 128), jnp.float32)
        for tap in range(CONV):
            back = CONV - 1 - tap
            value = value + padded[tap, 8 + back : 8 + back + span, :]
            edge = edge + padded[tap, back : back + 8, :]
        rim_out[:, at] = edge
        dconv[:, at] = value.astype(jnp.bfloat16)
        last_rows[:, at] = value[span - 16 :]
        return 0

    lax.fori_loop(0, conv_width // 128, convolve_back, 0)
    rim = remote(rim_out, rim_in, rim_s, rim_r, {"grp": lax.rem(grp + 2 * chips - 1, 2 * chips)})
    pl.when(grp > 0)(rim.start)
    run_out(reduction)

    def add_rim():
        rim.wait_recv()
        dconv[span - 16 : span - 8, 0:conv_width] = last_rows[0:8, :].astype(low)
        last = last_rows[8:16, :] + rim_in[...]
        dconv[span - 8 :, 0:conv_width] = last.astype(low)

    pl.when(grp + 1 < 2 * chips)(add_rim)
    pl.when(grp > 0)(rim.wait_send)

    half_car.wait_send()
    half_grad.wait_send()
    later_pass.wait_send()
    for k in range(1, reach + 1):

        def sent(k=k):
            sent_on[k].wait_send()
            for copy in state_along[k]:
                copy.wait_send()

        pl.when(chip - k >= 0)(sent)
    for back in range(reach + 1):
        for side in (0, 1):
            if (back, side) in ((0, 1),):
                continue
            live = slot_live((back, side), chip, core, reach)
            pl.when(jnp.logical_and(live, core != side))(passed[back, side].wait_send)


def mix_backward(reach, operands, plan):
    sums = plan.outs()
    chips = lax.axis_size("grp") // 2
    span = operands[0].shape[0]
    inner = SSM_HEADS * SSM_HEAD
    half = inner // 2
    kv_width = 2 * KV_HEADS * HEAD
    f32, low = jnp.float32, jnp.bfloat16
    shape = jax.ShapeDtypeStruct
    dma = pltpu.SemaphoreType.DMA
    vmem = pltpu.VMEM
    outs = [
        shape((span, HEADS * HEAD), f32),
        shape((span, kv_width), f32),
        shape((span, inner + 2 * STATE + SSM_HEADS), low),
        shape((8, inner + 2 * STATE), f32),
        shape((8, 128), f32),
    ]
    scratch = [
        vmem((HEADS, span, 128), low),
        vmem((HEADS, span, 128), low),
        vmem((span, span), f32),
        vmem((128, span), low),
        vmem((HEADS * HEAD, span), f32),
        vmem((HEADS, 1, span), f32),
        vmem((span, 128), f32),
        vmem((span, 128), f32),
        vmem((reach + 1, 2, span, kv_width), low),
        vmem((reach + 1, span, kv_width), low),
        vmem((reach + 1, span, kv_width), low),
        vmem((reach + 1, span, kv_width), low),
        vmem((span, inner), low),
        vmem((span, inner), low),
        vmem((span, inner), low),
        vmem((span, span), f32),
        vmem((span, span), f32),
        vmem((2, STATE, half), f32),
        vmem((STATE, half), low),
        vmem((STATE, half), low),
        vmem((8, half), f32),
        vmem((STATE, half), low),
        vmem((8, half), f32),
        vmem((reach + 1, STATE, half), low),
        vmem((reach + 1, 8, half), f32),
        vmem((STATE, half), f32),
        vmem((2, STATE, half), f32),
        vmem((STATE, half), f32),
        vmem((128, span), f32),
        vmem((span, 128), f32),
        vmem((span, inner + 2 * STATE), f32),
        vmem((3, span, 256), f32),
        vmem((inner, 128), low),
        vmem((8, 256), f32),
        vmem((CONV, span + 16, 128), f32),
        vmem((16, inner + 2 * STATE), f32),
        vmem((8, inner + 2 * STATE), f32),
        vmem((8, inner + 2 * STATE), f32),
        dma,
        dma,
        dma((reach + 1,)),
        dma((reach + 1,)),
        dma((reach + 1,)),
        dma((reach + 1,)),
        dma((2,)),
        dma((2,)),
        dma((reach + 1, 2)),
        dma((reach + 1, 2)),
        dma,
        dma,
    ]
    results = pl.pallas_call(
        functools.partial(mix_backward_kernel, reach, plan),
        out_shape=[*outs, *sums],
        in_specs=[pl.BlockSpec(memory_space=pltpu.VMEM)] * (len(operands) + len(plan.operands())),
        out_specs=[pl.BlockSpec(memory_space=pltpu.VMEM)] * (len(outs) + len(sums)),
        scratch_shapes=[*scratch, *plan.scratch()],
        compiler_params=pltpu.CompilerParams(
            collective_id=3, has_side_effects=True, vmem_limit_bytes=VMEM_LIMIT
        ),
        name="mix_backward",
    )(*operands, *plan.operands())
    return results[: len(outs)], results[len(outs) :]


def shards(
    tokens,
    segments,
    input_gain,
    attention_in,
    attention_out,
    mixer_in,
    filter_taps,
    filter_bias,
    step_bias,
    decay_log,
    skip_scale,
    mixer_gain,
    mixer_out,
    feed_gain,
    gate_up,
    down_proj,
    cotangent,
):
    seq_count, span_len, model_width = tokens.shape
    row_count = seq_count * span_len
    seq_len = segments.shape[1]
    group_devices = lax.axis_size("grp")
    position = lax.axis_index("grp") * span_len
    inner_width = SSM_HEADS * SSM_HEAD
    xbc_width = inner_width + 2 * STATE
    query_width = HEADS * HEAD
    kv_width = KV_HEADS * HEAD
    rim_rows = CONV - 1
    def padded(value):
        return jnp.pad(value, ((0, 0), (0, 256 - value.shape[1])))

    small = [filter_taps] + [p[None] for p in (filter_bias, input_gain, mixer_gain, feed_gain)]
    pack = jnp.concatenate([padded(part) for part in small])
    shares = [attention_in, mixer_in, gate_up, down_proj, mixer_out, attention_out]
    gather = Gather(
        shares,
        [
            column_chunks(n, n, share.shape[1], pieces)[i][1:]
            for n, (share, pieces) in enumerate(zip(shares, (1, 4, 4, 2, 2, 1)))
            for i in range(pieces)
        ],
        pack,
    )
    offsets = position + jnp.arange(span_len, dtype=jnp.int32)
    cosine_table, sine_table = rope_tables(offsets, HEAD)
    cosine = jnp.concatenate([cosine_table] * 4, axis=1)
    sine = jnp.concatenate([-sine_table, sine_table] * 2, axis=1)
    reach = min(seq_len // (4 * span_len), group_devices // 2 - 1)
    chip = lax.axis_index("grp") // 2
    docs = jnp.concatenate([jnp.full((2 * reach * span_len,), -1, jnp.int32), segments[0]])
    window = lax.dynamic_slice_in_dim(docs, 2 * chip * span_len, 2 * (reach + 1) * span_len)
    window = window.reshape(2 * (reach + 1), 1, span_len).astype(jnp.float32)
    own_docs = lax.dynamic_slice_in_dim(segments[0], position, span_len)
    heads_rows = jnp.stack([step_bias, decay_log, skip_scale])
    heads_rows = jnp.pad(heads_rows, ((0, 5), (0, 128 - SSM_HEADS)))
    results, full = run_forward(
        reach,
        gather,
        tokens[0],
        window,
        heads_rows,
        cosine,
        sine,
    )
    full_attn_in, full_mix_in, full_gate_up, full_down, full_mix_out, full_attn_out = full
    (
        normed_low,
        query_rows,
        gate_part,
        ext_rows,
        active,
        step_wide,
        steps,
        running,
        running_turned,
        enter_decay,
        tail_decay,
        carried_lanes,
        carried,
        attended,
        attended_turned,
        inverse_total,
        mixed,
        entering,
        kv_window,
        key_docs,
        packs,
        same_docs,
        taps_wide,
        gain_in,
    ) = results
    full_mix_gain, full_feed_gain = (
        packs[:, 6 + i, : part.shape[0]].reshape(-1) for i, part in enumerate((mixer_gain, feed_gain))
    )
    token_float = tokens.reshape(row_count, model_width).astype(jnp.float32)
    back_attn_in, back_attn_out, back_mix_in = full_attn_in, full_attn_out, full_mix_in
    back_mix_out, back_gate_up, back_down = full_mix_out, full_gate_up, full_down
    gate_part, mixed = gate_part[None], mixed[None]
    rate_scale = -jnp.exp(decay_log)
    recurrence = (
        active,
        steps,
        running,
        running_turned,
        enter_decay,
        tail_decay,
        carried_lanes,
        jnp.repeat(skip_scale, SSM_HEAD)[None, :],
    )
    normed_mix, gate_back = jax.vjp(gated_norm, mixed, gate_part, full_mix_gain.astype(jnp.float32))
    normed_mix_low = normed_mix.reshape(row_count, inner_width).astype(jnp.bfloat16)
    hidden = (
        token_float
        + jnp.dot(attended, full_attn_out, preferred_element_type=jnp.float32)
        + jnp.dot(normed_mix_low, full_mix_out, preferred_element_type=jnp.float32)
    )
    normed_feed, feed_back = jax.vjp(rms_scale, hidden, full_feed_gain.astype(jnp.float32))
    normed_feed_low = normed_feed.astype(jnp.bfloat16)
    gate_vals = jnp.dot(normed_feed_low, full_gate_up, preferred_element_type=jnp.float32)
    activation, act_back = jax.vjp(swiglu, gate_vals[:, :FF], gate_vals[:, FF:])
    activation_low = activation.astype(jnp.bfloat16)
    out_rows = (
        hidden + jnp.dot(activation_low, full_down, preferred_element_type=jnp.float32)
    ).astype(jnp.bfloat16)
    grad_rows = cotangent.reshape(row_count, model_width)
    grad_act = jnp.dot(grad_rows, back_down.T, preferred_element_type=jnp.float32)
    grad_gate, grad_upper = act_back(grad_act)
    grad_gu = jnp.concatenate([grad_gate, grad_upper], axis=-1).astype(jnp.bfloat16)
    grad_feed_in = jnp.dot(grad_gu, back_gate_up.T, preferred_element_type=jnp.float32)
    grad_hidden_norm, grad_feed = feed_back(grad_feed_in)
    grad_hidden = grad_rows.astype(jnp.float32) + grad_hidden_norm
    grad_hidden_low = grad_hidden.astype(jnp.bfloat16)
    grad_attended = jnp.dot(
        grad_hidden_low, back_attn_out.T, preferred_element_type=jnp.float32
    ).astype(jnp.bfloat16)
    grad_normed_mix = jnp.dot(grad_hidden_low, back_mix_out.T, preferred_element_type=jnp.float32)
    grad_mixed, grad_gate_part, grad_mix_gain = gate_back(
        grad_normed_mix.reshape(seq_count, span_len, inner_width)
    )
    heads_scale = jnp.stack([rate_scale, carried[0, :SSM_HEADS]])
    heads_scale = jnp.pad(heads_scale, ((0, 6), (0, 128 - SSM_HEADS)))
    operands = (
        query_rows,
        kv_window,
        key_docs,
        own_docs[None, :].astype(jnp.float32),
        *recurrence,
        attended_turned,
        inverse_total,
        entering,
        grad_attended,
        grad_mixed.reshape(row_count, inner_width),
        heads_scale,
        ext_rows,
        step_wide,
        heads_rows,
        taps_wide,
        same_docs,
    )
    early = GradPlan(
        [normed_feed_low, activation_low, normed_mix_low, attended_turned],
        [False, False, False, True],
        [grad_gu, grad_rows, grad_hidden_low],
        [
            *column_chunks(0, 0, 2 * FF, 4),
            *column_chunks(1, 1, model_width, 2),
            *column_chunks(2, 2, model_width, 2),
            (3, 2, 0, model_width),
        ],
        handed=HANDED,
    )
    (grad_query, grad_kv_own, grad_conv, conv_sums, grad_heads), early_sums = mix_backward(
        reach, operands, early
    )
    late = GradPlan(
        [normed_low],
        [False],
        [
            grad_gate_part.reshape(row_count, inner_width).astype(jnp.bfloat16),
            grad_conv,
            jax.ShapeDtypeStruct((row_count, attention_in.shape[1]), jnp.bfloat16),
        ],
        [
            *column_chunks(0, 0, inner_width, 2),
            (0, 2, 0, attention_in.shape[1]),
            *column_chunks(0, 1, xbc_width + SSM_HEADS, CONV_PIECES),
        ],
        later=(2,),
        received=early_sums[len(early_sums) - HANDED :],
    )
    done, own = len(early_sums) - HANDED, 3 + CONV_PIECES
    place = [*range(done), *range(done + own, done + own + HANDED)]
    joins = (
        place[:4],
        place[4:6],
        place[6:8],
        place[8:],
        [done, done + 1, *range(done + 3, done + own)],
        [done + 2],
    )
    grad_token, summed, joined = run_tail(
        late,
        early_sums[:done],
        joins,
        conv_sums,
        grad_query,
        grad_kv_own,
        cosine,
        sine,
        tokens[0],
        gain_in,
        grad_hidden,
        grad_heads,
        grad_feed[None],
        grad_mix_gain[None],
        full_mix_in,
        full_attn_in,
    )
    index = lax.axis_index("grp")

    def own_part(value):
        size = value.shape[-1] // group_devices
        return lax.dynamic_slice_in_dim(value, index * size, size, value.ndim - 1)

    own_gate_up, own_down, own_mix_out, own_attn_out, own_mix_in, own_attn_in = joined
    return (
        out_rows.reshape(seq_count, span_len, model_width),
        grad_token.reshape(seq_count, span_len, model_width),
        own_part(summed[7, :model_width]),
        own_attn_in,
        own_attn_out,
        own_mix_in,
        own_part(summed[:CONV]),
        own_part(summed[CONV]),
        *(summed[7, model_width + 128 * i :][:SSM_HEADS] for i in range(3)),
        own_part(summed[5, :inner_width]),
        own_mix_out,
        own_part(summed[6, :model_width]),
        own_gate_up,
        own_down,
    )


def solution(mesh):
    return jax.shard_map(
        shards,
        mesh=mesh,
        in_specs=(
            P("rep", "grp", None),
            P("rep", None),
            P("grp"),
            P("grp", None),
            P("grp", None),
            P("grp", None),
            P(None, "grp"),
            P("grp"),
            P(),
            P(),
            P(),
            P("grp"),
            P("grp", None),
            P("grp"),
            P("grp", None),
            P("grp", None),
            P("rep", "grp", None),
        ),
        out_specs=(
            P("rep", "grp", None),
            P("rep", "grp", None),
            P("grp"),
            P("grp", None),
            P("grp", None),
            P("grp", None),
            P(None, "grp"),
            P("grp"),
            P(),
            P(),
            P(),
            P("grp"),
            P("grp", None),
            P("grp"),
            P("grp", None),
            P("grp", None),
        ),
        check_vma=False,
    )
```

```python
import functools
import itertools
import math
from functools import partial

import jax
import jax.numpy as jnp
from jax import lax
from jax.experimental import pallas as pl
from jax.experimental.pallas import tpu as pltpu
from jax.sharding import PartitionSpec as P

HEADS = 8
KV_HEADS = 2
HEAD = 64
SSM_HEADS = 24
SSM_HEAD = 64
STATE = 128
CONV = 4
FF = 2048


NORM_EPS = 1e-05
ROPE_BASE = 100000000000.0
HIGHEST = lax.Precision.HIGHEST


def rms_scale(values, scales):
    return values * lax.rsqrt(jnp.mean(values * values, axis=-1, keepdims=True) + NORM_EPS) * scales


def rope_tables(positions, head_width):
    indices = jnp.arange(head_width // 2, dtype=jnp.float32)
    frequency = ROPE_BASE ** (-2.0 * indices / head_width)
    angles = positions.astype(jnp.float32)[:, None] * frequency[None, :]
    return (jnp.cos(angles), jnp.sin(angles))


def gated_norm(mixed, gate_part, scales):
    flat_mixed = mixed.reshape(gate_part.shape)
    return rms_scale(flat_mixed * jax.nn.silu(gate_part), scales)


def swiglu(gate_vals, up_vals):
    return jax.nn.silu(gate_vals) * up_vals


MESH = pl.DeviceIdType.MESH
HIDDEN = -1e30
VMEM_LIMIT = 67043328
TAIL_LAG = 1
WINDOW = 2
HANDED = 5
CONV_PIECES = 2
LAST_TICKS = (2, 5)


def seat():
    rep, grp = lax.axis_index("rep"), lax.axis_index("grp")
    chips = lax.axis_size("grp") // 2
    quarter = lax.rem(rep, 4)
    base = rep - quarter
    flip_x = quarter + 1 - 2 * lax.rem(quarter, 2)
    flip_y = lax.rem(quarter + 2, 4)
    chip, core = lax.div(grp, 2), lax.rem(grp, 2)
    return dict(
        quarter=quarter,
        qx=flip_x,
        qy=flip_y,
        qd=lax.rem(flip_x + 2, 4),
        chip=chip,
        core=core,
        x={"rep": base + flip_x},
        y={"rep": base + flip_y},
        partner={"grp": chip * 2 + 1 - core},
        along=[{"grp": lax.rem(chip + k, chips) * 2 + core} for k in range(chips)],
        chip_to=[lax.rem(chip + k, chips) for k in range(chips)],
        chip_from=[lax.rem(chip - k + chips, chips) for k in range(chips)],
    )


def remote(source, target, sent, arrived, device):
    return pltpu.make_async_remote_copy(
        src_ref=source,
        dst_ref=target,
        send_sem=sent,
        recv_sem=arrived,
        device_id=device,
        device_id_type=MESH,
    )


def greet(me, extra=()):
    barrier = pltpu.get_barrier_semaphore()
    others = [me["x"], me["y"], me["partner"], *me["along"][1:], *extra]
    for device in others:
        pl.semaphore_signal(barrier, inc=1, device_id=device, device_id_type=MESH)
    pl.semaphore_wait(barrier, len(others))


def near_first(chips):
    return sorted(range(1, chips), key=lambda k: min(k, chips - k))


class Gather:
    def __init__(self, shards, chunks, pack):
        self.group = lax.axis_size("grp")
        self.chips = self.group // 2
        self.cut = [s.reshape(4, s.shape[0] // 4, s.shape[1]) for s in shards]
        self.chunks = chunks
        self.pack = pack

    def outs(self):
        shape = jax.ShapeDtypeStruct
        return [shape((self.group, *part.shape), part.dtype) for part in self.cut]

    def scratch(self):
        dma = pltpu.SemaphoreType.DMA
        count = len(self.chunks) + 1
        own = [pltpu.VMEM(part.shape, part.dtype) for part in self.cut]
        return [*own, *[dma((count, self.chips))] * 10, dma((len(self.cut), 2))]

    def steps(self, me, ins, pack, packs, outs, scratch):
        chips, count = self.chips, len(self.chunks)
        own_copy = scratch[: len(ins)]
        zs, zr, xs, xr, ys, yr, ds, dr, cs, cr, ls = scratch[len(ins) :]
        own = me["chip"] * 2 + me["core"]
        order = near_first(chips)
        along, over_x, over_y, diagonal, self.across = {}, {}, {}, {}, {}

        def part(m, ref):
            n, start, width = self.chunks[m]
            return ref if width == outs[n].shape[-1] else ref.at[..., start : start + width]

        def weight(m):
            return self.chunks[m][0]

        def start_along(m):
            source = part(m, ins[weight(m)].at[me["quarter"]])
            place = part(m, outs[weight(m)].at[own, me["quarter"]])
            for k in order:
                along[m, k] = remote(source, place, zs.at[m, k], zr.at[m, k], me["along"][k])
                along[m, k].start()

        def block(m, k):
            return outs[weight(m)].at[me["chip_from"][k] * 2 + me["core"]]

        for k in order:
            along[count, k] = remote(
                pack, packs.at[own], zs.at[count, k], zr.at[count, k], me["along"][k]
            )
            along[count, k].start()
        self.across[count, 0] = remote(
            pack, packs.at[own], cs.at[count, 0], cr.at[count, 0], me["partner"]
        )
        self.across[count, 0].start()
        packs[own] = pack[...]
        for m in range(min(WINDOW, count)):
            start_along(m)
        load, store = [], []
        for n in range(len(ins)):
            load.append(pltpu.make_async_copy(ins[n], own_copy[n], ls.at[n, 0]))
            load[-1].start()
        for m in range(count):
            source, place = part(m, ins[weight(m)]), part(m, outs[weight(m)].at[own])
            self.across[m, 0] = remote(source, place, cs.at[m, 0], cr.at[m, 0], me["partner"])
            self.across[m, 0].start()
        for n in range(len(ins)):
            load[n].wait()
            store.append(pltpu.make_async_copy(own_copy[n], outs[n].at[own], ls.at[n, 1]))
            store[-1].start()
        for k in order:
            along[count, k].wait_recv()
            piece = packs.at[me["chip_from"][k] * 2 + me["core"]]
            self.across[count, k] = remote(
                piece, piece, cs.at[count, k], cr.at[count, k], me["partner"]
            )
            self.across[count, k].start()
        self.store = store
        yield
        for step in range(count + 2):
            m = step
            if m < count:
                for k in order:
                    along[m, k].wait_recv()
                    piece = part(m, block(m, k).at[me["quarter"]])
                    over_x[m, k] = remote(piece, piece, xs.at[m, k], xr.at[m, k], me["x"])
                    over_y[m, k] = remote(piece, piece, ys.at[m, k], yr.at[m, k], me["y"])
                    over_x[m, k].start()
                    over_y[m, k].start()
                if m + WINDOW < count:
                    start_along(m + WINDOW)
            m = step - 1
            if 0 <= m < count:
                for k in order:
                    if (m + k) % 2 == 0:
                        over_x[m, k].wait_recv()
                        q, device = me["qx"], me["y"]
                    else:
                        over_y[m, k].wait_recv()
                        q, device = me["qy"], me["x"]
                    piece = part(m, block(m, k).at[q])
                    diagonal[m, k] = remote(piece, piece, ds.at[m, k], dr.at[m, k], device)
                    diagonal[m, k].start()
            m = step - 2
            if 0 <= m < count:
                for k in order:
                    if (m + k) % 2 == 0:
                        over_y[m, k].wait_recv()
                    else:
                        over_x[m, k].wait_recv()
                    diagonal[m, k].wait_recv()
                    piece = part(m, block(m, k))
                    self.across[m, k] = remote(
                        piece, piece, cs.at[m, k], cr.at[m, k], me["partner"]
                    )
                    self.across[m, k].start()
            yield
        self.all_copies = (along, over_x, over_y, diagonal, self.across)

    def arrive(self, m):
        for k in range(self.chips):
            self.across[m, k].wait_recv()

    def finish(self, waited):
        for m in range(len(self.chunks)):
            if m not in waited:
                self.arrive(m)
        for copies in self.all_copies:
            for copy in copies.values():
                copy.wait_send()


def f32(value):
    return value.astype(jnp.float32)


def turn_rows(source, turned, chips, piece, is_turned):
    features = source.shape[0] if is_turned else source.shape[1]
    width = math.lcm(128, piece)
    for start in range(0, features, width):
        if is_turned:
            value = f32(source[start : start + width, :])
        else:
            value = f32(source[:, start : start + width]).T
        for i in range(width // piece):
            at = start // piece + i
            chip, core, quarter = at // 8, (at // 4) % 2, at % 4
            block = value[i * piece : (i + 1) * piece].astype(jnp.bfloat16)
            turned[core, quarter, chip * piece : (chip + 1) * piece, :] = block


class GradPlan:
    def __init__(self, lefts, turned, rights, chunks, later=(), handed=0, received=()):
        self.handed, self.received = handed, list(received)
        self.later, self.swap_right = later, {}
        self.chips = lax.axis_size("grp") // 2
        self.extras = lax.axis_size("rep") // 4
        self.lefts, self.turned, self.rights, self.chunks = lefts, turned, rights, chunks
        self.tokens = rights[0].shape[0]
        sizes = [x.shape[0] if flag else x.shape[1] for x, flag in zip(lefts, turned)]
        self.rows = [size // 8 for size in sizes]
        self.piece = [size // (8 * self.chips) for size in sizes]

    def operands(self):
        rights = [r for n, r in enumerate(self.rights) if n not in self.later]
        return [*self.lefts, *rights, *self.received]

    def outs(self):
        whole = len(self.chunks) - self.handed
        shapes = [
            (4 if m < whole else self.chips, self.piece[a], width)
            for m, (a, _, _, width) in enumerate(self.chunks)
        ]
        shapes += [(4, *total.shape[1:]) for total in self.received]
        return [jax.ShapeDtypeStruct(shape, jnp.bfloat16) for shape in shapes]

    def scratch(self):
        low, vmem, dma = jnp.bfloat16, pltpu.VMEM, pltpu.SemaphoreType.DMA
        lefts, rights, count = len(self.lefts), len(self.rights), len(self.chunks)
        work = [vmem((2, 4, rows, self.tokens), low) for rows in self.rows]
        work += [vmem((4, rows, self.tokens), low) for rows in self.rows]
        work += [vmem(right.shape, low) for right in self.rights]
        shapes = [(self.rows[a], self.piece[a], width) for a, _, _, width in self.chunks]
        work += [vmem((4, rows, width), low) for rows, _, width in shapes]
        work += [vmem((2, rows, width), low) for rows, _, width in shapes]
        work += [vmem((rows, width), low) for rows, _, width in shapes]
        work += [vmem((self.chips, piece, width), low) for _, piece, width in shapes]
        ends = [shape[1:] for shape in shapes] + [total.shape[1:] for total in self.received]
        count = len(ends)
        work += [vmem((self.chips - 1, *end), low) for end in ends]
        if self.extras > 1:
            work += [vmem((self.extras, *end), low) for end in ends]
        sems = [dma((lefts,))] * 2 + [dma((rights,))] * 2
        sems += [dma((count, 2)), dma((count, 2)), dma((count,)), dma((count,))]
        sems += [dma((count, self.chips))] * 2 + [dma((count, self.extras))] * 2
        sems += [dma((count, 3))] * 2
        return [*work, *sems]

    def steps(self, me, ins, outs, scratch, lag=2):
        chips, extras, count = self.chips, self.extras, len(self.chunks)
        whole, ends = count - self.handed, count + len(self.received)
        lefts, rights = ins[: len(self.lefts)], ins[len(self.lefts) :]
        rights, received = rights[: len(self.rights)], rights[len(self.rights) :]
        groups = []
        sizes = [len(lefts), len(lefts), len(rights), *[count] * 4, ends]
        for size in sizes + ([ends] if extras > 1 else []):
            groups.append(scratch[:size])
            scratch = scratch[size:]
        turned, turned_in, rights_in, parts, one, two, total, slots = groups[:8]
        extra_in = groups[8] if extras > 1 else ()
        la_s, la_r, ri_s, ri_r, s1, r1, s2, r2, zs, zr, es, er, gs, gr = scratch
        total = [*total, *received]
        core = me["core"]
        reps, rep = lax.axis_size("rep"), lax.axis_index("rep")
        beyond = [{"rep": lax.rem(rep + 4 * e, reps)} for e in range(1, extras)]
        swap_left, swap_right = {}, self.swap_right
        for n in range(len(rights)):
            swap_right[n] = remote(rights[n], rights_in[n], ri_s.at[n], ri_r.at[n], me["partner"])
            if n not in self.later and n == 0:
                swap_right[n].start()
        for n in range(len(lefts)):
            turn_rows(lefts[n], turned[n], chips, self.piece[n], self.turned[n])
            swap_left[n] = remote(
                turned[n].at[1 - core], turned_in[n], la_s.at[n], la_r.at[n], me["partner"]
            )
            if n == 0:
                swap_left[n].start()
            yield
        waiting = [swap_right[n] for n in range(1, len(rights)) if n not in self.later]
        waiting = [copy for pair in itertools.zip_longest([swap_left[n] for n in range(1, len(lefts))], waiting) for copy in pair if copy is not None]
        have = set()
        first, second, along, other, spread = {}, {}, {}, {}, {}

        def form(m):
            a, b, start, width = self.chunks[m]
            for key, copy in (("left", a), swap_left[a]), (("right", b), swap_right[b]):
                if key not in have:
                    have.add(key)
                    copy.wait_recv()
            at = slice(start, start + width)

            def quarter(q, _):
                value = dot_plain(turned[a][core, q], rights[b][:, at])
                value = value + dot_plain(turned_in[a][q], rights_in[b][:, at])
                parts[m][q] = value.astype(jnp.bfloat16)
                return 0

            lax.fori_loop(0, 4, quarter, 0)

        def send_first(m, i):
            device, mine = (me["x"], me["qx"]) if m % 2 == 0 else (me["y"], me["qy"])
            q = me["qd"] if i == 1 else mine
            first[m, i] = remote(parts[m].at[q], one[m].at[i], s1.at[m, i], r1.at[m, i], device)
            first[m, i].start()

        def send_second(m):
            rows = self.rows[self.chunks[m][0]]
            device, q = (me["y"], me["qy"]) if m % 2 == 0 else (me["x"], me["qx"])
            first[m, 1].wait_recv()

            def add(j, _):
                at = pl.ds(pl.multiple_of(j * 64, 64), 64)
                value = f32(parts[m][q, at, :]) + f32(one[m][1, at, :])
                parts[m][q, at, :] = value.astype(jnp.bfloat16)
                return 0

            lax.fori_loop(0, rows // 64, add, 0)
            second[m] = remote(parts[m].at[q], two[m], s2.at[m], r2.at[m], device)
            second[m].start()

        def send_along(m):
            piece = self.piece[self.chunks[m][0]]
            first[m, 0].wait_recv()
            second[m].wait_recv()
            for j in range(chips):
                at = slice(j * piece, (j + 1) * piece)
                value = f32(parts[m][me["quarter"], at, :]) + f32(one[m][0, at, :]) + f32(two[m][at, :])
                (total if m < whole else outs)[m][j] = value.astype(jnp.bfloat16)
            if m < whole:
                pass_along(m)

        def pass_along(m):
            for k in near_first(chips):
                along[m, k] = remote(
                    total[m].at[me["chip_to"][k]],
                    slots[m].at[k - 1],
                    zs.at[m, k],
                    zr.at[m, k],
                    me["along"][k],
                )
                along[m, k].start()

        def send_spread(m):
            value = f32(total[m][me["chip"]])
            for k in near_first(chips):
                along[m, k].wait_recv()
                value = value + f32(slots[m][k - 1])
            if extras > 1:
                extra_in[m][0] = value.astype(jnp.bfloat16)
                for e in range(1, extras):
                    other[m, e] = remote(
                        extra_in[m].at[0],
                        extra_in[m].at[e],
                        es.at[m, e],
                        er.at[m, e],
                        beyond[e - 1],
                    )
                    other[m, e].start()
                for e in range(1, extras):
                    other[m, e].wait_recv()
                    value = value + f32(extra_in[m][e])
            outs[m][me["quarter"]] = value.astype(jnp.bfloat16)
            piece = outs[m].at[me["quarter"]]
            for i, device in enumerate((me["x"], me["y"])):
                spread[m, i] = remote(piece, piece, gs.at[m, i], gr.at[m, i], device)
                spread[m, i].start()

        def send_diagonal(m):
            way = m % 2
            spread[m, way].wait_recv()
            q, device = (me["qx"], me["y"]) if way == 0 else (me["qy"], me["x"])
            piece = outs[m].at[q]
            spread[m, 2] = remote(piece, piece, gs.at[m, 2], gr.at[m, 2], device)
            spread[m, 2].start()

        for m in range(count, ends):
            pass_along(m)
        stages = (send_second, send_along, send_spread, send_diagonal)
        spans = (count, count, whole, whole)
        last = max([lag * (n + 1) + span for n, span in enumerate(spans)])
        for step in range(max(last, len(received) + 2 * lag)):
            if step < count:
                form(step)
                send_first(step, 1)
            if 1 <= step <= count:
                send_first(step - 1, 0)
            for _ in range(2):
                if waiting:
                    waiting.pop(0).start()
            for n, stage in enumerate(stages):
                m = step - lag * (n + 1)
                if 0 <= m < spans[n]:
                    stage(m)
                m = count + step - lag * (n - 1)
                if n >= 2 and count <= m < ends:
                    stage(m)
            yield
        for m in [*range(whole), *range(count, ends)]:
            spread[m, 1 - m % 2].wait_recv()
            spread[m, 2].wait_recv()
        for copies in (swap_left, swap_right, first, second, along, other, spread):
            for copy in copies.values():
                copy.wait_send()
        yield


def small_steps(me, chips, extras, vec, out, stage, slots, sems, more):
    ss, sr, zs, zr = sems
    copies = []
    value = vec[...]
    hops = [me["x"], me["y"], me["partner"]]
    for i, device in enumerate(hops):
        stage[i] = value
        copies.append(remote(stage.at[i], slots.at[i], ss.at[i], sr.at[i], device))
        copies[-1].start()
        yield
        copies[-1].wait_recv()
        value = value + slots[i]
    if extras > 1:
        stage[3] = value
        for e in range(1, extras):
            at = 3 + chips + e
            copies.append(remote(stage.at[3], slots.at[at], ss.at[2 + e], sr.at[2 + e], more[e - 1]))
            copies[-1].start()
        yield
        for e in range(1, extras):
            copies[-e].wait_recv()
        for e in range(1, extras):
            value = value + slots[3 + chips + e]
    stage[4] = value
    along = []
    for k in near_first(chips):
        along.append(remote(stage.at[4], slots.at[3 + k], zs.at[k], zr.at[k], me["along"][k]))
        along[-1].start()
    yield
    for copy in along:
        copy.wait_recv()
    for k in range(1, chips):
        value = value + slots[3 + k]
    out[...] = value
    for copy in copies + along:
        copy.wait_send()
    yield


def run_out(steps):
    for _ in steps:
        pass


def tail_kernel(plan, early, joins, *refs):
    groups = []
    kept = len(plan.outs())
    for size in (len(plan.operands()), 13 + len(early), 2 + len(joins), 6 + kept):
        groups.append(refs[:size])
        refs = refs[size:]
    normed_ref, dz_ref, dconv, *received = groups[0]
    (
        conv_sums,
        dq_ref,
        dkv_ref,
        cosine_ref,
        sine_ref,
        tokens_ref,
        gain_ref,
        hidden_ref,
        early_heads,
        feed_gain_ref,
        mixer_gain_ref,
        mixer_w,
        attention_w,
    ) = groups[1][len(early) :]
    token_grad_ref, total_ref, *joined = groups[2]
    (
        dproj,
        mixer_rows,
        attention_rows,
        dnormed,
        vec,
        fetch_sem,
        *sums,
    ) = groups[3]
    stage, slots, small_sems = refs[-6], refs[-5], refs[-4:]
    me = seat()
    rep, reps = lax.axis_index("rep"), lax.axis_size("rep")
    span, conv_width = dz_ref.shape[0], conv_sums.shape[1]
    width = tokens_ref.shape[1]
    inner = dz_ref.shape[1]
    beyond = [{"rep": lax.rem(rep + 4 * e, reps)} for e in range(1, plan.extras)]
    greet(me, beyond)
    large = plan.steps(me, [normed_ref, dz_ref, dconv, dproj, *received], sums, refs[:-6], lag=TAIL_LAG)
    next(large)

    blocks = width // 256
    fetched = (
        pltpu.make_async_copy(mixer_w, mixer_rows, fetch_sem.at[0]),
        pltpu.make_async_copy(attention_w, attention_rows, fetch_sem.at[1]),
    )
    for copy in fetched:
        copy.start()

    low_half = lanes((span, 128)) % HEAD < HEAD // 2

    def turned_back(value):
        other = jnp.where(low_half, pltpu.roll(value, 128 - HEAD // 2, 1), pltpu.roll(value, HEAD // 2, 1))
        return value * cosine_ref[...] - other * sine_ref[...]

    queries = dq_ref.shape[1]
    for start in range(0, queries, 128):
        at = slice(start, start + 128)
        dproj[:, at] = turned_back(dq_ref[:, at]).astype(jnp.bfloat16)
    dproj[:, queries : queries + 128] = turned_back(dkv_ref[:, 0:128]).astype(jnp.bfloat16)
    dproj[:, queries + 128 :] = dkv_ref[:, 128:].astype(jnp.bfloat16)
    next(large)
    plan.swap_right[2].start()
    next(large)

    for copy in fetched:
        copy.wait()
    for i in range(blocks):
        at = slice(i * 256, (i + 1) * 256)
        value = dot_rows(dz_ref[...], mixer_rows[at, 0:inner])
        value = value + dot_rows(dconv[:, 0:conv_width], mixer_rows[at, inner : inner + conv_width])
        value = value + dot_rows(dconv[:, conv_width:], mixer_rows[at, inner + conv_width :])
        dnormed[:, at] = value + dot_rows(dproj[...], attention_rows[at, :])
        if i % 2 == 1:
            next(large, None)

    def norm_back(i, gain_grad):
        at = pl.ds(pl.multiple_of(i * 64, 64), 64)
        value = f32(tokens_ref[at, :])
        scale = lax.rsqrt(jnp.mean(value * value, axis=-1, keepdims=True) + NORM_EPS)
        unit = value * scale
        grad = dnormed[at, :]
        inner_grad = grad * gain_ref[0:1]
        mean = jnp.mean(inner_grad * unit, axis=-1, keepdims=True)
        token_grad_ref[at, :] = hidden_ref[at, :] + scale * (inner_grad - unit * mean)
        return gain_grad + jnp.sum(grad * unit, axis=0, keepdims=True)

    gain_grad = lax.fori_loop(0, span // 64, norm_back, jnp.zeros((1, width), jnp.float32))
    vec[...] = conv_sums[...]
    vec[5:6, 0:inner] = mixer_gain_ref[...]
    vec[6:7, 0:width] = feed_gain_ref[...]
    vec[7:8, 0:width] = gain_grad
    for i, row in enumerate((2, 0, 1)):
        vec[7:8, width + 128 * i : width + 128 * (i + 1)] = early_heads[row : row + 1]
    next(large, None)
    small = small_steps(me, plan.chips, plan.extras, vec, total_ref, stage, slots, small_sems, beyond)
    for _ in small:
        next(large, None)
    pieces = [*groups[1][: len(early)], *sums]

    def join(wanted):
        for target, parts in zip(joined, joins):
            start = 0
            for part in parts:
                source = pieces[part]
                rows, columns = source.shape[1:]
                if part in wanted:
                    for q in range(4):
                        at = (slice(q * rows, (q + 1) * rows), slice(start, start + columns))
                        target[at] = f32(source[q])
                start += columns

    join(range(len(early)))
    run_out(large)
    join(range(len(early), len(pieces)))


def run_tail(plan, early, joins, *operands):
    dma, vmem = pltpu.SemaphoreType.DMA, pltpu.VMEM
    chips, extras = plan.chips, plan.extras
    f32, low = jnp.float32, jnp.bfloat16
    conv_width, span = operands[0].shape[1], operands[1].shape[0]
    width = operands[5].shape[1]
    mixer_w, attention_w = operands[-2:]
    vec = (8, conv_width)
    scratch = [
        vmem((span, attention_w.shape[1]), low),
        vmem(mixer_w.shape, low),
        vmem(attention_w.shape, low),
        vmem((span, width), f32),
        vmem(vec, f32),
        dma((2,)),
        *[vmem(out.shape, out.dtype) for out in plan.outs()],
    ]
    pieces = [*early, *plan.outs()]
    full = []
    for parts in joins:
        rows = 4 * pieces[parts[0]].shape[1]
        full.append(jax.ShapeDtypeStruct((rows, sum(pieces[p].shape[2] for p in parts)), f32))
    small = [vmem((5, *vec), f32), vmem((3 + chips + extras, *vec), f32)]
    small += [dma((2 + extras,)), dma((2 + extras,)), dma((chips,)), dma((chips,))]
    vm, anywhere = pl.BlockSpec(memory_space=pltpu.VMEM), pl.BlockSpec(memory_space=pl.ANY)
    token_grad, total, *joined = pl.pallas_call(
        functools.partial(tail_kernel, plan, early, joins),
        out_shape=[
            jax.ShapeDtypeStruct((span, width), f32),
            jax.ShapeDtypeStruct(vec, f32),
            *full,
        ],
        in_specs=[vm] * (len(plan.operands()) + len(early) + 11) + [anywhere] * 2,
        out_specs=[vm] * (2 + len(full)),
        scratch_shapes=[*scratch, *plan.scratch(), *small],
        compiler_params=pltpu.CompilerParams(
            collective_id=1, has_side_effects=True, vmem_limit_bytes=VMEM_LIMIT
        ),
        name="run_tail",
    )(*plan.operands(), *early, *operands)
    return token_grad, total, joined


def column_chunks(left, right, columns, pieces):
    width = columns // pieces // 128 * 128
    starts = [i * width for i in range(pieces)] + [columns]
    return [(left, right, low, high - low) for low, high in zip(starts, starts[1:])]


def axis_seat():
    grp = lax.axis_index("grp")
    return lax.div(grp, 2), lax.rem(grp, 2)


def greet_group(extra=()):
    size, grp = lax.axis_size("grp"), lax.axis_index("grp")
    barrier = pltpu.get_barrier_semaphore()
    others = [{"grp": lax.rem(grp + k, size)} for k in range(1, size)] + list(extra)
    for device in others:
        pl.semaphore_signal(barrier, inc=1, device_id=device, device_id_type=MESH)
    pl.semaphore_wait(barrier, len(others))


def lanes(shape):
    return lax.broadcasted_iota(jnp.int32, shape, len(shape) - 1)


def pair_columns(columns, pair):
    rows = columns.shape[0]
    low = jnp.broadcast_to(columns[:, 2 * pair : 2 * pair + 1], (rows, 128))
    high = jnp.broadcast_to(columns[:, 2 * pair + 1 : 2 * pair + 2], (rows, 128))
    return jnp.where(lanes((rows, 128)) < 64, low, high)


def dot_rows(left, right):
    return lax.dot_general(
        left, right, (((1,), (1,)), ((), ())), preferred_element_type=jnp.float32
    )


def dot_plain(left, right):
    return jnp.dot(left, right, preferred_element_type=jnp.float32)


def align_heads(source, target, scale):
    for pair in range(HEADS // 2):
        both = source[:, pair * 128 : (pair + 1) * 128].astype(jnp.float32) * scale
        swapped = pltpu.roll(both, 64, 1)
        for odd in range(2):
            head = 2 * pair + odd
            group = head // (HEADS // KV_HEADS)
            value = both if odd == group else swapped
            keep = lanes(value.shape) // 64 == group
            target[head] = jnp.where(keep, value, 0.0).astype(jnp.bfloat16)


def slot_plan(reach):
    return [(0, 0)] + [(k, core) for k in range(1, reach + 1) for core in (1, 0)]


def slot_live(slot, chip, core, reach):
    back, side = slot
    if back == 0:
        return core == 1
    live = chip - back >= 0
    if back == reach and side == 0:
        live = jnp.logical_and(live, core == 0)
    return live


def same_document(key_column, query_row, causal):
    size = query_row.shape[-1]
    allowed = across(key_column, size) == query_row
    if causal:
        rows = lax.broadcasted_iota(jnp.int32, (size, size), 0)
        allowed = jnp.logical_and(allowed, rows <= lanes((size, size)))
    return jnp.where(allowed, 0.0, HIDDEN)


def across(column, width):
    return jnp.concatenate([column] * (width // 128), axis=1)


def forward_kernel(reach, gather, *refs):
    chips, many = gather.chips, len(gather.cut)
    groups = []
    for size in (6, many, 24, many, 39):
        groups.append(refs[:size])
        refs = refs[size:]
    (
        tokens_ref,
        pack,
        docs_ref,
        heads_ref,
        cosine_ref,
        sine_ref,
    ) = groups[0]
    shards = groups[1]
    (
        normed_ref,
        q_ref,
        gate_ref,
        ext_ref,
        act_ref,
        step_ref,
        dt_ref,
        run_ref,
        runt_ref,
        e_ref,
        wd_ref,
        car_ref,
        carried_ref,
        att_ref,
        attt_ref,
        inv_ref,
        mixed_ref,
        ent_ref,
        kvw_ref,
        segk_ref,
        packs,
        same,
        taps,
        gain_ref,
    ) = groups[2]
    fulls = groups[3]
    (
        kv_ref,
        attention_w,
        mixer_w,
        rim_out,
        rim_in,
        seg_ext,
        skip_lanes,
        qa,
        bias,
        vt,
        ot,
        total,
        xdt,
        xw,
        runb,
        gram,
        own_state,
        half_out,
        half_in,
        car_in,
        chip_out,
        chip_car,
        chip_in,
        chip_car_in,
        enter_out,
        acc,
        fetch_sem,
        rim_s,
        rim_r,
        ka_s,
        ka_r,
        kp_s,
        kp_r,
        ha_s,
        ha_r,
        ca_s,
        ca_r,
        en_s,
        en_r,
    ) = groups[4]
    travel = refs
    chip, core = axis_seat()
    grp = lax.axis_index("grp")
    span = tokens_ref.shape[0]
    inner = SSM_HEADS * SSM_HEAD
    half = inner // 2
    partner = {"grp": chip * 2 + 1 - core}

    def ahead(k):
        return {"grp": lax.rem(grp + 2 * k, 2 * chips)}

    me = seat()
    greet_group([me["x"], me["y"]])
    gathering = gather.steps(me, shards, pack, packs, fulls, travel)

    def tick():
        next(gathering, None)

    tick()
    for i in range(2 * (reach + 1)):
        segk_ref[i] = jnp.broadcast_to(docs_ref[i], (128, span)).T
    own_row = docs_ref[2 * reach + core]
    own_docs = segk_ref[2 * reach + core]
    seg_ext[8:, :] = own_docs
    seg_ext[0:8, :] = segk_ref[2 * reach + core - 1][span - 8 :]
    prior, tail = seg_ext[7:8, :], own_docs[span - 1 :]
    for j in range(CONV - 1):
        same[j] = jnp.where(seg_ext[5 + j : 5 + j + span, :] == own_docs, 1.0, 0.0)

    for k in range(chips):
        gather.across[len(gather.chunks), k].wait_recv()

    def whole_rows(width):
        total = width * 2 * chips
        rows = lax.broadcasted_iota(jnp.int32, (pack.shape[1], total), 0)
        value = jnp.zeros((8, total), jnp.float32)
        for i in range(2 * chips):
            here = jnp.logical_and(lanes(rows.shape) == rows + width * i, rows < width)
            value = value + dot_plain(packs[i], jnp.where(here, 1.0, 0.0).astype(jnp.bfloat16))
        return value

    taps[...] = whole_rows(taps.shape[1] // (2 * chips))
    gain = whole_rows(tokens_ref.shape[1] // (2 * chips))[5:6]
    gain_ref[...] = jnp.broadcast_to(gain, gain_ref.shape)

    def norm(i, _):
        at = pl.ds(pl.multiple_of(i * 64, 64), 64)
        value = f32(tokens_ref[at, :])
        scale = lax.rsqrt(jnp.mean(value * value, axis=-1, keepdims=True) + NORM_EPS)
        normed_ref[at, :] = (value * scale * gain).astype(jnp.bfloat16)
        return 0

    lax.fori_loop(0, span // 64, norm, 0)
    for pair in range(SSM_HEADS // 2):
        at = slice(pair * 128, (pair + 1) * 128)
        skip_lanes[:, at] = pair_columns(jnp.broadcast_to(heads_ref[2:3], (8, 128)), pair)

    for _ in range(3):
        tick()
    gather.arrive(0)
    mixer_chunks = [m for m, chunk in enumerate(gather.chunks) if chunk[0] == 1]
    waited = {0}
    fetch = pltpu.make_async_copy(fulls[0], attention_w, fetch_sem.at[0])
    gather.store[0].wait()
    fetch.start()
    tick()
    fetch.wait()
    width = tokens_ref.shape[1]
    low_half = lanes((span, 128)) % HEAD < HEAD // 2

    def turned(value):
        other = jnp.where(low_half, pltpu.roll(value, 128 - HEAD // 2, 1), pltpu.roll(value, HEAD // 2, 1))
        return value * cosine_ref[...] + other * sine_ref[...]

    for j in range(3):
        part = attention_w[:, :, :, j * 256 : (j + 1) * 256].reshape(width, 256)
        value = dot_plain(normed_ref[...], part)
        one, two = value[:, 0:128], value[:, 128:256]
        if j < 2:
            q_ref[:, j * 256 : j * 256 + 128] = turned(one).astype(jnp.bfloat16)
            q_ref[:, j * 256 + 128 : (j + 1) * 256] = turned(two).astype(jnp.bfloat16)
        else:
            kv_ref[:, 0:128] = turned(one).astype(jnp.bfloat16)
            kv_ref[:, 128:256] = two.astype(jnp.bfloat16)

    for _ in mixer_chunks[1:]:
        tick()
    for m in mixer_chunks:
        gather.arrive(m)
        waited.add(m)
    fetch = pltpu.make_async_copy(fulls[1], mixer_w, fetch_sem.at[1])
    gather.store[1].wait()
    fetch.start()
    fetch.wait()

    def project(at):
        return dot_plain(normed_ref[...], mixer_w[:, :, :, at].reshape(width, -1))

    conv_width = inner + 2 * STATE
    rest = inner + conv_width

    def conv_block(j, _):
        value = project(pl.ds(pl.multiple_of(inner + j * 256, 256), 256)).astype(jnp.bfloat16)
        at = pl.ds(pl.multiple_of(j * 256, 256), 256)
        ext_ref[8:, at] = f32(value)
        rim_out[:, at] = value[span - 16 :]
        return 0

    lax.fori_loop(0, conv_width // 256, conv_block, 0)
    tick()
    step_ref[...] = jnp.zeros_like(step_ref)
    step_ref[:, 0:SSM_HEADS] = project(slice(rest, rest + SSM_HEADS))
    rim = remote(rim_out, rim_in, rim_s, rim_r, {"grp": lax.rem(grp + 1, 2 * chips)})
    pl.when(grp + 1 < 2 * chips)(rim.start)

    def gate_block(j, _):
        at = pl.ds(pl.multiple_of(j * 256, 256), 256)
        gate_ref[:, at] = project(at)
        return 0

    lax.fori_loop(0, inner // 256, gate_block, 0)
    tick()

    raw = step_ref[...] + heads_ref[0:1]
    dt_ref[...] = jnp.maximum(raw, 0.0) + jnp.log1p(jnp.exp(-jnp.abs(raw)))
    before = lax.broadcasted_iota(jnp.int32, (span, span), 0) >= lanes((span, span))
    running = lax.dot_general(
        jnp.where(before, 1.0, 0.0), dt_ref[...] * -jnp.exp(heads_ref[1:2]), (((1,), (0,)), ((), ())),
        precision=HIGHEST, preferred_element_type=jnp.float32,
    )
    run_ref[...] = running
    turned_run = running.T
    for head in range(SSM_HEADS):
        runt_ref[head] = turned_run[head : head + 1]
    final = running[span - 1 :]
    e_ref[...] = jnp.where(own_docs == prior, jnp.exp(running), 0.0)
    wd_ref[...] = jnp.where(own_docs == tail, jnp.exp(final - running), 0.0)
    carried = jnp.where(tail == prior, jnp.exp(final), 0.0)
    carried_ref[...] = jnp.broadcast_to(carried, (8, 128))
    for pair in range(SSM_HEADS // 2):
        at = pair * 128 % half
        car_ref[pair * 128 // half, :, at : at + 128] = pair_columns(carried_ref, pair)

    def rim_none():
        ext_ref[0:8, :] = jnp.zeros((8, conv_width), jnp.float32)

    def rim_some():
        rim.wait_recv()
        ext_ref[0:8, :] = f32(rim_in[8:16, :])

    pl.when(grp == 0)(rim_none)
    pl.when(grp > 0)(rim_some)

    def convolve(j, _):
        at = pl.ds(pl.multiple_of(j * 256, 256), 256)
        value = jnp.broadcast_to(taps[CONV : CONV + 1, at], (span, 256))
        for tap in range(CONV):
            term = ext_ref[5 + tap : 5 + tap + span, at] * taps[tap : tap + 1, at]
            if tap < CONV - 1:
                term = jnp.where(across(same[tap], 256) > 0.0, term, 0.0)
            value = value + term
        act_ref[:, at] = value / (1.0 + jnp.exp(-value))
        return 0

    lax.fori_loop(0, conv_width // 256, convolve, 0)
    tick()
    own_kv = remote(kv_ref, kvw_ref.at[0, core], kp_s.at[0], kp_r.at[0], partner)
    own_kv.start()
    kv_along = {}
    for k in range(1, reach + 1):
        kv_along[k] = remote(kv_ref, kvw_ref.at[k, core], ka_s.at[k], ka_r.at[k], ahead(k))
        pl.when(chip + k < chips)(kv_along[k].start)
    kvw_ref[0, core] = kv_ref[...]

    weight = wd_ref[...] * dt_ref[...]
    for pair in range(SSM_HEADS // 2):
        at = slice(pair * 128, (pair + 1) * 128)
        x_pair = act_ref[:, at]
        xdt[:, at] = (x_pair * pair_columns(dt_ref, pair)).astype(jnp.bfloat16)
        xw[:, at] = (x_pair * pair_columns(weight, pair)).astype(jnp.bfloat16)
    in_map = act_ref[:, inner : inner + STATE]
    out_map = act_ref[:, inner + STATE :]
    out_low = out_map.astype(jnp.bfloat16)
    in_turned = in_map.T.astype(jnp.bfloat16)
    for i in range(2):
        own_state[i] = dot_plain(in_turned, xw[:, i * half : (i + 1) * half])
    half_out[...] = own_state[1 - core].astype(jnp.bfloat16)
    align_heads(q_ref, qa, HEAD**-0.5)
    ot[...] = jnp.zeros_like(ot)
    total[...] = jnp.zeros_like(total)
    half_car = remote(car_ref.at[1 - core], car_in, ha_s.at[0], ha_r.at[0], partner)
    half_state = remote(half_out, half_in, ha_s.at[1], ha_r.at[1], partner)
    half_car.start()
    half_state.start()

    def attend_slot(keys, values, key_docs, causal):
        bias[...] = same_document(key_docs, own_row, causal)
        vt[...] = values.astype(jnp.float32).T.astype(jnp.bfloat16)

        def per_head(head, _):
            group = lax.div(head, HEADS // KV_HEADS)
            scores = dot_rows(keys[...], qa[head]) + bias[...]
            weights = jnp.exp(scores)
            total[head] += jnp.sum(weights, axis=0, keepdims=True)
            rows = pl.ds(pl.multiple_of(group * HEAD, HEAD), HEAD)
            into = pl.ds(pl.multiple_of(head * HEAD, HEAD), HEAD)
            ot[into, :] += dot_plain(vt[rows, :], weights.astype(jnp.bfloat16))
            return 0

        lax.fori_loop(0, HEADS, per_head, 0)

    def attend_ref(ref, key_docs, causal):
        attend_slot(ref.at[:, 0:128], ref[:, 128:256], key_docs, causal)

    attend_ref(kv_ref, segk_ref[2 * reach + core], True)
    tick()

    half_car.wait_recv()
    half_state.wait_recv()
    mine, theirs = own_state[core], half_in[...].astype(jnp.float32)
    car_mine, car_theirs = car_ref[core], car_in[...]
    first = core == 0
    car_0 = jnp.where(first, car_mine, car_theirs)
    car_1 = jnp.where(first, car_theirs, car_mine)
    state_0 = jnp.where(first, mine, theirs)
    state_1 = jnp.where(first, theirs, mine)
    chip_out[...] = (state_1 + car_1[0:1] * state_0).astype(jnp.bfloat16)
    chip_car[...] = car_0 * car_1

    for head in range(SSM_HEADS):
        runb[head] = jnp.broadcast_to(run_ref[:, head : head + 1], (span, 128))
    gram[...] = lax.dot_general(
        out_map, in_map, (((1,), (1,)), ((), ())), precision=HIGHEST,
        preferred_element_type=jnp.float32,
    )
    state_along = {}
    for k in range(1, reach + 1):
        state_along[k] = (
            remote(chip_out, chip_in.at[k], ca_s.at[k, 0], ca_r.at[k, 0], ahead(k)),
            remote(chip_car, chip_car_in.at[k], ca_s.at[k, 1], ca_r.at[k, 1], ahead(k)),
        )
        for copy in state_along[k]:
            pl.when(chip + k < chips)(copy.start)

    kv_pass = {}
    for k in range(1, reach + 1):
        place = kvw_ref.at[k, core]
        kv_pass[k] = remote(place, place, kp_s.at[k], kp_r.at[k], partner)

        def hand_on(k=k):
            kv_along[k].wait_recv()
            kv_pass[k].start()

        pl.when(chip - k >= 0)(hand_on)

    rows = lax.broadcasted_iota(jnp.int32, (span, span), 0)
    allowed = jnp.logical_and(
        across(segk_ref[2 * reach + core], span) == own_row, rows >= lanes((span, span))
    )
    bias[...] = jnp.where(allowed, 0.0, HIDDEN)

    def intra(quad, _):
        at = pl.ds(pl.multiple_of(quad * 256, 256), 256)
        value = jnp.zeros((span, 256), jnp.float32)
        for i in range(4):
            head = quad * 4 + i
            column = runb[head]
            spread = jnp.concatenate([column] * (span // 128), axis=1) - runt_ref[head]
            mixing = (jnp.exp(spread + bias[...]) * gram[...]).astype(jnp.bfloat16)
            part = dot_plain(mixing, xdt[:, at])
            value = jnp.where(lanes((span, 256)) // 64 == i, part, value)
        mixed_ref[:, at] = value + skip_lanes[0:1, at] * act_ref[:, at]
        return 0

    lax.fori_loop(0, SSM_HEADS // 4, intra, 0)
    tick()

    own_kv.wait_recv()
    for index, slot in enumerate(slot_plan(reach)):
        back, side = slot
        if slot == (1, 1):
            acc[...] = jnp.zeros_like(acc)
            for k in range(reach, 0, -1):

                def take(k=k):
                    for copy in state_along[k]:
                        copy.wait_recv()
                    acc[...] = chip_in[k].astype(jnp.float32) + chip_car_in[k, 0:1] * acc[...]

                pl.when(chip - k >= 0)(take)
            enter_0, enter_1 = acc[...], state_0 + car_0[0:1] * acc[...]
            ent_ref[core] = jnp.where(first, enter_0, enter_1)
            enter_out[...] = jnp.where(first, enter_1, enter_0)
            for k in range(1, reach + 1):
                pl.when(chip - k >= 0)(kv_pass[k].wait_recv)

        def visit(back=back, side=side):
            ref = kvw_ref.at[back, side]
            attend_ref(ref, segk_ref[2 * (reach - back) + side], False)

        pl.when(slot_live(slot, chip, core, reach))(visit)
        tick()
        if slot == (1, 1):
            enter_pass = remote(enter_out, ent_ref.at[core], en_s, en_r, partner)
            enter_pass.start()

    for head in range(HEADS):
        inverse = 1.0 / total[head]
        inv_ref[head] = inverse
        into = slice(head * HEAD, (head + 1) * HEAD)
        ot[into, :] = ot[into, :] * inverse
    attt_ref[...] = ot[...].astype(jnp.bfloat16)
    for pair in range(HEADS // 2):
        at = slice(pair * 128, (pair + 1) * 128)
        att_ref[:, at] = ot[at, :].T.astype(jnp.bfloat16)

    enter_pass.wait_recv()
    for i in range(2):
        carried_in = dot_plain(out_low, ent_ref[i].astype(jnp.bfloat16))
        for j in range(SSM_HEADS // 4):
            pair = i * (SSM_HEADS // 4) + j
            at = slice(pair * 128, (pair + 1) * 128)
            part = carried_in[:, j * 128 : (j + 1) * 128]
            mixed_ref[:, at] += pair_columns(e_ref, pair) * part

    run_out(gathering)
    gather.finish(waited)
    for copy in gather.store[2:]:
        copy.wait()
    own_kv.wait_send()
    pl.when(grp + 1 < 2 * chips)(rim.wait_send)
    half_car.wait_send()
    half_state.wait_send()
    enter_pass.wait_send()
    for k in range(1, reach + 1):

        def sent(k=k):
            kv_along[k].wait_send()
            for copy in state_along[k]:
                copy.wait_send()

        pl.when(chip + k < chips)(sent)
        pl.when(chip - k >= 0)(kv_pass[k].wait_send)


def run_forward(reach, gather, tokens, docs, heads, cosine, sine):
    chips, group = gather.chips, gather.group
    span, width = tokens.shape
    inner = SSM_HEADS * SSM_HEAD
    half, conv_width = inner // 2, inner + 2 * STATE
    kv_width = 2 * KV_HEADS * HEAD
    f32, low = jnp.float32, jnp.bfloat16
    shape = jax.ShapeDtypeStruct
    dma = pltpu.SemaphoreType.DMA
    vmem = pltpu.VMEM
    column = shape((span, 128), f32)
    outs = [
        shape((span, width), low),
        shape((span, HEADS * HEAD), low),
        shape((span, inner), f32),
        shape((span + 8, conv_width), f32),
        shape((span, conv_width), f32),
        column,
        column,
        column,
        shape((SSM_HEADS, 1, span), f32),
        column,
        column,
        shape((2, 8, half), f32),
        shape((8, 128), f32),
        shape((span, HEADS * HEAD), low),
        shape((HEADS * HEAD, span), low),
        shape((HEADS, 1, span), f32),
        shape((span, inner), f32),
        shape((2, STATE, half), f32),
        shape((reach + 1, 2, span, kv_width), low),
        shape((2 * (reach + 1), span, 128), f32),
        shape((group, *gather.pack.shape), low),
        shape((CONV - 1, span, 128), f32),
        shape((8, conv_width), f32),
        shape((8, width), f32),
    ]
    scratch = [
        vmem((span, kv_width), low),
        vmem((group, *gather.cut[0].shape), low),
        vmem((group, *gather.cut[1].shape), low),
        vmem((16, conv_width), low),
        vmem((16, conv_width), low),
        vmem((span + 8, 128), f32),
        vmem((8, inner), f32),
        vmem((HEADS, span, 128), low),
        vmem((span, span), f32),
        vmem((128, span), low),
        vmem((HEADS * HEAD, span), f32),
        vmem((HEADS, 1, span), f32),
        vmem((span, inner), low),
        vmem((span, inner), low),
        vmem((SSM_HEADS, span, 128), f32),
        vmem((span, span), f32),
        vmem((2, STATE, half), f32),
        vmem((STATE, half), low),
        vmem((STATE, half), low),
        vmem((8, half), f32),
        vmem((STATE, half), low),
        vmem((8, half), f32),
        vmem((reach + 1, STATE, half), low),
        vmem((reach + 1, 8, half), f32),
        vmem((STATE, half), f32),
        vmem((STATE, half), f32),
        dma((2,)),
        dma,
        dma,
        dma((reach + 1,)),
        dma((reach + 1,)),
        dma((reach + 1,)),
        dma((reach + 1,)),
        dma((2,)),
        dma((2,)),
        dma((reach + 1, 2)),
        dma((reach + 1, 2)),
        dma,
        dma,
    ]
    vm, anywhere = pl.BlockSpec(memory_space=pltpu.VMEM), pl.BlockSpec(memory_space=pl.ANY)
    many = len(gather.cut)
    results = pl.pallas_call(
        functools.partial(forward_kernel, reach, gather),
        out_shape=[*outs, *gather.outs()],
        in_specs=[vm] * 6 + [anywhere] * many,
        out_specs=[vm] * len(outs) + [anywhere] * many,
        scratch_shapes=[*scratch, *gather.scratch()],
        compiler_params=pltpu.CompilerParams(
            collective_id=2, has_side_effects=True, vmem_limit_bytes=VMEM_LIMIT
        ),
        name="run_forward",
    )(tokens, gather.pack, docs, heads, cosine, sine, *gather.cut)
    full = [part.reshape(-1, part.shape[-1]) for part in results[len(outs) :]]
    return results[: len(outs)], full


def mix_backward_kernel(reach, plan, *refs):
    chips, extras = plan.chips, plan.extras
    many = len(plan.chunks)
    cut = [23, len(plan.operands()), 5, many, 50]
    groups = []
    for size in cut:
        groups.append(refs[:size])
        refs = refs[size:]
    (
        q_ref,
        kvw_ref,
        segc_ref,
        segr_ref,
        act_ref,
        dt_ref,
        run_ref,
        runt_ref,
        e_ref,
        wd_ref,
        car_ref,
        skip_ref,
        attt_ref,
        inv_ref,
        ent_ref,
        gout_ref,
        gmix_ref,
        rate_ref,
        ext_ref,
        step_ref,
        rows_ref,
        taps_ref,
        same_ref,
    ) = groups[0]
    (
        dq_ref,
        dkv_ref,
        dconv,
        conv_sums,
        heads_ref,
    ) = groups[2]
    (
        qa,
        da,
        bias,
        kt,
        dqt,
        centre,
        dk,
        dv,
        part_out,
        part_in,
        sum_out,
        sum_in,
        xdt,
        xw,
        ge,
        gramt,
        dgram,
        own_grad,
        half_out,
        half_in,
        car_in,
        chip_out,
        chip_car,
        chip_in,
        chip_car_in,
        later_out,
        later,
        acc,
        qrow,
        qcol,
        dxdt,
        sums,
        fold_ref,
        skip_row,
        padded,
        last_rows,
        rim_out,
        rim_in,
        rim_s,
        rim_r,
        pp_s,
        pp_r,
        pa_s,
        pa_r,
        ha_s,
        ha_r,
        ca_s,
        ca_r,
        la_s,
        la_r,
    ) = groups[4]
    me = seat()
    rep, reps = lax.axis_index("rep"), lax.axis_size("rep")
    beyond = [{"rep": lax.rem(rep + 4 * e, reps)} for e in range(1, extras)]
    reduction = plan.steps(me, groups[1], groups[3], refs, lag=3)
    chip, core = axis_seat()
    grp = lax.axis_index("grp")
    span = q_ref.shape[0]
    inner = SSM_HEADS * SSM_HEAD
    half = inner // 2
    low = jnp.bfloat16
    partner = {"grp": chip * 2 + 1 - core}
    first = core == 0

    def behind(k):
        return {"grp": lax.rem(grp - 2 * k + 2 * chips, 2 * chips)}

    greet_group([me["x"], me["y"], *beyond])
    for _ in plan.lefts:
        next(reduction)
    in_map = act_ref[:, inner : inner + STATE]
    out_map = act_ref[:, inner + STATE :]
    in_low, out_low = in_map.astype(low), out_map.astype(low)
    weight = wd_ref[...] * dt_ref[...]
    for pair in range(SSM_HEADS // 2):
        at = slice(pair * 128, (pair + 1) * 128)
        x_pair = act_ref[:, at]
        ge[:, at] = (gmix_ref[:, at] * pair_columns(e_ref, pair)).astype(low)
        xdt[:, at] = (x_pair * pair_columns(dt_ref, pair)).astype(low)
        xw[:, at] = (x_pair * pair_columns(weight, pair)).astype(low)
    out_turned = out_map.T.astype(low)
    for i in range(2):
        own_grad[i] = dot_plain(out_turned, ge[:, i * half : (i + 1) * half])
    half_out[...] = own_grad[1 - core].astype(low)
    align_heads(q_ref, qa, HEAD**-0.5)
    align_heads(gout_ref, da, 1.0)
    half_car = remote(car_ref.at[1 - core], car_in, ha_s.at[0], ha_r.at[0], partner)
    half_grad = remote(half_out, half_in, ha_s.at[1], ha_r.at[1], partner)
    half_car.start()
    half_grad.start()

    next(reduction, None)
    next(reduction, None)
    for pair in range(HEADS // 2):
        at = slice(pair * 128, (pair + 1) * 128)
        product = gout_ref[:, at].astype(jnp.float32).T * attt_ref[at, :].astype(jnp.float32)
        for odd in range(2):
            rows = product[odd * HEAD : (odd + 1) * HEAD]
            centre[2 * pair + odd] = jnp.sum(rows, axis=0, keepdims=True)
    dqt[...] = jnp.zeros_like(dqt)

    def attend_back(ref, key_docs, causal):
        bias[...] = same_document(key_docs, segr_ref[...], causal)
        kt[...] = ref[:, 0:128].astype(jnp.float32).T.astype(low)
        dk[...] = jnp.zeros_like(dk)
        dv[...] = jnp.zeros_like(dv)

        def per_head(head, _):
            group = lax.div(head, HEADS // KV_HEADS)
            scores = dot_rows(ref[:, 0:128], qa[head]) + bias[...]
            probs = jnp.exp(scores) * inv_ref[head]
            grad_probs = dot_rows(ref[:, 128:256], da[head])
            grad_scores = (probs * (grad_probs - centre[head])).astype(low)
            dv[...] += dot_plain(probs.astype(low), da[head])
            dk[...] += dot_plain(grad_scores, qa[head])
            rows = pl.ds(pl.multiple_of(group * HEAD, HEAD), HEAD)
            into = pl.ds(pl.multiple_of(head * HEAD, HEAD), HEAD)
            dqt[into, :] += dot_plain(kt[rows, :], grad_scores)
            return 0

        lax.fori_loop(0, HEADS, per_head, 0)

    passed, sent_on = {}, {}

    def pass_slot(back, side):
        live = slot_live((back, side), chip, core, reach)

        def compute():
            attend_back(kvw_ref.at[back, side], segc_ref[2 * (reach - back) + side], False)
            part_out[back, side, :, 0:128] = dk[...].astype(low)
            part_out[back, side, :, 128:256] = dv[...].astype(low)

        pl.when(live)(compute)

    def start_part(back):
        for side in (0, 1):
            passed[back, side] = remote(
                part_out.at[back, side],
                part_in.at[back],
                pp_s.at[back],
                pp_r.at[back],
                partner,
            )
            live = slot_live((back, side), chip, core, reach)
            pl.when(jnp.logical_and(live, core != side))(passed[back, side].start)

    def send_sum(back):
        both = chip - back >= 0
        partner_has = jnp.logical_and(both, core == 1) if back == reach else both

        def add_partner():
            passed[back, 0].wait_recv()
            value = part_out[back, core].astype(jnp.float32) + part_in[back].astype(jnp.float32)
            sum_out[back] = value.astype(low)

        pl.when(partner_has)(add_partner)
        if back == reach:

            def alone():
                sum_out[back] = part_out[back, core]

            pl.when(jnp.logical_and(both, core == 0))(alone)

    def send_sum_start(back):
        sent_on[back] = remote(
            sum_out.at[back], sum_in.at[back], pa_s.at[back], pa_r.at[back], behind(back)
        )
        pl.when(chip - back >= 0)(sent_on[back].start)

    next(reduction, None)
    pass_slot(reach, 1)
    next(reduction, None)

    half_car.wait_recv()
    half_grad.wait_recv()
    mine, theirs = own_grad[core], half_in[...].astype(jnp.float32)
    car_mine, car_theirs = car_ref[core], car_in[...]
    car_0 = jnp.where(first, car_mine, car_theirs)
    car_1 = jnp.where(first, car_theirs, car_mine)
    grad_0 = jnp.where(first, mine, theirs)
    grad_1 = jnp.where(first, theirs, mine)
    chip_out[...] = (grad_0 + car_0[0:1] * grad_1).astype(low)
    chip_car[...] = car_0 * car_1
    pass_slot(reach, 0)
    next(reduction, None)
    state_along = {}
    for k in range(1, reach + 1):
        state_along[k] = (
            remote(chip_out, chip_in.at[k], ca_s.at[k, 0], ca_r.at[k, 0], behind(k)),
            remote(chip_car, chip_car_in.at[k], ca_s.at[k, 1], ca_r.at[k, 1], behind(k)),
        )
        for copy in state_along[k]:
            pl.when(chip - k >= 0)(copy.start)
    start_part(reach)
    for back in range(reach - 1, 0, -1):
        pass_slot(back, 1)
        next(reduction, None)
        send_sum(back + 1)
        pass_slot(back, 0)
        next(reduction, None)
        send_sum_start(back + 1)
        start_part(back)
    pass_slot(0, 0)
    next(reduction, None)
    start_part(0)
    send_sum(1)

    send_sum_start(1)
    bias[...] = same_document(segc_ref[2 * reach + core], segr_ref[...], True)
    gramt[...] = lax.dot_general(
        in_map, out_map, (((1,), (1,)), ((), ())), precision=HIGHEST,
        preferred_element_type=jnp.float32,
    )
    dgram[...] = jnp.zeros_like(dgram)
    qcol[...] = jnp.zeros_like(qcol)
    qrow[...] = jnp.zeros_like(qrow)
    heads_of = lax.broadcasted_iota(jnp.int32, (inner, 128), 0) // SSM_HEAD
    fold_ref[...] = jnp.where(heads_of == lanes((inner, 128)), 1.0, 0.0).astype(low)

    def intra(quad, _):
        at = pl.ds(pl.multiple_of(quad * 256, 256), 256)
        grads = gmix_ref[:, at].astype(low)
        inputs = xdt[:, at]
        place = lanes((span, 256)) // 64
        value = jnp.zeros((span, 256), jnp.float32)
        for i in range(4):
            head = quad * 4 + i
            column = jnp.broadcast_to(runt_ref[head], (128, span)).T
            spread = runt_ref[head] - across(column, span)
            decay = jnp.exp(spread + bias[...])
            mixing = decay * gramt[...]
            alone = jnp.where(place == i, inputs, jnp.zeros_like(inputs))
            grad_mixing = dot_rows(alone, grads)
            dgram[...] += decay * grad_mixing
            product = mixing * grad_mixing
            qrow[pl.ds(head, 1), :] = jnp.sum(product, axis=0, keepdims=True)
            by_row = jnp.sum(product, axis=1, keepdims=True)
            qcol[...] = jnp.where(lanes((span, 128)) == head, by_row, qcol[...])
            part = dot_plain(mixing.astype(low), grads)
            value = jnp.where(place == i, part, value)
        dxdt[:, at] = value
        return 0

    quads = SSM_HEADS // 4
    for low_quad, high_quad in ((0, quads // 2), (quads // 2, quads)):
        lax.fori_loop(low_quad, high_quad, intra, 0)
        next(reduction, None)

    acc[...] = jnp.zeros_like(acc)
    for k in range(reach, 0, -1):

        def take(k=k):
            for copy in state_along[k]:
                copy.wait_recv()
            acc[...] = chip_in[k].astype(jnp.float32) + chip_car_in[k, 0:1] * acc[...]

        pl.when(chip + k < chips)(take)
    later_1, later_0 = acc[...], grad_1 + car_1[0:1] * acc[...]
    later[core] = jnp.where(first, later_0, later_1)
    later_out[...] = jnp.where(first, later_1, later_0)

    attend_back(kvw_ref.at[0, core], segc_ref[2 * reach + core], True)
    next(reduction, None)
    later_pass = remote(later_out, later.at[core], la_s, la_r, partner)
    later_pass.start()
    for pair in range(HEADS // 2):
        at = slice(pair * 128, (pair + 1) * 128)
        dq_ref[:, at] = dqt[at, :].T * HEAD**-0.5

    dkv_ref[:, 0:128] = dk[...]
    dkv_ref[:, 128:256] = dv[...]

    def add_zero():
        passed[0, 0].wait_recv()
        dkv_ref[...] += part_in[0].astype(jnp.float32)

    pl.when(core == 0)(add_zero)
    for k in range(1, reach + 1):

        def add_ahead(k=k):
            sent_on[k].wait_recv()
            dkv_ref[...] += sum_in[k].astype(jnp.float32)

        pl.when(chip + k < chips)(add_ahead)

    grad_low = dgram[...].astype(low)
    grad_in = dot_plain(grad_low, out_low)
    grad_out = dot_plain(dgram[...].T.astype(low), in_low)
    later_pass.wait_recv()

    def fold(value, own):
        high = value.astype(low)
        rest = (value - high.astype(jnp.float32)).astype(low)
        return dot_plain(high, fold_ref[own, :]) + dot_plain(rest, fold_ref[own, :])

    carried = jnp.zeros((1, 128), jnp.float32)
    skip_sum = jnp.zeros((8, 128), jnp.float32)
    x_inside, x_part, g_reached = (jnp.zeros((span, 128), jnp.float32) for _ in range(3))
    for block in range(inner // 256):
        i, start = block * 256 // half, block * 256 % half
        own, wide = slice(block * 256, (block + 1) * 256), slice(start, start + 256)
        entering, grads = ent_ref[i, :, wide], later[i, :, wide]
        by_lane = jnp.sum(entering * grads, axis=0, keepdims=True)
        carried = carried + fold(jnp.broadcast_to(by_lane, (8, 256)), own)[0:1]
        enter_low, later_low = entering.astype(low), grads.astype(low)
        grad_out = grad_out + dot_rows(ge[:, own], enter_low)
        grad_in = grad_in + dot_rows(xw[:, own], later_low)
        reached = dot_plain(out_low, enter_low)
        grad_xw = dot_plain(in_low, later_low)
        for j in range(2):
            pair = block * 2 + j
            at = slice(pair * 128, (pair + 1) * 128)
            here = slice(j * 128, (j + 1) * 128)
            x_pair, g_pair = act_ref[:, at], gmix_ref[:, at]
            part = grad_xw[:, here]
            inside = dxdt[:, at]
            dxdt[:, at] = (
                skip_ref[:, at] * g_pair
                + pair_columns(dt_ref, pair) * inside
                + pair_columns(weight, pair) * part
            )
            sums[0, :, here] = x_pair * inside
            sums[1, :, here] = x_pair * part
            sums[2, :, here] = g_pair * reached[:, here]
            skip_row[0:1, here] = jnp.sum(x_pair * g_pair, axis=0, keepdims=True)
        x_inside, x_part, g_reached = (
            total + fold(sums[n], own) for n, total in enumerate((x_inside, x_part, g_reached))
        )
        skip_sum = skip_sum + fold(jnp.broadcast_to(skip_row[0:1], (8, 256)), own)
        if block in LAST_TICKS:
            next(reduction, None)
    dxdt[:, inner : inner + STATE] = grad_in
    dxdt[:, inner + STATE :] = grad_out

    w_part = weight * x_part
    drun = qrow[...].T - qcol[...] + e_ref[...] * g_reached - w_part
    last = jnp.sum(w_part, axis=0, keepdims=True) + rate_ref[1:2] * carried
    rows = lax.broadcasted_iota(jnp.int32, (span, 128), 0)
    drun = jnp.where(rows == span - 1, drun + last, drun)
    upper = lax.broadcasted_iota(jnp.int32, (span, span), 0) <= lanes((span, span))
    drate = lax.dot_general(
        jnp.where(upper, 1.0, 0.0), drun, (((1,), (0,)), ((), ())), precision=HIGHEST,
        preferred_element_type=jnp.float32,
    )
    rate = rate_ref[0:1]
    dstep = x_inside + wd_ref[...] * x_part + rate * drate
    dstep = dstep / (1.0 + jnp.exp(-(step_ref[...] + rows_ref[0:1])))
    heads_ref[...] = jnp.zeros_like(heads_ref)
    heads_ref[0:1] = jnp.sum(rate * dt_ref[...] * drate, axis=0, keepdims=True)
    heads_ref[1:2] = skip_sum[0:1]
    heads_ref[2:3] = jnp.sum(dstep, axis=0, keepdims=True)

    conv_width = inner + 2 * STATE
    conv_sums[...] = jnp.zeros_like(conv_sums)
    padded[...] = jnp.zeros_like(padded)
    dconv[:, conv_width:] = dstep[:, 0:SSM_HEADS].astype(low)

    def convolve_back(j, _):
        at = pl.ds(pl.multiple_of(j * 128, 128), 128)
        value = jnp.broadcast_to(taps_ref[CONV : CONV + 1, at], (span, 128))
        inside = [same_ref[tap] > 0.0 for tap in range(CONV - 1)]
        for tap in range(CONV):
            term = ext_ref[5 + tap : 5 + tap + span, at] * taps_ref[tap : tap + 1, at]
            value = value + (jnp.where(inside[tap], term, 0.0) if tap < CONV - 1 else term)
        gate = 1.0 / (1.0 + jnp.exp(-value))
        grad = dxdt[:, at] * gate * (1.0 + value * (1.0 - gate))
        conv_sums[CONV : CONV + 1, at] = jnp.sum(grad, axis=0, keepdims=True)
        for tap in range(CONV):
            kept = jnp.where(inside[tap], grad, 0.0) if tap < CONV - 1 else grad
            product = kept * ext_ref[5 + tap : 5 + tap + span, at]
            conv_sums[tap : tap + 1, at] = jnp.sum(product, axis=0, keepdims=True)
            padded[tap, 8 : 8 + span, :] = kept * taps_ref[tap : tap + 1, at]
        value = jnp.zeros((span, 128), jnp.float32)
        edge = jnp.zeros((8, 128), jnp.float32)
        for tap in range(CONV):
            back = CONV - 1 - tap
            value = value + padded[tap, 8 + back : 8 + back + span, :]
            edge = edge + padded[tap, back : back + 8, :]
        rim_out[:, at] = edge
        dconv[:, at] = value.astype(jnp.bfloat16)
        last_rows[:, at] = value[span - 16 :]
        return 0

    lax.fori_loop(0, conv_width // 128, convolve_back, 0)
    rim = remote(rim_out, rim_in, rim_s, rim_r, {"grp": lax.rem(grp + 2 * chips - 1, 2 * chips)})
    pl.when(grp > 0)(rim.start)
    run_out(reduction)

    def add_rim():
        rim.wait_recv()
        dconv[span - 16 : span - 8, 0:conv_width] = last_rows[0:8, :].astype(low)
        last = last_rows[8:16, :] + rim_in[...]
        dconv[span - 8 :, 0:conv_width] = last.astype(low)

    pl.when(grp + 1 < 2 * chips)(add_rim)
    pl.when(grp > 0)(rim.wait_send)

    half_car.wait_send()
    half_grad.wait_send()
    later_pass.wait_send()
    for k in range(1, reach + 1):

        def sent(k=k):
            sent_on[k].wait_send()
            for copy in state_along[k]:
                copy.wait_send()

        pl.when(chip - k >= 0)(sent)
    for back in range(reach + 1):
        for side in (0, 1):
            if (back, side) in ((0, 1),):
                continue
            live = slot_live((back, side), chip, core, reach)
            pl.when(jnp.logical_and(live, core != side))(passed[back, side].wait_send)


def mix_backward(reach, operands, plan):
    sums = plan.outs()
    chips = lax.axis_size("grp") // 2
    span = operands[0].shape[0]
    inner = SSM_HEADS * SSM_HEAD
    half = inner // 2
    kv_width = 2 * KV_HEADS * HEAD
    f32, low = jnp.float32, jnp.bfloat16
    shape = jax.ShapeDtypeStruct
    dma = pltpu.SemaphoreType.DMA
    vmem = pltpu.VMEM
    outs = [
        shape((span, HEADS * HEAD), f32),
        shape((span, kv_width), f32),
        shape((span, inner + 2 * STATE + SSM_HEADS), low),
        shape((8, inner + 2 * STATE), f32),
        shape((8, 128), f32),
    ]
    scratch = [
        vmem((HEADS, span, 128), low),
        vmem((HEADS, span, 128), low),
        vmem((span, span), f32),
        vmem((128, span), low),
        vmem((HEADS * HEAD, span), f32),
        vmem((HEADS, 1, span), f32),
        vmem((span, 128), f32),
        vmem((span, 128), f32),
        vmem((reach + 1, 2, span, kv_width), low),
        vmem((reach + 1, span, kv_width), low),
        vmem((reach + 1, span, kv_width), low),
        vmem((reach + 1, span, kv_width), low),
        vmem((span, inner), low),
        vmem((span, inner), low),
        vmem((span, inner), low),
        vmem((span, span), f32),
        vmem((span, span), f32),
        vmem((2, STATE, half), f32),
        vmem((STATE, half), low),
        vmem((STATE, half), low),
        vmem((8, half), f32),
        vmem((STATE, half), low),
        vmem((8, half), f32),
        vmem((reach + 1, STATE, half), low),
        vmem((reach + 1, 8, half), f32),
        vmem((STATE, half), f32),
        vmem((2, STATE, half), f32),
        vmem((STATE, half), f32),
        vmem((128, span), f32),
        vmem((span, 128), f32),
        vmem((span, inner + 2 * STATE), f32),
        vmem((3, span, 256), f32),
        vmem((inner, 128), low),
        vmem((8, 256), f32),
        vmem((CONV, span + 16, 128), f32),
        vmem((16, inner + 2 * STATE), f32),
        vmem((8, inner + 2 * STATE), f32),
        vmem((8, inner + 2 * STATE), f32),
        dma,
        dma,
        dma((reach + 1,)),
        dma((reach + 1,)),
        dma((reach + 1,)),
        dma((reach + 1,)),
        dma((2,)),
        dma((2,)),
        dma((reach + 1, 2)),
        dma((reach + 1, 2)),
        dma,
        dma,
    ]
    results = pl.pallas_call(
        functools.partial(mix_backward_kernel, reach, plan),
        out_shape=[*outs, *sums],
        in_specs=[pl.BlockSpec(memory_space=pltpu.VMEM)] * (len(operands) + len(plan.operands())),
        out_specs=[pl.BlockSpec(memory_space=pltpu.VMEM)] * (len(outs) + len(sums)),
        scratch_shapes=[*scratch, *plan.scratch()],
        compiler_params=pltpu.CompilerParams(
            collective_id=3, has_side_effects=True, vmem_limit_bytes=VMEM_LIMIT
        ),
        name="mix_backward",
    )(*operands, *plan.operands())
    return results[: len(outs)], results[len(outs) :]


def shards(
    tokens,
    segments,
    input_gain,
    attention_in,
    attention_out,
    mixer_in,
    filter_taps,
    filter_bias,
    step_bias,
    decay_log,
    skip_scale,
    mixer_gain,
    mixer_out,
    feed_gain,
    gate_up,
    down_proj,
    cotangent,
):
    seq_count, span_len, model_width = tokens.shape
    row_count = seq_count * span_len
    seq_len = segments.shape[1]
    group_devices = lax.axis_size("grp")
    position = lax.axis_index("grp") * span_len
    inner_width = SSM_HEADS * SSM_HEAD
    xbc_width = inner_width + 2 * STATE
    query_width = HEADS * HEAD
    kv_width = KV_HEADS * HEAD
    rim_rows = CONV - 1
    def padded(value):
        return jnp.pad(value, ((0, 0), (0, 256 - value.shape[1])))

    small = [filter_taps] + [p[None] for p in (filter_bias, input_gain, mixer_gain, feed_gain)]
    pack = jnp.concatenate([padded(part) for part in small])
    shares = [attention_in, mixer_in, gate_up, down_proj, mixer_out, attention_out]
    gather = Gather(
        shares,
        [
            column_chunks(n, n, share.shape[1], pieces)[i][1:]
            for n, (share, pieces) in enumerate(zip(shares, (1, 4, 4, 2, 2, 1)))
            for i in range(pieces)
        ],
        pack,
    )
    offsets = position + jnp.arange(span_len, dtype=jnp.int32)
    cosine_table, sine_table = rope_tables(offsets, HEAD)
    cosine = jnp.concatenate([cosine_table] * 4, axis=1)
    sine = jnp.concatenate([-sine_table, sine_table] * 2, axis=1)
    reach = min(seq_len // (4 * span_len), group_devices // 2 - 1)
    chip = lax.axis_index("grp") // 2
    docs = jnp.concatenate([jnp.full((2 * reach * span_len,), -1, jnp.int32), segments[0]])
    window = lax.dynamic_slice_in_dim(docs, 2 * chip * span_len, 2 * (reach + 1) * span_len)
    window = window.reshape(2 * (reach + 1), 1, span_len).astype(jnp.float32)
    own_docs = lax.dynamic_slice_in_dim(segments[0], position, span_len)
    heads_rows = jnp.stack([step_bias, decay_log, skip_scale])
    heads_rows = jnp.pad(heads_rows, ((0, 5), (0, 128 - SSM_HEADS)))
    results, full = run_forward(
        reach,
        gather,
        tokens[0],
        window,
        heads_rows,
        cosine,
        sine,
    )
    full_attn_in, full_mix_in, full_gate_up, full_down, full_mix_out, full_attn_out = full
    (
        normed_low,
        query_rows,
        gate_part,
        ext_rows,
        active,
        step_wide,
        steps,
        running,
        running_turned,
        enter_decay,
        tail_decay,
        carried_lanes,
        carried,
        attended,
        attended_turned,
        inverse_total,
        mixed,
        entering,
        kv_window,
        key_docs,
        packs,
        same_docs,
        taps_wide,
        gain_in,
    ) = results
    full_mix_gain, full_feed_gain = (
        packs[:, 6 + i, : part.shape[0]].reshape(-1) for i, part in enumerate((mixer_gain, feed_gain))
    )
    token_float = tokens.reshape(row_count, model_width).astype(jnp.float32)
    back_attn_in, back_attn_out, back_mix_in = full_attn_in, full_attn_out, full_mix_in
    back_mix_out, back_gate_up, back_down = full_mix_out, full_gate_up, full_down
    gate_part, mixed = gate_part[None], mixed[None]
    rate_scale = -jnp.exp(decay_log)
    recurrence = (
        active,
        steps,
        running,
        running_turned,
        enter_decay,
        tail_decay,
        carried_lanes,
        jnp.repeat(skip_scale, SSM_HEAD)[None, :],
    )
    normed_mix, gate_back = jax.vjp(gated_norm, mixed, gate_part, full_mix_gain.astype(jnp.float32))
    normed_mix_low = normed_mix.reshape(row_count, inner_width).astype(jnp.bfloat16)
    hidden = (
        token_float
        + jnp.dot(attended, full_attn_out, preferred_element_type=jnp.float32)
        + jnp.dot(normed_mix_low, full_mix_out, preferred_element_type=jnp.float32)
    )
    normed_feed, feed_back = jax.vjp(rms_scale, hidden, full_feed_gain.astype(jnp.float32))
    normed_feed_low = normed_feed.astype(jnp.bfloat16)
    gate_vals = jnp.dot(normed_feed_low, full_gate_up, preferred_element_type=jnp.float32)
    activation, act_back = jax.vjp(swiglu, gate_vals[:, :FF], gate_vals[:, FF:])
    activation_low = activation.astype(jnp.bfloat16)
    out_rows = (
        hidden + jnp.dot(activation_low, full_down, preferred_element_type=jnp.float32)
    ).astype(jnp.bfloat16)
    grad_rows = cotangent.reshape(row_count, model_width)
    grad_act = jnp.dot(grad_rows, back_down.T, preferred_element_type=jnp.float32)
    grad_gate, grad_upper = act_back(grad_act)
    grad_gu = jnp.concatenate([grad_gate, grad_upper], axis=-1).astype(jnp.bfloat16)
    grad_feed_in = jnp.dot(grad_gu, back_gate_up.T, preferred_element_type=jnp.float32)
    grad_hidden_norm, grad_feed = feed_back(grad_feed_in)
    grad_hidden = grad_rows.astype(jnp.float32) + grad_hidden_norm
    grad_hidden_low = grad_hidden.astype(jnp.bfloat16)
    grad_attended = jnp.dot(
        grad_hidden_low, back_attn_out.T, preferred_element_type=jnp.float32
    ).astype(jnp.bfloat16)
    grad_normed_mix = jnp.dot(grad_hidden_low, back_mix_out.T, preferred_element_type=jnp.float32)
    grad_mixed, grad_gate_part, grad_mix_gain = gate_back(
        grad_normed_mix.reshape(seq_count, span_len, inner_width)
    )
    heads_scale = jnp.stack([rate_scale, carried[0, :SSM_HEADS]])
    heads_scale = jnp.pad(heads_scale, ((0, 6), (0, 128 - SSM_HEADS)))
    operands = (
        query_rows,
        kv_window,
        key_docs,
        own_docs[None, :].astype(jnp.float32),
        *recurrence,
        attended_turned,
        inverse_total,
        entering,
        grad_attended,
        grad_mixed.reshape(row_count, inner_width),
        heads_scale,
        ext_rows,
        step_wide,
        heads_rows,
        taps_wide,
        same_docs,
    )
    early = GradPlan(
        [normed_feed_low, activation_low, normed_mix_low, attended_turned],
        [False, False, False, True],
        [grad_gu, grad_rows, grad_hidden_low],
        [
            *column_chunks(0, 0, 2 * FF, 4),
            *column_chunks(1, 1, model_width, 2),
            *column_chunks(2, 2, model_width, 2),
            (3, 2, 0, model_width),
        ],
        handed=HANDED,
    )
    (grad_query, grad_kv_own, grad_conv, conv_sums, grad_heads), early_sums = mix_backward(
        reach, operands, early
    )
    late = GradPlan(
        [normed_low],
        [False],
        [
            grad_gate_part.reshape(row_count, inner_width).astype(jnp.bfloat16),
            grad_conv,
            jax.ShapeDtypeStruct((row_count, attention_in.shape[1]), jnp.bfloat16),
        ],
        [
            *column_chunks(0, 0, inner_width, 2),
            (0, 2, 0, attention_in.shape[1]),
            *column_chunks(0, 1, xbc_width + SSM_HEADS, CONV_PIECES),
        ],
        later=(2,),
        received=early_sums[len(early_sums) - HANDED :],
    )
    done, own = len(early_sums) - HANDED, 3 + CONV_PIECES
    place = [*range(done), *range(done + own, done + own + HANDED)]
    joins = (
        place[:4],
        place[4:6],
        place[6:8],
        place[8:],
        [done, done + 1, *range(done + 3, done + own)],
        [done + 2],
    )
    grad_token, summed, joined = run_tail(
        late,
        early_sums[:done],
        joins,
        conv_sums,
        grad_query,
        grad_kv_own,
        cosine,
        sine,
        tokens[0],
        gain_in,
        grad_hidden,
        grad_heads,
        grad_feed[None],
        grad_mix_gain[None],
        full_mix_in,
        full_attn_in,
    )
    index = lax.axis_index("grp")

    def own_part(value):
        size = value.shape[-1] // group_devices
        return lax.dynamic_slice_in_dim(value, index * size, size, value.ndim - 1)

    own_gate_up, own_down, own_mix_out, own_attn_out, own_mix_in, own_attn_in = joined
    return (
        out_rows.reshape(seq_count, span_len, model_width),
        grad_token.reshape(seq_count, span_len, model_width),
        own_part(summed[7, :model_width]),
        own_attn_in,
        own_attn_out,
        own_mix_in,
        own_part(summed[:CONV]),
        own_part(summed[CONV]),
        *(summed[7, model_width + 128 * i :][:SSM_HEADS] for i in range(3)),
        own_part(summed[5, :inner_width]),
        own_mix_out,
        own_part(summed[6, :model_width]),
        own_gate_up,
        own_down,
    )


def solution(mesh):
    return jax.shard_map(
        shards,
        mesh=mesh,
        in_specs=(
            P("rep", "grp", None),
            P("rep", None),
            P("grp"),
            P("grp", None),
            P("grp", None),
            P("grp", None),
            P(None, "grp"),
            P("grp"),
            P(),
            P(),
            P(),
            P("grp"),
            P("grp", None),
            P("grp"),
            P("grp", None),
            P("grp", None),
            P("rep", "grp", None),
        ),
        out_specs=(
            P("rep", "grp", None),
            P("rep", "grp", None),
            P("grp"),
            P("grp", None),
            P("grp", None),
            P("grp", None),
            P(None, "grp"),
            P("grp"),
            P(),
            P(),
            P(),
            P("grp"),
            P("grp", None),
            P("grp"),
            P("grp", None),
            P("grp", None),
        ),
        check_vma=False,
    )
```
